32 devices in a mesh: fsdp: 4 (over z), ctx: 2 (over x), tp: 4 (over y, core).
Axes of the slice: x: 2, y: 2, z: 4, core: 2. Of those that a mesh axis runs over, the one named last changes fastest.
Arguments:
- inputs: float32 [4, 2048, 768], P('fsdp', 'ctx'), may hold values from -6 to 6
- lengths: int32 [4], P('fsdp'), may hold values from 1024 to 2048, as said below
- w_qkv: float32 [768, 2304], P(('fsdp', 'ctx'), 'tp'), may hold values from -0.3125 to 0.3125
- b_query: float32 [768], P('tp'), may hold values from -3 to 3
- b_value: float32 [768], P('tp'), may hold values from -0.3 to 0.3
- w_out: float32 [768, 768], P('tp', ('fsdp', 'ctx')), may hold values from -1.75 to 1.75
- b_out: float32 [768], replicated, may hold values from -2 to 2
- gain_attn: float32 [768], replicated, may hold values from 0.5 to 1.5
- shift_attn: float32 [768], replicated, may hold values from -2 to 2
- w_up: float32 [768, 3072], P(('fsdp', 'ctx'), 'tp'), may hold values from -0.21875 to 0.21875
- b_up: float32 [3072], P('tp'), may hold values from -3 to 3
- w_down: float32 [3072, 768], P('tp', ('fsdp', 'ctx')), may hold values from -0.109375 to 0.109375
- b_down: float32 [768], replicated, may hold values from -2 to 2
- gain_ffn: float32 [768], replicated, may hold values from 0.5 to 1.5
- shift_ffn: float32 [768], replicated, may hold values from -2 to 2
- cotangent: float32 [4, 2048, 768], P('fsdp', 'ctx'), may hold values from -6 to 6
Outputs:
- outputs: float32 [4, 2048, 768], P('fsdp', 'ctx')
- d_inputs: float32 [4, 2048, 768], P('fsdp', 'ctx')
- d_wqkv: float32 [768, 2304], P(('fsdp', 'ctx'), 'tp')
- d_bquery: float32 [768], P('tp')
- d_bvalue: float32 [768], P('tp')
- d_wout: float32 [768, 768], P('tp', ('fsdp', 'ctx'))
- d_bout: float32 [768], replicated
- d_gattn: float32 [768], replicated
- d_sattn: float32 [768], replicated
- d_wup: float32 [768, 3072], P(('fsdp', 'ctx'), 'tp')
- d_bup: float32 [3072], P('tp')
- d_wdown: float32 [3072, 768], P('tp', ('fsdp', 'ctx'))
- d_bdown: float32 [768], replicated
- d_gffn: float32 [768], replicated
- d_sffn: float32 [768], replicated
The draws below stay inside these ranges and needn't reach their ends.
Inputs may be any that keep to these rules, and one draw needn't show every extreme that they name: `lengths`: keys at positions at or past a sequence's length are padding; some sequence is full, some has exactly half of 2048 real positions.
All inputs are finite; a program needn't handle non-finite values.
Results may differ from the reference program's by a relative error of at most 0.0003.
Values sent between devices are 32-bit elements; how exact they have to be, the bound alone decides.
A program may use at most 256 MiB of HBM per device.

```python
import jax
import jax.numpy as jnp
from jax import lax

D = 768
H = 12
HD = 64
FF = 3072
LENGTH = 2048
NSEQ = 4


def draw_lengths(key, part):
    drawn = jax.random.randint(jax.random.fold_in(key, 11), (NSEQ,), LENGTH // 2, LENGTH + 1)
    order = jax.random.permutation(jax.random.fold_in(key, 12), NSEQ)
    drawn = drawn.at[order[0]].set(LENGTH)
    drawn = drawn.at[order[1]].set(LENGTH // 2)
    return drawn.astype(jnp.int32)


def block_scale(own_key, extent, cuts, low, top_value):
    loudness, own = 1.0, jax.random.fold_in(own_key, 6)
    for axis_at, parts in cuts:
        draws = jnp.exp(jax.random.uniform(jax.random.fold_in(own, axis_at), (parts,), jnp.float32, low / len(cuts), top_value / len(cuts)))
        loudness = loudness * jnp.repeat(draws, extent[axis_at] // parts).reshape([-1 if axis == axis_at else 1 for axis in range(len(extent))])
    return loudness


def noise(rng, dims, scale, reach, split=(), kind=jnp.bfloat16):
    level = block_scale(rng, dims, split, -0.22, 0.18) if split else 1.0
    values = jax.random.normal(rng, dims, jnp.float32) * scale * level
    return jnp.minimum(jnp.maximum(values, -reach), reach).astype(kind)


def setup_inputs(seed: int = 0) -> dict:
    key_list = jax.random.split(jax.random.key(seed), 17)
    inputs = noise(key_list[0], (NSEQ, LENGTH, D), 1.0, 6.0, ((0, 4), (1, 2)), jnp.float32)
    lengths = draw_lengths(jax.random.fold_in(key_list[16], 71), 0)
    w_qkv = noise(key_list[2], (D, 3 * D), (D // 2) ** -0.5, 0.3125, ((0, 8), (1, 4)), jnp.float32)
    b_query = noise(key_list[3], (D,), 0.5, 3.0, ((0, 4),), jnp.float32)
    b_value = noise(key_list[4], (D,), 0.05, 0.3, ((0, 4),), jnp.float32)
    w_out = noise(key_list[5], (D, D), (D // 64) ** -0.5, 1.75, ((0, 4), (1, 8)), jnp.float32)
    b_out = noise(key_list[6], (D,), 0.3, 2.0, (), jnp.float32)
    gain_attn = jnp.clip(1.0 + 0.1 * jax.random.normal(key_list[7], (D,), jnp.float32), 0.5, 1.5)
    shift_attn = noise(key_list[8], (D,), 0.3, 2.0, (), jnp.float32)
    w_up = noise(key_list[9], (D, FF), D ** -0.5, 0.21875, ((0, 8), (1, 4)), jnp.float32)
    b_up = noise(key_list[10], (FF,), 0.5, 3.0, ((0, 4),), jnp.float32)
    w_down = noise(key_list[11], (FF, D), FF ** -0.5, 0.109375, ((0, 4), (1, 8)), jnp.float32)
    b_down = noise(key_list[12], (D,), 0.3, 2.0, (), jnp.float32)
    gain_ffn = jnp.clip(1.0 + 0.1 * jax.random.normal(key_list[13], (D,), jnp.float32), 0.5, 1.5)
    shift_ffn = noise(key_list[14], (D,), 0.3, 2.0, (), jnp.float32)
    cotangent = noise(key_list[15], (NSEQ, LENGTH, D), 1.0, 6.0, ((0, 4), (1, 2)), jnp.float32)
    return dict(inputs=inputs, lengths=lengths, w_qkv=w_qkv, b_query=b_query, b_value=b_value, w_out=w_out, b_out=b_out, gain_attn=gain_attn, shift_attn=shift_attn, w_up=w_up, b_up=b_up, w_down=w_down, b_down=b_down, gain_ffn=gain_ffn, shift_ffn=shift_ffn, cotangent=cotangent)


NORM_EPS = 1e-12
MASKED = -1e+30
EXACT = lax.Precision.HIGHEST

@jax.custom_vjp
def low(v):
    return lax.optimization_barrier(v.astype(jnp.bfloat16)).astype(jnp.float32)

@jax.custom_vjp
def low_back(v):
    return v

def low_keep(v):
    return (low(v), None)

def low_pass(kept, grad):
    return (grad,)

def back_keep(v):
    return (v, None)

def back_low(kept, grad):
    return (low(grad),)
low.defvjp(low_keep, low_pass)
low_back.defvjp(back_keep, back_low)

def layer_norm(values, gain, shift):
    centred = values - lax.optimization_barrier(jnp.mean(values, axis=-1, keepdims=True))
    spread = lax.optimization_barrier(jnp.mean(centred * centred, axis=-1, keepdims=True))
    return centred * lax.rsqrt(spread + NORM_EPS) * gain + shift

def exact_gelu(values):
    return jax.nn.gelu(values, approximate=False)

def attend(queries, keys, values, key_mask):
    scores = jnp.einsum('qhd,khd->hqk', queries, keys, precision=EXACT) * HD ** (-0.5)
    scores = jnp.where(key_mask[None, None, :], scores, MASKED)
    key_probs = jax.nn.softmax(scores, axis=-1)
    mixture = jnp.einsum('hqk,khd->qhd', key_probs, values, precision=EXACT)
    return mixture.reshape(queries.shape[0], H * HD)

def one_sequence(params, tokens, length):
    w_qkv, b_query, b_value, w_out, b_out, gain_attn, shift_attn, w_up, b_up, w_down, b_down, gain_ffn, shift_ffn = params
    bias_qkv = jnp.stack([b_query.reshape(H, HD), jnp.zeros((H, HD), b_query.dtype), b_value.reshape(H, HD)], axis=1).reshape(3 * D)
    projected = (jnp.dot(tokens, w_qkv, precision=EXACT) + bias_qkv).reshape(LENGTH, H, 3, HD)
    queries = projected[:, :, 0]
    keys = projected[:, :, 1]
    values = projected[:, :, 2]
    key_mask = jnp.arange(LENGTH) < length
    query_rows = min(512, LENGTH)

    def query_block(block_queries):
        return attend(block_queries, keys, values, key_mask)
    attended = lax.map(jax.checkpoint(query_block), queries.reshape(LENGTH // query_rows, query_rows, H, HD)).reshape(LENGTH, D)
    attn_normed = layer_norm(tokens + jnp.dot(attended, w_out, precision=EXACT) + b_out, gain_attn, shift_attn)
    hidden_pre = jnp.dot(attn_normed, w_up, precision=EXACT) + b_up
    activated = exact_gelu(hidden_pre)
    ffn_resid = attn_normed + jnp.dot(activated, w_down, precision=EXACT) + b_down
    return layer_norm(ffn_resid, gain_ffn, shift_ffn)

def forward(all_inputs, params, lengths):

    def per_sequence(carry_val, seq_pair):
        tokens, length = seq_pair
        return (carry_val, jax.checkpoint(one_sequence)(params, tokens, length))
    _, layer_outs = lax.scan(per_sequence, jnp.zeros((), jnp.float32), (all_inputs, lengths))
    return layer_outs

def reference(inputs, lengths, w_qkv, b_query, b_value, w_out, b_out, gain_attn, shift_attn, w_up, b_up, w_down, b_down, gain_ffn, shift_ffn, cotangent):
    params = (w_qkv, b_query, b_value, w_out, b_out, gain_attn, shift_attn, w_up, b_up, w_down, b_down, gain_ffn, shift_ffn)

    def forward_all(all_inputs, all_params):
        return forward(all_inputs, all_params, lengths)
    outputs, pull_back = jax.vjp(forward_all, inputs, params)
    d_inputs, grads = pull_back(cotangent)
    return (outputs, d_inputs, grads[0], grads[1], grads[2], grads[3], grads[4], grads[5], grads[6], grads[7], grads[8], grads[9], grads[10], grads[11], grads[12])
```

```python
import functools
import math

import jax
import jax.numpy as jnp
from jax import lax
from jax.experimental import pallas as pl
from jax.experimental.pallas import tpu as pltpu
from jax.sharding import PartitionSpec as P

HD = 64
LOG2E = math.log2(math.e)
NORM_EPS = 1e-12
MASKED = -1e30
THREE = lax.Precision.HIGH
CHUNKS = 2


def contract(left, right, left_dim, right_dim):
    return lax.dot_general(
        left,
        right,
        (((left_dim,), (right_dim,)), ((), ())),
        precision=THREE,
        preferred_element_type=jnp.float32,
    )


def ringed(block, axis, distance):
    count = lax.axis_size(axis)
    return lax.ppermute(block, axis, [(i, (i + distance) % count) for i in range(count)])


def swapped(block, axis, bit):
    return lax.ppermute(block, axis, [(i, i ^ bit) for i in range(lax.axis_size(axis))])


def bits_of(axis):
    bits, bit = [], 1
    while bit < lax.axis_size(axis):
        bits.append(bit)
        bit *= 2
    return bits


def tp_offset(rows):
    rank, offset, size = lax.axis_index("tp"), 0, rows
    for bit in bits_of("tp"):
        size //= 2
        offset = offset + jnp.where(rank & bit != 0, size, 0)
    return offset, size


def own_rows(block):
    offset, size = tp_offset(block.shape[0])
    return lax.dynamic_slice_in_dim(block, offset, size, 0)


def tp_scatter(part):
    rank = lax.axis_index("tp")
    for bit in bits_of("tp"):
        half = part.shape[0] // 2
        upper = (rank & bit != 0).astype(jnp.int32)
        leaving = lax.dynamic_slice_in_dim(part, (1 - upper) * half, half, 0)
        staying = lax.dynamic_slice_in_dim(part, upper * half, half, 0)
        part = staying + swapped(leaving, "tp", bit)
    return part


def tp_gather(block):
    rank = lax.axis_index("tp")
    for bit in reversed(bits_of("tp")):
        other = swapped(block, "tp", bit)
        upper = rank & bit != 0
        block = jnp.where(
            upper,
            jnp.concatenate([other, block], axis=0),
            jnp.concatenate([block, other], axis=0),
        )
    return block


def small_sum(vector, axes):
    for axis in axes:
        for bit in bits_of(axis):
            vector = vector + swapped(vector, axis, bit)
    return vector


def weight_gather(shard, widths):
    rows = shard.shape[0]
    n_f, n_c = lax.axis_size("fsdp"), lax.axis_size("ctx")
    at_f, at_c = lax.axis_index("fsdp"), lax.axis_index("ctx")
    wholes = [jnp.zeros((n_f * n_c * rows, width), jnp.float32) for width in widths]
    along_f = shard
    for k in range(n_f):
        if k:
            along_f = ringed(along_f, "fsdp", 1)
        along_c = along_f
        for m in range(n_c):
            if m:
                along_c = ringed(along_c, "ctx", 1)
            place = ((at_f - k) % n_f * n_c + (at_c - m) % n_c) * rows
            start = 0
            for i, width in enumerate(widths):
                wholes[i] = lax.dynamic_update_slice(
                    wholes[i], along_c[:, start : start + width], (place, 0)
                )
                start += width
    return wholes


def grad_scatter(pieces):
    n_f, n_c = lax.axis_size("fsdp"), lax.axis_size("ctx")
    at_f, at_c = lax.axis_index("fsdp"), lax.axis_index("ctx")
    rows = pieces[0].shape[0] // (n_f * n_c)

    def piece(f, c):
        start = (f % n_f * n_c + c % n_c) * rows
        cut = [lax.dynamic_slice_in_dim(p, start, rows, 0) for p in pieces]
        return cut[0] if len(cut) == 1 else jnp.concatenate(cut, axis=1)

    total = None
    for k in range(1, n_f + 1):
        over_c = piece(at_f - k, at_c - 1)
        for m in range(2, n_c + 1):
            over_c = ringed(over_c, "ctx", 1) + piece(at_f - k, at_c - m)
        total = over_c if total is None else ringed(total, "fsdp", 1) + over_c
    return total


def normalized(values):
    centred = values - jnp.mean(values, axis=-1, keepdims=True)
    spread = jnp.mean(centred * centred, axis=-1, keepdims=True)
    recip = lax.rsqrt(spread + NORM_EPS)
    return centred * recip, recip


def norm_back(grad, gain, normed, recip):
    scaled = grad * gain
    return recip * (
        scaled
        - jnp.mean(scaled, axis=-1, keepdims=True)
        - normed * jnp.mean(scaled * normed, axis=-1, keepdims=True)
    )


def halves(values):
    high = values.astype(jnp.bfloat16)
    return high, (values - high.astype(jnp.float32)).astype(jnp.bfloat16)


def low_half(shape):
    return lax.broadcasted_iota(jnp.int32, shape, 1) < HD


def dot(left, right, left_dim, right_dim):
    return lax.dot_general(
        left, right, (((left_dim,), (right_dim,)), ((), ())), preferred_element_type=jnp.float32
    )


def doubled(ref, rows, head, scratch, heads):
    for j in range(heads):

        @pl.when(head == j)
        def _():
            piece = ref[rows, j * HD : (j + 1) * HD]
            scratch[...] = jnp.concatenate([piece, piece], axis=1)


def packed(pair, first):
    low = low_half(pair.shape)
    turned = pltpu.roll(pair, HD, 1)
    twice = jnp.where(low, pair, turned) if first else jnp.where(low, turned, pair)
    high, rest = halves(twice)
    return jnp.where(low, high.astype(jnp.float32), rest.astype(jnp.float32)).astype(jnp.bfloat16)


def stacked(half):
    high, rest = halves(half)
    return jnp.concatenate([high, rest], axis=0)


def key_bias(meta_ref, block, start, count, width):
    place = meta_ref[1 + block] + start + lax.broadcasted_iota(jnp.int32, (count, width), 0)
    return jnp.where(place < meta_ref[0], 0.0, MASKED)


def forward_kernel(heads, blocks, tile, rows, meta_ref, q_ref, *refs):
    kv_refs, (out_ref, lse_ref, kp, vt, bias, qd, acc) = refs[:blocks], refs[blocks:]
    head, step = pl.program_id(0), pl.program_id(1)
    span = kv_refs[0].shape[0]
    per = span // tile

    @pl.when(step == 0)
    def _():
        for b in range(blocks):

            def prepare(j, _, b=b):
                at = pl.ds(pl.multiple_of(j * tile, tile), tile)
                to = pl.ds(pl.multiple_of(b * span + j * tile, tile), tile)
                pair = kv_refs[b][at, :]
                kp[to, :] = packed(pair, True)
                vt[:, to] = stacked(pair.T[HD:, :])
                bias[to, :] = key_bias(meta_ref, b, j * tile, tile, 128)
                return 0

            lax.fori_loop(0, per, prepare, 0)

    here = pl.ds(pl.multiple_of(step * rows, rows), rows)
    doubled(q_ref, here, head, qd, heads)
    q_high, q_low = halves(qd[...] * (LOG2E * HD**-0.5))
    q_four = jnp.concatenate([q_high, q_low], axis=1)
    acc[...] = jnp.zeros_like(acc)

    def key_tile(j, carry):
        top, total = carry
        at = pl.ds(pl.multiple_of(j * tile, tile), tile)
        k_two = kp[at, :]
        scores = dot(jnp.concatenate([k_two, k_two], axis=1), q_four, 1, 1)
        scores = scores + jnp.concatenate([bias[at, :]] * (rows // 128), axis=1)
        new_top = jnp.maximum(top, jnp.max(scores, axis=0, keepdims=True))
        fade = jnp.exp2(top - new_top)
        probs = jnp.exp2(scores - new_top)
        total = total * fade + jnp.sum(probs, axis=0, keepdims=True)
        high, low = halves(probs)
        v_two = vt[:, at]
        acc[...] = acc[...] * fade + (dot(v_two, high, 1, 0) + dot(v_two, low, 1, 0))
        return new_top, total

    top, total = lax.fori_loop(
        0,
        blocks * per,
        key_tile,
        (jnp.full((1, rows), MASKED, jnp.float32), jnp.zeros((1, rows), jnp.float32)),
    )
    result = acc[:HD, :] + acc[HD:, :]
    result = (result / total).T
    for j in range(heads):

        @pl.when(head == j)
        def _():
            out_ref[here, j * HD : (j + 1) * HD] = result
            lse_ref[j : j + 1, here] = top + jnp.log2(total)


def attention(queries, kv_blocks, meta, heads, rows=256, tile=512):
    count, span, blocks = queries.shape[0], kv_blocks[0].shape[0], len(kv_blocks)
    keys = span * blocks
    whole = lambda h, i, m: (0, 0)
    return pl.pallas_call(
        functools.partial(forward_kernel, heads, blocks, tile, rows),
        grid_spec=pltpu.PrefetchScalarGridSpec(
            num_scalar_prefetch=1,
            grid=(heads, count // rows),
            in_specs=[pl.BlockSpec((count, heads * HD), whole)]
            + [pl.BlockSpec((span, 2 * HD), lambda h, i, m: (0, h))] * blocks,
            out_specs=[
                pl.BlockSpec((count, heads * HD), whole),
                pl.BlockSpec((heads, count), whole),
            ],
            scratch_shapes=[
                pltpu.VMEM((keys, 2 * HD), jnp.bfloat16),
                pltpu.VMEM((2 * HD, keys), jnp.bfloat16),
                pltpu.VMEM((keys, 128), jnp.float32),
                pltpu.VMEM((rows, 2 * HD), jnp.float32),
                pltpu.VMEM((2 * HD, rows), jnp.float32),
            ],
        ),
        out_shape=[
            jax.ShapeDtypeStruct((count, heads * HD), jnp.float32),
            jax.ShapeDtypeStruct((heads, count), jnp.float32),
        ],
        compiler_params=pltpu.CompilerParams(dimension_semantics=("arbitrary", "arbitrary")),
        cost_estimate=pl.CostEstimate(
            flops=24 * heads * count * keys * HD,
            bytes_accessed=8 * keys * heads * HD + 8 * count * heads * HD,
            transcendentals=heads * count * keys,
        ),
        name="attention_forward",
    )(meta, queries, *kv_blocks)


def backward_kernel(heads, blocks, tile, rows, meta_ref, q_ref, do_ref, out_ref, lse_ref, *refs):
    kv_refs = refs[:blocks]
    dq_ref, dkv_refs = refs[blocks], refs[blocks + 1 : 2 * blocks + 1]
    kp, vp, kt, bias, qd, dd, od, dk, dv, acc = refs[2 * blocks + 1 :]
    head, step = pl.program_id(0), pl.program_id(1)
    span = kv_refs[0].shape[0]
    per = span // tile

    @pl.when(step == 0)
    def _():
        dk[...] = jnp.zeros_like(dk)
        dv[...] = jnp.zeros_like(dv)
        for b in range(blocks):

            def prepare(j, _, b=b):
                at = pl.ds(pl.multiple_of(j * tile, tile), tile)
                to = pl.ds(pl.multiple_of(b * span + j * tile, tile), tile)
                pair = kv_refs[b][at, :]
                kp[to, :] = packed(pair, True)
                vp[to, :] = packed(pair, False)
                kt[:, to] = stacked(pair.T[:HD, :])
                bias[to, :] = key_bias(meta_ref, b, j * tile, tile, 128)
                return 0

            lax.fori_loop(0, per, prepare, 0)

    here = pl.ds(pl.multiple_of(step * rows, rows), rows)
    doubled(q_ref, here, head, qd, heads)
    doubled(do_ref, here, head, dd, heads)
    doubled(out_ref, here, head, od, heads)
    low = low_half((rows, 2 * HD))

    def both(values):
        high, rest = halves(values)
        mixed = jnp.where(low, high.astype(jnp.float32), rest.astype(jnp.float32))
        return jnp.concatenate([high, rest], axis=1), mixed.astype(jnp.bfloat16)

    q_four, q_two = both(qd[...] * (LOG2E * HD**-0.5))
    do_four, do_two = both(dd[...])
    delta = jnp.sum((dd[...] * od[...]).T[:HD, :], axis=0, keepdims=True)
    lse = lse_ref[0:1, here]
    for j in range(1, heads):
        lse = jnp.where(head == j, lse_ref[j : j + 1, here], lse)
    acc[...] = jnp.zeros_like(acc)

    def key_tile(j, _):
        at = pl.ds(pl.multiple_of(j * tile, tile), tile)
        k_two, v_two = kp[at, :], vp[at, :]
        scores = dot(jnp.concatenate([k_two, k_two], axis=1), q_four, 1, 1)
        scores = scores + jnp.concatenate([bias[at, :]] * (rows // 128), axis=1)
        probs = jnp.exp2(scores - lse)
        high, rest = halves(probs)
        dv[at, :] += dot(high, do_two, 1, 0) + dot(rest, do_two, 1, 0)
        grad_p = dot(jnp.concatenate([v_two, v_two], axis=1), do_four, 1, 1)
        grad_s = probs * (grad_p - delta)
        high, rest = halves(grad_s)
        dk[at, :] += dot(high, q_two, 1, 0) + dot(rest, q_two, 1, 0)
        k_t = kt[:, at]
        acc[...] += dot(k_t, high, 1, 0) + dot(k_t, rest, 1, 0)
        return 0

    lax.fori_loop(0, blocks * per, key_tile, 0)
    result = ((acc[:HD, :] + acc[HD:, :]) * HD**-0.5).T
    for j in range(heads):

        @pl.when(head == j)
        def _():
            dq_ref[here, j * HD : (j + 1) * HD] = result

    @pl.when(step == pl.num_programs(1) - 1)
    def _():
        for b in range(blocks):

            def finish(j, _, b=b):
                at = pl.ds(pl.multiple_of(j * tile, tile), tile)
                to = pl.ds(pl.multiple_of(b * span + j * tile, tile), tile)
                grad_k, grad_v = dk[to, :], dv[to, :]
                grad_k = (grad_k + pltpu.roll(grad_k, HD, 1)) * (1.0 / LOG2E)
                grad_v = grad_v + pltpu.roll(grad_v, HD, 1)
                dkv_refs[b][at, :] = jnp.where(low_half(grad_k.shape), grad_k, grad_v)
                return 0

            lax.fori_loop(0, per, finish, 0)


def attention_back(queries, grads, result, lse, kv_blocks, meta, heads, rows=256, tile=512):
    count, span, blocks = queries.shape[0], kv_blocks[0].shape[0], len(kv_blocks)
    keys = span * blocks
    whole = lambda h, i, m: (0, 0)
    wide = pl.BlockSpec((count, heads * HD), whole)
    kv_spec = pl.BlockSpec((span, 2 * HD), lambda h, i, m: (0, h))
    return pl.pallas_call(
        functools.partial(backward_kernel, heads, blocks, tile, rows),
        grid_spec=pltpu.PrefetchScalarGridSpec(
            num_scalar_prefetch=1,
            grid=(heads, count // rows),
            in_specs=[wide] * 3 + [pl.BlockSpec((heads, count), whole)] + [kv_spec] * blocks,
            out_specs=[wide] + [kv_spec] * blocks,
            scratch_shapes=[
                pltpu.VMEM((keys, 2 * HD), jnp.bfloat16),
                pltpu.VMEM((keys, 2 * HD), jnp.bfloat16),
                pltpu.VMEM((2 * HD, keys), jnp.bfloat16),
                pltpu.VMEM((keys, 128), jnp.float32),
                pltpu.VMEM((rows, 2 * HD), jnp.float32),
                pltpu.VMEM((rows, 2 * HD), jnp.float32),
                pltpu.VMEM((rows, 2 * HD), jnp.float32),
                pltpu.VMEM((keys, 2 * HD), jnp.float32),
                pltpu.VMEM((keys, 2 * HD), jnp.float32),
                pltpu.VMEM((2 * HD, rows), jnp.float32),
            ],
        ),
        out_shape=[jax.ShapeDtypeStruct((count, heads * HD), jnp.float32)]
        + [jax.ShapeDtypeStruct((span, 2 * heads * HD), jnp.float32)] * blocks,
        compiler_params=pltpu.CompilerParams(dimension_semantics=("arbitrary", "arbitrary")),
        cost_estimate=pl.CostEstimate(
            flops=60 * heads * count * keys * HD,
            bytes_accessed=16 * keys * heads * HD + 16 * count * heads * HD,
            transcendentals=heads * count * keys,
        ),
        name="attention_backward",
    )(meta, queries, grads, result, lse, *kv_blocks)


def per_device(
    inputs,
    lengths,
    w_qkv,
    b_query,
    b_value,
    w_out,
    b_out,
    gain_attn,
    shift_attn,
    w_up,
    b_up,
    w_down,
    b_down,
    gain_ffn,
    shift_ffn,
    cotangent,
):
    width = inputs.shape[-1]
    block_len = inputs.shape[1]
    heads = b_query.shape[0] // HD
    split_at = heads * HD
    hidden = b_up.shape[0]
    tokens = inputs.reshape(block_len, width)
    cot = cotangent.reshape(block_len, width)
    length = lengths[0]
    n_c = lax.axis_size("ctx")
    at_c = lax.axis_index("ctx")

    def regroup(columns):
        parts = columns.reshape(columns.shape[:-1] + (heads, 3 * HD))
        lead = columns.shape[:-1]
        return jnp.concatenate(
            [
                parts[..., HD:].reshape(lead + (2 * split_at,)),
                parts[..., :HD].reshape(lead + (split_at,)),
            ],
            axis=-1,
        )

    bias_kv = jnp.stack(
        [jnp.zeros((heads, HD), jnp.float32), b_value.reshape(heads, HD)], axis=1
    ).reshape(-1)
    wide_kv, wide_q = weight_gather(regroup(w_qkv), [2 * split_at, split_at])
    rest = jnp.concatenate([w_up, w_down.T, w_out.T], axis=1)
    wide_up, wide_down_t, wide_out_t = weight_gather(rest, [hidden, hidden, split_at])

    kv_blocks = [contract(tokens, wide_kv, 1, 0) + bias_kv]
    for m in range(1, n_c):
        kv_blocks.append(ringed(kv_blocks[-1], "ctx", 1))
    queries = contract(tokens, wide_q, 1, 0) + b_query
    meta = jnp.stack([length] + [(at_c - m) % n_c * block_len for m in range(n_c)])
    attended, log_sums = attention(queries, kv_blocks, meta, heads)

    chunk = block_len // CHUNKS
    outs, grad_atts, grad_mids = [], [], []
    d_up = d_down_t = d_out_t = None
    vec_rows = jnp.zeros((6, width), jnp.float32)
    d_bup = jnp.zeros((hidden,), jnp.float32)

    def plus(total, term):
        return term if total is None else total + term

    for i in range(CHUNKS):
        rows = slice(i * chunk, (i + 1) * chunk)
        att_c = attended[rows]
        resid = own_rows(tokens[rows]) + tp_scatter(contract(att_c, wide_out_t, 1, 1)) + b_out
        n1, r1 = normalized(resid)
        normed_own = n1 * gain_attn + shift_attn
        normed = tp_gather(normed_own)
        pre = contract(normed, wide_up, 1, 0) + b_up
        cdf = 0.5 * lax.erfc(pre * (-math.sqrt(0.5)))
        act = pre * cdf
        slope = cdf + pre * (jnp.exp(-0.5 * pre * pre) * (1.0 / math.sqrt(2.0 * math.pi)))
        ffn = normed_own + tp_scatter(contract(act, wide_down_t, 1, 1)) + b_down
        n2, r2 = normalized(ffn)
        outs.append(n2 * gain_ffn + shift_ffn)
        cot_own = own_rows(cot[rows])
        second_own = norm_back(cot_own, gain_ffn, n2, r2)
        second = tp_gather(second_own)
        d_down_t = plus(d_down_t, contract(second, act, 0, 0))
        grad_pre = contract(second, wide_down_t, 1, 0) * slope
        d_up = plus(d_up, contract(normed, grad_pre, 0, 0))
        d_bup = d_bup + jnp.sum(grad_pre, axis=0)
        first_own = second_own + tp_scatter(contract(grad_pre, wide_up, 1, 1))
        mid_own = norm_back(first_own, gain_attn, n1, r1)
        grad_mids.append(mid_own)
        mid = tp_gather(mid_own)
        d_out_t = plus(d_out_t, contract(mid, att_c, 0, 0))
        grad_atts.append(contract(mid, wide_out_t, 1, 0))
        vec_rows = vec_rows + jnp.stack(
            [
                jnp.sum(mid_own, axis=0),
                jnp.sum(first_own * n1, axis=0),
                jnp.sum(first_own, axis=0),
                jnp.sum(second_own, axis=0),
                jnp.sum(cot_own * n2, axis=0),
                jnp.sum(cot_own, axis=0),
            ]
        )

    outputs = jnp.concatenate([tp_gather(o) for o in outs], axis=0)
    sums = small_sum(vec_rows, ("tp", "fsdp", "ctx"))
    rest_sum = grad_scatter([d_up, d_down_t, d_out_t])
    d_wup = rest_sum[:, :hidden]
    d_wdown = rest_sum[:, hidden : 2 * hidden].T
    d_wout = rest_sum[:, 2 * hidden :].T

    grad_att = jnp.concatenate(grad_atts, axis=0)
    grad_q, *grad_blocks = attention_back(
        queries, grad_att, attended, log_sums, kv_blocks, meta, heads
    )
    grad_kv = grad_blocks[0]
    for m in range(1, n_c):
        grad_kv = grad_kv + ringed(grad_blocks[m], "ctx", -m)
    back = contract(grad_kv, wide_kv, 1, 1) + contract(grad_q, wide_q, 1, 1)
    tail_sums = small_sum(
        jnp.concatenate([jnp.sum(grad_kv, axis=0), jnp.sum(grad_q, axis=0), d_bup]),
        ("fsdp", "ctx"),
    )
    d_bvalue = tail_sums[: 2 * split_at].reshape(heads, 2, HD)[:, 1].reshape(-1)
    d_bquery = tail_sums[2 * split_at : 3 * split_at]
    d_bup = tail_sums[3 * split_at :]
    own = grad_scatter([contract(tokens, grad_kv, 0, 0), contract(tokens, grad_q, 0, 0)])
    own_rows_count = own.shape[0]
    d_wqkv = jnp.concatenate(
        [
            own[:, 2 * split_at :].reshape(own_rows_count, heads, HD),
            own[:, : 2 * split_at].reshape(own_rows_count, heads, 2 * HD),
        ],
        axis=2,
    ).reshape(own_rows_count, 3 * split_at)
    d_in = []
    for i in range(CHUNKS):
        rows = slice(i * chunk, (i + 1) * chunk)
        d_in.append(tp_gather(grad_mids[i] + tp_scatter(back[rows])))
    d_inputs = jnp.concatenate(d_in, axis=0)
    return (
        outputs.reshape(1, block_len, width),
        d_inputs.reshape(1, block_len, width),
        d_wqkv,
        d_bquery,
        d_bvalue,
        d_wout,
        sums[0],
        sums[1],
        sums[2],
        d_wup,
        d_bup,
        d_wdown,
        sums[3],
        sums[4],
        sums[5],
    )


def solution(mesh):
    rows_of, cols_of = P(("fsdp", "ctx"), "tp"), P("tp", ("fsdp", "ctx"))
    seq, by_tp, same = P("fsdp", "ctx", None), P("tp"), P()
    in_specs = (
        seq, P("fsdp"), rows_of, by_tp, by_tp, cols_of, same, same, same,
        rows_of, by_tp, cols_of, same, same, same, seq,
    )
    out_specs = (
        seq, seq, rows_of, by_tp, by_tp, cols_of, same, same, same,
        rows_of, by_tp, cols_of, same, same, same,
    )
    return jax.shard_map(
        per_device, mesh=mesh, in_specs=in_specs, out_specs=out_specs, check_vma=False
    )
```

```python
import functools
import math

import jax
import jax.numpy as jnp
from jax import lax
from jax.experimental import pallas as pl
from jax.experimental.pallas import tpu as pltpu
from jax.sharding import PartitionSpec as P

HD = 64
LOG2E = math.log2(math.e)
NORM_EPS = 1e-12
MASKED = -1e30
THREE = lax.Precision.HIGH


def contract(left, right, left_dim, right_dim):
    return lax.dot_general(
        left,
        right,
        (((left_dim,), (right_dim,)), ((), ())),
        precision=THREE,
        preferred_element_type=jnp.float32,
    )


def ringed(block, axis, distance):
    count = lax.axis_size(axis)
    return lax.ppermute(block, axis, [(i, (i + distance) % count) for i in range(count)])


def swapped(block, axis, bit):
    return lax.ppermute(block, axis, [(i, i ^ bit) for i in range(lax.axis_size(axis))])


def bits_of(axis):
    bits, bit = [], 1
    while bit < lax.axis_size(axis):
        bits.append(bit)
        bit *= 2
    return bits


def quarter_scatter(part, chunks):
    rank = lax.axis_index("tp")
    count, width = part.shape
    block = part.reshape(chunks, 2, 2, count // (4 * chunks), width)
    for bit, axis in ((1, 1), (2, 1)):
        upper = rank // bit % 2
        leaving = lax.dynamic_index_in_dim(block, 1 - upper, axis, keepdims=False)
        staying = lax.dynamic_index_in_dim(block, upper, axis, keepdims=False)
        block = staying + swapped(leaving, "tp", bit)
    return block


def quarter_gather(block):
    rank = lax.axis_index("tp")
    for bit in (2, 1):
        other = swapped(block, "tp", bit)
        upper = rank // bit % 2 == 1
        block = jnp.where(
            upper, jnp.stack([other, block], axis=1), jnp.stack([block, other], axis=1)
        )
    return block.reshape(-1, block.shape[-1])


def small_sum(vector, axes):
    for axis in axes:
        for bit in bits_of(axis):
            vector = vector + swapped(vector, axis, bit)
    return vector


def weight_gather(shard, widths):
    rows = shard.shape[0]
    n_f, n_c = lax.axis_size("fsdp"), lax.axis_size("ctx")
    at_f, at_c = lax.axis_index("fsdp"), lax.axis_index("ctx")
    wholes = [jnp.zeros((n_f * n_c * rows, width), jnp.float32) for width in widths]
    along_f = shard
    for k in range(n_f):
        if k:
            along_f = ringed(along_f, "fsdp", 1)
        along_c = along_f
        for m in range(n_c):
            if m:
                along_c = ringed(along_c, "ctx", 1)
            place = ((at_f - k) % n_f * n_c + (at_c - m) % n_c) * rows
            start = 0
            for i, width in enumerate(widths):
                wholes[i] = lax.dynamic_update_slice(
                    wholes[i], along_c[:, start : start + width], (place, 0)
                )
                start += width
    return wholes


def grad_scatter(pieces):
    n_f, n_c = lax.axis_size("fsdp"), lax.axis_size("ctx")
    at_f, at_c = lax.axis_index("fsdp"), lax.axis_index("ctx")
    rows = pieces[0].shape[0] // (n_f * n_c)

    def piece(f, c):
        start = (f % n_f * n_c + c % n_c) * rows
        cut = [lax.dynamic_slice_in_dim(p, start, rows, 0) for p in pieces]
        return cut[0] if len(cut) == 1 else jnp.concatenate(cut, axis=1)

    total = None
    for k in range(1, n_f + 1):
        over_c = piece(at_f - k, at_c - 1)
        for m in range(2, n_c + 1):
            over_c = ringed(over_c, "ctx", 1) + piece(at_f - k, at_c - m)
        total = over_c if total is None else ringed(total, "fsdp", 1) + over_c
    return total


def normalized(values):
    centred = values - jnp.mean(values, axis=-1, keepdims=True)
    spread = jnp.mean(centred * centred, axis=-1, keepdims=True)
    recip = lax.rsqrt(spread + NORM_EPS)
    return centred * recip, recip


def norm_back(grad, gain, normed, recip):
    scaled = grad * gain
    return recip * (
        scaled
        - jnp.mean(scaled, axis=-1, keepdims=True)
        - normed * jnp.mean(scaled * normed, axis=-1, keepdims=True)
    )


def halves(values):
    high = values.astype(jnp.bfloat16)
    return high, (values - high.astype(jnp.float32)).astype(jnp.bfloat16)


def low_half(shape):
    return lax.broadcasted_iota(jnp.int32, shape, 1) < HD


def dot(left, right, left_dim, right_dim):
    return lax.dot_general(
        left, right, (((left_dim,), (right_dim,)), ((), ())), preferred_element_type=jnp.float32
    )


def doubled(ref, rows, head, scratch, heads):
    for j in range(heads):

        @pl.when(head == j)
        def _():
            piece = ref[rows, j * HD : (j + 1) * HD]
            scratch[...] = jnp.concatenate([piece, piece], axis=1)


def packed(pair, first):
    low = low_half(pair.shape)
    turned = pltpu.roll(pair, HD, 1)
    twice = jnp.where(low, pair, turned) if first else jnp.where(low, turned, pair)
    high, rest = halves(twice)
    return jnp.where(low, high.astype(jnp.float32), rest.astype(jnp.float32)).astype(jnp.bfloat16)


def stacked(half):
    high, rest = halves(half)
    return jnp.concatenate([high, rest], axis=0)


def key_bias(meta_ref, block, start, count, width):
    place = meta_ref[1 + block] + start + lax.broadcasted_iota(jnp.int32, (count, width), 0)
    return jnp.where(place < meta_ref[0], 0.0, MASKED)


def forward_kernel(heads, blocks, tile, rows, meta_ref, q_ref, *refs):
    kv_refs, (out_ref, lse_ref, kp, vt, bias, qd, acc) = refs[:blocks], refs[blocks:]
    head, step = pl.program_id(0), pl.program_id(1)
    span = kv_refs[0].shape[0]
    per = span // tile

    @pl.when(step == 0)
    def _():
        for b in range(blocks):

            def prepare(j, _, b=b):
                at = pl.ds(pl.multiple_of(j * tile, tile), tile)
                to = pl.ds(pl.multiple_of(b * span + j * tile, tile), tile)
                pair = kv_refs[b][at, :]
                kp[to, :] = packed(pair, True)
                vt[:, to] = stacked(pair.T[HD:, :])
                bias[to, :] = key_bias(meta_ref, b, j * tile, tile, 128)
                return 0

            lax.fori_loop(0, per, prepare, 0)

    here = pl.ds(pl.multiple_of(step * rows, rows), rows)
    doubled(q_ref, here, head, qd, heads)
    q_high, q_low = halves(qd[...] * (LOG2E * HD**-0.5))
    q_four = jnp.concatenate([q_high, q_low], axis=1)
    acc[...] = jnp.zeros_like(acc)

    def key_tile(j, carry):
        top, total = carry
        at = pl.ds(pl.multiple_of(j * tile, tile), tile)
        k_two = kp[at, :]
        scores = dot(jnp.concatenate([k_two, k_two], axis=1), q_four, 1, 1)
        scores = scores + jnp.concatenate([bias[at, :]] * (rows // 128), axis=1)
        new_top = jnp.maximum(top, jnp.max(scores, axis=0, keepdims=True))
        fade = jnp.exp2(top - new_top)
        probs = jnp.exp2(scores - new_top)
        total = total * fade + jnp.sum(probs, axis=0, keepdims=True)
        high, low = halves(probs)
        v_two = vt[:, at]
        acc[...] = acc[...] * fade + (dot(v_two, high, 1, 0) + dot(v_two, low, 1, 0))
        return new_top, total

    top, total = lax.fori_loop(
        0,
        blocks * per,
        key_tile,
        (jnp.full((1, rows), MASKED, jnp.float32), jnp.zeros((1, rows), jnp.float32)),
    )
    result = acc[:HD, :] + acc[HD:, :]
    result = (result / total).T
    for j in range(heads):

        @pl.when(head == j)
        def _():
            out_ref[here, j * HD : (j + 1) * HD] = result
            lse_ref[j : j + 1, here] = top + jnp.log2(total)


def attention(queries, kv_blocks, meta, heads, rows=256, tile=512):
    count, span, blocks = queries.shape[0], kv_blocks[0].shape[0], len(kv_blocks)
    keys = span * blocks
    whole = lambda h, i, m: (0, 0)
    return pl.pallas_call(
        functools.partial(forward_kernel, heads, blocks, tile, rows),
        grid_spec=pltpu.PrefetchScalarGridSpec(
            num_scalar_prefetch=1,
            grid=(heads, count // rows),
            in_specs=[pl.BlockSpec((count, heads * HD), whole)]
            + [pl.BlockSpec((span, 2 * HD), lambda h, i, m: (0, h))] * blocks,
            out_specs=[
                pl.BlockSpec((count, heads * HD), whole),
                pl.BlockSpec((heads, count), whole),
            ],
            scratch_shapes=[
                pltpu.VMEM((keys, 2 * HD), jnp.bfloat16),
                pltpu.VMEM((2 * HD, keys), jnp.bfloat16),
                pltpu.VMEM((keys, 128), jnp.float32),
                pltpu.VMEM((rows, 2 * HD), jnp.float32),
                pltpu.VMEM((2 * HD, rows), jnp.float32),
            ],
        ),
        out_shape=[
            jax.ShapeDtypeStruct((count, heads * HD), jnp.float32),
            jax.ShapeDtypeStruct((heads, count), jnp.float32),
        ],
        compiler_params=pltpu.CompilerParams(dimension_semantics=("arbitrary", "arbitrary")),
        cost_estimate=pl.CostEstimate(
            flops=24 * heads * count * keys * HD,
            bytes_accessed=8 * keys * heads * HD + 8 * count * heads * HD,
            transcendentals=heads * count * keys,
        ),
        name="attention_forward",
    )(meta, queries, *kv_blocks)


def backward_kernel(heads, blocks, tile, rows, meta_ref, q_ref, do_ref, out_ref, lse_ref, *refs):
    kv_refs = refs[:blocks]
    dq_ref, dkv_refs = refs[blocks], refs[blocks + 1 : 2 * blocks + 1]
    kp, vp, kt, bias, qd, dd, od, dk, dv, acc = refs[2 * blocks + 1 :]
    head, step = pl.program_id(0), pl.program_id(1)
    span = kv_refs[0].shape[0]
    per = span // tile

    @pl.when(step == 0)
    def _():
        dk[...] = jnp.zeros_like(dk)
        dv[...] = jnp.zeros_like(dv)
        for b in range(blocks):

            def prepare(j, _, b=b):
                at = pl.ds(pl.multiple_of(j * tile, tile), tile)
                to = pl.ds(pl.multiple_of(b * span + j * tile, tile), tile)
                pair = kv_refs[b][at, :]
                kp[to, :] = packed(pair, True)
                vp[to, :] = packed(pair, False)
                kt[:, to] = stacked(pair.T[:HD, :])
                bias[to, :] = key_bias(meta_ref, b, j * tile, tile, 128)
                return 0

            lax.fori_loop(0, per, prepare, 0)

    here = pl.ds(pl.multiple_of(step * rows, rows), rows)
    doubled(q_ref, here, head, qd, heads)
    doubled(do_ref, here, head, dd, heads)
    doubled(out_ref, here, head, od, heads)
    low = low_half((rows, 2 * HD))

    def both(values):
        high, rest = halves(values)
        mixed = jnp.where(low, high.astype(jnp.float32), rest.astype(jnp.float32))
        return jnp.concatenate([high, rest], axis=1), mixed.astype(jnp.bfloat16)

    q_four, q_two = both(qd[...] * (LOG2E * HD**-0.5))
    do_four, do_two = both(dd[...])
    delta = jnp.sum((dd[...] * od[...]).T[:HD, :], axis=0, keepdims=True)
    lse = lse_ref[0:1, here]
    for j in range(1, heads):
        lse = jnp.where(head == j, lse_ref[j : j + 1, here], lse)
    acc[...] = jnp.zeros_like(acc)

    def key_tile(j, _):
        at = pl.ds(pl.multiple_of(j * tile, tile), tile)
        k_two, v_two = kp[at, :], vp[at, :]
        scores = dot(jnp.concatenate([k_two, k_two], axis=1), q_four, 1, 1)
        scores = scores + jnp.concatenate([bias[at, :]] * (rows // 128), axis=1)
        probs = jnp.exp2(scores - lse)
        high, rest = halves(probs)
        dv[at, :] += dot(high, do_two, 1, 0) + dot(rest, do_two, 1, 0)
        grad_p = dot(jnp.concatenate([v_two, v_two], axis=1), do_four, 1, 1)
        grad_s = probs * (grad_p - delta)
        high, rest = halves(grad_s)
        dk[at, :] += dot(high, q_two, 1, 0) + dot(rest, q_two, 1, 0)
        k_t = kt[:, at]
        acc[...] += dot(k_t, high, 1, 0) + dot(k_t, rest, 1, 0)
        return 0

    lax.fori_loop(0, blocks * per, key_tile, 0)
    result = ((acc[:HD, :] + acc[HD:, :]) * HD**-0.5).T
    for j in range(heads):

        @pl.when(head == j)
        def _():
            dq_ref[here, j * HD : (j + 1) * HD] = result

    @pl.when(step == pl.num_programs(1) - 1)
    def _():
        for b in range(blocks):

            def finish(j, _, b=b):
                at = pl.ds(pl.multiple_of(j * tile, tile), tile)
                to = pl.ds(pl.multiple_of(b * span + j * tile, tile), tile)
                grad_k, grad_v = dk[to, :], dv[to, :]
                grad_k = (grad_k + pltpu.roll(grad_k, HD, 1)) * (1.0 / LOG2E)
                grad_v = grad_v + pltpu.roll(grad_v, HD, 1)
                dkv_refs[b][at, :] = jnp.where(low_half(grad_k.shape), grad_k, grad_v)
                return 0

            lax.fori_loop(0, per, finish, 0)


def attention_back(queries, grads, result, lse, kv_blocks, meta, heads, rows=256, tile=512):
    count, span, blocks = queries.shape[0], kv_blocks[0].shape[0], len(kv_blocks)
    keys = span * blocks
    whole = lambda h, i, m: (0, 0)
    wide = pl.BlockSpec((count, heads * HD), whole)
    kv_spec = pl.BlockSpec((span, 2 * HD), lambda h, i, m: (0, h))
    return pl.pallas_call(
        functools.partial(backward_kernel, heads, blocks, tile, rows),
        grid_spec=pltpu.PrefetchScalarGridSpec(
            num_scalar_prefetch=1,
            grid=(heads, count // rows),
            in_specs=[wide] * 3 + [pl.BlockSpec((heads, count), whole)] + [kv_spec] * blocks,
            out_specs=[wide] + [kv_spec] * blocks,
            scratch_shapes=[
                pltpu.VMEM((keys, 2 * HD), jnp.bfloat16),
                pltpu.VMEM((keys, 2 * HD), jnp.bfloat16),
                pltpu.VMEM((2 * HD, keys), jnp.bfloat16),
                pltpu.VMEM((keys, 128), jnp.float32),
                pltpu.VMEM((rows, 2 * HD), jnp.float32),
                pltpu.VMEM((rows, 2 * HD), jnp.float32),
                pltpu.VMEM((rows, 2 * HD), jnp.float32),
                pltpu.VMEM((keys, 2 * HD), jnp.float32),
                pltpu.VMEM((keys, 2 * HD), jnp.float32),
                pltpu.VMEM((2 * HD, rows), jnp.float32),
            ],
        ),
        out_shape=[jax.ShapeDtypeStruct((count, heads * HD), jnp.float32)]
        + [jax.ShapeDtypeStruct((span, 2 * heads * HD), jnp.float32)] * blocks,
        compiler_params=pltpu.CompilerParams(dimension_semantics=("arbitrary", "arbitrary")),
        cost_estimate=pl.CostEstimate(
            flops=60 * heads * count * keys * HD,
            bytes_accessed=16 * keys * heads * HD + 16 * count * heads * HD,
            transcendentals=heads * count * keys,
        ),
        name="attention_backward",
    )(meta, queries, grads, result, lse, *kv_blocks)


def dot_three(left, right, left_dim, right_dim):
    left_high, left_low = left
    right_high, right_low = right
    return dot(left_high, right_high, left_dim, right_dim) + (
        dot(left_high, right_low, left_dim, right_dim)
        + dot(left_low, right_high, left_dim, right_dim)
    )


def tiles_of(count, body):
    tile = 256 if count % 256 == 0 else count

    def step(n, _):
        body(pl.ds(pl.multiple_of(n * tile, tile), tile))
        return 0

    lax.fori_loop(0, count // tile, step, 0)


def middle_kernel(
    chunks, rows,
    att_ref, up_ref, down_ref, outw_ref,
    b_out, gain_1, shift_1, b_up, b_down, gain_2, shift_2, tok_hbm, cot_hbm,
    out_own, mid_own, gatt, d_up, d_down, d_out, vec, d_bup,
    part, rx0, rx1, full, act_hi, act_lo, slope, tok, cot, norm_1, recip_1,
    up_s, down_s, outw_s, xs, ys, ts, send0, recv0, send1, recv1, own_sem,
):
    half, quarter = rows // 2, rows // 4
    me = lax.axis_index("tp")
    bit0, bit1 = me % 2, me // 2 % 2
    peer0, peer1 = me + 1 - 2 * bit0, me + 2 - 4 * bit1
    home0 = pl.multiple_of(bit0 * half, half)
    away0 = pl.multiple_of((1 - bit0) * half, half)
    mine = pl.multiple_of(home0 + bit1 * quarter, quarter)
    away1 = pl.multiple_of(home0 + (1 - bit1) * quarter, quarter)
    own = pl.ds(mine, quarter)

    def remote(src, dst, send, recv, peer):
        return pltpu.make_async_remote_copy(
            src_ref=src,
            dst_ref=dst,
            send_sem=send,
            recv_sem=recv,
            device_id={"tp": peer},
            device_id_type=pl.DeviceIdType.MESH,
        )

    def scatter0(s, c):
        return remote(
            part.at[c, pl.ds(away0, half)], rx0.at[s, c], send0.at[0, s, c], recv0.at[0, s, c], peer0
        )

    def scatter1(s, c):
        return remote(
            part.at[c, pl.ds(away1, quarter)],
            rx1.at[s, c],
            send1.at[0, s, c],
            recv1.at[0, s, c],
            peer1,
        )

    def gather1(s, c):
        return remote(
            full.at[s, c, own], full.at[s, c, own], send1.at[1, s, c], recv1.at[1, s, c], peer1
        )

    def gather0(s, c):
        place = pl.ds(home0, half)
        return remote(
            full.at[s, c, place], full.at[s, c, place], send0.at[1, s, c], recv0.at[1, s, c], peer0
        )

    def own_copies(c):
        where = pl.ds(pl.multiple_of(c * rows + mine, quarter), quarter)
        return (
            pltpu.make_async_copy(tok_hbm.at[where], tok.at[c], own_sem.at[0, c]),
            pltpu.make_async_copy(cot_hbm.at[where], cot.at[c], own_sem.at[1, c]),
        )

    for c in range(chunks):
        for copy in own_copies(c):
            copy.start()
    barrier = pltpu.get_barrier_semaphore()
    for peer in (peer0, peer1):
        pl.semaphore_signal(
            barrier, inc=1, device_id={"tp": peer}, device_id_type=pl.DeviceIdType.MESH
        )

    def split_rows(source, target):
        count = source.shape[0]
        step = 128

        def one(i, _):
            at = pl.ds(pl.multiple_of(i * step, step), step)
            target[0, at, :], target[1, at, :] = halves(source[at, :])
            return 0

        lax.fori_loop(0, count // step, one, 0)

    split_rows(outw_ref, outw_s)
    split_rows(up_ref, up_s)
    split_rows(down_ref, down_s)
    d_bup[...] = jnp.zeros_like(d_bup)
    vec[...] = jnp.zeros_like(vec)
    d_up[...] = jnp.zeros_like(d_up)
    d_down[...] = jnp.zeros_like(d_down)
    d_out[...] = jnp.zeros_like(d_out)
    for c in range(chunks):
        for copy in own_copies(c):
            copy.wait()
    pl.semaphore_wait(barrier, 2)

    def split_into(target, value):
        target[0], target[1] = halves(value)

    def finish0(s, c):
        scatter0(s, c).wait()
        away = pl.ds(away1 - home0, quarter)
        part[c, pl.ds(away1, quarter), :] += rx0[s, c, away, :]
        scatter1(s, c).start()
        stay = pl.ds(mine - home0, quarter)
        part[c, own, :] += rx0[s, c, stay, :]

    def finish1(s, c):
        scatter1(s, c).wait()
        return part[c, own, :] + rx1[s, c]

    def forward1(s, c):
        gather1(s, c).wait()
        gather0(s, c).start()

    def trailing(c, now, before):
        if before is not None:

            @pl.when(c == 0)
            def _():
                before(chunks - 1)

        if now is not None:

            @pl.when(c > 0)
            def _():
                now(c - 1)

    def stage(body):
        def one(c, _):
            body(c)
            return 0

        lax.fori_loop(0, chunks, one, 0)

    def at_rows(c):
        return pl.ds(pl.multiple_of(c * rows, rows), rows)

    width = up_ref.shape[0]
    hidden = up_ref.shape[1]

    def attention_out(c):
        left = halves(att_ref[at_rows(c), :])

        def columns(n):
            part[c, :, n] = dot_three(left, (outw_s[0, n, :], outw_s[1, n, :]), 1, 1)

        tiles_of(width, columns)
        scatter0(0, c).start()
        trailing(c, functools.partial(finish0, 0), None)

    stage(attention_out)

    def first_norm(c):
        trailing(c, None, functools.partial(finish0, 0))
        resid = finish1(0, c) + tok[c] + b_out[...]
        n_1, r_1 = normalized(resid)
        norm_1[c] = n_1
        recip_1[c] = jnp.broadcast_to(r_1, recip_1.shape[1:])
        full[0, c, own, :] = n_1 * gain_1[...] + shift_1[...]
        gather1(0, c).start()
        trailing(c, functools.partial(forward1, 0), None)

    stage(first_norm)

    def feed_forward(c):
        gather0(0, c).wait()
        split_into(xs, full[0, c])

        def columns(n):
            pre = dot_three((xs[0], xs[1]), (up_s[0, :, n], up_s[1, :, n]), 1, 0) + b_up[:, n]
            cdf = 0.5 + 0.5 * lax.erf(pre * math.sqrt(0.5))
            slope[c, :, n] = cdf + pre * (
                jnp.exp(-0.5 * pre * pre) * (1.0 / math.sqrt(2.0 * math.pi))
            )
            act_hi[c, :, n], act_lo[c, :, n] = halves(pre * cdf)

        tiles_of(hidden, columns)

        def back(n):
            part[c, :, n] = dot_three(
                (act_hi[c], act_lo[c]), (down_s[0, n, :], down_s[1, n, :]), 1, 1
            )

        tiles_of(width, back)
        scatter0(1, c).start()
        trailing(c, functools.partial(finish0, 1), functools.partial(forward1, 0))

    def second_norm(c):
        trailing(c, None, functools.partial(finish0, 1))
        ffn = finish1(1, c) + full[0, c, own, :] + b_down[...]
        n_2, r_2 = normalized(ffn)
        out_own[c] = n_2 * gain_2[...] + shift_2[...]
        grad = cot[c]
        second = norm_back(grad, gain_2[...], n_2, r_2)
        full[1, c, own, :] = second
        gather1(1, c).start()
        vec[3:4, :] += jnp.sum(second, axis=0, keepdims=True)
        vec[4:5, :] += jnp.sum(grad * n_2, axis=0, keepdims=True)
        vec[5:6, :] += jnp.sum(grad, axis=0, keepdims=True)
        trailing(c, functools.partial(forward1, 1), None)

    def feed_back(c):
        gather0(1, c).wait()
        split_into(xs, full[1, c])

        def columns(n):
            grad = dot_three((xs[0], xs[1]), (down_s[0, :, n], down_s[1, :, n]), 1, 0)
            grad = grad * slope[c, :, n]
            slope[c, :, n] = grad
            ys[0, :, n], ys[1, :, n] = halves(grad)
            d_bup[:, n] += jnp.sum(grad, axis=0, keepdims=True)

        tiles_of(hidden, columns)

        def back(n):
            part[c, :, n] = dot_three((ys[0], ys[1]), (up_s[0, n, :], up_s[1, n, :]), 1, 1)

        tiles_of(width, back)
        scatter0(2, c).start()
        trailing(c, functools.partial(finish0, 2), functools.partial(forward1, 1))

    def middle_norm(c):
        trailing(c, None, functools.partial(finish0, 2))
        first = finish1(2, c) + full[1, c, own, :]
        n_1 = norm_1[c]
        mid = norm_back(first, gain_1[...], n_1, recip_1[c, :, :1])
        mid_own[c] = mid
        full[2, c, own, :] = mid
        gather1(2, c).start()
        vec[0:1, :] += jnp.sum(mid, axis=0, keepdims=True)
        vec[1:2, :] += jnp.sum(first * n_1, axis=0, keepdims=True)
        vec[2:3, :] += jnp.sum(first, axis=0, keepdims=True)
        trailing(c, functools.partial(forward1, 2), None)
        split_into(ts, full[1, c].T)

        def columns(n):
            d_down[:, n] += dot_three((ts[0], ts[1]), (act_hi[c, :, n], act_lo[c, :, n]), 1, 0)

        tiles_of(hidden, columns)

    def last(c):
        gather0(2, c).wait()
        mid = full[2, c]
        gatt[at_rows(c), :] = dot_three(halves(mid), (outw_s[0], outw_s[1]), 1, 0)
        trailing(c, None, functools.partial(forward1, 2))
        split_into(ts, mid.T)
        d_out[...] += dot_three((ts[0], ts[1]), halves(att_ref[at_rows(c), :]), 1, 0)
        split_into(ts, full[0, c].T)

        def columns(n):
            d_up[:, n] += dot_three((ts[0], ts[1]), halves(slope[c, :, n]), 1, 0)

        tiles_of(hidden, columns)

    stage(feed_forward)
    stage(second_norm)
    stage(feed_back)
    stage(middle_norm)
    stage(last)


def middle(attended, wide_up, wide_down_t, wide_out_t, vectors, tokens, cot, chunks=4):
    count, width = tokens.shape
    hidden, split_at = wide_up.shape[1], attended.shape[1]
    rows = count // chunks
    half, quarter = rows // 2, rows // 4
    vmem = pl.BlockSpec(memory_space=pltpu.VMEM)
    anywhere = pl.BlockSpec(memory_space=pl.ANY)
    f32, bf16 = jnp.float32, jnp.bfloat16
    sems = pltpu.SemaphoreType.DMA((2, 3, chunks))
    shape = jax.ShapeDtypeStruct
    return pl.pallas_call(
        functools.partial(middle_kernel, chunks, rows),
        in_specs=[vmem] * 11 + [anywhere] * 2,
        out_specs=[vmem] * 8,
        out_shape=[
            shape((chunks, quarter, width), f32),
            shape((chunks, quarter, width), f32),
            shape((count, split_at), f32),
            shape((width, hidden), f32),
            shape((width, hidden), f32),
            shape((width, split_at), f32),
            shape((8, width), f32),
            shape((1, hidden), f32),
        ],
        scratch_shapes=[
            pltpu.VMEM((chunks, rows, width), f32),
            pltpu.VMEM((3, chunks, half, width), f32),
            pltpu.VMEM((3, chunks, quarter, width), f32),
            pltpu.VMEM((3, chunks, rows, width), f32),
            pltpu.VMEM((chunks, rows, hidden), bf16),
            pltpu.VMEM((chunks, rows, hidden), bf16),
            pltpu.VMEM((chunks, rows, hidden), f32),
            pltpu.VMEM((chunks, quarter, width), f32),
            pltpu.VMEM((chunks, quarter, width), f32),
            pltpu.VMEM((chunks, quarter, width), f32),
            pltpu.VMEM((chunks, quarter, 128), f32),
            pltpu.VMEM((2, width, hidden), bf16),
            pltpu.VMEM((2, width, hidden), bf16),
            pltpu.VMEM((2, width, split_at), bf16),
            pltpu.VMEM((2, rows, width), bf16),
            pltpu.VMEM((2, rows, hidden), bf16),
            pltpu.VMEM((2, width, rows), bf16),
            sems, sems, sems, sems,
            pltpu.SemaphoreType.DMA((2, chunks)),
        ],
        compiler_params=pltpu.CompilerParams(
            collective_id=1, has_side_effects=True, vmem_limit_bytes=62 << 20
        ),
        cost_estimate=pl.CostEstimate(
            flops=6 * count * width * (6 * hidden + 3 * split_at),
            bytes_accessed=4 * width * (5 * hidden + 3 * split_at),
            transcendentals=2 * count * hidden,
        ),
        name="middle",
    )(attended, wide_up, wide_down_t, wide_out_t, *vectors, tokens, cot)


def per_device(
    inputs,
    lengths,
    w_qkv,
    b_query,
    b_value,
    w_out,
    b_out,
    gain_attn,
    shift_attn,
    w_up,
    b_up,
    w_down,
    b_down,
    gain_ffn,
    shift_ffn,
    cotangent,
):
    width = inputs.shape[-1]
    block_len = inputs.shape[1]
    heads = b_query.shape[0] // HD
    split_at = heads * HD
    hidden = b_up.shape[0]
    tokens = inputs.reshape(block_len, width)
    cot = cotangent.reshape(block_len, width)
    length = lengths[0]
    n_c = lax.axis_size("ctx")
    at_c = lax.axis_index("ctx")

    def regroup(columns):
        parts = columns.reshape(columns.shape[:-1] + (heads, 3 * HD))
        lead = columns.shape[:-1]
        return jnp.concatenate(
            [
                parts[..., HD:].reshape(lead + (2 * split_at,)),
                parts[..., :HD].reshape(lead + (split_at,)),
            ],
            axis=-1,
        )

    bias_kv = jnp.stack(
        [jnp.zeros((heads, HD), jnp.float32), b_value.reshape(heads, HD)], axis=1
    ).reshape(-1)
    wide_kv, wide_q = weight_gather(regroup(w_qkv), [2 * split_at, split_at])
    rest = jnp.concatenate([w_up, w_down.T, w_out.T], axis=1)
    wide_up, wide_down_t, wide_out_t = weight_gather(rest, [hidden, hidden, split_at])

    kv_blocks = [contract(tokens, wide_kv, 1, 0) + bias_kv]
    for m in range(1, n_c):
        kv_blocks.append(ringed(kv_blocks[-1], "ctx", 1))
    queries = contract(tokens, wide_q, 1, 0) + b_query
    meta = jnp.stack([length] + [(at_c - m) % n_c * block_len for m in range(n_c)])
    attended, log_sums = attention(queries, kv_blocks, meta, heads)

    flat = lambda v: v.reshape(1, -1)
    vectors = [flat(v) for v in (b_out, gain_attn, shift_attn, b_up, b_down, gain_ffn, shift_ffn)]
    outs, grad_mid, grad_att, d_up, d_down_t, d_out_t, vec_rows, d_bup = middle(
        attended, wide_up, wide_down_t, wide_out_t, vectors, tokens, cot
    )
    outputs = quarter_gather(outs)
    sums = small_sum(vec_rows, ("tp", "fsdp", "ctx"))
    rest_sum = grad_scatter([d_up, d_down_t, d_out_t])
    d_wup = rest_sum[:, :hidden]
    d_wdown = rest_sum[:, hidden : 2 * hidden].T
    d_wout = rest_sum[:, 2 * hidden :].T

    grad_q, *grad_blocks = attention_back(
        queries, grad_att, attended, log_sums, kv_blocks, meta, heads
    )
    grad_kv = grad_blocks[0]
    for m in range(1, n_c):
        grad_kv = grad_kv + ringed(grad_blocks[m], "ctx", -m)
    back = contract(grad_kv, wide_kv, 1, 1) + contract(grad_q, wide_q, 1, 1)
    tail_sums = small_sum(
        jnp.concatenate([jnp.sum(grad_kv, axis=0), jnp.sum(grad_q, axis=0), d_bup[0]]),
        ("fsdp", "ctx"),
    )
    d_bvalue = tail_sums[: 2 * split_at].reshape(heads, 2, HD)[:, 1].reshape(-1)
    d_bquery = tail_sums[2 * split_at : 3 * split_at]
    d_bup = tail_sums[3 * split_at :]
    own = grad_scatter([contract(tokens, grad_kv, 0, 0), contract(tokens, grad_q, 0, 0)])
    own_rows_count = own.shape[0]
    d_wqkv = jnp.concatenate(
        [
            own[:, 2 * split_at :].reshape(own_rows_count, heads, HD),
            own[:, : 2 * split_at].reshape(own_rows_count, heads, 2 * HD),
        ],
        axis=2,
    ).reshape(own_rows_count, 3 * split_at)
    d_inputs = quarter_gather(grad_mid + quarter_scatter(back, grad_mid.shape[0]))
    return (
        outputs.reshape(1, block_len, width),
        d_inputs.reshape(1, block_len, width),
        d_wqkv,
        d_bquery,
        d_bvalue,
        d_wout,
        sums[0],
        sums[1],
        sums[2],
        d_wup,
        d_bup,
        d_wdown,
        sums[3],
        sums[4],
        sums[5],
    )


def solution(mesh):
    rows_of, cols_of = P(("fsdp", "ctx"), "tp"), P("tp", ("fsdp", "ctx"))
    seq, by_tp, same = P("fsdp", "ctx", None), P("tp"), P()
    in_specs = (
        seq, P("fsdp"), rows_of, by_tp, by_tp, cols_of, same, same, same,
        rows_of, by_tp, cols_of, same, same, same, seq,
    )
    out_specs = (
        seq, seq, rows_of, by_tp, by_tp, cols_of, same, same, same,
        rows_of, by_tp, cols_of, same, same, same,
    )
    return jax.shard_map(
        per_device, mesh=mesh, in_specs=in_specs, out_specs=out_specs, check_vma=False
    )
```

```python
import functools
import math

import jax
import jax.numpy as jnp
from jax import lax
from jax.experimental import pallas as pl
from jax.experimental.pallas import tpu as pltpu
from jax.sharding import PartitionSpec as P

HD = 64
LOG2E = math.log2(math.e)
NORM_EPS = 1e-12
MASKED = -1e30
THREE = lax.Precision.HIGH


def contract(left, right, left_dim, right_dim):
    return lax.dot_general(
        left,
        right,
        (((left_dim,), (right_dim,)), ((), ())),
        precision=THREE,
        preferred_element_type=jnp.float32,
    )


def ringed(block, axis, distance):
    count = lax.axis_size(axis)
    return lax.ppermute(block, axis, [(i, (i + distance) % count) for i in range(count)])


def swapped(block, axis, bit):
    return lax.ppermute(block, axis, [(i, i ^ bit) for i in range(lax.axis_size(axis))])


def bits_of(axis):
    bits, bit = [], 1
    while bit < lax.axis_size(axis):
        bits.append(bit)
        bit *= 2
    return bits


def quarter_scatter(part, chunks):
    rank = lax.axis_index("tp")
    count, width = part.shape
    block = part.reshape(chunks, 2, 2, count // (4 * chunks), width)
    for bit, axis in ((1, 1), (2, 1)):
        upper = rank // bit % 2
        leaving = lax.dynamic_index_in_dim(block, 1 - upper, axis, keepdims=False)
        staying = lax.dynamic_index_in_dim(block, upper, axis, keepdims=False)
        block = staying + swapped(leaving, "tp", bit)
    return block


def quarter_gather(block):
    rank = lax.axis_index("tp")
    for bit in (2, 1):
        other = swapped(block, "tp", bit)
        upper = rank // bit % 2 == 1
        block = jnp.where(
            upper, jnp.stack([other, block], axis=1), jnp.stack([block, other], axis=1)
        )
    return block.reshape(-1, block.shape[-1])


def small_sum(vector, axes):
    for axis in axes:
        for bit in bits_of(axis):
            vector = vector + swapped(vector, axis, bit)
    return vector


def weight_gather(shard, widths):
    rows = shard.shape[0]
    n_f, n_c = lax.axis_size("fsdp"), lax.axis_size("ctx")
    at_f, at_c = lax.axis_index("fsdp"), lax.axis_index("ctx")
    wholes = [jnp.zeros((n_f * n_c * rows, width), jnp.float32) for width in widths]
    along_f = shard
    for k in range(n_f):
        if k:
            along_f = ringed(along_f, "fsdp", 1)
        along_c = along_f
        for m in range(n_c):
            if m:
                along_c = ringed(along_c, "ctx", 1)
            place = ((at_f - k) % n_f * n_c + (at_c - m) % n_c) * rows
            start = 0
            for i, width in enumerate(widths):
                wholes[i] = lax.dynamic_update_slice(
                    wholes[i], along_c[:, start : start + width], (place, 0)
                )
                start += width
    return wholes


def grad_scatter(pieces):
    n_f, n_c = lax.axis_size("fsdp"), lax.axis_size("ctx")
    at_f, at_c = lax.axis_index("fsdp"), lax.axis_index("ctx")
    rows = pieces[0].shape[0] // (n_f * n_c)

    def piece(f, c):
        start = (f % n_f * n_c + c % n_c) * rows
        cut = [lax.dynamic_slice_in_dim(p, start, rows, 0) for p in pieces]
        return cut[0] if len(cut) == 1 else jnp.concatenate(cut, axis=1)

    total = None
    for k in range(1, n_f + 1):
        over_c = piece(at_f - k, at_c - 1)
        for m in range(2, n_c + 1):
            over_c = ringed(over_c, "ctx", 1) + piece(at_f - k, at_c - m)
        total = over_c if total is None else ringed(total, "fsdp", 1) + over_c
    return total


def normalized(values):
    centred = values - jnp.mean(values, axis=-1, keepdims=True)
    spread = jnp.mean(centred * centred, axis=-1, keepdims=True)
    recip = lax.rsqrt(spread + NORM_EPS)
    return centred * recip, recip


def norm_back(grad, gain, normed, recip):
    scaled = grad * gain
    return recip * (
        scaled
        - jnp.mean(scaled, axis=-1, keepdims=True)
        - normed * jnp.mean(scaled * normed, axis=-1, keepdims=True)
    )


def halves(values):
    high = values.astype(jnp.bfloat16)
    return high, (values - high.astype(jnp.float32)).astype(jnp.bfloat16)


def low_half(shape):
    return lax.broadcasted_iota(jnp.int32, shape, 1) < HD


def dot(left, right, left_dim, right_dim):
    return lax.dot_general(
        left, right, (((left_dim,), (right_dim,)), ((), ())), preferred_element_type=jnp.float32
    )


def doubled(ref, rows, head, scratch, heads):
    for j in range(heads):

        @pl.when(head == j)
        def _():
            piece = ref[rows, j * HD : (j + 1) * HD]
            scratch[...] = jnp.concatenate([piece, piece], axis=1)


def packed(pair, first):
    low = low_half(pair.shape)
    turned = pltpu.roll(pair, HD, 1)
    twice = jnp.where(low, pair, turned) if first else jnp.where(low, turned, pair)
    high, rest = halves(twice)
    return jnp.where(low, high.astype(jnp.float32), rest.astype(jnp.float32)).astype(jnp.bfloat16)


def stacked(half):
    high, rest = halves(half)
    return jnp.concatenate([high, rest], axis=0)


def key_bias(meta_ref, block, start, count, width):
    place = meta_ref[1 + block] + start + lax.broadcasted_iota(jnp.int32, (count, width), 0)
    return jnp.where(place < meta_ref[0], 0.0, MASKED)


def forward_kernel(heads, blocks, tile, rows, meta_ref, q_ref, *refs):
    kv_refs, (out_ref, lse_ref, kp, vt, bias, qd, acc) = refs[:blocks], refs[blocks:]
    head, step = pl.program_id(0), pl.program_id(1)
    span = kv_refs[0].shape[0]
    per = span // tile

    @pl.when(step == 0)
    def _():
        for b in range(blocks):

            def prepare(j, _, b=b):
                at = pl.ds(pl.multiple_of(j * tile, tile), tile)
                to = pl.ds(pl.multiple_of(b * span + j * tile, tile), tile)
                pair = kv_refs[b][at, :]
                kp[to, :] = packed(pair, True)
                vt[:, to] = stacked(pair.T[HD:, :])
                bias[to, :] = key_bias(meta_ref, b, j * tile, tile, 128)
                return 0

            lax.fori_loop(0, per, prepare, 0)

    here = pl.ds(pl.multiple_of(step * rows, rows), rows)
    doubled(q_ref, here, head, qd, heads)
    q_high, q_low = halves(qd[...] * (LOG2E * HD**-0.5))
    q_four = jnp.concatenate([q_high, q_low], axis=1)
    acc[...] = jnp.zeros_like(acc)

    def key_tile(j, carry):
        top, total = carry
        at = pl.ds(pl.multiple_of(j * tile, tile), tile)
        k_two = kp[at, :]
        scores = dot(jnp.concatenate([k_two, k_two], axis=1), q_four, 1, 1)
        scores = scores + jnp.concatenate([bias[at, :]] * (rows // 128), axis=1)
        new_top = jnp.maximum(top, jnp.max(scores, axis=0, keepdims=True))
        fade = jnp.exp2(top - new_top)
        probs = jnp.exp2(scores - new_top)
        total = total * fade + jnp.sum(probs, axis=0, keepdims=True)
        high, low = halves(probs)
        v_two = vt[:, at]
        acc[...] = acc[...] * fade + (dot(v_two, high, 1, 0) + dot(v_two, low, 1, 0))
        return new_top, total

    top, total = lax.fori_loop(
        0,
        blocks * per,
        key_tile,
        (jnp.full((1, rows), MASKED, jnp.float32), jnp.zeros((1, rows), jnp.float32)),
    )
    result = acc[:HD, :] + acc[HD:, :]
    result = (result / total).T
    for j in range(heads):

        @pl.when(head == j)
        def _():
            out_ref[here, j * HD : (j + 1) * HD] = result
            lse_ref[j : j + 1, here] = top + jnp.log2(total)


def attention(queries, kv_blocks, meta, heads, rows=256, tile=512):
    count, span, blocks = queries.shape[0], kv_blocks[0].shape[0], len(kv_blocks)
    keys = span * blocks
    whole = lambda h, i, m: (0, 0)
    return pl.pallas_call(
        functools.partial(forward_kernel, heads, blocks, tile, rows),
        grid_spec=pltpu.PrefetchScalarGridSpec(
            num_scalar_prefetch=1,
            grid=(heads, count // rows),
            in_specs=[pl.BlockSpec((count, heads * HD), whole)]
            + [pl.BlockSpec((span, 2 * HD), lambda h, i, m: (0, h))] * blocks,
            out_specs=[
                pl.BlockSpec((count, heads * HD), whole),
                pl.BlockSpec((heads, count), whole),
            ],
            scratch_shapes=[
                pltpu.VMEM((keys, 2 * HD), jnp.bfloat16),
                pltpu.VMEM((2 * HD, keys), jnp.bfloat16),
                pltpu.VMEM((keys, 128), jnp.float32),
                pltpu.VMEM((rows, 2 * HD), jnp.float32),
                pltpu.VMEM((2 * HD, rows), jnp.float32),
            ],
        ),
        out_shape=[
            jax.ShapeDtypeStruct((count, heads * HD), jnp.float32),
            jax.ShapeDtypeStruct((heads, count), jnp.float32),
        ],
        compiler_params=pltpu.CompilerParams(dimension_semantics=("arbitrary", "arbitrary")),
        cost_estimate=pl.CostEstimate(
            flops=24 * heads * count * keys * HD,
            bytes_accessed=8 * keys * heads * HD + 8 * count * heads * HD,
            transcendentals=heads * count * keys,
        ),
        name="attention_forward",
    )(meta, queries, *kv_blocks)


def backward_kernel(
    heads, blocks, n_f, tile, rows, meta_ref, q_ref, do_ref, out_ref, lse_ref, up_g, down_g, outs,
    *refs,
):
    kv_refs = refs[:blocks]
    dq_ref, dkv_ref, up_out, down_out, kv_far, outs_all = refs[blocks : blocks + 6]
    kp, vp, kt, bias, qd, dd, od, dk, dv, acc, stage = refs[blocks + 6 : blocks + 17]
    transfers = Transfers(
        blocks, n_f, heads, up_g, down_g, outs, up_out, down_out, kv_far, outs_all, stage,
        *refs[blocks + 17 :],
    )
    head, step = pl.program_id(0), pl.program_id(1)
    steps = pl.num_programs(1)
    transfers.run(head * steps + step, before=True)
    span = kv_refs[0].shape[0]
    per = span // tile

    @pl.when(step == 0)
    def _():
        dk[...] = jnp.zeros_like(dk)
        dv[...] = jnp.zeros_like(dv)
        for b in range(blocks):

            def prepare(j, _, b=b):
                at = pl.ds(pl.multiple_of(j * tile, tile), tile)
                to = pl.ds(pl.multiple_of(b * span + j * tile, tile), tile)
                pair = kv_refs[b][at, :]
                kp[to, :] = packed(pair, True)
                vp[to, :] = packed(pair, False)
                kt[:, to] = stacked(pair.T[:HD, :])
                bias[to, :] = key_bias(meta_ref, b, j * tile, tile, 128)
                return 0

            lax.fori_loop(0, per, prepare, 0)

    here = pl.ds(pl.multiple_of(step * rows, rows), rows)
    doubled(q_ref, here, head, qd, heads)
    doubled(do_ref, here, head, dd, heads)
    doubled(out_ref, here, head, od, heads)
    low = low_half((rows, 2 * HD))

    def both(values):
        high, rest = halves(values)
        mixed = jnp.where(low, high.astype(jnp.float32), rest.astype(jnp.float32))
        return jnp.concatenate([high, rest], axis=1), mixed.astype(jnp.bfloat16)

    q_four, q_two = both(qd[...] * (LOG2E * HD**-0.5))
    do_four, do_two = both(dd[...])
    delta = jnp.sum((dd[...] * od[...]).T[:HD, :], axis=0, keepdims=True)
    lse = lse_ref[0:1, here]
    for j in range(1, heads):
        lse = jnp.where(head == j, lse_ref[j : j + 1, here], lse)
    acc[...] = jnp.zeros_like(acc)

    def key_tile(j, _):
        at = pl.ds(pl.multiple_of(j * tile, tile), tile)
        k_two, v_two = kp[at, :], vp[at, :]
        scores = dot(jnp.concatenate([k_two, k_two], axis=1), q_four, 1, 1)
        scores = scores + jnp.concatenate([bias[at, :]] * (rows // 128), axis=1)
        probs = jnp.exp2(scores - lse)
        high, rest = halves(probs)
        dv[at, :] += dot(high, do_two, 1, 0) + dot(rest, do_two, 1, 0)
        grad_p = dot(jnp.concatenate([v_two, v_two], axis=1), do_four, 1, 1)
        grad_s = probs * (grad_p - delta)
        high, rest = halves(grad_s)
        dk[at, :] += dot(high, q_two, 1, 0) + dot(rest, q_two, 1, 0)
        k_t = kt[:, at]
        acc[...] += dot(k_t, high, 1, 0) + dot(k_t, rest, 1, 0)
        return 0

    lax.fori_loop(0, blocks * per, key_tile, 0)
    result = ((acc[:HD, :] + acc[HD:, :]) * HD**-0.5).T
    for j in range(heads):

        @pl.when(head == j)
        def _():
            dq_ref[here, j * HD : (j + 1) * HD] = result

    def turned(rows_at):
        grad_k, grad_v = dk[rows_at, :], dv[rows_at, :]
        grad_k = (grad_k + pltpu.roll(grad_k, HD, 1)) * (1.0 / LOG2E)
        grad_v = grad_v + pltpu.roll(grad_v, HD, 1)
        return jnp.where(low_half(grad_k.shape), grad_k, grad_v)

    @pl.when(step == steps - 1)
    def _():
        for b in range(1, blocks):

            @pl.when(head >= 2)
            def _(b=b):
                transfers.kv_copy(head - 2, b).wait_send()

            def finish(j, _, b=b):
                at = pl.ds(pl.multiple_of(j * tile, tile), tile)
                to = pl.ds(pl.multiple_of(b * span + j * tile, tile), tile)
                stage[head % 2, b - 1, at, :] = turned(to)
                return 0

            lax.fori_loop(0, per, finish, 0)
            transfers.kv_copy(head, b).start()

        def keep(j, _):
            at = pl.ds(pl.multiple_of(j * tile, tile), tile)
            dkv_ref[at, :] = turned(at)
            return 0

        lax.fori_loop(0, per, keep, 0)

    transfers.run(head * steps + step, before=False)


def remote(src, dst, send, recv, **peer):
    return pltpu.make_async_remote_copy(
        src_ref=src,
        dst_ref=dst,
        send_sem=send,
        recv_sem=recv,
        device_id=peer,
        device_id_type=pl.DeviceIdType.MESH,
    )


class Transfers:
    def __init__(
        self, n_c, n_f, heads, up_g, down_g, outs, up_out, down_out, kv_far, outs_all, stage,
        up_z, up_x, down_x, down_z, up_z_sem, up_x_sem, down_x_sem, down_z_sem, kv_sem, out_sem,
    ):
        self.n_c, self.n_f, self.heads = n_c, n_f, heads
        self.up_g, self.down_g, self.outs = up_g, down_g, outs
        self.up_out, self.down_out, self.kv_far, self.outs_all = up_out, down_out, kv_far, outs_all
        self.stage = stage
        self.up_z, self.up_x, self.down_x, self.down_z = up_z, up_x, down_x, down_z
        self.up_z_sem, self.up_x_sem = up_z_sem, up_x_sem
        self.down_x_sem, self.down_z_sem, self.kv_sem = down_x_sem, down_z_sem, kv_sem
        self.out_sem = out_sem
        self.f, self.c, me = lax.axis_index("fsdp"), lax.axis_index("ctx"), lax.axis_index("tp")
        self.bit0, self.bit1 = me % 2, me // 2 % 2
        self.peer0, self.peer1 = me + 1 - 2 * self.bit0, me + 2 - 4 * self.bit1

    def at_f(self, k):
        return (self.f + (self.n_f - k)) % self.n_f

    def at_c(self, m):
        return (self.c + (self.n_c - m)) % self.n_c

    def up_hop(self, m):
        src = self.up_g.at[self.at_f(1)] if m == 1 else self.up_z.at[m - 2]
        sem = self.up_z_sem
        return remote(
            src, self.up_z.at[m - 1], sem.at[0, m - 1], sem.at[1, m - 1], fsdp=self.at_f(-1)
        )

    def up_side(self, m):
        src = self.up_z.at[self.n_f - 2, self.at_c(1)] if m == 1 else self.up_x.at[m - 2]
        sem = self.up_x_sem
        return remote(
            src, self.up_x.at[m - 1], sem.at[0, m - 1], sem.at[1, m - 1], ctx=self.at_c(-1)
        )

    def down_side(self, k, m):
        if m == 1:
            src = self.down_g.at[self.at_f(k), self.at_c(1)]
        else:
            src = self.down_x.at[k - 1, m - 2]
        sem = self.down_x_sem
        return remote(
            src,
            self.down_x.at[k - 1, m - 1],
            sem.at[0, k - 1, m - 1],
            sem.at[1, k - 1, m - 1],
            ctx=self.at_c(-1),
        )

    def down_hop(self, k):
        src = self.down_x.at[0, self.n_c - 2] if k == 1 else self.down_z.at[k - 2]
        sem = self.down_z_sem
        return remote(
            src, self.down_z.at[k - 1], sem.at[0, k - 1], sem.at[1, k - 1], fsdp=self.at_f(-1)
        )

    def kv_copy(self, head, m):
        lanes = pl.ds(pl.multiple_of(head * 2 * HD, 2 * HD), 2 * HD)
        return remote(
            self.stage.at[head % 2, m - 1],
            self.kv_far.at[m - 1, :, lanes],
            self.kv_sem.at[0, head, m - 1],
            self.kv_sem.at[1, head, m - 1],
            ctx=self.at_c(m),
        )

    def out_local(self):
        return pltpu.make_async_copy(
            self.outs, self.outs_all.at[:, self.bit0, self.bit1], self.out_sem.at[0, 2]
        )

    def out_far(self):
        return remote(
            self.outs,
            self.outs_all.at[:, self.bit0, self.bit1],
            self.out_sem.at[0, 0],
            self.out_sem.at[1, 0],
            tp=self.peer1,
        )

    def out_near(self):
        pair = self.outs_all.at[:, self.bit0]
        return remote(pair, pair, self.out_sem.at[0, 1], self.out_sem.at[1, 1], tp=self.peer0)

    def begin(self):
        barrier = pltpu.get_barrier_semaphore()
        peers = [{"tp": self.peer0}, {"tp": self.peer1}, {"fsdp": self.at_f(-1)}]
        if self.n_f > 2:
            peers.append({"fsdp": self.at_f(1)})
        peers += [{"ctx": self.at_c(m)} for m in range(1, self.n_c)]
        for peer in peers:
            pl.semaphore_signal(
                barrier, inc=1, device_id=peer, device_id_type=pl.DeviceIdType.MESH
            )
        pl.semaphore_wait(barrier, len(peers))
        self.up_hop(1).start()
        for k in range(1, self.n_f + 1):
            self.down_side(k, 1).start()
        self.out_local().start()
        self.out_far().start()

    def up_event(self, m):
        self.up_hop(m - 1).wait()
        self.up_z[m - 2] += self.up_g[self.at_f(m)]
        if m < self.n_f:
            self.up_hop(m).start()
        else:
            self.up_side(1).start()

    def up_side_event(self, m):
        self.up_side(m - 1).wait()
        total = self.up_x[m - 2] + self.up_z[self.n_f - 2, self.at_c(m)]
        if m < self.n_c:
            self.up_x[m - 2] = total
            self.up_side(m).start()
        else:
            self.up_out[...] = total

    def down_event(self, k):
        for m in range(2, self.n_c + 1):
            self.down_side(k, m - 1).wait()
            self.down_x[k - 1, m - 2] += self.down_g[self.at_f(k), self.at_c(m)]
            if m < self.n_c:
                self.down_side(k, m).start()
        if k > 1:
            self.down_hop(k - 1).wait()
            total = self.down_z[k - 2] + self.down_x[k - 1, self.n_c - 2]
            if k < self.n_f:
                self.down_z[k - 2] = total
            else:
                self.down_out[...] = total
        if k < self.n_f:
            self.down_hop(k).start()

    def out_event(self):
        self.out_local().wait()
        self.out_far().wait()
        self.out_near().start()

    def end(self):
        self.out_near().wait()
        for head in range(self.heads):
            for m in range(1, self.n_c):
                if head >= self.heads - 2:
                    self.kv_copy(head, m).wait_send()
                self.kv_copy(head, m).wait_recv()

    def run(self, now, before):
        count = self.heads * STEPS_PER_HEAD
        plan = []
        for k in range(1, self.n_f + 1):
            plan.append(((k - 0.3) / (self.n_f + 0.3), lambda k=k: self.down_event(k)))
        for m in range(2, self.n_f + 1):
            plan.append(((m - 1.0) / (self.n_f - 0.2), lambda m=m: self.up_event(m)))
        plan.append((0.45, self.out_event))
        plan.sort(key=lambda item: item[0])
        late = [lambda m=m: self.up_side_event(m) for m in range(2, self.n_c + 1)] + [self.end]
        if before:

            @pl.when(now == 0)
            def _():
                self.begin()

            return
        for at in range(count):
            todo = [f for p, f in plan if min(int(p * count), count - 1) == at]
            if at == count - 1:
                todo = todo + late
            if todo:

                @pl.when(now == at)
                def _(todo=todo):
                    for f in todo:
                        f()


STEPS_PER_HEAD = 4


def attention_back(
    queries, grads, result, lse, kv_blocks, meta, heads, up_g, down_g, outs, tile=512
):
    rows = queries.shape[0] // STEPS_PER_HEAD
    n_f, n_c, own, wide_up = up_g.shape
    wide_down = down_g.shape[-1]
    count, span, blocks = queries.shape[0], kv_blocks[0].shape[0], len(kv_blocks)
    keys = span * blocks
    whole = lambda h, i, m: (0, 0)
    wide = pl.BlockSpec((count, heads * HD), whole)
    kv_spec = pl.BlockSpec((span, 2 * HD), lambda h, i, m: (0, h))
    anywhere = pl.BlockSpec(memory_space=pl.ANY)
    sem, shape = pltpu.SemaphoreType.DMA, jax.ShapeDtypeStruct

    def held(array):
        return pl.BlockSpec(array.shape, lambda h, i, m: (0,) * array.ndim)

    return pl.pallas_call(
        functools.partial(backward_kernel, heads, blocks, n_f, tile, rows),
        grid_spec=pltpu.PrefetchScalarGridSpec(
            num_scalar_prefetch=1,
            grid=(heads, count // rows),
            in_specs=[wide] * 3
            + [pl.BlockSpec((heads, count), whole)]
            + [held(up_g), held(down_g), held(outs)]
            + [kv_spec] * blocks,
            out_specs=[
                wide,
                kv_spec,
                pl.BlockSpec((own, wide_up), whole),
                pl.BlockSpec((own, wide_down), whole),
                anywhere,
                anywhere,
            ],
            scratch_shapes=[
                pltpu.VMEM((keys, 2 * HD), jnp.bfloat16),
                pltpu.VMEM((keys, 2 * HD), jnp.bfloat16),
                pltpu.VMEM((2 * HD, keys), jnp.bfloat16),
                pltpu.VMEM((keys, 128), jnp.float32),
                pltpu.VMEM((rows, 2 * HD), jnp.float32),
                pltpu.VMEM((rows, 2 * HD), jnp.float32),
                pltpu.VMEM((rows, 2 * HD), jnp.float32),
                pltpu.VMEM((keys, 2 * HD), jnp.float32),
                pltpu.VMEM((keys, 2 * HD), jnp.float32),
                pltpu.VMEM((2 * HD, rows), jnp.float32),
                pltpu.VMEM((2, n_c - 1, span, 2 * HD), jnp.float32),
                pltpu.VMEM((n_f - 1, n_c, own, wide_up), jnp.float32),
                pltpu.VMEM((n_c - 1, own, wide_up), jnp.float32),
                pltpu.VMEM((n_f, n_c - 1, own, wide_down), jnp.float32),
                pltpu.VMEM((n_f - 1, own, wide_down), jnp.float32),
                sem((2, n_f - 1)),
                sem((2, n_c - 1)),
                sem((2, n_f, n_c - 1)),
                sem((2, n_f - 1)),
                sem((2, heads, n_c - 1)),
                sem((2, 3)),
            ],
        ),
        out_shape=[
            shape((count, heads * HD), jnp.float32),
            shape((span, 2 * heads * HD), jnp.float32),
            shape((own, wide_up), jnp.float32),
            shape((own, wide_down), jnp.float32),
            shape((n_c - 1, span, 2 * heads * HD), jnp.float32),
            shape((outs.shape[0], 2, 2) + outs.shape[1:], jnp.float32),
        ],
        compiler_params=pltpu.CompilerParams(
            dimension_semantics=("arbitrary", "arbitrary"),
            collective_id=2,
            has_side_effects=True,
            vmem_limit_bytes=62 << 20,
        ),
        cost_estimate=pl.CostEstimate(
            flops=60 * heads * count * keys * HD,
            bytes_accessed=16 * keys * heads * HD + 16 * count * heads * HD,
            transcendentals=heads * count * keys,
        ),
        name="attention_backward",
    )(meta, queries, grads, result, lse, up_g, down_g, outs, *kv_blocks)


def dot_three(left, right, left_dim, right_dim):
    left_high, left_low = left
    right_high, right_low = right
    return dot(left_high, right_high, left_dim, right_dim) + (
        dot(left_high, right_low, left_dim, right_dim)
        + dot(left_low, right_high, left_dim, right_dim)
    )


def tiles_of(count, body):
    tile = 256 if count % 256 == 0 else count

    def step(n, _):
        body(pl.ds(pl.multiple_of(n * tile, tile), tile))
        return 0

    lax.fori_loop(0, count // tile, step, 0)


def middle_kernel(
    chunks, rows,
    att_ref, up_ref, down_ref, outw_ref,
    b_out, gain_1, shift_1, b_up, b_down, gain_2, shift_2, tok_hbm, cot_hbm,
    out_own, mid_own, gatt, d_up, d_down, vec, d_bup,
    part, rx0, rx1, full, act_hi, act_lo, slope, tok, cot, norm_1, recip_1,
    up_s, down_s, outw_s, xs, ys, ts, send0, recv0, send1, recv1, own_sem,
):
    half, quarter = rows // 2, rows // 4
    me = lax.axis_index("tp")
    bit0, bit1 = me % 2, me // 2 % 2
    peer0, peer1 = me + 1 - 2 * bit0, me + 2 - 4 * bit1
    home0 = pl.multiple_of(bit0 * half, half)
    away0 = pl.multiple_of((1 - bit0) * half, half)
    mine = pl.multiple_of(home0 + bit1 * quarter, quarter)
    away1 = pl.multiple_of(home0 + (1 - bit1) * quarter, quarter)
    own = pl.ds(mine, quarter)

    def remote(src, dst, send, recv, peer):
        return pltpu.make_async_remote_copy(
            src_ref=src,
            dst_ref=dst,
            send_sem=send,
            recv_sem=recv,
            device_id={"tp": peer},
            device_id_type=pl.DeviceIdType.MESH,
        )

    def scatter0(s, c):
        return remote(
            part.at[c, pl.ds(away0, half)], rx0.at[s, c], send0.at[0, s, c], recv0.at[0, s, c], peer0
        )

    def scatter1(s, c):
        return remote(
            part.at[c, pl.ds(away1, quarter)],
            rx1.at[s, c],
            send1.at[0, s, c],
            recv1.at[0, s, c],
            peer1,
        )

    def gather1(s, c):
        return remote(
            full.at[s, c, own], full.at[s, c, own], send1.at[1, s, c], recv1.at[1, s, c], peer1
        )

    def gather0(s, c):
        place = pl.ds(home0, half)
        return remote(
            full.at[s, c, place], full.at[s, c, place], send0.at[1, s, c], recv0.at[1, s, c], peer0
        )

    def own_copies(c):
        where = pl.ds(pl.multiple_of(c * rows + mine, quarter), quarter)
        return (
            pltpu.make_async_copy(tok_hbm.at[where], tok.at[c], own_sem.at[0, c]),
            pltpu.make_async_copy(cot_hbm.at[where], cot.at[c], own_sem.at[1, c]),
        )

    for c in range(chunks):
        for copy in own_copies(c):
            copy.start()
    barrier = pltpu.get_barrier_semaphore()
    for peer in (peer0, peer1):
        pl.semaphore_signal(
            barrier, inc=1, device_id={"tp": peer}, device_id_type=pl.DeviceIdType.MESH
        )

    def split_rows(source, target):
        count = source.shape[0]
        step = 128

        def one(i, _):
            at = pl.ds(pl.multiple_of(i * step, step), step)
            target[0, at, :], target[1, at, :] = halves(source[at, :])
            return 0

        lax.fori_loop(0, count // step, one, 0)

    split_rows(outw_ref, outw_s)
    split_rows(up_ref, up_s)
    split_rows(down_ref, down_s)
    d_bup[...] = jnp.zeros_like(d_bup)
    vec[...] = jnp.zeros_like(vec)
    d_up[...] = jnp.zeros_like(d_up)
    d_down[...] = jnp.zeros_like(d_down)
    for c in range(chunks):
        for copy in own_copies(c):
            copy.wait()
    pl.semaphore_wait(barrier, 2)

    def split_into(target, value):
        target[0], target[1] = halves(value)

    def finish0(s, c):
        scatter0(s, c).wait()
        away = pl.ds(away1 - home0, quarter)
        part[c, pl.ds(away1, quarter), :] += rx0[s, c, away, :]
        scatter1(s, c).start()
        stay = pl.ds(mine - home0, quarter)
        part[c, own, :] += rx0[s, c, stay, :]

    def finish1(s, c):
        scatter1(s, c).wait()
        return part[c, own, :] + rx1[s, c]

    def forward1(s, c):
        gather1(s, c).wait()
        gather0(s, c).start()

    def trailing(c, now, before):
        if before is not None:

            @pl.when(c == 0)
            def _():
                before(chunks - 1)

        if now is not None:

            @pl.when(c > 0)
            def _():
                now(c - 1)

    def stage(body):
        def one(c, _):
            body(c)
            return 0

        lax.fori_loop(0, chunks, one, 0)

    def at_rows(c):
        return pl.ds(pl.multiple_of(c * rows, rows), rows)

    width = up_ref.shape[0]
    hidden = up_ref.shape[1]

    def attention_out(c):
        left = halves(att_ref[at_rows(c), :])

        def columns(n):
            part[c, :, n] = dot_three(left, (outw_s[0, n, :], outw_s[1, n, :]), 1, 1)

        tiles_of(width, columns)
        scatter0(0, c).start()
        trailing(c, functools.partial(finish0, 0), None)

    stage(attention_out)

    def first_norm(c):
        trailing(c, None, functools.partial(finish0, 0))
        resid = finish1(0, c) + tok[c] + b_out[...]
        n_1, r_1 = normalized(resid)
        norm_1[c] = n_1
        recip_1[c] = jnp.broadcast_to(r_1, recip_1.shape[1:])
        full[0, c, own, :] = n_1 * gain_1[...] + shift_1[...]
        gather1(0, c).start()
        trailing(c, functools.partial(forward1, 0), None)

    stage(first_norm)

    def feed_forward(c):
        gather0(0, c).wait()
        split_into(xs, full[0, c])

        def columns(n):
            pre = dot_three((xs[0], xs[1]), (up_s[0, :, n], up_s[1, :, n]), 1, 0) + b_up[:, n]
            cdf = 0.5 + 0.5 * lax.erf(pre * math.sqrt(0.5))
            slope[c, :, n] = cdf + pre * (
                jnp.exp(-0.5 * pre * pre) * (1.0 / math.sqrt(2.0 * math.pi))
            )
            act_hi[c, :, n], act_lo[c, :, n] = halves(pre * cdf)

        tiles_of(hidden, columns)

        def back(n):
            part[c, :, n] = dot_three(
                (act_hi[c], act_lo[c]), (down_s[0, n, :], down_s[1, n, :]), 1, 1
            )

        tiles_of(width, back)
        scatter0(1, c).start()
        trailing(c, functools.partial(finish0, 1), functools.partial(forward1, 0))

    def second_norm(c):
        trailing(c, None, functools.partial(finish0, 1))
        ffn = finish1(1, c) + full[0, c, own, :] + b_down[...]
        n_2, r_2 = normalized(ffn)
        out_own[c] = n_2 * gain_2[...] + shift_2[...]
        grad = cot[c]
        second = norm_back(grad, gain_2[...], n_2, r_2)
        full[1, c, own, :] = second
        gather1(1, c).start()
        vec[3:4, :] += jnp.sum(second, axis=0, keepdims=True)
        vec[4:5, :] += jnp.sum(grad * n_2, axis=0, keepdims=True)
        vec[5:6, :] += jnp.sum(grad, axis=0, keepdims=True)
        trailing(c, functools.partial(forward1, 1), None)

    def feed_back(c):
        gather0(1, c).wait()
        split_into(xs, full[1, c])

        def columns(n):
            grad = dot_three((xs[0], xs[1]), (down_s[0, :, n], down_s[1, :, n]), 1, 0)
            grad = grad * slope[c, :, n]
            slope[c, :, n] = grad
            ys[0, :, n], ys[1, :, n] = halves(grad)
            d_bup[:, n] += jnp.sum(grad, axis=0, keepdims=True)

        tiles_of(hidden, columns)

        def back(n):
            part[c, :, n] = dot_three((ys[0], ys[1]), (up_s[0, n, :], up_s[1, n, :]), 1, 1)

        tiles_of(width, back)
        scatter0(2, c).start()
        trailing(c, functools.partial(finish0, 2), functools.partial(forward1, 1))

    def middle_norm(c):
        trailing(c, None, functools.partial(finish0, 2))
        first = finish1(2, c) + full[1, c, own, :]
        n_1 = norm_1[c]
        mid = norm_back(first, gain_1[...], n_1, recip_1[c, :, :1])
        mid_own[c] = mid
        full[2, c, own, :] = mid
        gather1(2, c).start()
        vec[0:1, :] += jnp.sum(mid, axis=0, keepdims=True)
        vec[1:2, :] += jnp.sum(first * n_1, axis=0, keepdims=True)
        vec[2:3, :] += jnp.sum(first, axis=0, keepdims=True)
        trailing(c, functools.partial(forward1, 2), None)
        split_into(ts, full[1, c].T)

        def columns(n):
            d_down[:, n] += dot_three((ts[0], ts[1]), (act_hi[c, :, n], act_lo[c, :, n]), 1, 0)

        tiles_of(hidden, columns)

    def last(c):
        gather0(2, c).wait()
        mid = full[2, c]
        gatt[at_rows(c), :] = dot_three(halves(mid), (outw_s[0], outw_s[1]), 1, 0)
        trailing(c, None, functools.partial(forward1, 2))
        split_into(ts, mid.T)
        d_down[:, hidden:] += dot_three((ts[0], ts[1]), halves(att_ref[at_rows(c), :]), 1, 0)
        split_into(ts, full[0, c].T)

        def columns(n):
            d_up[:, n] += dot_three((ts[0], ts[1]), halves(slope[c, :, n]), 1, 0)

        tiles_of(hidden, columns)

    stage(feed_forward)
    stage(second_norm)
    stage(feed_back)
    stage(middle_norm)
    stage(last)


def middle(attended, wide_up, wide_down_t, wide_out_t, vectors, tokens, cot, chunks=4):
    count, width = tokens.shape
    hidden, split_at = wide_up.shape[1], attended.shape[1]
    rows = count // chunks
    half, quarter = rows // 2, rows // 4
    vmem = pl.BlockSpec(memory_space=pltpu.VMEM)
    anywhere = pl.BlockSpec(memory_space=pl.ANY)
    f32, bf16 = jnp.float32, jnp.bfloat16
    sems = pltpu.SemaphoreType.DMA((2, 3, chunks))
    shape = jax.ShapeDtypeStruct
    return pl.pallas_call(
        functools.partial(middle_kernel, chunks, rows),
        in_specs=[vmem] * 11 + [anywhere] * 2,
        out_specs=[vmem] * 7,
        out_shape=[
            shape((chunks, quarter, width), f32),
            shape((chunks, quarter, width), f32),
            shape((count, split_at), f32),
            shape((width, hidden), f32),
            shape((width, hidden + split_at), f32),
            shape((8, width), f32),
            shape((1, hidden), f32),
        ],
        scratch_shapes=[
            pltpu.VMEM((chunks, rows, width), f32),
            pltpu.VMEM((3, chunks, half, width), f32),
            pltpu.VMEM((3, chunks, quarter, width), f32),
            pltpu.VMEM((3, chunks, rows, width), f32),
            pltpu.VMEM((chunks, rows, hidden), bf16),
            pltpu.VMEM((chunks, rows, hidden), bf16),
            pltpu.VMEM((chunks, rows, hidden), f32),
            pltpu.VMEM((chunks, quarter, width), f32),
            pltpu.VMEM((chunks, quarter, width), f32),
            pltpu.VMEM((chunks, quarter, width), f32),
            pltpu.VMEM((chunks, quarter, 128), f32),
            pltpu.VMEM((2, width, hidden), bf16),
            pltpu.VMEM((2, width, hidden), bf16),
            pltpu.VMEM((2, width, split_at), bf16),
            pltpu.VMEM((2, rows, width), bf16),
            pltpu.VMEM((2, rows, hidden), bf16),
            pltpu.VMEM((2, width, rows), bf16),
            sems, sems, sems, sems,
            pltpu.SemaphoreType.DMA((2, chunks)),
        ],
        compiler_params=pltpu.CompilerParams(
            collective_id=1, has_side_effects=True, vmem_limit_bytes=62 << 20
        ),
        cost_estimate=pl.CostEstimate(
            flops=6 * count * width * (6 * hidden + 3 * split_at),
            bytes_accessed=4 * width * (5 * hidden + 3 * split_at),
            transcendentals=2 * count * hidden,
        ),
        name="middle",
    )(attended, wide_up, wide_down_t, wide_out_t, *vectors, tokens, cot)


def per_device(
    inputs,
    lengths,
    w_qkv,
    b_query,
    b_value,
    w_out,
    b_out,
    gain_attn,
    shift_attn,
    w_up,
    b_up,
    w_down,
    b_down,
    gain_ffn,
    shift_ffn,
    cotangent,
):
    width = inputs.shape[-1]
    block_len = inputs.shape[1]
    heads = b_query.shape[0] // HD
    split_at = heads * HD
    hidden = b_up.shape[0]
    tokens = inputs.reshape(block_len, width)
    cot = cotangent.reshape(block_len, width)
    length = lengths[0]
    n_c = lax.axis_size("ctx")
    at_c = lax.axis_index("ctx")

    def regroup(columns):
        parts = columns.reshape(columns.shape[:-1] + (heads, 3 * HD))
        lead = columns.shape[:-1]
        return jnp.concatenate(
            [
                parts[..., HD:].reshape(lead + (2 * split_at,)),
                parts[..., :HD].reshape(lead + (split_at,)),
            ],
            axis=-1,
        )

    bias_kv = jnp.stack(
        [jnp.zeros((heads, HD), jnp.float32), b_value.reshape(heads, HD)], axis=1
    ).reshape(-1)
    wide_kv, wide_q = weight_gather(regroup(w_qkv), [2 * split_at, split_at])
    rest = jnp.concatenate([w_up, w_down.T, w_out.T], axis=1)
    wide_up, wide_down_t, wide_out_t = weight_gather(rest, [hidden, hidden, split_at])

    kv_blocks = [contract(tokens, wide_kv, 1, 0) + bias_kv]
    for m in range(1, n_c):
        kv_blocks.append(ringed(kv_blocks[-1], "ctx", 1))
    queries = contract(tokens, wide_q, 1, 0) + b_query
    meta = jnp.stack([length] + [(at_c - m) % n_c * block_len for m in range(n_c)])
    attended, log_sums = attention(queries, kv_blocks, meta, heads)

    flat = lambda v: v.reshape(1, -1)
    vectors = [flat(v) for v in (b_out, gain_attn, shift_attn, b_up, b_down, gain_ffn, shift_ffn)]
    outs, grad_mid, grad_att, d_up, d_down_out, vec_rows, d_bup = middle(
        attended, wide_up, wide_down_t, wide_out_t, vectors, tokens, cot
    )
    sums = small_sum(vec_rows, ("tp", "fsdp", "ctx"))
    blocked = (lax.axis_size("fsdp"), n_c, w_up.shape[0])
    grad_q, grad_kv, d_wup, down_out, kv_far, outputs = attention_back(
        queries,
        grad_att,
        attended,
        log_sums,
        kv_blocks,
        meta,
        heads,
        d_up.reshape(blocked + (hidden,)),
        d_down_out.reshape(blocked + (hidden + split_at,)),
        outs,
    )
    d_wdown = down_out[:, :hidden].T
    d_wout = down_out[:, hidden:].T
    for m in range(n_c - 1):
        grad_kv = grad_kv + kv_far[m]
    back = contract(grad_kv, wide_kv, 1, 1) + contract(grad_q, wide_q, 1, 1)
    tail_sums = small_sum(
        jnp.concatenate([jnp.sum(grad_kv, axis=0), jnp.sum(grad_q, axis=0), d_bup[0]]),
        ("fsdp", "ctx"),
    )
    d_bvalue = tail_sums[: 2 * split_at].reshape(heads, 2, HD)[:, 1].reshape(-1)
    d_bquery = tail_sums[2 * split_at : 3 * split_at]
    d_bup = tail_sums[3 * split_at :]
    own = grad_scatter([contract(tokens, grad_kv, 0, 0), contract(tokens, grad_q, 0, 0)])
    own_rows_count = own.shape[0]
    d_wqkv = jnp.concatenate(
        [
            own[:, 2 * split_at :].reshape(own_rows_count, heads, HD),
            own[:, : 2 * split_at].reshape(own_rows_count, heads, 2 * HD),
        ],
        axis=2,
    ).reshape(own_rows_count, 3 * split_at)
    d_inputs = quarter_gather(grad_mid + quarter_scatter(back, grad_mid.shape[0]))
    return (
        outputs.reshape(1, block_len, width),
        d_inputs.reshape(1, block_len, width),
        d_wqkv,
        d_bquery,
        d_bvalue,
        d_wout,
        sums[0],
        sums[1],
        sums[2],
        d_wup,
        d_bup,
        d_wdown,
        sums[3],
        sums[4],
        sums[5],
    )


def solution(mesh):
    rows_of, cols_of = P(("fsdp", "ctx"), "tp"), P("tp", ("fsdp", "ctx"))
    seq, by_tp, same = P("fsdp", "ctx", None), P("tp"), P()
    in_specs = (
        seq, P("fsdp"), rows_of, by_tp, by_tp, cols_of, same, same, same,
        rows_of, by_tp, cols_of, same, same, same, seq,
    )
    out_specs = (
        seq, seq, rows_of, by_tp, by_tp, cols_of, same, same, same,
        rows_of, by_tp, cols_of, same, same, same,
    )
    return jax.shard_map(
        per_device, mesh=mesh, in_specs=in_specs, out_specs=out_specs, check_vma=False
    )
```

```python
import functools
import math

import jax
import jax.numpy as jnp
from jax import lax
from jax.experimental import pallas as pl
from jax.experimental.pallas import tpu as pltpu
from jax.sharding import PartitionSpec as P

HD = 64
LOG2E = math.log2(math.e)
NORM_EPS = 1e-12
MASKED = -1e30
THREE = lax.Precision.HIGH


def contract(left, right, left_dim, right_dim):
    return lax.dot_general(
        left,
        right,
        (((left_dim,), (right_dim,)), ((), ())),
        precision=THREE,
        preferred_element_type=jnp.float32,
    )


def ringed(block, axis, distance):
    count = lax.axis_size(axis)
    return lax.ppermute(block, axis, [(i, (i + distance) % count) for i in range(count)])


def swapped(block, axis, bit):
    return lax.ppermute(block, axis, [(i, i ^ bit) for i in range(lax.axis_size(axis))])


def bits_of(axis):
    bits, bit = [], 1
    while bit < lax.axis_size(axis):
        bits.append(bit)
        bit *= 2
    return bits


def quarter_scatter(part, chunks):
    rank = lax.axis_index("tp")
    count, width = part.shape
    block = part.reshape(chunks, 2, 2, count // (4 * chunks), width)
    for bit, axis in ((1, 1), (2, 1)):
        upper = rank // bit % 2
        leaving = lax.dynamic_index_in_dim(block, 1 - upper, axis, keepdims=False)
        staying = lax.dynamic_index_in_dim(block, upper, axis, keepdims=False)
        block = staying + swapped(leaving, "tp", bit)
    return block


def quarter_gather(block):
    rank = lax.axis_index("tp")
    for bit in (2, 1):
        other = swapped(block, "tp", bit)
        upper = rank // bit % 2 == 1
        block = jnp.where(
            upper, jnp.stack([other, block], axis=1), jnp.stack([block, other], axis=1)
        )
    return block.reshape(-1, block.shape[-1])


def small_sum(vector, axes):
    for axis in axes:
        for bit in bits_of(axis):
            vector = vector + swapped(vector, axis, bit)
    return vector


def weight_gather(shard, widths):
    rows = shard.shape[0]
    n_f, n_c = lax.axis_size("fsdp"), lax.axis_size("ctx")
    at_f, at_c = lax.axis_index("fsdp"), lax.axis_index("ctx")
    wholes = [jnp.zeros((n_f * n_c * rows, width), jnp.float32) for width in widths]
    along_f = shard
    for k in range(n_f):
        if k:
            along_f = ringed(along_f, "fsdp", 1)
        along_c = along_f
        for m in range(n_c):
            if m:
                along_c = ringed(along_c, "ctx", 1)
            place = ((at_f - k) % n_f * n_c + (at_c - m) % n_c) * rows
            start = 0
            for i, width in enumerate(widths):
                wholes[i] = lax.dynamic_update_slice(
                    wholes[i], along_c[:, start : start + width], (place, 0)
                )
                start += width
    return wholes


def grad_scatter(pieces):
    n_f, n_c = lax.axis_size("fsdp"), lax.axis_size("ctx")
    at_f, at_c = lax.axis_index("fsdp"), lax.axis_index("ctx")
    rows = pieces[0].shape[0] // (n_f * n_c)

    def piece(f, c):
        start = (f % n_f * n_c + c % n_c) * rows
        cut = [lax.dynamic_slice_in_dim(p, start, rows, 0) for p in pieces]
        return cut[0] if len(cut) == 1 else jnp.concatenate(cut, axis=1)

    total = None
    for k in range(1, n_f + 1):
        over_c = piece(at_f - k, at_c - 1)
        for m in range(2, n_c + 1):
            over_c = ringed(over_c, "ctx", 1) + piece(at_f - k, at_c - m)
        total = over_c if total is None else ringed(total, "fsdp", 1) + over_c
    return total


def normalized(values):
    centred = values - jnp.mean(values, axis=-1, keepdims=True)
    spread = jnp.mean(centred * centred, axis=-1, keepdims=True)
    recip = lax.rsqrt(spread + NORM_EPS)
    return centred * recip, recip


def norm_back(grad, gain, normed, recip):
    scaled = grad * gain
    return recip * (
        scaled
        - jnp.mean(scaled, axis=-1, keepdims=True)
        - normed * jnp.mean(scaled * normed, axis=-1, keepdims=True)
    )


def halves(values):
    high = values.astype(jnp.bfloat16)
    return high, (values - high.astype(jnp.float32)).astype(jnp.bfloat16)


def low_half(shape):
    return lax.broadcasted_iota(jnp.int32, shape, 1) < HD


def dot(left, right, left_dim, right_dim):
    return lax.dot_general(
        left, right, (((left_dim,), (right_dim,)), ((), ())), preferred_element_type=jnp.float32
    )


def doubled(ref, rows, head, scratch, heads):
    for j in range(heads):

        @pl.when(head == j)
        def _():
            piece = ref[rows, j * HD : (j + 1) * HD]
            scratch[...] = jnp.concatenate([piece, piece], axis=1)


def packed(pair, first):
    low = low_half(pair.shape)
    turned = pltpu.roll(pair, HD, 1)
    twice = jnp.where(low, pair, turned) if first else jnp.where(low, turned, pair)
    high, rest = halves(twice)
    return jnp.where(low, high.astype(jnp.float32), rest.astype(jnp.float32)).astype(jnp.bfloat16)


def stacked(half):
    high, rest = halves(half)
    return jnp.concatenate([high, rest], axis=0)


def key_bias(meta_ref, block, start, count, width):
    place = meta_ref[1 + block] + start + lax.broadcasted_iota(jnp.int32, (count, width), 0)
    return jnp.where(place < meta_ref[0], 0.0, MASKED)


def forward_kernel(heads, blocks, tile, rows, meta_ref, q_ref, *refs):
    kv_refs, (out_ref, lse_ref, kp, vt, bias, qd, acc) = refs[:blocks], refs[blocks:]
    head, step = pl.program_id(0), pl.program_id(1)
    span = kv_refs[0].shape[0]
    per = span // tile

    @pl.when(step == 0)
    def _():
        for b in range(blocks):

            def prepare(j, _, b=b):
                at = pl.ds(pl.multiple_of(j * tile, tile), tile)
                to = pl.ds(pl.multiple_of(b * span + j * tile, tile), tile)
                pair = kv_refs[b][at, :]
                kp[to, :] = packed(pair, True)
                vt[:, to] = stacked(pair.T[HD:, :])
                bias[to, :] = key_bias(meta_ref, b, j * tile, tile, 128)
                return 0

            lax.fori_loop(0, per, prepare, 0)

    here = pl.ds(pl.multiple_of(step * rows, rows), rows)
    doubled(q_ref, here, head, qd, heads)
    q_high, q_low = halves(qd[...] * (LOG2E * HD**-0.5))
    q_four = jnp.concatenate([q_high, q_low], axis=1)
    acc[...] = jnp.zeros_like(acc)

    def key_tile(j, carry):
        top, total = carry
        at = pl.ds(pl.multiple_of(j * tile, tile), tile)
        k_two = kp[at, :]
        scores = dot(jnp.concatenate([k_two, k_two], axis=1), q_four, 1, 1)
        scores = scores + jnp.concatenate([bias[at, :]] * (rows // 128), axis=1)
        new_top = jnp.maximum(top, jnp.max(scores, axis=0, keepdims=True))
        fade = jnp.exp2(top - new_top)
        probs = jnp.exp2(scores - new_top)
        total = total * fade + jnp.sum(probs, axis=0, keepdims=True)
        high, low = halves(probs)
        v_two = vt[:, at]
        acc[...] = acc[...] * fade + (dot(v_two, high, 1, 0) + dot(v_two, low, 1, 0))
        return new_top, total

    top, total = lax.fori_loop(
        0,
        blocks * per,
        key_tile,
        (jnp.full((1, rows), MASKED, jnp.float32), jnp.zeros((1, rows), jnp.float32)),
    )
    result = acc[:HD, :] + acc[HD:, :]
    result = (result / total).T
    for j in range(heads):

        @pl.when(head == j)
        def _():
            out_ref[here, j * HD : (j + 1) * HD] = result
            lse_ref[j : j + 1, here] = top + jnp.log2(total)


def attention(queries, kv_blocks, meta, heads, rows=256, tile=512):
    count, span, blocks = queries.shape[0], kv_blocks[0].shape[0], len(kv_blocks)
    keys = span * blocks
    whole = lambda h, i, m: (0, 0)
    return pl.pallas_call(
        functools.partial(forward_kernel, heads, blocks, tile, rows),
        grid_spec=pltpu.PrefetchScalarGridSpec(
            num_scalar_prefetch=1,
            grid=(heads, count // rows),
            in_specs=[pl.BlockSpec((count, heads * HD), whole)]
            + [pl.BlockSpec((span, 2 * HD), lambda h, i, m: (0, h))] * blocks,
            out_specs=[
                pl.BlockSpec((count, heads * HD), whole),
                pl.BlockSpec((heads, count), whole),
            ],
            scratch_shapes=[
                pltpu.VMEM((keys, 2 * HD), jnp.bfloat16),
                pltpu.VMEM((2 * HD, keys), jnp.bfloat16),
                pltpu.VMEM((keys, 128), jnp.float32),
                pltpu.VMEM((rows, 2 * HD), jnp.float32),
                pltpu.VMEM((2 * HD, rows), jnp.float32),
            ],
        ),
        out_shape=[
            jax.ShapeDtypeStruct((count, heads * HD), jnp.float32),
            jax.ShapeDtypeStruct((heads, count), jnp.float32),
        ],
        compiler_params=pltpu.CompilerParams(dimension_semantics=("arbitrary", "arbitrary")),
        cost_estimate=pl.CostEstimate(
            flops=24 * heads * count * keys * HD,
            bytes_accessed=8 * keys * heads * HD + 8 * count * heads * HD,
            transcendentals=heads * count * keys,
        ),
        name="attention_forward",
    )(meta, queries, *kv_blocks)


def backward_kernel(
    heads, blocks, n_f, tile, rows, meta_ref, q_ref, do_ref, out_ref, lse_ref, up_g, down_g, outs,
    *refs,
):
    kv_refs = refs[:blocks]
    dq_ref, dkv_ref, up_out, down_out, kv_far, outs_all = refs[blocks : blocks + 6]
    kp, vp, kt, bias, qd, dd, od, dk, dv, acc, stage = refs[blocks + 6 : blocks + 17]
    transfers = Transfers(
        blocks, n_f, heads, up_g, down_g, outs, up_out, down_out, kv_far, outs_all, stage,
        *refs[blocks + 17 :],
    )
    head, step = pl.program_id(0), pl.program_id(1)
    steps = pl.num_programs(1)
    transfers.run(head * steps + step, before=True)
    span = kv_refs[0].shape[0]
    per = span // tile

    @pl.when(step == 0)
    def _():
        dk[...] = jnp.zeros_like(dk)
        dv[...] = jnp.zeros_like(dv)
        for b in range(blocks):

            def prepare(j, _, b=b):
                at = pl.ds(pl.multiple_of(j * tile, tile), tile)
                to = pl.ds(pl.multiple_of(b * span + j * tile, tile), tile)
                pair = kv_refs[b][at, :]
                kp[to, :] = packed(pair, True)
                vp[to, :] = packed(pair, False)
                kt[:, to] = stacked(pair.T[:HD, :])
                bias[to, :] = key_bias(meta_ref, b, j * tile, tile, 128)
                return 0

            lax.fori_loop(0, per, prepare, 0)

    here = pl.ds(pl.multiple_of(step * rows, rows), rows)
    doubled(q_ref, here, head, qd, heads)
    doubled(do_ref, here, head, dd, heads)
    doubled(out_ref, here, head, od, heads)
    low = low_half((rows, 2 * HD))

    def both(values):
        high, rest = halves(values)
        mixed = jnp.where(low, high.astype(jnp.float32), rest.astype(jnp.float32))
        return jnp.concatenate([high, rest], axis=1), mixed.astype(jnp.bfloat16)

    q_four, q_two = both(qd[...] * (LOG2E * HD**-0.5))
    do_four, do_two = both(dd[...])
    delta = jnp.sum((dd[...] * od[...]).T[:HD, :], axis=0, keepdims=True)
    lse = lse_ref[0:1, here]
    for j in range(1, heads):
        lse = jnp.where(head == j, lse_ref[j : j + 1, here], lse)
    acc[...] = jnp.zeros_like(acc)

    def key_tile(j, _):
        at = pl.ds(pl.multiple_of(j * tile, tile), tile)
        k_two, v_two = kp[at, :], vp[at, :]
        scores = dot(jnp.concatenate([k_two, k_two], axis=1), q_four, 1, 1)
        scores = scores + jnp.concatenate([bias[at, :]] * (rows // 128), axis=1)
        probs = jnp.exp2(scores - lse)
        high, rest = halves(probs)
        dv[at, :] += dot(high, do_two, 1, 0) + dot(rest, do_two, 1, 0)
        grad_p = dot(jnp.concatenate([v_two, v_two], axis=1), do_four, 1, 1)
        grad_s = probs * (grad_p - delta)
        high, rest = halves(grad_s)
        dk[at, :] += dot(high, q_two, 1, 0) + dot(rest, q_two, 1, 0)
        k_t = kt[:, at]
        acc[...] += dot(k_t, high, 1, 0) + dot(k_t, rest, 1, 0)
        return 0

    lax.fori_loop(0, blocks * per, key_tile, 0)
    result = ((acc[:HD, :] + acc[HD:, :]) * HD**-0.5).T
    for j in range(heads):

        @pl.when(head == j)
        def _():
            dq_ref[here, j * HD : (j + 1) * HD] = result

    def turned(rows_at):
        grad_k, grad_v = dk[rows_at, :], dv[rows_at, :]
        grad_k = (grad_k + pltpu.roll(grad_k, HD, 1)) * (1.0 / LOG2E)
        grad_v = grad_v + pltpu.roll(grad_v, HD, 1)
        return jnp.where(low_half(grad_k.shape), grad_k, grad_v)

    @pl.when(step == steps - 1)
    def _():
        for b in range(1, blocks):

            @pl.when(head >= 2)
            def _(b=b):
                transfers.kv_copy(head - 2, b).wait_send()

            def finish(j, _, b=b):
                at = pl.ds(pl.multiple_of(j * tile, tile), tile)
                to = pl.ds(pl.multiple_of(b * span + j * tile, tile), tile)
                stage[head % 2, b - 1, at, :] = turned(to)
                return 0

            lax.fori_loop(0, per, finish, 0)
            transfers.kv_copy(head, b).start()

        def keep(j, _):
            at = pl.ds(pl.multiple_of(j * tile, tile), tile)
            dkv_ref[at, :] = turned(at)
            return 0

        lax.fori_loop(0, per, keep, 0)

    transfers.run(head * steps + step, before=False)


def remote(src, dst, send, recv, **peer):
    return pltpu.make_async_remote_copy(
        src_ref=src,
        dst_ref=dst,
        send_sem=send,
        recv_sem=recv,
        device_id=peer,
        device_id_type=pl.DeviceIdType.MESH,
    )


class Transfers:
    def __init__(
        self, n_c, n_f, heads, up_g, down_g, outs, up_out, down_out, kv_far, outs_all, stage,
        up_z, up_x, down_x, down_z, up_z_sem, up_x_sem, down_x_sem, down_z_sem, kv_sem, out_sem,
    ):
        self.n_c, self.n_f, self.heads = n_c, n_f, heads
        self.up_g, self.down_g, self.outs = up_g, down_g, outs
        self.up_out, self.down_out, self.kv_far, self.outs_all = up_out, down_out, kv_far, outs_all
        self.stage = stage
        self.up_z, self.up_x, self.down_x, self.down_z = up_z, up_x, down_x, down_z
        self.up_z_sem, self.up_x_sem = up_z_sem, up_x_sem
        self.down_x_sem, self.down_z_sem, self.kv_sem = down_x_sem, down_z_sem, kv_sem
        self.out_sem = out_sem
        self.f, self.c, me = lax.axis_index("fsdp"), lax.axis_index("ctx"), lax.axis_index("tp")
        self.bit0, self.bit1 = me % 2, me // 2 % 2
        self.peer0, self.peer1 = me + 1 - 2 * self.bit0, me + 2 - 4 * self.bit1

    def at_f(self, k):
        return (self.f + (self.n_f - k)) % self.n_f

    def at_c(self, m):
        return (self.c + (self.n_c - m)) % self.n_c

    def up_hop(self, m):
        src = self.up_g.at[self.at_f(1)] if m == 1 else self.up_z.at[m - 2]
        sem = self.up_z_sem
        return remote(
            src, self.up_z.at[m - 1], sem.at[0, m - 1], sem.at[1, m - 1], fsdp=self.at_f(-1)
        )

    def up_side(self, m):
        src = self.up_z.at[self.n_f - 2, self.at_c(1)] if m == 1 else self.up_x.at[m - 2]
        sem = self.up_x_sem
        return remote(
            src, self.up_x.at[m - 1], sem.at[0, m - 1], sem.at[1, m - 1], ctx=self.at_c(-1)
        )

    def down_side(self, k, m):
        if m == 1:
            src = self.down_g.at[self.at_f(k), self.at_c(1)]
        else:
            src = self.down_x.at[k - 1, m - 2]
        sem = self.down_x_sem
        return remote(
            src,
            self.down_x.at[k - 1, m - 1],
            sem.at[0, k - 1, m - 1],
            sem.at[1, k - 1, m - 1],
            ctx=self.at_c(-1),
        )

    def down_hop(self, k):
        src = self.down_x.at[0, self.n_c - 2] if k == 1 else self.down_z.at[k - 2]
        sem = self.down_z_sem
        return remote(
            src, self.down_z.at[k - 1], sem.at[0, k - 1], sem.at[1, k - 1], fsdp=self.at_f(-1)
        )

    def kv_copy(self, head, m):
        lanes = pl.ds(pl.multiple_of(head * 2 * HD, 2 * HD), 2 * HD)
        return remote(
            self.stage.at[head % 2, m - 1],
            self.kv_far.at[m - 1, :, lanes],
            self.kv_sem.at[0, head, m - 1],
            self.kv_sem.at[1, head, m - 1],
            ctx=self.at_c(m),
        )

    def out_local(self):
        return pltpu.make_async_copy(
            self.outs, self.outs_all.at[:, self.bit0, self.bit1], self.out_sem.at[0, 2]
        )

    def out_far(self):
        return remote(
            self.outs,
            self.outs_all.at[:, self.bit0, self.bit1],
            self.out_sem.at[0, 0],
            self.out_sem.at[1, 0],
            tp=self.peer1,
        )

    def out_near(self):
        pair = self.outs_all.at[:, self.bit0]
        return remote(pair, pair, self.out_sem.at[0, 1], self.out_sem.at[1, 1], tp=self.peer0)

    def begin(self):
        barrier = pltpu.get_barrier_semaphore()
        peers = [{"tp": self.peer0}, {"tp": self.peer1}, {"fsdp": self.at_f(-1)}]
        if self.n_f > 2:
            peers.append({"fsdp": self.at_f(1)})
        peers += [{"ctx": self.at_c(m)} for m in range(1, self.n_c)]
        for peer in peers:
            pl.semaphore_signal(
                barrier, inc=1, device_id=peer, device_id_type=pl.DeviceIdType.MESH
            )
        pl.semaphore_wait(barrier, len(peers))
        self.up_hop(1).start()
        for k in range(1, self.n_f + 1):
            self.down_side(k, 1).start()
        self.out_local().start()
        self.out_far().start()

    def up_event(self, m):
        self.up_hop(m - 1).wait()
        self.up_z[m - 2] += self.up_g[self.at_f(m)]
        if m < self.n_f:
            self.up_hop(m).start()
        else:
            self.up_side(1).start()

    def up_side_event(self, m):
        self.up_side(m - 1).wait()
        total = self.up_x[m - 2] + self.up_z[self.n_f - 2, self.at_c(m)]
        if m < self.n_c:
            self.up_x[m - 2] = total
            self.up_side(m).start()
        else:
            self.up_out[...] = total

    def down_event(self, k):
        for m in range(2, self.n_c + 1):
            self.down_side(k, m - 1).wait()
            self.down_x[k - 1, m - 2] += self.down_g[self.at_f(k), self.at_c(m)]
            if m < self.n_c:
                self.down_side(k, m).start()
        if k > 1:
            self.down_hop(k - 1).wait()
            total = self.down_z[k - 2] + self.down_x[k - 1, self.n_c - 2]
            if k < self.n_f:
                self.down_z[k - 2] = total
            else:
                self.down_out[...] = total
        if k < self.n_f:
            self.down_hop(k).start()

    def out_event(self):
        self.out_local().wait()
        self.out_far().wait()
        self.out_near().start()

    def end(self):
        self.out_near().wait()
        for head in range(self.heads):
            for m in range(1, self.n_c):
                if head >= self.heads - 2:
                    self.kv_copy(head, m).wait_send()
                self.kv_copy(head, m).wait_recv()

    def run(self, now, before):
        count = self.heads * STEPS_PER_HEAD
        plan = []
        for k in range(1, self.n_f + 1):
            plan.append(((k - 0.3) / (self.n_f + 0.3), lambda k=k: self.down_event(k)))
        for m in range(2, self.n_f + 1):
            plan.append(((m - 1.0) / (self.n_f - 0.2), lambda m=m: self.up_event(m)))
        plan.append((0.45, self.out_event))
        plan.sort(key=lambda item: item[0])
        late = [lambda m=m: self.up_side_event(m) for m in range(2, self.n_c + 1)] + [self.end]
        if before:

            @pl.when(now == 0)
            def _():
                self.begin()

            return
        for at in range(count):
            todo = [f for p, f in plan if min(int(p * count), count - 1) == at]
            if at == count - 1:
                todo = todo + late
            if todo:

                @pl.when(now == at)
                def _(todo=todo):
                    for f in todo:
                        f()


STEPS_PER_HEAD = 4


def attention_back(
    queries, grads, result, lse, kv_blocks, meta, heads, up_g, down_g, outs, tile=512
):
    rows = queries.shape[0] // STEPS_PER_HEAD
    n_f, n_c, own, wide_up = up_g.shape
    wide_down = down_g.shape[-1]
    count, span, blocks = queries.shape[0], kv_blocks[0].shape[0], len(kv_blocks)
    keys = span * blocks
    whole = lambda h, i, m: (0, 0)
    wide = pl.BlockSpec((count, heads * HD), whole)
    kv_spec = pl.BlockSpec((span, 2 * HD), lambda h, i, m: (0, h))
    anywhere = pl.BlockSpec(memory_space=pl.ANY)
    sem, shape = pltpu.SemaphoreType.DMA, jax.ShapeDtypeStruct

    def held(array):
        return pl.BlockSpec(array.shape, lambda h, i, m: (0,) * array.ndim)

    return pl.pallas_call(
        functools.partial(backward_kernel, heads, blocks, n_f, tile, rows),
        grid_spec=pltpu.PrefetchScalarGridSpec(
            num_scalar_prefetch=1,
            grid=(heads, count // rows),
            in_specs=[wide] * 3
            + [pl.BlockSpec((heads, count), whole)]
            + [held(up_g), held(down_g), held(outs)]
            + [kv_spec] * blocks,
            out_specs=[
                wide,
                kv_spec,
                pl.BlockSpec((own, wide_up), whole),
                pl.BlockSpec((own, wide_down), whole),
                anywhere,
                anywhere,
            ],
            scratch_shapes=[
                pltpu.VMEM((keys, 2 * HD), jnp.bfloat16),
                pltpu.VMEM((keys, 2 * HD), jnp.bfloat16),
                pltpu.VMEM((2 * HD, keys), jnp.bfloat16),
                pltpu.VMEM((keys, 128), jnp.float32),
                pltpu.VMEM((rows, 2 * HD), jnp.float32),
                pltpu.VMEM((rows, 2 * HD), jnp.float32),
                pltpu.VMEM((rows, 2 * HD), jnp.float32),
                pltpu.VMEM((keys, 2 * HD), jnp.float32),
                pltpu.VMEM((keys, 2 * HD), jnp.float32),
                pltpu.VMEM((2 * HD, rows), jnp.float32),
                pltpu.VMEM((2, n_c - 1, span, 2 * HD), jnp.float32),
                pltpu.VMEM((n_f - 1, n_c, own, wide_up), jnp.float32),
                pltpu.VMEM((n_c - 1, own, wide_up), jnp.float32),
                pltpu.VMEM((n_f, n_c - 1, own, wide_down), jnp.float32),
                pltpu.VMEM((n_f - 1, own, wide_down), jnp.float32),
                sem((2, n_f - 1)),
                sem((2, n_c - 1)),
                sem((2, n_f, n_c - 1)),
                sem((2, n_f - 1)),
                sem((2, heads, n_c - 1)),
                sem((2, 3)),
            ],
        ),
        out_shape=[
            shape((count, heads * HD), jnp.float32),
            shape((span, 2 * heads * HD), jnp.float32),
            shape((own, wide_up), jnp.float32),
            shape((own, wide_down), jnp.float32),
            shape((n_c - 1, span, 2 * heads * HD), jnp.float32),
            shape((outs.shape[0], 2, 2) + outs.shape[1:], jnp.float32),
        ],
        compiler_params=pltpu.CompilerParams(
            dimension_semantics=("arbitrary", "arbitrary"),
            collective_id=2,
            has_side_effects=True,
            vmem_limit_bytes=62 << 20,
        ),
        cost_estimate=pl.CostEstimate(
            flops=60 * heads * count * keys * HD,
            bytes_accessed=16 * keys * heads * HD + 16 * count * heads * HD,
            transcendentals=heads * count * keys,
        ),
        name="attention_backward",
    )(meta, queries, grads, result, lse, up_g, down_g, outs, *kv_blocks)


def dot_three(left, right, left_dim, right_dim):
    left_high, left_low = left
    right_high, right_low = right
    return dot(left_high, right_high, left_dim, right_dim) + (
        dot(left_high, right_low, left_dim, right_dim)
        + dot(left_low, right_high, left_dim, right_dim)
    )


def tiles_of(count, body):
    tile = 256 if count % 256 == 0 else count

    def step(n, _):
        body(pl.ds(pl.multiple_of(n * tile, tile), tile))
        return 0

    lax.fori_loop(0, count // tile, step, 0)


def middle_kernel(
    chunks, rows, n_c,
    att_ref, weights, outw_ref,
    b_out, gain_1, shift_1, b_up, b_down, gain_2, shift_2, tok_hbm, cot_hbm,
    out_own, mid_own, gatt, d_up, d_down, vec, d_bup,
    part, rx0, rx1, full, act_hi, act_lo, slope, tok, cot, norm_1, recip_1,
    up_s, down_s, outw_s, xs, ys, ts, send0, recv0, send1, recv1, own_sem,
    *blocked,
):
    half, quarter = rows // 2, rows // 4
    me = lax.axis_index("tp")
    bit0, bit1 = me % 2, me // 2 % 2
    peer0, peer1 = me + 1 - 2 * bit0, me + 2 - 4 * bit1
    home0 = pl.multiple_of(bit0 * half, half)
    away0 = pl.multiple_of((1 - bit0) * half, half)
    mine = pl.multiple_of(home0 + bit1 * quarter, quarter)
    away1 = pl.multiple_of(home0 + (1 - bit1) * quarter, quarter)
    own = pl.ds(mine, quarter)

    def remote_tp(src, dst, send, recv, peer):
        return remote(src, dst, send, recv, tp=peer)

    width, hidden = up_s.shape[1], up_s.shape[2]
    if blocked:
        whole, w_sem, wl_sem = blocked
        n_f, own_w = weights.shape[0], weights.shape[1]
        at = lax.axis_index("ctx")

        def columns_of(part_at):
            return pl.ds(part_at * hidden, hidden)

        def w_copies(part_at):
            cols = columns_of(part_at)
            for k in range(n_f):
                yield pltpu.make_async_copy(
                    weights.at[k, :, cols], whole.at[k, at, :, cols], wl_sem.at[part_at, k]
                )
                for m in range(1, n_c):
                    yield remote(
                        weights.at[k, :, cols],
                        whole.at[k, at, :, cols],
                        w_sem.at[0, part_at, k, m - 1],
                        w_sem.at[1, part_at, k, m - 1],
                        ctx=(at + m) % n_c,
                    )

    def scatter0(s, c):
        return remote_tp(
            part.at[c, pl.ds(away0, half)], rx0.at[s, c], send0.at[0, s, c], recv0.at[0, s, c], peer0
        )

    def scatter1(s, c):
        return remote_tp(
            part.at[c, pl.ds(away1, quarter)],
            rx1.at[s, c],
            send1.at[0, s, c],
            recv1.at[0, s, c],
            peer1,
        )

    def gather1(s, c):
        return remote_tp(
            full.at[s, c, own], full.at[s, c, own], send1.at[1, s, c], recv1.at[1, s, c], peer1
        )

    def gather0(s, c):
        place = pl.ds(home0, half)
        return remote_tp(
            full.at[s, c, place], full.at[s, c, place], send0.at[1, s, c], recv0.at[1, s, c], peer0
        )

    def own_copies(c):
        where = pl.ds(pl.multiple_of(c * rows + mine, quarter), quarter)
        return (
            pltpu.make_async_copy(tok_hbm.at[where], tok.at[c], own_sem.at[0, c]),
            pltpu.make_async_copy(cot_hbm.at[where], cot.at[c], own_sem.at[1, c]),
        )

    for c in range(chunks):
        for copy in own_copies(c):
            copy.start()
    barrier = pltpu.get_barrier_semaphore()
    peers = [{"tp": peer0}, {"tp": peer1}]
    if blocked:
        peers += [{"ctx": (at + m) % n_c} for m in range(1, n_c)]
    for peer in peers:
        pl.semaphore_signal(barrier, inc=1, device_id=peer, device_id_type=pl.DeviceIdType.MESH)

    def split_rows(source, target):
        count = source.shape[0]
        step = 128

        def one(i, _):
            at = pl.ds(pl.multiple_of(i * step, step), step)
            target[0, at, :], target[1, at, :] = halves(source[at, :])
            return 0

        lax.fori_loop(0, count // step, one, 0)

    split_rows(outw_ref, outw_s)

    def weights_ready(part_at, target):
        if not blocked:
            split_rows(weights[part_at], target)
            return
        for copy in w_copies(part_at):
            copy.wait()

        def one(j, _):
            to = pl.ds(pl.multiple_of(j * own_w, own_w), own_w)
            piece = whole[j // n_c, j % n_c, :, columns_of(part_at)]
            target[0, to, :], target[1, to, :] = halves(piece)
            return 0

        lax.fori_loop(0, n_f * n_c, one, 0)

    d_bup[...] = jnp.zeros_like(d_bup)
    vec[...] = jnp.zeros_like(vec)
    d_up[...] = jnp.zeros_like(d_up)
    d_down[...] = jnp.zeros_like(d_down)
    for c in range(chunks):
        for copy in own_copies(c):
            copy.wait()
    pl.semaphore_wait(barrier, len(peers))
    if blocked:
        for part_at in range(2):
            for copy in w_copies(part_at):
                copy.start()

    def split_into(target, value):
        target[0], target[1] = halves(value)

    def finish0(s, c):
        scatter0(s, c).wait()
        away = pl.ds(away1 - home0, quarter)
        part[c, pl.ds(away1, quarter), :] += rx0[s, c, away, :]
        scatter1(s, c).start()
        stay = pl.ds(mine - home0, quarter)
        part[c, own, :] += rx0[s, c, stay, :]

    def finish1(s, c):
        scatter1(s, c).wait()
        return part[c, own, :] + rx1[s, c]

    def forward1(s, c):
        gather1(s, c).wait()
        gather0(s, c).start()

    def trailing(c, now, before):
        if before is not None:

            @pl.when(c == 0)
            def _():
                before(chunks - 1)

        if now is not None:

            @pl.when(c > 0)
            def _():
                now(c - 1)

    def stage(body):
        def one(c, _):
            body(c)
            return 0

        lax.fori_loop(0, chunks, one, 0)

    def at_rows(c):
        return pl.ds(pl.multiple_of(c * rows, rows), rows)

    def attention_out(c):
        left = halves(att_ref[at_rows(c), :])

        def columns(n):
            part[c, :, n] = dot_three(left, (outw_s[0, n, :], outw_s[1, n, :]), 1, 1)

        tiles_of(width, columns)
        scatter0(0, c).start()
        trailing(c, functools.partial(finish0, 0), None)

    stage(attention_out)

    def first_norm(c):
        trailing(c, None, functools.partial(finish0, 0))
        resid = finish1(0, c) + tok[c] + b_out[...]
        n_1, r_1 = normalized(resid)
        norm_1[c] = n_1
        recip_1[c] = jnp.broadcast_to(r_1, recip_1.shape[1:])
        full[0, c, own, :] = n_1 * gain_1[...] + shift_1[...]
        gather1(0, c).start()
        trailing(c, functools.partial(forward1, 0), None)

    stage(first_norm)

    def feed_forward(c):
        gather0(0, c).wait()
        split_into(xs, full[0, c])

        def columns(n):
            pre = dot_three((xs[0], xs[1]), (up_s[0, :, n], up_s[1, :, n]), 1, 0) + b_up[:, n]
            cdf = 0.5 + 0.5 * lax.erf(pre * math.sqrt(0.5))
            slope[c, :, n] = cdf + pre * (
                jnp.exp(-0.5 * pre * pre) * (1.0 / math.sqrt(2.0 * math.pi))
            )
            act_hi[c, :, n], act_lo[c, :, n] = halves(pre * cdf)

        tiles_of(hidden, columns)

        @pl.when(c == 0)
        def _():
            weights_ready(1, down_s)

        def back(n):
            part[c, :, n] = dot_three(
                (act_hi[c], act_lo[c]), (down_s[0, n, :], down_s[1, n, :]), 1, 1
            )

        tiles_of(width, back)
        scatter0(1, c).start()
        trailing(c, functools.partial(finish0, 1), functools.partial(forward1, 0))

    def second_norm(c):
        trailing(c, None, functools.partial(finish0, 1))
        ffn = finish1(1, c) + full[0, c, own, :] + b_down[...]
        n_2, r_2 = normalized(ffn)
        out_own[c] = n_2 * gain_2[...] + shift_2[...]
        grad = cot[c]
        second = norm_back(grad, gain_2[...], n_2, r_2)
        full[1, c, own, :] = second
        gather1(1, c).start()
        vec[3:4, :] += jnp.sum(second, axis=0, keepdims=True)
        vec[4:5, :] += jnp.sum(grad * n_2, axis=0, keepdims=True)
        vec[5:6, :] += jnp.sum(grad, axis=0, keepdims=True)
        trailing(c, functools.partial(forward1, 1), None)

    def feed_back(c):
        gather0(1, c).wait()
        split_into(xs, full[1, c])

        def columns(n):
            grad = dot_three((xs[0], xs[1]), (down_s[0, :, n], down_s[1, :, n]), 1, 0)
            grad = grad * slope[c, :, n]
            slope[c, :, n] = grad
            ys[0, :, n], ys[1, :, n] = halves(grad)
            d_bup[:, n] += jnp.sum(grad, axis=0, keepdims=True)

        tiles_of(hidden, columns)

        def back(n):
            part[c, :, n] = dot_three((ys[0], ys[1]), (up_s[0, n, :], up_s[1, n, :]), 1, 1)

        tiles_of(width, back)
        scatter0(2, c).start()
        trailing(c, functools.partial(finish0, 2), functools.partial(forward1, 1))

    def middle_norm(c):
        trailing(c, None, functools.partial(finish0, 2))
        first = finish1(2, c) + full[1, c, own, :]
        n_1 = norm_1[c]
        mid = norm_back(first, gain_1[...], n_1, recip_1[c, :, :1])
        mid_own[c] = mid
        full[2, c, own, :] = mid
        gather1(2, c).start()
        vec[0:1, :] += jnp.sum(mid, axis=0, keepdims=True)
        vec[1:2, :] += jnp.sum(first * n_1, axis=0, keepdims=True)
        vec[2:3, :] += jnp.sum(first, axis=0, keepdims=True)
        trailing(c, functools.partial(forward1, 2), None)
        split_into(ts, full[1, c].T)

        def columns(n):
            d_down[:, n] += dot_three((ts[0], ts[1]), (act_hi[c, :, n], act_lo[c, :, n]), 1, 0)

        tiles_of(hidden, columns)

    def last(c):
        gather0(2, c).wait()
        mid = full[2, c]
        gatt[at_rows(c), :] = dot_three(halves(mid), (outw_s[0], outw_s[1]), 1, 0)
        trailing(c, None, functools.partial(forward1, 2))
        split_into(ts, mid.T)
        d_down[:, hidden:] += dot_three((ts[0], ts[1]), halves(att_ref[at_rows(c), :]), 1, 0)
        split_into(ts, full[0, c].T)

        def columns(n):
            d_up[:, n] += dot_three((ts[0], ts[1]), halves(slope[c, :, n]), 1, 0)

        tiles_of(hidden, columns)

    weights_ready(0, up_s)
    stage(feed_forward)
    stage(second_norm)
    stage(feed_back)
    stage(middle_norm)
    stage(last)


def middle_whole(chunks, rows, n_c, att, up, down, *refs):
    middle_kernel(chunks, rows, n_c, att, (up, down), *refs)


def middle(attended, weights, wide_out_t, vectors, tokens, cot, hidden, n_c, chunks=4):
    blocked = not isinstance(weights, tuple)
    count, width = tokens.shape
    split_at = attended.shape[1]
    rows = count // chunks
    half, quarter = rows // 2, rows // 4
    vmem = pl.BlockSpec(memory_space=pltpu.VMEM)
    anywhere = pl.BlockSpec(memory_space=pl.ANY)
    f32, bf16 = jnp.float32, jnp.bfloat16
    sems = pltpu.SemaphoreType.DMA((2, 3, chunks))
    extra = []
    if blocked:
        n_f, own = weights.shape[0], weights.shape[1]
        extra = [
            pltpu.VMEM((n_f, n_c, own, 2 * hidden), f32),
            pltpu.SemaphoreType.DMA((2, 2, n_f, n_c - 1)),
            pltpu.SemaphoreType.DMA((2, n_f)),
        ]
    shape = jax.ShapeDtypeStruct
    return pl.pallas_call(
        functools.partial(middle_kernel if blocked else middle_whole, chunks, rows, n_c),
        in_specs=[vmem]
        + ([anywhere] if blocked else [vmem] * 2)
        + [vmem] * 8
        + [anywhere] * 2,
        out_specs=[vmem] * 7,
        out_shape=[
            shape((chunks, quarter, width), f32),
            shape((chunks, quarter, width), f32),
            shape((count, split_at), f32),
            shape((width, hidden), f32),
            shape((width, hidden + split_at), f32),
            shape((8, width), f32),
            shape((1, hidden), f32),
        ],
        scratch_shapes=[
            pltpu.VMEM((chunks, rows, width), f32),
            pltpu.VMEM((3, chunks, half, width), f32),
            pltpu.VMEM((3, chunks, quarter, width), f32),
            pltpu.VMEM((3, chunks, rows, width), f32),
            pltpu.VMEM((chunks, rows, hidden), bf16),
            pltpu.VMEM((chunks, rows, hidden), bf16),
            pltpu.VMEM((chunks, rows, hidden), f32),
            pltpu.VMEM((chunks, quarter, width), f32),
            pltpu.VMEM((chunks, quarter, width), f32),
            pltpu.VMEM((chunks, quarter, width), f32),
            pltpu.VMEM((chunks, quarter, 128), f32),
            pltpu.VMEM((2, width, hidden), bf16),
            pltpu.VMEM((2, width, hidden), bf16),
            pltpu.VMEM((2, width, split_at), bf16),
            pltpu.VMEM((2, rows, width), bf16),
            pltpu.VMEM((2, rows, hidden), bf16),
            pltpu.VMEM((2, width, rows), bf16),
            sems, sems, sems, sems,
            pltpu.SemaphoreType.DMA((2, chunks)),
            *extra,
        ],
        compiler_params=pltpu.CompilerParams(
            collective_id=1, has_side_effects=True, vmem_limit_bytes=62 << 20
        ),
        cost_estimate=pl.CostEstimate(
            flops=6 * count * width * (6 * hidden + 3 * split_at),
            bytes_accessed=4 * width * (5 * hidden + 3 * split_at),
            transcendentals=2 * count * hidden,
        ),
        name="middle",
    )(
        attended,
        *([weights] if blocked else weights),
        wide_out_t,
        *vectors,
        tokens,
        cot,
    )


def front_kernel(
    heads, n_c, n_f, tile, rows, meta_ref, tok, shard, up, down, outw, b_q, b_kv,
    att, lse, q_out, kv_out, kv_far, wide, up_down, out_all,
    q_s, kv_s, kv_t, wv, w_s, ud_own, ow_own, kp, vt, bias, qd, acc, top_s, total_s,
    hop_sem, side_sem, ud_sem, ow_sem, ow_side_sem, kv_sem, local_sem,
):
    block, head, step = pl.program_id(0), pl.program_id(1), pl.program_id(2)
    n_q = pl.num_programs(2)
    span, hidden, split_at = tok.shape[0], up.shape[1], heads * HD
    own = shard.shape[0]
    f, c = lax.axis_index("fsdp"), lax.axis_index("ctx")

    def at_f(k):
        return (f + (n_f - k)) % n_f

    def at_c(m):
        return (c + (n_c - m)) % n_c

    def lanes(h):
        return pl.ds(pl.multiple_of(h * 2 * HD, 2 * HD), 2 * HD)

    def hop(k):
        src = shard if k == 1 else wv.at[at_f(k - 1), c]
        return remote(
            src, wv.at[at_f(k - 1), c], hop_sem.at[0, k - 1], hop_sem.at[1, k - 1], fsdp=at_f(-1)
        )

    def side(k, m):
        src = shard if k == 0 else wv.at[at_f(k), c]
        return remote(
            src, wv.at[at_f(k), c], side_sem.at[0, k, m - 1], side_sem.at[1, k, m - 1], ctx=at_c(-m)
        )

    def ud_hop(k):
        src = ud_own if k == 1 else up_down.at[at_f(k - 1)]
        return remote(
            src, up_down.at[at_f(k - 1)], ud_sem.at[0, k - 1], ud_sem.at[1, k - 1], fsdp=at_f(-1)
        )

    def ow_hop(k):
        src = ow_own if k == 1 else out_all.at[at_f(k - 1), c]
        return remote(
            src, out_all.at[at_f(k - 1), c], ow_sem.at[0, k - 1], ow_sem.at[1, k - 1], fsdp=at_f(-1)
        )

    def ow_side(k, m):
        src = ow_own if k == 0 else out_all.at[at_f(k), c]
        return remote(
            src,
            out_all.at[at_f(k), c],
            ow_side_sem.at[0, k, m - 1],
            ow_side_sem.at[1, k, m - 1],
            ctx=at_c(-m),
        )

    def kv_send(h, m):
        return remote(
            kv_s.at[:, lanes(h)],
            kv_far.at[m - 1, :, lanes(h)],
            kv_sem.at[0, h, m - 1],
            kv_sem.at[1, h, m - 1],
            ctx=at_c(-m),
        )

    def locals_of():
        return [
            pltpu.make_async_copy(a, b, local_sem.at[i])
            for i, (a, b) in enumerate(
                (
                    (ud_own, up_down.at[f]),
                    (ow_own, out_all.at[f, c]),
                    (wv, wide),
                    (q_s, q_out),
                    (kv_s, kv_out),
                )
            )
        ]

    @pl.when((block == 0) & (head == 0) & (step == 0))
    def _():
        barrier = pltpu.get_barrier_semaphore()
        peers = [{"fsdp": at_f(-1)}] + ([{"fsdp": at_f(1)}] if n_f > 2 else [])
        peers += [{"ctx": at_c(m)} for m in range(1, n_c)]
        for peer in peers:
            pl.semaphore_signal(
                barrier, inc=1, device_id=peer, device_id_type=pl.DeviceIdType.MESH
            )
        pl.semaphore_wait(barrier, len(peers))
        hop(1).start()
        for m in range(1, n_c):
            side(0, m).start()
        wv[f, c] = shard[...]
        ud_own[:, :hidden] = up[...]
        ud_own[:, hidden:] = down[...].T
        ow_own[...] = outw[...].T
        for k in range(1, n_f):
            hop(k).wait()
            if k < n_f - 1:
                hop(k + 1).start()
            for m in range(1, n_c):
                side(k, m).start()
        ud_hop(1).start()
        ow_hop(1).start()
        copies = locals_of()
        copies[0].start()
        copies[1].start()
        for k in range(n_f):
            for m in range(1, n_c):
                side(k, m).wait()

        def split(j, _):
            to = pl.ds(pl.multiple_of(j * own, own), own)
            w_s[0, to, :], w_s[1, to, :] = halves(wv[j // n_c, j % n_c])
            return 0

        lax.fori_loop(0, n_f * n_c, split, 0)
        copies[2].start()

        def keys(i, _):
            at = pl.ds(pl.multiple_of(i * rows, rows), rows)
            right = (w_s[0, :, : 2 * split_at], w_s[1, :, : 2 * split_at])
            kv_s[at, :] = dot_three(halves(tok[at, :]), right, 1, 0) + b_kv[...]
            return 0

        lax.fori_loop(0, span // rows, keys, 0)
        for h in range(heads):
            for m in range(1, n_c):
                kv_send(h, m).start()

        def asking(i, _):
            at = pl.ds(pl.multiple_of(i * rows, rows), rows)
            right = (w_s[0, :, 2 * split_at :], w_s[1, :, 2 * split_at :])
            q_s[at, :] = dot_three(halves(tok[at, :]), right, 1, 0) + b_q[...]
            return 0

        lax.fori_loop(0, span // rows, asking, 0)
        copies[3].start()
        copies[4].start()
        for m in range(1, n_c):
            ow_side(0, m).start()

    @pl.when((block == 0) & (step == 0))
    def _():
        kv_t[...] = kv_s[:, lanes(head)]

    @pl.when((block > 0) & (step == 0))
    def _():
        kv_send(head, block).wait_recv()
        copy = pltpu.make_async_copy(
            kv_far.at[block - 1, :, lanes(head)], kv_t, local_sem.at[5]
        )
        copy.start()
        copy.wait()

    @pl.when(step == 0)
    def _():
        def prepare(j, _):
            at = pl.ds(pl.multiple_of(j * tile, tile), tile)
            pair = kv_t[at, :]
            kp[at, :] = packed(pair, True)
            vt[:, at] = stacked(pair.T[HD:, :])
            bias[at, :] = key_bias(meta_ref, block, j * tile, tile, 128)
            return 0

        lax.fori_loop(0, span // tile, prepare, 0)

    here = pl.ds(pl.multiple_of(step * rows, rows), rows)

    @pl.when(block == 0)
    def _():
        acc[head, :, here] = jnp.zeros((2 * HD, rows), jnp.float32)
        top_s[head, :, here] = jnp.full((1, rows), MASKED, jnp.float32)
        total_s[head, :, here] = jnp.zeros((1, rows), jnp.float32)

    doubled(q_s, here, head, qd, heads)
    q_high, q_low = halves(qd[...] * (LOG2E * HD**-0.5))
    q_four = jnp.concatenate([q_high, q_low], axis=1)

    def key_tile(j, carry):
        top, total = carry
        at = pl.ds(pl.multiple_of(j * tile, tile), tile)
        k_two = kp[at, :]
        scores = dot(jnp.concatenate([k_two, k_two], axis=1), q_four, 1, 1)
        scores = scores + jnp.concatenate([bias[at, :]] * (rows // 128), axis=1)
        new_top = jnp.maximum(top, jnp.max(scores, axis=0, keepdims=True))
        fade = jnp.exp2(top - new_top)
        probs = jnp.exp2(scores - new_top)
        total = total * fade + jnp.sum(probs, axis=0, keepdims=True)
        high, low = halves(probs)
        v_two = vt[:, at]
        acc[head, :, here] = acc[head, :, here] * fade + (
            dot(v_two, high, 1, 0) + dot(v_two, low, 1, 0)
        )
        return new_top, total

    top, total = lax.fori_loop(
        0, span // tile, key_tile, (top_s[head, :, here], total_s[head, :, here])
    )
    top_s[head, :, here] = top
    total_s[head, :, here] = total

    @pl.when(block == n_c - 1)
    def _():
        result = ((acc[head, :HD, here] + acc[head, HD:, here]) / total).T
        for j in range(heads):

            @pl.when(head == j)
            def _(j=j):
                att[here, j * HD : (j + 1) * HD] = result
                lse[j : j + 1, here] = top + jnp.log2(total)

    def arrived(k):
        ud_hop(k).wait()
        ow_hop(k).wait()
        if k < n_f - 1:
            ud_hop(k + 1).start()
            ow_hop(k + 1).start()
        for m in range(1, n_c):
            ow_side(k, m).start()

    count = n_c * heads * STEPS_PER_HEAD
    now = (block * heads + head) * n_q + step
    for k in range(1, n_f):

        @pl.when(now == min(count - 1, k * count // (n_f - 1) - 1))
        def _(k=k):
            arrived(k)

    @pl.when(now == count - 1)
    def _():
        for k in range(n_f):
            for m in range(1, n_c):
                ow_side(k, m).wait()
        for h in range(heads):
            for m in range(1, n_c):
                kv_send(h, m).wait_send()
        for copy in locals_of():
            copy.wait()


def front(tokens, shard, w_up, w_down, w_out, b_query, b_kv, meta, heads, n_f, n_c, tile=512):
    span, width = tokens.shape
    own, total = shard.shape
    hidden, split_at = w_up.shape[1], heads * HD
    rows = span // STEPS_PER_HEAD
    shape, sem, f32, bf16 = jax.ShapeDtypeStruct, pltpu.SemaphoreType.DMA, jnp.float32, jnp.bfloat16
    anywhere = pl.BlockSpec(memory_space=pl.ANY)

    def held(dims):
        return pl.BlockSpec(dims, lambda b, h, i, m: (0,) * len(dims))

    operands = (tokens, shard, w_up, w_down, w_out, b_query, b_kv)
    return pl.pallas_call(
        functools.partial(front_kernel, heads, n_c, n_f, tile, rows),
        grid_spec=pltpu.PrefetchScalarGridSpec(
            num_scalar_prefetch=1,
            grid=(n_c, heads, STEPS_PER_HEAD),
            in_specs=[held(x.shape) for x in operands],
            out_specs=[held((span, split_at)), held((heads, span))] + [anywhere] * 6,
            scratch_shapes=[
                pltpu.VMEM((span, split_at), f32),
                pltpu.VMEM((span, 2 * split_at), f32),
                pltpu.VMEM((span, 2 * HD), f32),
                pltpu.VMEM((n_f, n_c, own, total), f32),
                pltpu.VMEM((2, width, total), bf16),
                pltpu.VMEM((own, 2 * hidden), f32),
                pltpu.VMEM((own, split_at), f32),
                pltpu.VMEM((span, 2 * HD), bf16),
                pltpu.VMEM((2 * HD, span), bf16),
                pltpu.VMEM((span, 128), f32),
                pltpu.VMEM((rows, 2 * HD), f32),
                pltpu.VMEM((heads, 2 * HD, span), f32),
                pltpu.VMEM((heads, 1, span), f32),
                pltpu.VMEM((heads, 1, span), f32),
                sem((2, n_f - 1)),
                sem((2, n_f, n_c - 1)),
                sem((2, n_f - 1)),
                sem((2, n_f - 1)),
                sem((2, n_f, n_c - 1)),
                sem((2, heads, n_c - 1)),
                sem((6,)),
            ],
        ),
        out_shape=[
            shape((span, split_at), f32),
            shape((heads, span), f32),
            shape((span, split_at), f32),
            shape((span, 2 * split_at), f32),
            shape((n_c - 1, span, 2 * split_at), f32),
            shape((n_f, n_c, own, total), f32),
            shape((n_f, own, 2 * hidden), f32),
            shape((n_f, n_c, own, split_at), f32),
        ],
        compiler_params=pltpu.CompilerParams(
            dimension_semantics=("arbitrary",) * 3,
            collective_id=3,
            has_side_effects=True,
            vmem_limit_bytes=62 << 20,
        ),
        name="front",
    )(meta, *operands)

def per_device(
    inputs,
    lengths,
    w_qkv,
    b_query,
    b_value,
    w_out,
    b_out,
    gain_attn,
    shift_attn,
    w_up,
    b_up,
    w_down,
    b_down,
    gain_ffn,
    shift_ffn,
    cotangent,
):
    width = inputs.shape[-1]
    block_len = inputs.shape[1]
    heads = b_query.shape[0] // HD
    split_at = heads * HD
    hidden = b_up.shape[0]
    tokens = inputs.reshape(block_len, width)
    cot = cotangent.reshape(block_len, width)
    length = lengths[0]
    n_c = lax.axis_size("ctx")
    at_c = lax.axis_index("ctx")

    def regroup(columns):
        parts = columns.reshape(columns.shape[:-1] + (heads, 3 * HD))
        lead = columns.shape[:-1]
        return jnp.concatenate(
            [
                parts[..., HD:].reshape(lead + (2 * split_at,)),
                parts[..., :HD].reshape(lead + (split_at,)),
            ],
            axis=-1,
        )

    bias_kv = jnp.stack(
        [jnp.zeros((heads, HD), jnp.float32), b_value.reshape(heads, HD)], axis=1
    ).reshape(-1)
    n_f, own = lax.axis_size("fsdp"), w_up.shape[0]
    meta = jnp.stack([length] + [(at_c - m) % n_c * block_len for m in range(n_c)])
    if own % 16 == 0 and n_c > 1 and n_f > 1:
        attended, log_sums, queries, kv_own, kv_far, wide, weights, wide_out_t = front(
            tokens, regroup(w_qkv), w_up, w_down, w_out, b_query.reshape(1, -1),
            bias_kv.reshape(1, -1), meta, heads, n_f, n_c,
        )
        wide = wide.reshape(width, 3 * split_at)
        wide_kv, wide_q = wide[:, : 2 * split_at], wide[:, 2 * split_at :]
        wide_out_t = wide_out_t.reshape(width, split_at)
        kv_blocks = [kv_own] + [kv_far[m] for m in range(n_c - 1)]
    else:
        wide_kv, wide_q = weight_gather(regroup(w_qkv), [2 * split_at, split_at])
        rest = jnp.concatenate([w_up, w_down.T, w_out.T], axis=1)
        wide_up, wide_down_t, wide_out_t = weight_gather(rest, [hidden, hidden, split_at])
        weights = (wide_up, wide_down_t)
        kv_blocks = [contract(tokens, wide_kv, 1, 0) + bias_kv]
        for m in range(1, n_c):
            kv_blocks.append(ringed(kv_blocks[-1], "ctx", 1))
        queries = contract(tokens, wide_q, 1, 0) + b_query
        attended, log_sums = attention(queries, kv_blocks, meta, heads)

    flat = lambda v: v.reshape(1, -1)
    vectors = [flat(v) for v in (b_out, gain_attn, shift_attn, b_up, b_down, gain_ffn, shift_ffn)]
    outs, grad_mid, grad_att, d_up, d_down_out, vec_rows, d_bup = middle(
        attended, weights, wide_out_t, vectors, tokens, cot, hidden, n_c
    )
    sums = small_sum(vec_rows, ("tp", "fsdp", "ctx"))
    blocked = (lax.axis_size("fsdp"), n_c, w_up.shape[0])
    grad_q, grad_kv, d_wup, down_out, kv_far, outputs = attention_back(
        queries,
        grad_att,
        attended,
        log_sums,
        kv_blocks,
        meta,
        heads,
        d_up.reshape(blocked + (hidden,)),
        d_down_out.reshape(blocked + (hidden + split_at,)),
        outs,
    )
    d_wdown = down_out[:, :hidden].T
    d_wout = down_out[:, hidden:].T
    for m in range(n_c - 1):
        grad_kv = grad_kv + kv_far[m]
    back = contract(grad_kv, wide_kv, 1, 1) + contract(grad_q, wide_q, 1, 1)
    tail_sums = small_sum(
        jnp.concatenate([jnp.sum(grad_kv, axis=0), jnp.sum(grad_q, axis=0), d_bup[0]]),
        ("fsdp", "ctx"),
    )
    d_bvalue = tail_sums[: 2 * split_at].reshape(heads, 2, HD)[:, 1].reshape(-1)
    d_bquery = tail_sums[2 * split_at : 3 * split_at]
    d_bup = tail_sums[3 * split_at :]
    own = grad_scatter([contract(tokens, grad_kv, 0, 0), contract(tokens, grad_q, 0, 0)])
    own_rows_count = own.shape[0]
    d_wqkv = jnp.concatenate(
        [
            own[:, 2 * split_at :].reshape(own_rows_count, heads, HD),
            own[:, : 2 * split_at].reshape(own_rows_count, heads, 2 * HD),
        ],
        axis=2,
    ).reshape(own_rows_count, 3 * split_at)
    d_inputs = quarter_gather(grad_mid + quarter_scatter(back, grad_mid.shape[0]))
    return (
        outputs.reshape(1, block_len, width),
        d_inputs.reshape(1, block_len, width),
        d_wqkv,
        d_bquery,
        d_bvalue,
        d_wout,
        sums[0],
        sums[1],
        sums[2],
        d_wup,
        d_bup,
        d_wdown,
        sums[3],
        sums[4],
        sums[5],
    )


def solution(mesh):
    rows_of, cols_of = P(("fsdp", "ctx"), "tp"), P("tp", ("fsdp", "ctx"))
    seq, by_tp, same = P("fsdp", "ctx", None), P("tp"), P()
    in_specs = (
        seq, P("fsdp"), rows_of, by_tp, by_tp, cols_of, same, same, same,
        rows_of, by_tp, cols_of, same, same, same, seq,
    )
    out_specs = (
        seq, seq, rows_of, by_tp, by_tp, cols_of, same, same, same,
        rows_of, by_tp, cols_of, same, same, same,
    )
    return jax.shard_map(
        per_device, mesh=mesh, in_specs=in_specs, out_specs=out_specs, check_vma=False
    )
```

```python
import functools
import math

import jax
import jax.numpy as jnp
from jax import lax
from jax.experimental import pallas as pl
from jax.experimental.pallas import tpu as pltpu
from jax.sharding import PartitionSpec as P

HD = 64
LOG2E = math.log2(math.e)
NORM_EPS = 1e-12
MASKED = -1e30
THREE = lax.Precision.HIGH


def contract(left, right, left_dim, right_dim):
    return lax.dot_general(
        left,
        right,
        (((left_dim,), (right_dim,)), ((), ())),
        precision=THREE,
        preferred_element_type=jnp.float32,
    )


def ringed(block, axis, distance):
    count = lax.axis_size(axis)
    return lax.ppermute(block, axis, [(i, (i + distance) % count) for i in range(count)])


def swapped(block, axis, bit):
    return lax.ppermute(block, axis, [(i, i ^ bit) for i in range(lax.axis_size(axis))])


def bits_of(axis):
    bits, bit = [], 1
    while bit < lax.axis_size(axis):
        bits.append(bit)
        bit *= 2
    return bits


def quarter_scatter(part, chunks):
    rank = lax.axis_index("tp")
    count, width = part.shape
    block = part.reshape(chunks, 2, 2, count // (4 * chunks), width)
    for bit, axis in ((1, 1), (2, 1)):
        upper = rank // bit % 2
        leaving = lax.dynamic_index_in_dim(block, 1 - upper, axis, keepdims=False)
        staying = lax.dynamic_index_in_dim(block, upper, axis, keepdims=False)
        block = staying + swapped(leaving, "tp", bit)
    return block


def quarter_gather(block):
    rank = lax.axis_index("tp")
    for bit in (2, 1):
        other = swapped(block, "tp", bit)
        upper = rank // bit % 2 == 1
        block = jnp.where(
            upper, jnp.stack([other, block], axis=1), jnp.stack([block, other], axis=1)
        )
    return block.reshape(-1, block.shape[-1])


def small_sum(vector, axes):
    for axis in axes:
        for bit in bits_of(axis):
            vector = vector + swapped(vector, axis, bit)
    return vector


def weight_gather(shard, widths):
    rows = shard.shape[0]
    n_f, n_c = lax.axis_size("fsdp"), lax.axis_size("ctx")
    at_f, at_c = lax.axis_index("fsdp"), lax.axis_index("ctx")
    wholes = [jnp.zeros((n_f * n_c * rows, width), jnp.float32) for width in widths]
    along_f = shard
    for k in range(n_f):
        if k:
            along_f = ringed(along_f, "fsdp", 1)
        along_c = along_f
        for m in range(n_c):
            if m:
                along_c = ringed(along_c, "ctx", 1)
            place = ((at_f - k) % n_f * n_c + (at_c - m) % n_c) * rows
            start = 0
            for i, width in enumerate(widths):
                wholes[i] = lax.dynamic_update_slice(
                    wholes[i], along_c[:, start : start + width], (place, 0)
                )
                start += width
    return wholes


def grad_scatter(pieces):
    n_f, n_c = lax.axis_size("fsdp"), lax.axis_size("ctx")
    at_f, at_c = lax.axis_index("fsdp"), lax.axis_index("ctx")
    rows = pieces[0].shape[0] // (n_f * n_c)

    def piece(f, c):
        start = (f % n_f * n_c + c % n_c) * rows
        cut = [lax.dynamic_slice_in_dim(p, start, rows, 0) for p in pieces]
        return cut[0] if len(cut) == 1 else jnp.concatenate(cut, axis=1)

    total = None
    for k in range(1, n_f + 1):
        over_c = piece(at_f - k, at_c - 1)
        for m in range(2, n_c + 1):
            over_c = ringed(over_c, "ctx", 1) + piece(at_f - k, at_c - m)
        total = over_c if total is None else ringed(total, "fsdp", 1) + over_c
    return total


def normalized(values):
    centred = values - jnp.mean(values, axis=-1, keepdims=True)
    spread = jnp.mean(centred * centred, axis=-1, keepdims=True)
    recip = lax.rsqrt(spread + NORM_EPS)
    return centred * recip, recip


def norm_back(grad, gain, normed, recip):
    scaled = grad * gain
    return recip * (
        scaled
        - jnp.mean(scaled, axis=-1, keepdims=True)
        - normed * jnp.mean(scaled * normed, axis=-1, keepdims=True)
    )


def halves(values):
    high = values.astype(jnp.bfloat16)
    return high, (values - high.astype(jnp.float32)).astype(jnp.bfloat16)


def low_half(shape):
    return lax.broadcasted_iota(jnp.int32, shape, 1) < HD


def dot(left, right, left_dim, right_dim):
    return lax.dot_general(
        left, right, (((left_dim,), (right_dim,)), ((), ())), preferred_element_type=jnp.float32
    )


def doubled(ref, rows, head, scratch, heads):
    for j in range(heads):

        @pl.when(head == j)
        def _():
            piece = ref[rows, j * HD : (j + 1) * HD]
            scratch[...] = jnp.concatenate([piece, piece], axis=1)


def packed(pair, first):
    low = low_half(pair.shape)
    turned = pltpu.roll(pair, HD, 1)
    twice = jnp.where(low, pair, turned) if first else jnp.where(low, turned, pair)
    high, rest = halves(twice)
    return jnp.where(low, high.astype(jnp.float32), rest.astype(jnp.float32)).astype(jnp.bfloat16)


def stacked(half):
    high, rest = halves(half)
    return jnp.concatenate([high, rest], axis=0)


def key_bias(limit, first, count, width):
    place = first + lax.broadcasted_iota(jnp.int32, (count, width), 0)
    return jnp.where(place < limit, 0.0, MASKED)


def row(ref):
    return ref[...].reshape(1, -1)


def forward_kernel(heads, blocks, tile, rows, meta_ref, q_ref, *refs):
    kv_refs, (out_ref, lse_ref, kp, vt, bias, qd, acc) = refs[:blocks], refs[blocks:]
    head, step = pl.program_id(0), pl.program_id(1)
    span = kv_refs[0].shape[0]
    per = span // tile

    @pl.when(step == 0)
    def _():
        for b in range(blocks):

            def prepare(j, _, b=b):
                at = pl.ds(pl.multiple_of(j * tile, tile), tile)
                to = pl.ds(pl.multiple_of(b * span + j * tile, tile), tile)
                pair = kv_refs[b][at, :]
                kp[to, :] = packed(pair, True)
                vt[:, to] = stacked(pair.T[HD:, :])
                bias[to, :] = key_bias(meta_ref[0], meta_ref[1 + b] + j * tile, tile, 128)
                return 0

            lax.fori_loop(0, per, prepare, 0)

    here = pl.ds(pl.multiple_of(step * rows, rows), rows)
    doubled(q_ref, here, head, qd, heads)
    q_high, q_low = halves(qd[...] * (LOG2E * HD**-0.5))
    q_four = jnp.concatenate([q_high, q_low], axis=1)
    acc[...] = jnp.zeros_like(acc)

    def key_tile(j, carry):
        top, total = carry
        at = pl.ds(pl.multiple_of(j * tile, tile), tile)
        k_two = kp[at, :]
        scores = dot(jnp.concatenate([k_two, k_two], axis=1), q_four, 1, 1)
        scores = scores + jnp.concatenate([bias[at, :]] * (rows // 128), axis=1)
        new_top = jnp.maximum(top, jnp.max(scores, axis=0, keepdims=True))
        fade = jnp.exp2(top - new_top)
        probs = jnp.exp2(scores - new_top)
        total = total * fade + jnp.sum(probs, axis=0, keepdims=True)
        high, low = halves(probs)
        v_two = vt[:, at]
        acc[...] = acc[...] * fade + (dot(v_two, high, 1, 0) + dot(v_two, low, 1, 0))
        return new_top, total

    top, total = lax.fori_loop(
        0,
        blocks * per,
        key_tile,
        (jnp.full((1, rows), MASKED, jnp.float32), jnp.zeros((1, rows), jnp.float32)),
    )
    result = acc[:HD, :] + acc[HD:, :]
    result = (result / total).T
    for j in range(heads):

        @pl.when(head == j)
        def _():
            out_ref[here, j * HD : (j + 1) * HD] = result
            lse_ref[j : j + 1, here] = top + jnp.log2(total)


def attention(queries, kv_blocks, meta, heads, rows=256, tile=512):
    count, span, blocks = queries.shape[0], kv_blocks[0].shape[0], len(kv_blocks)
    keys = span * blocks
    whole = lambda h, i, m: (0, 0)
    return pl.pallas_call(
        functools.partial(forward_kernel, heads, blocks, tile, rows),
        grid_spec=pltpu.PrefetchScalarGridSpec(
            num_scalar_prefetch=1,
            grid=(heads, count // rows),
            in_specs=[pl.BlockSpec((count, heads * HD), whole)]
            + [pl.BlockSpec((span, 2 * HD), lambda h, i, m: (0, h))] * blocks,
            out_specs=[
                pl.BlockSpec((count, heads * HD), whole),
                pl.BlockSpec((heads, count), whole),
            ],
            scratch_shapes=[
                pltpu.VMEM((keys, 2 * HD), jnp.bfloat16),
                pltpu.VMEM((2 * HD, keys), jnp.bfloat16),
                pltpu.VMEM((keys, 128), jnp.float32),
                pltpu.VMEM((rows, 2 * HD), jnp.float32),
                pltpu.VMEM((2 * HD, rows), jnp.float32),
            ],
        ),
        out_shape=[
            jax.ShapeDtypeStruct((count, heads * HD), jnp.float32),
            jax.ShapeDtypeStruct((heads, count), jnp.float32),
        ],
        compiler_params=pltpu.CompilerParams(dimension_semantics=("arbitrary", "arbitrary")),
        cost_estimate=pl.CostEstimate(
            flops=24 * heads * count * keys * HD,
            bytes_accessed=8 * keys * heads * HD + 8 * count * heads * HD,
            transcendentals=heads * count * keys,
        ),
        name="attention_forward",
    )(meta, queries, *kv_blocks)


def backward_kernel(
    heads, blocks, n_f, tile, rows, meta_ref, q_ref, do_ref, out_ref, lse_ref, up_g, down_g, outs,
    *refs,
):
    kv_refs = refs[:blocks]
    dq_ref, dkv_ref, up_out, down_out, out_out, kv_far, outs_all = refs[blocks : blocks + 7]
    kp, vp, kt, bias, qd, dd, od, dk, dv, acc, stage = refs[blocks + 7 : blocks + 18]
    transfers = Transfers(
        blocks, n_f, heads, up_g, down_g, outs, up_out, (down_out, out_out), kv_far, outs_all, stage,
        *refs[blocks + 18 :],
    )
    head, step = pl.program_id(0), pl.program_id(1)
    steps = pl.num_programs(1)
    transfers.run(head * steps + step, before=True)
    span = kv_refs[0].shape[0]
    per = span // tile

    @pl.when(step == 0)
    def _():
        dk[...] = jnp.zeros_like(dk)
        dv[...] = jnp.zeros_like(dv)
        for b in range(blocks):

            def prepare(j, _, b=b):
                at = pl.ds(pl.multiple_of(j * tile, tile), tile)
                to = pl.ds(pl.multiple_of(b * span + j * tile, tile), tile)
                pair = kv_refs[b][at, :]
                kp[to, :] = packed(pair, True)
                vp[to, :] = packed(pair, False)
                kt[:, to] = stacked(pair.T[:HD, :])
                bias[to, :] = key_bias(
                    meta_ref[0], transfers.at_c(b) * span + j * tile, tile, 128
                )
                return 0

            lax.fori_loop(0, per, prepare, 0)

    here = pl.ds(pl.multiple_of(step * rows, rows), rows)
    doubled(q_ref, here, head, qd, heads)
    doubled(do_ref, here, head, dd, heads)
    doubled(out_ref, here, head, od, heads)
    low = low_half((rows, 2 * HD))

    def both(values):
        high, rest = halves(values)
        mixed = jnp.where(low, high.astype(jnp.float32), rest.astype(jnp.float32))
        return jnp.concatenate([high, rest], axis=1), mixed.astype(jnp.bfloat16)

    q_four, q_two = both(qd[...] * (LOG2E * HD**-0.5))
    do_four, do_two = both(dd[...])
    delta = jnp.sum((dd[...] * od[...]).T[:HD, :], axis=0, keepdims=True)
    lse = lse_ref[0:1, here]
    for j in range(1, heads):
        lse = jnp.where(head == j, lse_ref[j : j + 1, here], lse)
    acc[...] = jnp.zeros_like(acc)

    def key_tile(j, _):
        at = pl.ds(pl.multiple_of(j * tile, tile), tile)
        k_two, v_two = kp[at, :], vp[at, :]
        scores = dot(jnp.concatenate([k_two, k_two], axis=1), q_four, 1, 1)
        scores = scores + jnp.concatenate([bias[at, :]] * (rows // 128), axis=1)
        probs = jnp.exp2(scores - lse)
        high, rest = halves(probs)
        dv[at, :] += dot(high, do_two, 1, 0) + dot(rest, do_two, 1, 0)
        grad_p = dot(jnp.concatenate([v_two, v_two], axis=1), do_four, 1, 1)
        grad_s = probs * (grad_p - delta)
        high, rest = halves(grad_s)
        dk[at, :] += dot(high, q_two, 1, 0) + dot(rest, q_two, 1, 0)
        k_t = kt[:, at]
        acc[...] += dot(k_t, high, 1, 0) + dot(k_t, rest, 1, 0)
        return 0

    lax.fori_loop(0, blocks * per, key_tile, 0)
    result = ((acc[:HD, :] + acc[HD:, :]) * HD**-0.5).T
    for j in range(heads):

        @pl.when(head == j)
        def _():
            dq_ref[here, j * HD : (j + 1) * HD] = result

    def turned(rows_at):
        grad_k, grad_v = dk[rows_at, :], dv[rows_at, :]
        grad_k = (grad_k + pltpu.roll(grad_k, HD, 1)) * (1.0 / LOG2E)
        grad_v = grad_v + pltpu.roll(grad_v, HD, 1)
        return jnp.where(low_half(grad_k.shape), grad_k, grad_v)

    @pl.when(step == steps - 1)
    def _():
        for b in range(1, blocks):

            @pl.when(head >= 2)
            def _(b=b):
                transfers.kv_copy(head - 2, b).wait_send()

            def finish(j, _, b=b):
                at = pl.ds(pl.multiple_of(j * tile, tile), tile)
                to = pl.ds(pl.multiple_of(b * span + j * tile, tile), tile)
                stage[head % 2, b - 1, at, :] = turned(to)
                return 0

            lax.fori_loop(0, per, finish, 0)
            transfers.kv_copy(head, b).start()

        def keep(j, _):
            at = pl.ds(pl.multiple_of(j * tile, tile), tile)
            dkv_ref[at, :] = turned(at)
            return 0

        lax.fori_loop(0, per, keep, 0)

    transfers.run(head * steps + step, before=False)


def remote(src, dst, send, recv, **peer):
    return pltpu.make_async_remote_copy(
        src_ref=src,
        dst_ref=dst,
        send_sem=send,
        recv_sem=recv,
        device_id=peer,
        device_id_type=pl.DeviceIdType.MESH,
    )


class Transfers:
    def __init__(
        self, n_c, n_f, heads, up_g, down_g, outs, up_out, down_out, kv_far, outs_all, stage,
        up_z, up_x, down_x, down_z, up_z_sem, up_x_sem, down_x_sem, down_z_sem, kv_sem, out_sem,
    ):
        self.n_c, self.n_f, self.heads = n_c, n_f, heads
        self.up_g, self.down_g, self.outs = up_g, down_g, outs
        self.up_out, self.down_out, self.kv_far, self.outs_all = up_out, down_out, kv_far, outs_all
        self.stage = stage
        self.up_z, self.up_x, self.down_x, self.down_z = up_z, up_x, down_x, down_z
        self.up_z_sem, self.up_x_sem = up_z_sem, up_x_sem
        self.down_x_sem, self.down_z_sem, self.kv_sem = down_x_sem, down_z_sem, kv_sem
        self.out_sem = out_sem
        self.f, self.c, me = lax.axis_index("fsdp"), lax.axis_index("ctx"), lax.axis_index("tp")
        self.bit0, self.bit1 = me % 2, me // 2 % 2
        self.peer0, self.peer1 = me + 1 - 2 * self.bit0, me + 2 - 4 * self.bit1

    def at_f(self, k):
        return (self.f + (self.n_f - k)) % self.n_f

    def at_c(self, m):
        return (self.c + (self.n_c - m)) % self.n_c

    def up_hop(self, m):
        src = self.up_g.at[self.at_f(1)] if m == 1 else self.up_z.at[m - 2]
        sem = self.up_z_sem
        return remote(
            src, self.up_z.at[m - 1], sem.at[0, m - 1], sem.at[1, m - 1], fsdp=self.at_f(-1)
        )

    def up_side(self, m):
        src = self.up_z.at[self.n_f - 2, self.at_c(1)] if m == 1 else self.up_x.at[m - 2]
        sem = self.up_x_sem
        return remote(
            src, self.up_x.at[m - 1], sem.at[0, m - 1], sem.at[1, m - 1], ctx=self.at_c(-1)
        )

    def down_side(self, k, m):
        if m == 1:
            src = self.down_g.at[self.at_f(k), self.at_c(1)]
        else:
            src = self.down_x.at[k - 1, m - 2]
        sem = self.down_x_sem
        return remote(
            src,
            self.down_x.at[k - 1, m - 1],
            sem.at[0, k - 1, m - 1],
            sem.at[1, k - 1, m - 1],
            ctx=self.at_c(-1),
        )

    def down_hop(self, k):
        src = self.down_x.at[0, self.n_c - 2] if k == 1 else self.down_z.at[k - 2]
        sem = self.down_z_sem
        return remote(
            src, self.down_z.at[k - 1], sem.at[0, k - 1], sem.at[1, k - 1], fsdp=self.at_f(-1)
        )

    def kv_copy(self, head, m):
        lanes = pl.ds(pl.multiple_of(head * 2 * HD, 2 * HD), 2 * HD)
        return remote(
            self.stage.at[head % 2, m - 1],
            self.kv_far.at[m - 1, :, lanes],
            self.kv_sem.at[0, head, m - 1],
            self.kv_sem.at[1, head, m - 1],
            ctx=self.at_c(m),
        )

    def out_local(self):
        return pltpu.make_async_copy(
            self.outs, self.outs_all.at[:, self.bit0, self.bit1], self.out_sem.at[0, 2]
        )

    def out_far(self):
        return remote(
            self.outs,
            self.outs_all.at[:, self.bit0, self.bit1],
            self.out_sem.at[0, 0],
            self.out_sem.at[1, 0],
            tp=self.peer1,
        )

    def out_near(self):
        pair = self.outs_all.at[:, self.bit0]
        return remote(pair, pair, self.out_sem.at[0, 1], self.out_sem.at[1, 1], tp=self.peer0)

    def begin(self):
        barrier = pltpu.get_barrier_semaphore()
        peers = [{"tp": self.peer0}, {"tp": self.peer1}, {"fsdp": self.at_f(-1)}]
        if self.n_f > 2:
            peers.append({"fsdp": self.at_f(1)})
        peers += [{"ctx": self.at_c(m)} for m in range(1, self.n_c)]
        for peer in peers:
            pl.semaphore_signal(
                barrier, inc=1, device_id=peer, device_id_type=pl.DeviceIdType.MESH
            )
        pl.semaphore_wait(barrier, len(peers))
        self.up_hop(1).start()
        for k in range(1, self.n_f + 1):
            self.down_side(k, 1).start()
        self.out_local().start()
        self.out_far().start()

    def up_event(self, m):
        self.up_hop(m - 1).wait()
        self.up_z[m - 2] += self.up_g[self.at_f(m)]
        if m < self.n_f:
            self.up_hop(m).start()
        else:
            self.up_side(1).start()

    def up_side_event(self, m):
        self.up_side(m - 1).wait()
        total = self.up_x[m - 2] + self.up_z[self.n_f - 2, self.at_c(m)]
        if m < self.n_c:
            self.up_x[m - 2] = total
            self.up_side(m).start()
        else:
            self.up_out[...] = total

    def down_event(self, k):
        for m in range(2, self.n_c + 1):
            self.down_side(k, m - 1).wait()
            self.down_x[k - 1, m - 2] += self.down_g[self.at_f(k), self.at_c(m)]
            if m < self.n_c:
                self.down_side(k, m).start()
        if k > 1:
            self.down_hop(k - 1).wait()
            total = self.down_z[k - 2] + self.down_x[k - 1, self.n_c - 2]
            if k < self.n_f:
                self.down_z[k - 2] = total
            else:
                down_out, out_out = self.down_out
                down_out[...] = total[:, : down_out.shape[1]]
                out_out[...] = total[:, down_out.shape[1] :]
        if k < self.n_f:
            self.down_hop(k).start()

    def out_event(self):
        self.out_local().wait()
        self.out_far().wait()
        self.out_near().start()

    def end(self):
        self.out_near().wait()
        for head in range(self.heads):
            for m in range(1, self.n_c):
                if head >= self.heads - 2:
                    self.kv_copy(head, m).wait_send()
                self.kv_copy(head, m).wait_recv()

    def run(self, now, before):
        count = self.heads * STEPS_PER_HEAD
        plan = []
        for k in range(1, self.n_f + 1):
            plan.append(((k - 0.3) / (self.n_f + 0.3), lambda k=k: self.down_event(k)))
        for m in range(2, self.n_f + 1):
            plan.append(((m - 1.0) / (self.n_f - 0.2), lambda m=m: self.up_event(m)))
        plan.append((0.45, self.out_event))
        plan.sort(key=lambda item: item[0])
        late = [lambda m=m: self.up_side_event(m) for m in range(2, self.n_c + 1)] + [self.end]
        if before:

            @pl.when(now == 0)
            def _():
                self.begin()

            return
        for at in range(count):
            todo = [f for p, f in plan if min(int(p * count), count - 1) == at]
            if at == count - 1:
                todo = todo + late
            if todo:

                @pl.when(now == at)
                def _(todo=todo):
                    for f in todo:
                        f()


STEPS_PER_HEAD = 4


def attention_back(
    queries, grads, result, lse, kv_blocks, meta, heads, up_g, down_g, outs, tile=512
):
    rows = queries.shape[0] // STEPS_PER_HEAD
    n_f, n_c, own, wide_up = up_g.shape
    wide_down = down_g.shape[-1]
    count, span, blocks = queries.shape[0], kv_blocks[0].shape[0], len(kv_blocks)
    keys = span * blocks
    whole = lambda h, i, m: (0, 0)
    wide = pl.BlockSpec((count, heads * HD), whole)
    kv_spec = pl.BlockSpec((span, 2 * HD), lambda h, i, m: (0, h))
    anywhere = pl.BlockSpec(memory_space=pl.ANY)
    sem, shape = pltpu.SemaphoreType.DMA, jax.ShapeDtypeStruct

    def held(array):
        return pl.BlockSpec(array.shape, lambda h, i, m: (0,) * array.ndim)

    return pl.pallas_call(
        functools.partial(backward_kernel, heads, blocks, n_f, tile, rows),
        grid_spec=pltpu.PrefetchScalarGridSpec(
            num_scalar_prefetch=1,
            grid=(heads, count // rows),
            in_specs=[wide] * 3
            + [pl.BlockSpec((heads, count), whole)]
            + [held(up_g), held(down_g), held(outs)]
            + [kv_spec] * blocks,
            out_specs=[
                wide,
                kv_spec,
                pl.BlockSpec((own, wide_up), whole),
                pl.BlockSpec((own, wide_up), whole),
                pl.BlockSpec((own, wide_down - wide_up), whole),
                anywhere,
                anywhere,
            ],
            scratch_shapes=[
                pltpu.VMEM((keys, 2 * HD), jnp.bfloat16),
                pltpu.VMEM((keys, 2 * HD), jnp.bfloat16),
                pltpu.VMEM((2 * HD, keys), jnp.bfloat16),
                pltpu.VMEM((keys, 128), jnp.float32),
                pltpu.VMEM((rows, 2 * HD), jnp.float32),
                pltpu.VMEM((rows, 2 * HD), jnp.float32),
                pltpu.VMEM((rows, 2 * HD), jnp.float32),
                pltpu.VMEM((keys, 2 * HD), jnp.float32),
                pltpu.VMEM((keys, 2 * HD), jnp.float32),
                pltpu.VMEM((2 * HD, rows), jnp.float32),
                pltpu.VMEM((2, n_c - 1, span, 2 * HD), jnp.float32),
                pltpu.VMEM((n_f - 1, n_c, own, wide_up), jnp.float32),
                pltpu.VMEM((n_c - 1, own, wide_up), jnp.float32),
                pltpu.VMEM((n_f, n_c - 1, own, wide_down), jnp.float32),
                pltpu.VMEM((n_f - 1, own, wide_down), jnp.float32),
                sem((2, n_f - 1)),
                sem((2, n_c - 1)),
                sem((2, n_f, n_c - 1)),
                sem((2, n_f - 1)),
                sem((2, heads, n_c - 1)),
                sem((2, 3)),
            ],
        ),
        out_shape=[
            shape((count, heads * HD), jnp.float32),
            shape((span, 2 * heads * HD), jnp.float32),
            shape((own, wide_up), jnp.float32),
            shape((own, wide_up), jnp.float32),
            shape((own, wide_down - wide_up), jnp.float32),
            shape((n_c - 1, span, 2 * heads * HD), jnp.float32),
            shape((outs.shape[0], 2, 2) + outs.shape[1:], jnp.float32),
        ],
        compiler_params=pltpu.CompilerParams(
            dimension_semantics=("arbitrary", "arbitrary"),
            collective_id=2,
            has_side_effects=True,
            vmem_limit_bytes=62 << 20,
        ),
        cost_estimate=pl.CostEstimate(
            flops=60 * heads * count * keys * HD,
            bytes_accessed=16 * keys * heads * HD + 16 * count * heads * HD,
            transcendentals=heads * count * keys,
        ),
        name="attention_backward",
    )(meta, queries, grads, result, lse, up_g, down_g, outs, *kv_blocks)


def dot_three(left, right, left_dim, right_dim):
    left_high, left_low = left
    right_high, right_low = right
    return dot(left_high, right_high, left_dim, right_dim) + (
        dot(left_high, right_low, left_dim, right_dim)
        + dot(left_low, right_high, left_dim, right_dim)
    )


def tiles_of(count, body):
    tile = 256 if count % 256 == 0 else count

    def step(n, _):
        body(pl.ds(pl.multiple_of(n * tile, tile), tile))
        return 0

    lax.fori_loop(0, count // tile, step, 0)


def middle_kernel(
    chunks, rows, n_c,
    att_ref, weights, outw_ref,
    b_out_1, gain_1_1, shift_1_1, b_up_1, b_down_1, gain_2_1, shift_2_1, tok_hbm, cot_hbm,
    out_own, mid_own, gatt, d_up, d_down, vec, d_bup,
    part, rx0, rx1, full, act_hi, act_lo, slope, tok, cot, norm_1, recip_1,
    up_s, down_s, outw_s, xs, ys, ts, send0, recv0, send1, recv1, own_sem,
    lines, b_up, *blocked,
):
    half, quarter = rows // 2, rows // 4
    me = lax.axis_index("tp")
    bit0, bit1 = me % 2, me // 2 % 2
    peer0, peer1 = me + 1 - 2 * bit0, me + 2 - 4 * bit1
    home0 = pl.multiple_of(bit0 * half, half)
    away0 = pl.multiple_of((1 - bit0) * half, half)
    mine = pl.multiple_of(home0 + bit1 * quarter, quarter)
    away1 = pl.multiple_of(home0 + (1 - bit1) * quarter, quarter)
    own = pl.ds(mine, quarter)

    def remote_tp(src, dst, send, recv, peer):
        return remote(src, dst, send, recv, tp=peer)

    width, hidden = up_s.shape[1], up_s.shape[2]
    if blocked:
        whole, w_sem, wl_sem = blocked
        n_f, own_w = weights.shape[0], weights.shape[1]
        at = lax.axis_index("ctx")

        def columns_of(part_at):
            return pl.ds(part_at * hidden, hidden)

        def w_copies(part_at):
            cols = columns_of(part_at)
            for k in range(n_f):
                yield pltpu.make_async_copy(
                    weights.at[k, :, cols], whole.at[k, at, :, cols], wl_sem.at[part_at, k]
                )
                for m in range(1, n_c):
                    yield remote(
                        weights.at[k, :, cols],
                        whole.at[k, at, :, cols],
                        w_sem.at[0, part_at, k, m - 1],
                        w_sem.at[1, part_at, k, m - 1],
                        ctx=(at + m) % n_c,
                    )

    def scatter0(s, c):
        return remote_tp(
            part.at[c, pl.ds(away0, half)], rx0.at[s, c], send0.at[0, s, c], recv0.at[0, s, c], peer0
        )

    def scatter1(s, c):
        return remote_tp(
            part.at[c, pl.ds(away1, quarter)],
            rx1.at[s, c],
            send1.at[0, s, c],
            recv1.at[0, s, c],
            peer1,
        )

    def gather1(s, c):
        return remote_tp(
            full.at[s, c, own], full.at[s, c, own], send1.at[1, s, c], recv1.at[1, s, c], peer1
        )

    def gather0(s, c):
        place = pl.ds(home0, half)
        return remote_tp(
            full.at[s, c, place], full.at[s, c, place], send0.at[1, s, c], recv0.at[1, s, c], peer0
        )

    def own_copies(c):
        where = pl.ds(pl.multiple_of(c * rows + mine, quarter), quarter)
        return (
            pltpu.make_async_copy(tok_hbm.at[where], tok.at[c], own_sem.at[0, c]),
            pltpu.make_async_copy(cot_hbm.at[where], cot.at[c], own_sem.at[1, c]),
        )

    for c in range(chunks):
        for copy in own_copies(c):
            copy.start()
    barrier = pltpu.get_barrier_semaphore()
    peers = [{"tp": peer0}, {"tp": peer1}]
    if blocked:
        peers += [{"ctx": (at + m) % n_c} for m in range(1, n_c)]
    for peer in peers:
        pl.semaphore_signal(barrier, inc=1, device_id=peer, device_id_type=pl.DeviceIdType.MESH)

    firsts = (b_out_1, gain_1_1, shift_1_1, b_down_1, gain_2_1, shift_2_1)
    for i, vector in enumerate(firsts):
        lines[i : i + 1, :] = row(vector)
    b_up[...] = row(b_up_1)
    b_out, gain_1, shift_1, b_down, gain_2, shift_2 = (
        lines.at[i : i + 1] for i in range(len(firsts))
    )

    def split_rows(source, target):
        count = source.shape[0]
        step = 128

        def one(i, _):
            at = pl.ds(pl.multiple_of(i * step, step), step)
            target[0, at, :], target[1, at, :] = halves(source[at, :])
            return 0

        lax.fori_loop(0, count // step, one, 0)

    split_rows(outw_ref, outw_s)

    def weights_ready(part_at, target):
        if not blocked:
            split_rows(weights[part_at], target)
            return
        for copy in w_copies(part_at):
            copy.wait()

        def one(j, _):
            to = pl.ds(pl.multiple_of(j * own_w, own_w), own_w)
            piece = whole[j // n_c, j % n_c, :, columns_of(part_at)]
            target[0, to, :], target[1, to, :] = halves(piece)
            return 0

        lax.fori_loop(0, n_f * n_c, one, 0)

    d_bup[...] = jnp.zeros_like(d_bup)
    vec[...] = jnp.zeros_like(vec)
    d_up[...] = jnp.zeros_like(d_up)
    d_down[...] = jnp.zeros_like(d_down)
    for c in range(chunks):
        for copy in own_copies(c):
            copy.wait()
    pl.semaphore_wait(barrier, len(peers))
    if blocked:
        for part_at in range(2):
            for copy in w_copies(part_at):
                copy.start()

    def split_into(target, value):
        target[0], target[1] = halves(value)

    def finish0(s, c):
        scatter0(s, c).wait()
        away = pl.ds(away1 - home0, quarter)
        part[c, pl.ds(away1, quarter), :] += rx0[s, c, away, :]
        scatter1(s, c).start()
        stay = pl.ds(mine - home0, quarter)
        part[c, own, :] += rx0[s, c, stay, :]

    def finish1(s, c):
        scatter1(s, c).wait()
        return part[c, own, :] + rx1[s, c]

    def forward1(s, c):
        gather1(s, c).wait()
        gather0(s, c).start()

    def trailing(c, now, before):
        if before is not None:

            @pl.when(c == 0)
            def _():
                before(chunks - 1)

        if now is not None:

            @pl.when(c > 0)
            def _():
                now(c - 1)

    def stage(body):
        def one(c, _):
            body(c)
            return 0

        lax.fori_loop(0, chunks, one, 0)

    def at_rows(c):
        return pl.ds(pl.multiple_of(c * rows, rows), rows)

    def attention_out(c):
        left = halves(att_ref[at_rows(c), :])

        def columns(n):
            part[c, :, n] = dot_three(left, (outw_s[0, n, :], outw_s[1, n, :]), 1, 1)

        tiles_of(width, columns)
        scatter0(0, c).start()
        trailing(c, functools.partial(finish0, 0), None)

    stage(attention_out)

    def first_norm(c):
        trailing(c, None, functools.partial(finish0, 0))
        resid = finish1(0, c) + tok[c] + b_out[...]
        n_1, r_1 = normalized(resid)
        norm_1[c] = n_1
        recip_1[c] = jnp.broadcast_to(r_1, recip_1.shape[1:])
        full[0, c, own, :] = n_1 * gain_1[...] + shift_1[...]
        gather1(0, c).start()
        trailing(c, functools.partial(forward1, 0), None)

    stage(first_norm)

    def feed_forward(c):
        gather0(0, c).wait()
        split_into(xs, full[0, c])

        def columns(n):
            pre = dot_three((xs[0], xs[1]), (up_s[0, :, n], up_s[1, :, n]), 1, 0) + b_up[:, n]
            cdf = 0.5 + 0.5 * lax.erf(pre * math.sqrt(0.5))
            slope[c, :, n] = cdf + pre * (
                jnp.exp(-0.5 * pre * pre) * (1.0 / math.sqrt(2.0 * math.pi))
            )
            act_hi[c, :, n], act_lo[c, :, n] = halves(pre * cdf)

        tiles_of(hidden, columns)

        @pl.when(c == 0)
        def _():
            weights_ready(1, down_s)

        def back(n):
            part[c, :, n] = dot_three(
                (act_hi[c], act_lo[c]), (down_s[0, n, :], down_s[1, n, :]), 1, 1
            )

        tiles_of(width, back)
        scatter0(1, c).start()
        trailing(c, functools.partial(finish0, 1), functools.partial(forward1, 0))

    def second_norm(c):
        trailing(c, None, functools.partial(finish0, 1))
        ffn = finish1(1, c) + full[0, c, own, :] + b_down[...]
        n_2, r_2 = normalized(ffn)
        out_own[c] = n_2 * gain_2[...] + shift_2[...]
        grad = cot[c]
        second = norm_back(grad, gain_2[...], n_2, r_2)
        full[1, c, own, :] = second
        gather1(1, c).start()
        vec[3:4, :] += jnp.sum(second, axis=0, keepdims=True)
        vec[4:5, :] += jnp.sum(grad * n_2, axis=0, keepdims=True)
        vec[5:6, :] += jnp.sum(grad, axis=0, keepdims=True)
        trailing(c, functools.partial(forward1, 1), None)

    def feed_back(c):
        gather0(1, c).wait()
        split_into(xs, full[1, c])

        def columns(n):
            grad = dot_three((xs[0], xs[1]), (down_s[0, :, n], down_s[1, :, n]), 1, 0)
            grad = grad * slope[c, :, n]
            slope[c, :, n] = grad
            ys[0, :, n], ys[1, :, n] = halves(grad)
            d_bup[:, n] += jnp.sum(grad, axis=0, keepdims=True)

        tiles_of(hidden, columns)

        def back(n):
            part[c, :, n] = dot_three((ys[0], ys[1]), (up_s[0, n, :], up_s[1, n, :]), 1, 1)

        tiles_of(width, back)
        scatter0(2, c).start()
        trailing(c, functools.partial(finish0, 2), functools.partial(forward1, 1))

    def middle_norm(c):
        trailing(c, None, functools.partial(finish0, 2))
        first = finish1(2, c) + full[1, c, own, :]
        n_1 = norm_1[c]
        mid = norm_back(first, gain_1[...], n_1, recip_1[c, :, :1])
        mid_own[c] = mid
        full[2, c, own, :] = mid
        gather1(2, c).start()
        vec[0:1, :] += jnp.sum(mid, axis=0, keepdims=True)
        vec[1:2, :] += jnp.sum(first * n_1, axis=0, keepdims=True)
        vec[2:3, :] += jnp.sum(first, axis=0, keepdims=True)
        trailing(c, functools.partial(forward1, 2), None)
        split_into(ts, full[1, c].T)

        def columns(n):
            d_down[:, n] += dot_three((ts[0], ts[1]), (act_hi[c, :, n], act_lo[c, :, n]), 1, 0)

        tiles_of(hidden, columns)

    def last(c):
        gather0(2, c).wait()
        mid = full[2, c]
        gatt[at_rows(c), :] = dot_three(halves(mid), (outw_s[0], outw_s[1]), 1, 0)
        trailing(c, None, functools.partial(forward1, 2))
        split_into(ts, mid.T)
        d_down[:, hidden:] += dot_three((ts[0], ts[1]), halves(att_ref[at_rows(c), :]), 1, 0)
        split_into(ts, full[0, c].T)

        def columns(n):
            d_up[:, n] += dot_three((ts[0], ts[1]), halves(slope[c, :, n]), 1, 0)

        tiles_of(hidden, columns)

    weights_ready(0, up_s)
    stage(feed_forward)
    stage(second_norm)
    stage(feed_back)
    stage(middle_norm)
    stage(last)


def middle_whole(chunks, rows, n_c, att, up, down, *refs):
    middle_kernel(chunks, rows, n_c, att, (up, down), *refs)


def middle(attended, weights, wide_out_t, vectors, tokens, cot, hidden, n_c, chunks=4):
    blocked = not isinstance(weights, tuple)
    count, width = tokens.shape
    split_at = attended.shape[1]
    rows = count // chunks
    half, quarter = rows // 2, rows // 4
    vmem = pl.BlockSpec(memory_space=pltpu.VMEM)
    anywhere = pl.BlockSpec(memory_space=pl.ANY)
    f32, bf16 = jnp.float32, jnp.bfloat16
    sems = pltpu.SemaphoreType.DMA((2, 3, chunks))
    extra = [pltpu.VMEM((8, width), f32), pltpu.VMEM((1, hidden), f32)]
    if blocked:
        n_f, own = weights.shape[0], weights.shape[1]
        extra += [
            pltpu.VMEM((n_f, n_c, own, 2 * hidden), f32),
            pltpu.SemaphoreType.DMA((2, 2, n_f, n_c - 1)),
            pltpu.SemaphoreType.DMA((2, n_f)),
        ]
    shape = jax.ShapeDtypeStruct
    return pl.pallas_call(
        functools.partial(middle_kernel if blocked else middle_whole, chunks, rows, n_c),
        in_specs=[vmem]
        + ([anywhere] if blocked else [vmem] * 2)
        + [vmem] * 8
        + [anywhere] * 2,
        out_specs=[vmem] * 7,
        out_shape=[
            shape((chunks, quarter, width), f32),
            shape((chunks, quarter, width), f32),
            shape((count, split_at), f32),
            shape((width, hidden), f32),
            shape((width, hidden + split_at), f32),
            shape((8, width), f32),
            shape((1, hidden), f32),
        ],
        scratch_shapes=[
            pltpu.VMEM((chunks, rows, width), f32),
            pltpu.VMEM((3, chunks, half, width), f32),
            pltpu.VMEM((3, chunks, quarter, width), f32),
            pltpu.VMEM((3, chunks, rows, width), f32),
            pltpu.VMEM((chunks, rows, hidden), bf16),
            pltpu.VMEM((chunks, rows, hidden), bf16),
            pltpu.VMEM((chunks, rows, hidden), f32),
            pltpu.VMEM((chunks, quarter, width), f32),
            pltpu.VMEM((chunks, quarter, width), f32),
            pltpu.VMEM((chunks, quarter, width), f32),
            pltpu.VMEM((chunks, quarter, 128), f32),
            pltpu.VMEM((2, width, hidden), bf16),
            pltpu.VMEM((2, width, hidden), bf16),
            pltpu.VMEM((2, width, split_at), bf16),
            pltpu.VMEM((2, rows, width), bf16),
            pltpu.VMEM((2, rows, hidden), bf16),
            pltpu.VMEM((2, width, rows), bf16),
            sems, sems, sems, sems,
            pltpu.SemaphoreType.DMA((2, chunks)),
            *extra,
        ],
        compiler_params=pltpu.CompilerParams(
            collective_id=1, has_side_effects=True, vmem_limit_bytes=62 << 20
        ),
        cost_estimate=pl.CostEstimate(
            flops=6 * count * width * (6 * hidden + 3 * split_at),
            bytes_accessed=4 * width * (5 * hidden + 3 * split_at),
            transcendentals=2 * count * hidden,
        ),
        name="middle",
    )(
        attended,
        *([weights] if blocked else weights),
        wide_out_t,
        *vectors,
        tokens,
        cot,
    )


def front_kernel(
    heads, n_c, n_f, tile, rows, meta_ref, tok, w_qkv, up, down_t, outw_t, b_q, b_v,
    att, lse, q_out, kv_out, kv_far, wide, up_down, out_all,
    shard, q_s, kv_s, kv_t, wv, w_s, ud_own, ow_own, kp, vt, bias, qd, acc, top_s, total_s,
    hop_sem, side_sem, ud_sem, ow_sem, ow_side_sem, kv_sem, local_sem,
):
    block, head, step = pl.program_id(0), pl.program_id(1), pl.program_id(2)
    n_q = pl.num_programs(2)
    span, hidden, split_at = tok.shape[0], up.shape[1], heads * HD
    own = shard.shape[0]
    f, c = lax.axis_index("fsdp"), lax.axis_index("ctx")

    def at_f(k):
        return (f + (n_f - k)) % n_f

    def at_c(m):
        return (c + (n_c - m)) % n_c

    def lanes(h):
        return pl.ds(pl.multiple_of(h * 2 * HD, 2 * HD), 2 * HD)

    def hop(k):
        src = shard if k == 1 else wv.at[at_f(k - 1), c]
        return remote(
            src, wv.at[at_f(k - 1), c], hop_sem.at[0, k - 1], hop_sem.at[1, k - 1], fsdp=at_f(-1)
        )

    def side(k, m):
        src = shard if k == 0 else wv.at[at_f(k), c]
        return remote(
            src, wv.at[at_f(k), c], side_sem.at[0, k, m - 1], side_sem.at[1, k, m - 1], ctx=at_c(-m)
        )

    def ud_hop(k):
        src = ud_own if k == 1 else up_down.at[at_f(k - 1)]
        return remote(
            src, up_down.at[at_f(k - 1)], ud_sem.at[0, k - 1], ud_sem.at[1, k - 1], fsdp=at_f(-1)
        )

    def ow_hop(k):
        src = ow_own if k == 1 else out_all.at[at_f(k - 1), c]
        return remote(
            src, out_all.at[at_f(k - 1), c], ow_sem.at[0, k - 1], ow_sem.at[1, k - 1], fsdp=at_f(-1)
        )

    def ow_side(k, m):
        src = ow_own if k == 0 else out_all.at[at_f(k), c]
        return remote(
            src,
            out_all.at[at_f(k), c],
            ow_side_sem.at[0, k, m - 1],
            ow_side_sem.at[1, k, m - 1],
            ctx=at_c(-m),
        )

    def kv_send(h, m):
        return remote(
            kv_s.at[:, lanes(h)],
            kv_far.at[m - 1, :, lanes(h)],
            kv_sem.at[0, h, m - 1],
            kv_sem.at[1, h, m - 1],
            ctx=at_c(-m),
        )

    def locals_of():
        return [
            pltpu.make_async_copy(a, b, local_sem.at[i])
            for i, (a, b) in enumerate(
                (
                    (ud_own, up_down.at[f]),
                    (ow_own, out_all.at[f, c]),
                    (wv, wide),
                    (q_s, q_out),
                    (kv_s, kv_out),
                )
            )
        ]

    @pl.when((block == 0) & (head == 0) & (step == 0))
    def _():
        barrier = pltpu.get_barrier_semaphore()
        peers = [{"fsdp": at_f(-1)}] + ([{"fsdp": at_f(1)}] if n_f > 2 else [])
        peers += [{"ctx": at_c(m)} for m in range(1, n_c)]
        for peer in peers:
            pl.semaphore_signal(
                barrier, inc=1, device_id=peer, device_id_type=pl.DeviceIdType.MESH
            )
        for h in range(heads):
            at = 3 * HD * h
            shard[:, 2 * HD * h : 2 * HD * (h + 1)] = w_qkv[:, at + HD : at + 3 * HD]
            shard[:, 2 * split_at + HD * h : 2 * split_at + HD * (h + 1)] = w_qkv[:, at : at + HD]
        pl.semaphore_wait(barrier, len(peers))
        hop(1).start()
        for m in range(1, n_c):
            side(0, m).start()
        wv[f, c] = shard[...]
        ud_own[:, :hidden] = up[...]
        ud_own[:, hidden:] = down_t[...]
        ow_own[...] = outw_t[...]
        for k in range(1, n_f):
            hop(k).wait()
            if k < n_f - 1:
                hop(k + 1).start()
            for m in range(1, n_c):
                side(k, m).start()
        ud_hop(1).start()
        ow_hop(1).start()
        copies = locals_of()
        copies[0].start()
        copies[1].start()
        for k in range(n_f):
            for m in range(1, n_c):
                side(k, m).wait()

        def split(j, _):
            to = pl.ds(pl.multiple_of(j * own, own), own)
            w_s[0, to, :], w_s[1, to, :] = halves(wv[j // n_c, j % n_c])
            return 0

        lax.fori_loop(0, n_f * n_c, split, 0)
        copies[2].start()

        blank = jnp.zeros((1, HD), jnp.float32)
        v_row = row(b_v)
        b_kv = jnp.concatenate(
            sum(([blank, v_row[:, h * HD : (h + 1) * HD]] for h in range(heads)), []), axis=1
        )
        q_row = row(b_q)

        def keys(i, _):
            at = pl.ds(pl.multiple_of(i * rows, rows), rows)
            right = (w_s[0, :, : 2 * split_at], w_s[1, :, : 2 * split_at])
            kv_s[at, :] = dot_three(halves(tok[at, :]), right, 1, 0) + b_kv
            return 0

        lax.fori_loop(0, span // rows, keys, 0)
        for h in range(heads):
            for m in range(1, n_c):
                kv_send(h, m).start()

        def asking(i, _):
            at = pl.ds(pl.multiple_of(i * rows, rows), rows)
            right = (w_s[0, :, 2 * split_at :], w_s[1, :, 2 * split_at :])
            q_s[at, :] = dot_three(halves(tok[at, :]), right, 1, 0) + q_row
            return 0

        lax.fori_loop(0, span // rows, asking, 0)
        copies[3].start()
        copies[4].start()
        for m in range(1, n_c):
            ow_side(0, m).start()

    @pl.when((block == 0) & (step == 0))
    def _():
        kv_t[...] = kv_s[:, lanes(head)]

    @pl.when((block > 0) & (step == 0))
    def _():
        kv_send(head, block).wait_recv()
        copy = pltpu.make_async_copy(
            kv_far.at[block - 1, :, lanes(head)], kv_t, local_sem.at[5]
        )
        copy.start()
        copy.wait()

    @pl.when(step == 0)
    def _():
        def prepare(j, _):
            at = pl.ds(pl.multiple_of(j * tile, tile), tile)
            pair = kv_t[at, :]
            kp[at, :] = packed(pair, True)
            vt[:, at] = stacked(pair.T[HD:, :])
            bias[at, :] = key_bias(meta_ref[0], at_c(block) * span + j * tile, tile, 128)
            return 0

        lax.fori_loop(0, span // tile, prepare, 0)

    here = pl.ds(pl.multiple_of(step * rows, rows), rows)

    @pl.when(block == 0)
    def _():
        acc[head, :, here] = jnp.zeros((2 * HD, rows), jnp.float32)
        top_s[head, :, here] = jnp.full((1, rows), MASKED, jnp.float32)
        total_s[head, :, here] = jnp.zeros((1, rows), jnp.float32)

    doubled(q_s, here, head, qd, heads)
    q_high, q_low = halves(qd[...] * (LOG2E * HD**-0.5))
    q_four = jnp.concatenate([q_high, q_low], axis=1)

    def key_tile(j, carry):
        top, total = carry
        at = pl.ds(pl.multiple_of(j * tile, tile), tile)
        k_two = kp[at, :]
        scores = dot(jnp.concatenate([k_two, k_two], axis=1), q_four, 1, 1)
        scores = scores + jnp.concatenate([bias[at, :]] * (rows // 128), axis=1)
        new_top = jnp.maximum(top, jnp.max(scores, axis=0, keepdims=True))
        fade = jnp.exp2(top - new_top)
        probs = jnp.exp2(scores - new_top)
        total = total * fade + jnp.sum(probs, axis=0, keepdims=True)
        high, low = halves(probs)
        v_two = vt[:, at]
        acc[head, :, here] = acc[head, :, here] * fade + (
            dot(v_two, high, 1, 0) + dot(v_two, low, 1, 0)
        )
        return new_top, total

    top, total = lax.fori_loop(
        0, span // tile, key_tile, (top_s[head, :, here], total_s[head, :, here])
    )
    top_s[head, :, here] = top
    total_s[head, :, here] = total

    @pl.when(block == n_c - 1)
    def _():
        result = ((acc[head, :HD, here] + acc[head, HD:, here]) / total).T
        for j in range(heads):

            @pl.when(head == j)
            def _(j=j):
                att[here, j * HD : (j + 1) * HD] = result
                lse[j : j + 1, here] = top + jnp.log2(total)

    def arrived(k):
        ud_hop(k).wait()
        ow_hop(k).wait()
        if k < n_f - 1:
            ud_hop(k + 1).start()
            ow_hop(k + 1).start()
        for m in range(1, n_c):
            ow_side(k, m).start()

    count = n_c * heads * STEPS_PER_HEAD
    now = (block * heads + head) * n_q + step
    for k in range(1, n_f):

        @pl.when(now == min(count - 1, k * count // (n_f - 1) - 1))
        def _(k=k):
            arrived(k)

    @pl.when(now == count - 1)
    def _():
        for k in range(n_f):
            for m in range(1, n_c):
                ow_side(k, m).wait()
        for h in range(heads):
            for m in range(1, n_c):
                kv_send(h, m).wait_send()
        for copy in locals_of():
            copy.wait()


def front(tokens, w_qkv, w_up, w_down_t, w_out_t, b_query, b_value, lengths, heads, n_f, n_c, tile=512):
    span, width = tokens.shape
    own, total = w_qkv.shape
    hidden, split_at = w_up.shape[1], heads * HD
    rows = span // STEPS_PER_HEAD
    shape, sem, f32, bf16 = jax.ShapeDtypeStruct, pltpu.SemaphoreType.DMA, jnp.float32, jnp.bfloat16
    anywhere = pl.BlockSpec(memory_space=pl.ANY)

    def held(dims):
        return pl.BlockSpec(dims, lambda b, h, i, m: (0,) * len(dims))

    operands = (tokens, w_qkv, w_up, w_down_t, w_out_t, b_query, b_value)
    return pl.pallas_call(
        functools.partial(front_kernel, heads, n_c, n_f, tile, rows),
        grid_spec=pltpu.PrefetchScalarGridSpec(
            num_scalar_prefetch=1,
            grid=(n_c, heads, STEPS_PER_HEAD),
            in_specs=[held(x.shape) for x in operands],
            out_specs=[held((span, split_at)), held((heads, span))] + [anywhere] * 6,
            scratch_shapes=[
                pltpu.VMEM((own, total), f32),
                pltpu.VMEM((span, split_at), f32),
                pltpu.VMEM((span, 2 * split_at), f32),
                pltpu.VMEM((span, 2 * HD), f32),
                pltpu.VMEM((n_f, n_c, own, total), f32),
                pltpu.VMEM((2, width, total), bf16),
                pltpu.VMEM((own, 2 * hidden), f32),
                pltpu.VMEM((own, split_at), f32),
                pltpu.VMEM((span, 2 * HD), bf16),
                pltpu.VMEM((2 * HD, span), bf16),
                pltpu.VMEM((span, 128), f32),
                pltpu.VMEM((rows, 2 * HD), f32),
                pltpu.VMEM((heads, 2 * HD, span), f32),
                pltpu.VMEM((heads, 1, span), f32),
                pltpu.VMEM((heads, 1, span), f32),
                sem((2, n_f - 1)),
                sem((2, n_f, n_c - 1)),
                sem((2, n_f - 1)),
                sem((2, n_f - 1)),
                sem((2, n_f, n_c - 1)),
                sem((2, heads, n_c - 1)),
                sem((6,)),
            ],
        ),
        out_shape=[
            shape((span, split_at), f32),
            shape((heads, span), f32),
            shape((span, split_at), f32),
            shape((span, 2 * split_at), f32),
            shape((n_c - 1, span, 2 * split_at), f32),
            shape((n_f, n_c, own, total), f32),
            shape((n_f, own, 2 * hidden), f32),
            shape((n_f, n_c, own, split_at), f32),
        ],
        compiler_params=pltpu.CompilerParams(
            dimension_semantics=("arbitrary",) * 3,
            collective_id=3,
            has_side_effects=True,
            vmem_limit_bytes=62 << 20,
        ),
        name="front",
    )(lengths, *operands)

def tail_kernel(
    chunks, rows, n_c, n_f, own,
    tok, grad_q, grad_kv, far, wide, mid, vec, d_bup,
    d_in, d_w, d_bq, d_bv, d_bu, s_0, s_1, s_2, s_3, s_4, s_5,
    part, rx0, rx1, full, w_s, gs, ts, dw, side_rx, hop_rx, small, small_rx,
    near_sem, far_sem, side_sem, hop_sem, small_sem, local_sem,
):
    half, quarter = rows // 2, rows // 4
    me, f, c_at = lax.axis_index("tp"), lax.axis_index("fsdp"), lax.axis_index("ctx")
    bit0, bit1 = me % 2, me // 2 % 2
    peer0, peer1 = me + 1 - 2 * bit0, me + 2 - 4 * bit1
    home0 = pl.multiple_of(bit0 * half, half)
    away0 = pl.multiple_of((1 - bit0) * half, half)
    mine = pl.multiple_of(home0 + bit1 * quarter, quarter)
    away1 = pl.multiple_of(home0 + (1 - bit1) * quarter, quarter)
    keep = pl.ds(mine, quarter)
    width, kv_width, total = tok.shape[1], grad_kv.shape[1], wide.shape[1]

    def at_f(k):
        return (f + (n_f - k)) % n_f

    def at_c(m):
        return (c_at + (n_c - m)) % n_c

    def exchange(src, dst, sems, kind, c, peer):
        return remote(src, dst, sems.at[0, kind, c], sems.at[1, kind, c], tp=peer)

    def scatter0(c):
        return exchange(part.at[c, pl.ds(away0, half)], rx0.at[c], near_sem, 0, c, peer0)

    def scatter1(c):
        return exchange(part.at[c, pl.ds(away1, quarter)], rx1.at[c], far_sem, 0, c, peer1)

    def gather1(c):
        return exchange(full.at[c, keep], full.at[c, keep], far_sem, 1, c, peer1)

    def gather0(c):
        place = pl.ds(home0, half)
        return exchange(full.at[c, place], full.at[c, place], near_sem, 1, c, peer0)

    def block(k, m):
        return pl.ds(pl.multiple_of((at_f(k) * n_c + at_c(m)) * own, own), own)

    def side(k, m):
        src = dw.at[block(k, 1)] if m == 1 else side_rx.at[k - 1, m - 2]
        return remote(
            src,
            side_rx.at[k - 1, m - 1],
            side_sem.at[0, k - 1, m - 1],
            side_sem.at[1, k - 1, m - 1],
            ctx=at_c(-1),
        )

    def hop(k):
        src = side_rx.at[0, n_c - 2] if k == 1 else hop_rx.at[k - 2]
        return remote(
            src, hop_rx.at[k - 1], hop_sem.at[0, k - 1], hop_sem.at[1, k - 1], fsdp=at_f(-1)
        )

    def powers(count):
        bits, bit = [], 1
        while bit < count:
            bits.append(bit)
            bit *= 2
        return bits

    def flipped(at, bit):
        return at + bit - 2 * bit * (at // bit % 2)

    rounds = [("tp", peer0), ("tp", peer1)]
    rounds += [("fsdp", flipped(f, bit)) for bit in powers(n_f)]
    rounds += [("ctx", flipped(c_at, bit)) for bit in powers(n_c)]

    def small_copy(r):
        axis, peer = rounds[r]
        return remote(
            small.at[r], small_rx.at[r], small_sem.at[0, r], small_sem.at[1, r], **{axis: peer}
        )

    def small_event(r):
        small_copy(r).wait()
        if rounds[r][0] == "tp":
            small[r + 1, :8, :] = small[r, :8, :] + small_rx[r, :8, :]
            small[r + 1, 8:, :] = small[r, 8:, :]
        else:
            small[r + 1] = small[r] + small_rx[r]
        if r + 1 < len(rounds):
            small_copy(r + 1).start()

    barrier = pltpu.get_barrier_semaphore()
    peers = [{"tp": peer0}, {"tp": peer1}]
    peers += [{"fsdp": at_f(k)} for k in range(1, n_f)]
    peers += [{"ctx": at_c(m)} for m in range(1, n_c)]
    for peer in peers:
        pl.semaphore_signal(barrier, inc=1, device_id=peer, device_id_type=pl.DeviceIdType.MESH)

    def split(i, _):
        at = pl.ds(pl.multiple_of(i * 128, 128), 128)
        w_s[0, at, :], w_s[1, at, :] = halves(wide[at, :])
        return 0

    lax.fori_loop(0, width // 128, split, 0)
    small[0, :8, :] = vec[...]
    small[0, 8:, :] = jnp.zeros_like(small[0, 8:, :])
    small[0, 8:9, :] = d_bup[...]
    dw[...] = jnp.zeros_like(dw)
    pl.semaphore_wait(barrier, len(peers))

    def finish0(c):
        scatter0(c).wait()
        part[c, pl.ds(away1, quarter), :] += rx0[c, pl.ds(away1 - home0, quarter), :]
        scatter1(c).start()
        part[c, keep, :] += rx0[c, pl.ds(mine - home0, quarter), :]

    def partial(c, _):
        at = pl.ds(pl.multiple_of(c * rows, rows), rows)
        kv = grad_kv[at, :]
        for m in range(n_c - 1):
            kv = kv + far[m, at, :]
        grad = jnp.concatenate([kv, grad_q[at, :]], axis=1)
        gs[c, 0], gs[c, 1] = halves(grad)
        small[0, 9:10, :total] += jnp.sum(grad, axis=0, keepdims=True)

        def columns(n):
            part[c, :, n] = dot_three((gs[c, 0], gs[c, 1]), (w_s[0, n, :], w_s[1, n, :]), 1, 1)

        tiles_of(width, columns)
        scatter0(c).start()

        @pl.when(c > 0)
        def _():
            finish0(c - 1)

        return 0

    lax.fori_loop(0, chunks, partial, 0)
    finish0(chunks - 1)
    small_copy(0).start()

    def weights(c, _):
        at = pl.ds(pl.multiple_of(c * rows, rows), rows)
        ts[0], ts[1] = halves(tok[at, :].T)

        def lines(n):
            dw[n, :] += dot_three((ts[0, n, :], ts[1, n, :]), (gs[c, 0], gs[c, 1]), 1, 0)

        tiles_of(width, lines)
        return 0

    lax.fori_loop(0, chunks, weights, 0)
    for k in range(1, n_f + 1):
        side(k, 1).start()

    heads = (total - kv_width) // HD

    def grouped(target, value):
        for h in range(heads):
            at = 3 * HD * h
            target[:, at : at + HD] = value[:, kv_width + HD * h : kv_width + HD * (h + 1)]
            target[:, at + HD : at + 3 * HD] = value[:, 2 * HD * h : 2 * HD * (h + 1)]

    def weight_event(k):
        for m in range(2, n_c + 1):
            side(k, m - 1).wait()
            side_rx[k - 1, m - 2] += dw[block(k, m), :]
            if m < n_c:
                side(k, m).start()
        if k > 1:
            hop(k - 1).wait()
            result = hop_rx[k - 2] + side_rx[k - 1, n_c - 2]
            if k < n_f:
                hop_rx[k - 2] = result
            else:
                grouped(d_w, result)
        if k < n_f:
            hop(k).start()

    def finish1(c):
        scatter1(c).wait()
        full[c, keep, :] = part[c, keep, :] + rx1[c] + mid[c]
        gather1(c).start()

    def forward1(c):
        gather1(c).wait()
        gather0(c).start()

    def leave(c):
        return pltpu.make_async_copy(full.at[c], d_in.at[c], local_sem.at[c])

    plan = [(c + 0.0, lambda c=c: finish1(c)) for c in range(chunks)]
    plan += [(chunks + 0.5 + c, lambda c=c: forward1(c)) for c in range(chunks)]
    plan += [
        (2 * chunks * k / (n_f + 0.5), lambda k=k: weight_event(k)) for k in range(1, n_f + 1)
    ]
    plan += [
        (2 * chunks * (r + 0.7) / (len(rounds) + 0.5), lambda r=r: small_event(r))
        for r in range(len(rounds))
    ]
    plan.sort(key=lambda item: item[0])
    for _, event in plan:
        event()
    last = len(rounds)
    for i, target in enumerate((s_0, s_1, s_2, s_3, s_4, s_5)):
        target[...] = small[last, i : i + 1, :].reshape(-1)
    d_bu[...] = small[last, 8:9, :].reshape(-1)
    d_bq[...] = small[last, 9:10, kv_width:total].reshape(-1)
    by_value = [
        small[last, 9:10, 2 * HD * h + HD : 2 * HD * (h + 1)] for h in range(heads)
    ]
    d_bv[...] = jnp.concatenate(by_value, axis=1).reshape(-1)
    for c in range(chunks):
        gather0(c).wait()
        leave(c).start()
    for c in range(chunks):
        leave(c).wait()


def tail(tokens, grad_q, grad_kv, far, wide, mid, vec, d_bup, n_f, n_c, own):
    count, width = tokens.shape
    total, chunks, quarter = wide.shape[1], mid.shape[0], mid.shape[1]
    rows = 4 * quarter
    vmem, anywhere = pl.BlockSpec(memory_space=pltpu.VMEM), pl.BlockSpec(memory_space=pl.ANY)
    shape, sem, f32, bf16 = jax.ShapeDtypeStruct, pltpu.SemaphoreType.DMA, jnp.float32, jnp.bfloat16
    rounds = 2 + (n_f - 1).bit_length() + (n_c - 1).bit_length()
    return pl.pallas_call(
        functools.partial(tail_kernel, chunks, rows, n_c, n_f, own),
        in_specs=[vmem] * 8,
        out_specs=[anywhere] + [vmem] * 10,
        out_shape=[
            shape((chunks, rows, width), f32),
            shape((own, total), f32),
            shape((total - grad_kv.shape[1],), f32),
            shape((total - grad_kv.shape[1],), f32),
        ]
        + [shape((width,), f32)] * 7,
        scratch_shapes=[
            pltpu.VMEM((chunks, rows, width), f32),
            pltpu.VMEM((chunks, rows // 2, width), f32),
            pltpu.VMEM((chunks, quarter, width), f32),
            pltpu.VMEM((chunks, rows, width), f32),
            pltpu.VMEM((2, width, total), bf16),
            pltpu.VMEM((chunks, 2, rows, total), bf16),
            pltpu.VMEM((2, width, rows), bf16),
            pltpu.VMEM((width, total), f32),
            pltpu.VMEM((n_f, n_c - 1, own, total), f32),
            pltpu.VMEM((n_f - 1, own, total), f32),
            pltpu.VMEM((rounds + 1, 16, width), f32),
            pltpu.VMEM((rounds, 16, width), f32),
            sem((2, 2, chunks)),
            sem((2, 2, chunks)),
            sem((2, n_f, n_c - 1)),
            sem((2, n_f - 1)),
            sem((2, rounds)),
            sem((chunks,)),
        ],
        compiler_params=pltpu.CompilerParams(
            collective_id=4, has_side_effects=True, vmem_limit_bytes=62 << 20
        ),
        name="tail",
    )(tokens, grad_q, grad_kv, far, wide, mid, vec, d_bup)

def per_device(
    inputs,
    lengths,
    w_qkv,
    b_query,
    b_value,
    w_out,
    b_out,
    gain_attn,
    shift_attn,
    w_up,
    b_up,
    w_down,
    b_down,
    gain_ffn,
    shift_ffn,
    cotangent,
):
    width = inputs.shape[-1]
    block_len = inputs.shape[1]
    heads = b_query.shape[0] // HD
    split_at = heads * HD
    hidden = b_up.shape[0]
    tokens = inputs.reshape(block_len, width)
    cot = cotangent.reshape(block_len, width)
    length = lengths[0]
    n_c = lax.axis_size("ctx")
    at_c = lax.axis_index("ctx")

    def regroup(columns):
        parts = columns.reshape(columns.shape[:-1] + (heads, 3 * HD))
        lead = columns.shape[:-1]
        return jnp.concatenate(
            [
                parts[..., HD:].reshape(lead + (2 * split_at,)),
                parts[..., :HD].reshape(lead + (split_at,)),
            ],
            axis=-1,
        )

    bias_kv = jnp.stack(
        [jnp.zeros((heads, HD), jnp.float32), b_value.reshape(heads, HD)], axis=1
    ).reshape(-1)
    n_f, own = lax.axis_size("fsdp"), w_up.shape[0]
    fused = own % 16 == 0 and n_c > 1 and n_f > 1 and hidden == width
    if fused:
        attended, log_sums, queries, kv_own, kv_far, wide, weights, wide_out_t = front(
            tokens, w_qkv, w_up, w_down.T, w_out.T, b_query, b_value, lengths, heads, n_f, n_c,
        )
        wide = wide.reshape(width, 3 * split_at)
        wide_kv, wide_q = wide[:, : 2 * split_at], wide[:, 2 * split_at :]
        wide_out_t = wide_out_t.reshape(width, split_at)
        kv_blocks = [kv_own] + [kv_far[m] for m in range(n_c - 1)]
    else:
        wide_kv, wide_q = weight_gather(regroup(w_qkv), [2 * split_at, split_at])
        rest = jnp.concatenate([w_up, w_down.T, w_out.T], axis=1)
        wide_up, wide_down_t, wide_out_t = weight_gather(rest, [hidden, hidden, split_at])
        weights = (wide_up, wide_down_t)
        kv_blocks = [contract(tokens, wide_kv, 1, 0) + bias_kv]
        for m in range(1, n_c):
            kv_blocks.append(ringed(kv_blocks[-1], "ctx", 1))
        queries = contract(tokens, wide_q, 1, 0) + b_query
        meta = jnp.stack([length] + [(at_c - m) % n_c * block_len for m in range(n_c)])
        attended, log_sums = attention(queries, kv_blocks, meta, heads)

    vectors = (b_out, gain_attn, shift_attn, b_up, b_down, gain_ffn, shift_ffn)
    outs, grad_mid, grad_att, d_up, d_down_out, vec_rows, d_bup = middle(
        attended, weights, wide_out_t, vectors, tokens, cot, hidden, n_c
    )
    blocked = (lax.axis_size("fsdp"), n_c, w_up.shape[0])
    grad_q, grad_kv, d_wup, d_wdown_t, d_wout_t, kv_back, outputs = attention_back(
        queries,
        grad_att,
        attended,
        log_sums,
        kv_blocks,
        lengths,
        heads,
        d_up.reshape(blocked + (hidden,)),
        d_down_out.reshape(blocked + (hidden + split_at,)),
        outs,
    )
    d_wdown, d_wout = d_wdown_t.T, d_wout_t.T
    if fused:
        d_inputs, d_wqkv, d_bquery, d_bvalue, d_bup, *sums = tail(
            tokens, grad_q, grad_kv, kv_back, wide, grad_mid, vec_rows, d_bup, n_f, n_c, own
        )
        d_inputs = d_inputs.reshape(block_len, width)
    else:
        for m in range(n_c - 1):
            grad_kv = grad_kv + kv_back[m]
        back = contract(grad_kv, wide_kv, 1, 1) + contract(grad_q, wide_q, 1, 1)
        tail_sums = small_sum(
            jnp.concatenate([jnp.sum(grad_kv, axis=0), jnp.sum(grad_q, axis=0), d_bup[0]]),
            ("fsdp", "ctx"),
        )
        proj_sums, d_bup = tail_sums[: 3 * split_at], tail_sums[3 * split_at :]
        sums = small_sum(vec_rows, ("tp", "fsdp", "ctx"))
        d_inputs = quarter_gather(grad_mid + quarter_scatter(back, grad_mid.shape[0]))
        own_dw = grad_scatter([contract(tokens, grad_kv, 0, 0), contract(tokens, grad_q, 0, 0)])
        d_wqkv = jnp.concatenate(
            [
                own_dw[:, 2 * split_at :].reshape(own, heads, HD),
                own_dw[:, : 2 * split_at].reshape(own, heads, 2 * HD),
            ],
            axis=2,
        ).reshape(own, 3 * split_at)
        d_bvalue = proj_sums[: 2 * split_at].reshape(heads, 2, HD)[:, 1].reshape(-1)
        d_bquery = proj_sums[2 * split_at : 3 * split_at]
    return (
        outputs.reshape(1, block_len, width),
        d_inputs.reshape(1, block_len, width),
        d_wqkv,
        d_bquery,
        d_bvalue,
        d_wout,
        sums[0],
        sums[1],
        sums[2],
        d_wup,
        d_bup,
        d_wdown,
        sums[3],
        sums[4],
        sums[5],
    )


def solution(mesh):
    rows_of, cols_of = P(("fsdp", "ctx"), "tp"), P("tp", ("fsdp", "ctx"))
    seq, by_tp, same = P("fsdp", "ctx", None), P("tp"), P()
    in_specs = (
        seq, P("fsdp"), rows_of, by_tp, by_tp, cols_of, same, same, same,
        rows_of, by_tp, cols_of, same, same, same, seq,
    )
    out_specs = (
        seq, seq, rows_of, by_tp, by_tp, cols_of, same, same, same,
        rows_of, by_tp, cols_of, same, same, same,
    )
    return jax.shard_map(
        per_device, mesh=mesh, in_specs=in_specs, out_specs=out_specs, check_vma=False
    )
```

```python
import functools
import math

import jax
import jax.numpy as jnp
from jax import lax
from jax.experimental import pallas as pl
from jax.experimental.pallas import tpu as pltpu
from jax.sharding import PartitionSpec as P

HD = 64
LOG2E = math.log2(math.e)
NORM_EPS = 1e-12
MASKED = -1e30
THREE = lax.Precision.HIGH


def contract(left, right, left_dim, right_dim):
    return lax.dot_general(
        left,
        right,
        (((left_dim,), (right_dim,)), ((), ())),
        precision=THREE,
        preferred_element_type=jnp.float32,
    )


def ringed(block, axis, distance):
    count = lax.axis_size(axis)
    return lax.ppermute(block, axis, [(i, (i + distance) % count) for i in range(count)])


def swapped(block, axis, bit):
    return lax.ppermute(block, axis, [(i, i ^ bit) for i in range(lax.axis_size(axis))])


def bits_of(axis):
    bits, bit = [], 1
    while bit < lax.axis_size(axis):
        bits.append(bit)
        bit *= 2
    return bits


def quarter_scatter(part, chunks):
    rank = lax.axis_index("tp")
    count, width = part.shape
    block = part.reshape(chunks, 2, 2, count // (4 * chunks), width)
    for bit, axis in ((1, 1), (2, 1)):
        upper = rank // bit % 2
        leaving = lax.dynamic_index_in_dim(block, 1 - upper, axis, keepdims=False)
        staying = lax.dynamic_index_in_dim(block, upper, axis, keepdims=False)
        block = staying + swapped(leaving, "tp", bit)
    return block


def quarter_gather(block):
    rank = lax.axis_index("tp")
    for bit in (2, 1):
        other = swapped(block, "tp", bit)
        upper = rank // bit % 2 == 1
        block = jnp.where(
            upper, jnp.stack([other, block], axis=1), jnp.stack([block, other], axis=1)
        )
    return block.reshape(-1, block.shape[-1])


def small_sum(vector, axes):
    for axis in axes:
        for bit in bits_of(axis):
            vector = vector + swapped(vector, axis, bit)
    return vector


def weight_gather(shard, widths):
    rows = shard.shape[0]
    n_f, n_c = lax.axis_size("fsdp"), lax.axis_size("ctx")
    at_f, at_c = lax.axis_index("fsdp"), lax.axis_index("ctx")
    wholes = [jnp.zeros((n_f * n_c * rows, width), jnp.float32) for width in widths]
    along_f = shard
    for k in range(n_f):
        if k:
            along_f = ringed(along_f, "fsdp", 1)
        along_c = along_f
        for m in range(n_c):
            if m:
                along_c = ringed(along_c, "ctx", 1)
            place = ((at_f - k) % n_f * n_c + (at_c - m) % n_c) * rows
            start = 0
            for i, width in enumerate(widths):
                wholes[i] = lax.dynamic_update_slice(
                    wholes[i], along_c[:, start : start + width], (place, 0)
                )
                start += width
    return wholes


def grad_scatter(pieces):
    n_f, n_c = lax.axis_size("fsdp"), lax.axis_size("ctx")
    at_f, at_c = lax.axis_index("fsdp"), lax.axis_index("ctx")
    rows = pieces[0].shape[0] // (n_f * n_c)

    def piece(f, c):
        start = (f % n_f * n_c + c % n_c) * rows
        cut = [lax.dynamic_slice_in_dim(p, start, rows, 0) for p in pieces]
        return cut[0] if len(cut) == 1 else jnp.concatenate(cut, axis=1)

    total = None
    for k in range(1, n_f + 1):
        over_c = piece(at_f - k, at_c - 1)
        for m in range(2, n_c + 1):
            over_c = ringed(over_c, "ctx", 1) + piece(at_f - k, at_c - m)
        total = over_c if total is None else ringed(total, "fsdp", 1) + over_c
    return total


def normalized(values):
    centred = values - jnp.mean(values, axis=-1, keepdims=True)
    spread = jnp.mean(centred * centred, axis=-1, keepdims=True)
    recip = lax.rsqrt(spread + NORM_EPS)
    return centred * recip, recip


def norm_back(grad, gain, normed, recip):
    scaled = grad * gain
    return recip * (
        scaled
        - jnp.mean(scaled, axis=-1, keepdims=True)
        - normed * jnp.mean(scaled * normed, axis=-1, keepdims=True)
    )


def halves(values):
    high = values.astype(jnp.bfloat16)
    return high, (values - high.astype(jnp.float32)).astype(jnp.bfloat16)


def low_half(shape):
    return lax.broadcasted_iota(jnp.int32, shape, 1) < HD


def dot(left, right, left_dim, right_dim):
    return lax.dot_general(
        left, right, (((left_dim,), (right_dim,)), ((), ())), preferred_element_type=jnp.float32
    )


def doubled(ref, rows, head, scratch, heads):
    for j in range(heads):

        @pl.when(head == j)
        def _():
            piece = ref[rows, j * HD : (j + 1) * HD]
            scratch[...] = jnp.concatenate([piece, piece], axis=1)


def packed(pair, first):
    low = low_half(pair.shape)
    turned = pltpu.roll(pair, HD, 1)
    twice = jnp.where(low, pair, turned) if first else jnp.where(low, turned, pair)
    high, rest = halves(twice)
    return jnp.where(low, high.astype(jnp.float32), rest.astype(jnp.float32)).astype(jnp.bfloat16)


def stacked(half):
    high, rest = halves(half)
    return jnp.concatenate([high, rest], axis=0)


def key_bias(limit, first, count, width):
    place = first + lax.broadcasted_iota(jnp.int32, (count, width), 0)
    return jnp.where(place < limit, 0.0, MASKED)


def row(ref):
    return ref[...].reshape(1, -1)


def forward_kernel(heads, blocks, tile, rows, meta_ref, q_ref, *refs):
    kv_refs, (out_ref, lse_ref, kp, vt, bias, qd, acc) = refs[:blocks], refs[blocks:]
    head, step = pl.program_id(0), pl.program_id(1)
    span = kv_refs[0].shape[0]
    per = span // tile

    @pl.when(step == 0)
    def _():
        for b in range(blocks):

            def prepare(j, _, b=b):
                at = pl.ds(pl.multiple_of(j * tile, tile), tile)
                to = pl.ds(pl.multiple_of(b * span + j * tile, tile), tile)
                pair = kv_refs[b][at, :]
                kp[to, :] = packed(pair, True)
                vt[:, to] = stacked(pair.T[HD:, :])
                bias[to, :] = key_bias(meta_ref[0], meta_ref[1 + b] + j * tile, tile, 128)
                return 0

            lax.fori_loop(0, per, prepare, 0)

    here = pl.ds(pl.multiple_of(step * rows, rows), rows)
    doubled(q_ref, here, head, qd, heads)
    q_high, q_low = halves(qd[...] * (LOG2E * HD**-0.5))
    q_four = jnp.concatenate([q_high, q_low], axis=1)
    acc[...] = jnp.zeros_like(acc)

    def key_tile(j, carry):
        top, total = carry
        at = pl.ds(pl.multiple_of(j * tile, tile), tile)
        k_two = kp[at, :]
        scores = dot(jnp.concatenate([k_two, k_two], axis=1), q_four, 1, 1)
        scores = scores + jnp.concatenate([bias[at, :]] * (rows // 128), axis=1)
        new_top = jnp.maximum(top, jnp.max(scores, axis=0, keepdims=True))
        fade = jnp.exp2(top - new_top)
        probs = jnp.exp2(scores - new_top)
        total = total * fade + jnp.sum(probs, axis=0, keepdims=True)
        high, low = halves(probs)
        v_two = vt[:, at]
        acc[...] = acc[...] * fade + (dot(v_two, high, 1, 0) + dot(v_two, low, 1, 0))
        return new_top, total

    top, total = lax.fori_loop(
        0,
        blocks * per,
        key_tile,
        (jnp.full((1, rows), MASKED, jnp.float32), jnp.zeros((1, rows), jnp.float32)),
    )
    result = acc[:HD, :] + acc[HD:, :]
    result = (result / total).T
    for j in range(heads):

        @pl.when(head == j)
        def _():
            out_ref[here, j * HD : (j + 1) * HD] = result
            lse_ref[j : j + 1, here] = top + jnp.log2(total)


def attention(queries, kv_blocks, meta, heads, rows=256, tile=512):
    count, span, blocks = queries.shape[0], kv_blocks[0].shape[0], len(kv_blocks)
    keys = span * blocks
    whole = lambda h, i, m: (0, 0)
    return pl.pallas_call(
        functools.partial(forward_kernel, heads, blocks, tile, rows),
        grid_spec=pltpu.PrefetchScalarGridSpec(
            num_scalar_prefetch=1,
            grid=(heads, count // rows),
            in_specs=[pl.BlockSpec((count, heads * HD), whole)]
            + [pl.BlockSpec((span, 2 * HD), lambda h, i, m: (0, h))] * blocks,
            out_specs=[
                pl.BlockSpec((count, heads * HD), whole),
                pl.BlockSpec((heads, count), whole),
            ],
            scratch_shapes=[
                pltpu.VMEM((keys, 2 * HD), jnp.bfloat16),
                pltpu.VMEM((2 * HD, keys), jnp.bfloat16),
                pltpu.VMEM((keys, 128), jnp.float32),
                pltpu.VMEM((rows, 2 * HD), jnp.float32),
                pltpu.VMEM((2 * HD, rows), jnp.float32),
            ],
        ),
        out_shape=[
            jax.ShapeDtypeStruct((count, heads * HD), jnp.float32),
            jax.ShapeDtypeStruct((heads, count), jnp.float32),
        ],
        compiler_params=pltpu.CompilerParams(dimension_semantics=("arbitrary", "arbitrary")),
        cost_estimate=pl.CostEstimate(
            flops=24 * heads * count * keys * HD,
            bytes_accessed=8 * keys * heads * HD + 8 * count * heads * HD,
            transcendentals=heads * count * keys,
        ),
        name="attention_forward",
    )(meta, queries, *kv_blocks)


def backward_kernel(
    heads, blocks, n_f, tile, rows, meta_ref, q_ref, do_ref, out_ref, lse_ref, up_g, outs,
    *refs,
):
    kv_refs = refs[:blocks]
    dq_ref, dkv_ref, up_out, kv_far, outs_all = refs[blocks : blocks + 5]
    (
        kp, vp, kt, bias, qd, dd, od, dk, dv, acc, stage, q_all, do_all, q_mix, do_mix, delta_all
    ) = refs[blocks + 5 : blocks + 21]
    transfers = Transfers(
        blocks, n_f, heads, up_g, outs, up_out, kv_far, outs_all, stage,
        *refs[blocks + 21 :],
    )
    head, order, step = pl.program_id(0), pl.program_id(1), pl.program_id(2)
    steps = pl.num_programs(2)
    now = (head * blocks + order) * steps + step
    transfers.run(now, before=True)
    span = kv_refs[0].shape[0]
    per = span // tile

    @pl.when(step == 0)
    def _():
        dk[...] = jnp.zeros_like(dk)
        dv[...] = jnp.zeros_like(dv)
        for b in range(blocks):

            @pl.when((order + 1) % blocks == b)
            def _(b=b):
                def prepare(j, _):
                    at = pl.ds(pl.multiple_of(j * tile, tile), tile)
                    pair = kv_refs[b][at, :]
                    kp[at, :] = packed(pair, True)
                    vp[at, :] = packed(pair, False)
                    kt[:, at] = stacked(pair.T[:HD, :])
                    bias[at, :] = key_bias(
                        meta_ref[0], transfers.at_c(b) * span + j * tile, tile, 128
                    )
                    return 0

                lax.fori_loop(0, per, prepare, 0)

    here = pl.ds(pl.multiple_of(step * rows, rows), rows)

    @pl.when(order == 0)
    def _():
        doubled(q_ref, here, head, qd, heads)
        doubled(do_ref, here, head, dd, heads)
        doubled(out_ref, here, head, od, heads)
        low = low_half((rows, 2 * HD))
        for value, four, mix in (
            (qd[...] * (LOG2E * HD**-0.5), q_all, q_mix),
            (dd[...], do_all, do_mix),
        ):
            high, rest = halves(value)
            four[here, : 2 * HD] = high
            four[here, 2 * HD :] = rest
            mixed = jnp.where(low, high.astype(jnp.float32), rest.astype(jnp.float32))
            mix[here, :] = mixed.astype(jnp.bfloat16)
        delta_all[:, here] = jnp.sum((dd[...] * od[...]).T[:HD, :], axis=0, keepdims=True)
        acc[:, here] = jnp.zeros((2 * HD, rows), jnp.float32)

    q_four, q_two, do_four, do_two = q_all[here, :], q_mix[here, :], do_all[here, :], do_mix[here, :]
    delta = delta_all[:, here]
    lse = lse_ref[0:1, here]
    for j in range(1, heads):
        lse = jnp.where(head == j, lse_ref[j : j + 1, here], lse)
    def key_tile(j, _):
        at = pl.ds(pl.multiple_of(j * tile, tile), tile)
        k_two, v_two = kp[at, :], vp[at, :]
        scores = dot(jnp.concatenate([k_two, k_two], axis=1), q_four, 1, 1)
        scores = scores + jnp.concatenate([bias[at, :]] * (rows // 128), axis=1)
        probs = jnp.exp2(scores - lse)
        high, rest = halves(probs)
        dv[at, :] += dot(high, do_two, 1, 0) + dot(rest, do_two, 1, 0)
        grad_p = dot(jnp.concatenate([v_two, v_two], axis=1), do_four, 1, 1)
        grad_s = probs * (grad_p - delta)
        high, rest = halves(grad_s)
        dk[at, :] += dot(high, q_two, 1, 0) + dot(rest, q_two, 1, 0)
        k_t = kt[:, at]
        acc[:, here] += dot(k_t, high, 1, 0) + dot(k_t, rest, 1, 0)
        return 0

    lax.fori_loop(0, per, key_tile, 0)

    @pl.when(order == blocks - 1)
    def _():
        result = ((acc[:HD, here] + acc[HD:, here]) * HD**-0.5).T
        for j in range(heads):

            @pl.when(head == j)
            def _(j=j):
                dq_ref[here, j * HD : (j + 1) * HD] = result

    def turned(at):
        grad_k, grad_v = dk[at, :], dv[at, :]
        grad_k = (grad_k + pltpu.roll(grad_k, HD, 1)) * (1.0 / LOG2E)
        grad_v = grad_v + pltpu.roll(grad_v, HD, 1)
        return jnp.where(low_half(grad_k.shape), grad_k, grad_v)

    for b in range(1, blocks):

        @pl.when((step == steps - 1) & (order == b - 1))
        def _(b=b):
            @pl.when(head >= 2)
            def _():
                transfers.kv_copy(head - 2, b).wait_send()

            def far(j, _):
                at = pl.ds(pl.multiple_of(j * tile, tile), tile)
                stage[head % 2, b - 1, at, :] = turned(at)
                return 0

            lax.fori_loop(0, per, far, 0)
            transfers.kv_copy(head, b).start()

    @pl.when((step == steps - 1) & (order == blocks - 1))
    def _():
        def keep(j, _):
            at = pl.ds(pl.multiple_of(j * tile, tile), tile)
            dkv_ref[at, :] = turned(at)
            return 0

        lax.fori_loop(0, per, keep, 0)

    transfers.run(now, before=False)


def remote(src, dst, send, recv, **peer):
    return pltpu.make_async_remote_copy(
        src_ref=src,
        dst_ref=dst,
        send_sem=send,
        recv_sem=recv,
        device_id=peer,
        device_id_type=pl.DeviceIdType.MESH,
    )


class Ring:
    def __init__(self, n_f, n_c, pick, side_rx, hop_rx, side_sem, hop_sem, emit):
        self.n_f, self.n_c, self.pick, self.emit = n_f, n_c, pick, emit
        self.side_rx, self.hop_rx, self.side_sem, self.hop_sem = side_rx, hop_rx, side_sem, hop_sem
        self.next_f = (lax.axis_index("fsdp") + 1) % n_f
        self.next_c = (lax.axis_index("ctx") + 1) % n_c

    def side(self, k, m):
        return remote(
            self.pick(k, 1) if m == 1 else self.side_rx.at[k - 1, m - 2],
            self.side_rx.at[k - 1, m - 1],
            self.side_sem.at[0, k - 1, m - 1],
            self.side_sem.at[1, k - 1, m - 1],
            ctx=self.next_c,
        )

    def hop(self, k):
        src = self.side_rx.at[0, self.n_c - 2] if k == 1 else self.hop_rx.at[k - 2]
        sem = self.hop_sem
        return remote(
            src, self.hop_rx.at[k - 1], sem.at[0, k - 1], sem.at[1, k - 1], fsdp=self.next_f
        )

    def begin(self):
        for k in range(1, self.n_f + 1):
            self.side(k, 1).start()

    def event(self, k):
        for m in range(2, self.n_c + 1):
            self.side(k, m - 1).wait()
            self.side_rx[k - 1, m - 2] += self.pick(k, m)[...]
            if m < self.n_c:
                self.side(k, m).start()
        if k > 1:
            self.hop(k - 1).wait()
            result = self.hop_rx[k - 2] + self.side_rx[k - 1, self.n_c - 2]
            if k < self.n_f:
                self.hop_rx[k - 2] = result
            else:
                self.emit(result)
        if k < self.n_f:
            self.hop(k).start()


def ring_scratch(n_f, n_c, own, wide):
    sem = pltpu.SemaphoreType.DMA
    return [
        pltpu.VMEM((n_f, n_c - 1, own, wide), jnp.float32),
        pltpu.VMEM((n_f - 1, own, wide), jnp.float32),
        sem((2, n_f, n_c - 1)),
        sem((2, n_f - 1)),
    ]


def row_block(ref, own, n_f, n_c):
    f, c = lax.axis_index("fsdp"), lax.axis_index("ctx")

    def pick(k, m):
        at = (f + (n_f - k)) % n_f * n_c + (c + (n_c - m)) % n_c
        return ref.at[pl.ds(pl.multiple_of(at * own, own), own)]

    return pick


def keeper(target):
    def emit(value):
        target[...] = value

    return emit


class Transfers:
    def __init__(
        self, n_c, n_f, heads, up_g, outs, up_out, kv_far, outs_all, stage,
        side_rx, hop_rx, side_sem, hop_sem, kv_sem, out_sem,
    ):
        self.n_c, self.n_f, self.heads = n_c, n_f, heads
        self.outs, self.kv_far, self.outs_all = outs, kv_far, outs_all
        self.stage = stage
        self.kv_sem = kv_sem
        self.out_sem = out_sem
        self.f, self.c, me = lax.axis_index("fsdp"), lax.axis_index("ctx"), lax.axis_index("tp")
        self.bit0, self.bit1 = me % 2, me // 2 % 2
        self.peer0, self.peer1 = me + 1 - 2 * self.bit0, me + 2 - 4 * self.bit1
        self.ring = Ring(
            n_f, n_c, lambda k, m: up_g.at[self.at_f(k), self.at_c(m)],
            side_rx, hop_rx, side_sem, hop_sem, keeper(up_out),
        )

    def at_f(self, k):
        return (self.f + (self.n_f - k)) % self.n_f

    def at_c(self, m):
        return (self.c + (self.n_c - m)) % self.n_c

    def kv_copy(self, head, m):
        lanes = pl.ds(pl.multiple_of(head * 2 * HD, 2 * HD), 2 * HD)
        return remote(
            self.stage.at[head % 2, m - 1],
            self.kv_far.at[m - 1, :, lanes],
            self.kv_sem.at[0, head, m - 1],
            self.kv_sem.at[1, head, m - 1],
            ctx=self.at_c(m),
        )

    def out_local(self):
        return pltpu.make_async_copy(
            self.outs, self.outs_all.at[:, self.bit0, self.bit1], self.out_sem.at[0, 2]
        )

    def out_far(self):
        return remote(
            self.outs,
            self.outs_all.at[:, self.bit0, self.bit1],
            self.out_sem.at[0, 0],
            self.out_sem.at[1, 0],
            tp=self.peer1,
        )

    def out_near(self):
        pair = self.outs_all.at[:, self.bit0]
        return remote(pair, pair, self.out_sem.at[0, 1], self.out_sem.at[1, 1], tp=self.peer0)

    def begin(self):
        barrier = pltpu.get_barrier_semaphore()
        peers = [{"tp": self.peer0}, {"tp": self.peer1}, {"fsdp": self.at_f(-1)}]
        if self.n_f > 2:
            peers.append({"fsdp": self.at_f(1)})
        peers += [{"ctx": self.at_c(m)} for m in range(1, self.n_c)]
        for peer in peers:
            pl.semaphore_signal(
                barrier, inc=1, device_id=peer, device_id_type=pl.DeviceIdType.MESH
            )
        pl.semaphore_wait(barrier, len(peers))
        self.ring.begin()
        self.out_local().start()
        self.out_far().start()

    def out_event(self):
        self.out_local().wait()
        self.out_far().wait()
        self.out_near().start()

    def end(self):
        self.out_near().wait()
        for head in range(self.heads):
            for m in range(1, self.n_c):
                if head >= self.heads - 2:
                    self.kv_copy(head, m).wait_send()
                self.kv_copy(head, m).wait_recv()

    def run(self, now, before):
        count = self.heads * self.n_c * STEPS_PER_HEAD
        plan = []
        for k in range(1, self.n_f + 1):
            plan.append((0.85 * k / self.n_f, lambda k=k: self.ring.event(k)))
        plan.append((0.45, self.out_event))
        plan.sort(key=lambda item: item[0])
        late = [self.end]
        if before:

            @pl.when(now == 0)
            def _():
                self.begin()

            return
        for at in range(count):
            todo = [f for p, f in plan if min(int(p * count), count - 1) == at]
            if at == count - 1:
                todo = todo + late
            if todo:

                @pl.when(now == at)
                def _(todo=todo):
                    for f in todo:
                        f()


STEPS_PER_HEAD = 4


def attention_back(
    queries, grads, result, lse, kv_blocks, meta, heads, up_g, outs, tile=512
):
    rows = queries.shape[0] // STEPS_PER_HEAD
    n_f, n_c, own, wide_up = up_g.shape
    count, span, blocks = queries.shape[0], kv_blocks[0].shape[0], len(kv_blocks)
    keys = span * blocks
    whole = lambda h, b, i, m: (0, 0)
    wide = pl.BlockSpec((count, heads * HD), whole)
    kv_spec = pl.BlockSpec((span, 2 * HD), lambda h, b, i, m: (0, h))
    anywhere = pl.BlockSpec(memory_space=pl.ANY)
    sem, shape = pltpu.SemaphoreType.DMA, jax.ShapeDtypeStruct

    def held(array):
        return pl.BlockSpec(array.shape, lambda h, b, i, m: (0,) * array.ndim)

    return pl.pallas_call(
        functools.partial(backward_kernel, heads, blocks, n_f, tile, rows),
        grid_spec=pltpu.PrefetchScalarGridSpec(
            num_scalar_prefetch=1,
            grid=(heads, blocks, count // rows),
            in_specs=[wide] * 3
            + [pl.BlockSpec((heads, count), whole)]
            + [held(up_g), held(outs)]
            + [kv_spec] * blocks,
            out_specs=[
                wide,
                kv_spec,
                pl.BlockSpec((own, wide_up), whole),
                anywhere,
                anywhere,
            ],
            scratch_shapes=[
                pltpu.VMEM((span, 2 * HD), jnp.bfloat16),
                pltpu.VMEM((span, 2 * HD), jnp.bfloat16),
                pltpu.VMEM((2 * HD, span), jnp.bfloat16),
                pltpu.VMEM((span, 128), jnp.float32),
                pltpu.VMEM((rows, 2 * HD), jnp.float32),
                pltpu.VMEM((rows, 2 * HD), jnp.float32),
                pltpu.VMEM((rows, 2 * HD), jnp.float32),
                pltpu.VMEM((span, 2 * HD), jnp.float32),
                pltpu.VMEM((span, 2 * HD), jnp.float32),
                pltpu.VMEM((2 * HD, count), jnp.float32),
                pltpu.VMEM((2, n_c - 1, span, 2 * HD), jnp.float32),
                pltpu.VMEM((count, 4 * HD), jnp.bfloat16),
                pltpu.VMEM((count, 4 * HD), jnp.bfloat16),
                pltpu.VMEM((count, 2 * HD), jnp.bfloat16),
                pltpu.VMEM((count, 2 * HD), jnp.bfloat16),
                pltpu.VMEM((1, count), jnp.float32),
                *ring_scratch(n_f, n_c, own, wide_up),
                sem((2, heads, n_c - 1)),
                sem((2, 3)),
            ],
        ),
        out_shape=[
            shape((count, heads * HD), jnp.float32),
            shape((span, 2 * heads * HD), jnp.float32),
            shape((own, wide_up), jnp.float32),
            shape((n_c - 1, span, 2 * heads * HD), jnp.float32),
            shape((outs.shape[0], 2, 2) + outs.shape[1:], jnp.float32),
        ],
        compiler_params=pltpu.CompilerParams(
            dimension_semantics=("arbitrary",) * 3,
            collective_id=2,
            has_side_effects=True,
            vmem_limit_bytes=62 << 20,
        ),
        cost_estimate=pl.CostEstimate(
            flops=60 * heads * count * keys * HD,
            bytes_accessed=16 * keys * heads * HD + 16 * count * heads * HD,
            transcendentals=heads * count * keys,
        ),
        name="attention_backward",
    )(meta, queries, grads, result, lse, up_g, outs, *kv_blocks)


def dot_three(left, right, left_dim, right_dim):
    left_high, left_low = left
    right_high, right_low = right
    return dot(left_high, right_high, left_dim, right_dim) + (
        dot(left_high, right_low, left_dim, right_dim)
        + dot(left_low, right_high, left_dim, right_dim)
    )


def tiles_of(count, body):
    tile = 256 if count % 256 == 0 else count

    def step(n, _):
        body(pl.ds(pl.multiple_of(n * tile, tile), tile))
        return 0

    lax.fori_loop(0, count // tile, step, 0)


def middle_kernel(
    chunks, rows, n_c,
    att_ref, weights, outw_ref,
    b_out_1, gain_1_1, shift_1_1, b_up_1, b_down_1, gain_2_1, shift_2_1, tok_hbm, cot_hbm,
    out_own, mid_own, gatt, d_up, d_out, d_down_out, vec, d_bup,
    part, rx0, rx1, full, act_hi, act_lo, slope, tok, cot, norm_1, recip_1,
    up_s, down_s, outw_s, xs, ys, ts, send0, recv0, send1, recv1, own_sem,
    lines, b_up, *blocked,
):
    half, quarter = rows // 2, rows // 4
    me = lax.axis_index("tp")
    bit0, bit1 = me % 2, me // 2 % 2
    peer0, peer1 = me + 1 - 2 * bit0, me + 2 - 4 * bit1
    home0 = pl.multiple_of(bit0 * half, half)
    away0 = pl.multiple_of((1 - bit0) * half, half)
    mine = pl.multiple_of(home0 + bit1 * quarter, quarter)
    away1 = pl.multiple_of(home0 + (1 - bit1) * quarter, quarter)
    own = pl.ds(mine, quarter)

    def remote_tp(src, dst, send, recv, peer):
        return remote(src, dst, send, recv, tp=peer)

    width, hidden = up_s.shape[1], up_s.shape[2]
    d_down = d_down_out
    if blocked:
        whole, w_sem, wl_sem, d_down, *ring_refs = blocked
        n_f, own_w = weights.shape[0], weights.shape[1]
        at = lax.axis_index("ctx")
        ring = Ring(
            n_f, n_c, row_block(d_down, own_w, n_f, n_c), *ring_refs, keeper(d_down_out)
        )

        def columns_of(part_at):
            return pl.ds(part_at * hidden, hidden)

        def w_copies(part_at):
            cols = columns_of(part_at)
            for k in range(n_f):
                yield pltpu.make_async_copy(
                    weights.at[k, :, cols], whole.at[k, at, :, cols], wl_sem.at[part_at, k]
                )
                for m in range(1, n_c):
                    yield remote(
                        weights.at[k, :, cols],
                        whole.at[k, at, :, cols],
                        w_sem.at[0, part_at, k, m - 1],
                        w_sem.at[1, part_at, k, m - 1],
                        ctx=(at + m) % n_c,
                    )

    def scatter0(s, c):
        return remote_tp(
            part.at[c, pl.ds(away0, half)], rx0.at[s, c], send0.at[0, s, c], recv0.at[0, s, c], peer0
        )

    def scatter1(s, c):
        return remote_tp(
            part.at[c, pl.ds(away1, quarter)],
            rx1.at[s, c],
            send1.at[0, s, c],
            recv1.at[0, s, c],
            peer1,
        )

    def gather1(s, c):
        return remote_tp(
            full.at[s, c, own], full.at[s, c, own], send1.at[1, s, c], recv1.at[1, s, c], peer1
        )

    def gather0(s, c):
        place = pl.ds(home0, half)
        return remote_tp(
            full.at[s, c, place], full.at[s, c, place], send0.at[1, s, c], recv0.at[1, s, c], peer0
        )

    def own_copies(c):
        where = pl.ds(pl.multiple_of(c * rows + mine, quarter), quarter)
        return (
            pltpu.make_async_copy(tok_hbm.at[where], tok.at[c], own_sem.at[0, c]),
            pltpu.make_async_copy(cot_hbm.at[where], cot.at[c], own_sem.at[1, c]),
        )

    for c in range(chunks):
        for copy in own_copies(c):
            copy.start()
    barrier = pltpu.get_barrier_semaphore()
    peers = [{"tp": peer0}, {"tp": peer1}]
    if blocked:
        peers += [{"ctx": (at + m) % n_c} for m in range(1, n_c)]
        at_f = lax.axis_index("fsdp")
        peers += [{"fsdp": (at_f + k) % n_f} for k in sorted({1, n_f - 1})]
    for peer in peers:
        pl.semaphore_signal(barrier, inc=1, device_id=peer, device_id_type=pl.DeviceIdType.MESH)

    firsts = (b_out_1, gain_1_1, shift_1_1, b_down_1, gain_2_1, shift_2_1)
    for i, vector in enumerate(firsts):
        lines[i : i + 1, :] = row(vector)
    b_up[...] = row(b_up_1)
    b_out, gain_1, shift_1, b_down, gain_2, shift_2 = (
        lines.at[i : i + 1] for i in range(len(firsts))
    )

    def split_rows(source, target):
        count = source.shape[0]
        step = 128

        def one(i, _):
            at = pl.ds(pl.multiple_of(i * step, step), step)
            target[0, at, :], target[1, at, :] = halves(source[at, :])
            return 0

        lax.fori_loop(0, count // step, one, 0)

    split_rows(outw_ref, outw_s)

    def weights_ready(part_at, target):
        if not blocked:
            split_rows(weights[part_at], target)
            return
        for copy in w_copies(part_at):
            copy.wait()

        def one(j, _):
            to = pl.ds(pl.multiple_of(j * own_w, own_w), own_w)
            piece = whole[j // n_c, j % n_c, :, columns_of(part_at)]
            target[0, to, :], target[1, to, :] = halves(piece)
            return 0

        lax.fori_loop(0, n_f * n_c, one, 0)

    d_bup[...] = jnp.zeros_like(d_bup)
    vec[...] = jnp.zeros_like(vec)
    d_up[...] = jnp.zeros_like(d_up)
    d_down[...] = jnp.zeros_like(d_down)
    d_out[...] = jnp.zeros_like(d_out)
    for c in range(chunks):
        for copy in own_copies(c):
            copy.wait()
    pl.semaphore_wait(barrier, len(peers))
    if blocked:
        for part_at in range(2):
            for copy in w_copies(part_at):
                copy.start()

    def split_into(target, value):
        target[0], target[1] = halves(value)

    def finish0(s, c):
        scatter0(s, c).wait()
        away = pl.ds(away1 - home0, quarter)
        part[c, pl.ds(away1, quarter), :] += rx0[s, c, away, :]
        scatter1(s, c).start()
        stay = pl.ds(mine - home0, quarter)
        part[c, own, :] += rx0[s, c, stay, :]

    def finish1(s, c):
        scatter1(s, c).wait()
        return part[c, own, :] + rx1[s, c]

    def forward1(s, c):
        gather1(s, c).wait()
        gather0(s, c).start()

    def trailing(c, now, before):
        if before is not None:

            @pl.when(c == 0)
            def _():
                before(chunks - 1)

        if now is not None:

            @pl.when(c > 0)
            def _():
                now(c - 1)

    def stage(body):
        def one(c, _):
            body(c)
            return 0

        lax.fori_loop(0, chunks, one, 0)

    def at_rows(c):
        return pl.ds(pl.multiple_of(c * rows, rows), rows)

    def attention_out(c):
        left = halves(att_ref[at_rows(c), :])

        def columns(n):
            part[c, :, n] = dot_three(left, (outw_s[0, n, :], outw_s[1, n, :]), 1, 1)

        tiles_of(width, columns)
        scatter0(0, c).start()
        trailing(c, functools.partial(finish0, 0), None)

    stage(attention_out)

    def first_norm(c):
        trailing(c, None, functools.partial(finish0, 0))
        resid = finish1(0, c) + tok[c] + b_out[...]
        n_1, r_1 = normalized(resid)
        norm_1[c] = n_1
        recip_1[c] = jnp.broadcast_to(r_1, recip_1.shape[1:])
        full[0, c, own, :] = n_1 * gain_1[...] + shift_1[...]
        gather1(0, c).start()
        trailing(c, functools.partial(forward1, 0), None)

    stage(first_norm)

    def feed_forward(c):
        gather0(0, c).wait()
        split_into(xs, full[0, c])

        def columns(n):
            pre = dot_three((xs[0], xs[1]), (up_s[0, :, n], up_s[1, :, n]), 1, 0) + b_up[:, n]
            cdf = 0.5 + 0.5 * lax.erf(pre * math.sqrt(0.5))
            slope[c, :, n] = cdf + pre * (
                jnp.exp(-0.5 * pre * pre) * (1.0 / math.sqrt(2.0 * math.pi))
            )
            act_hi[c, :, n], act_lo[c, :, n] = halves(pre * cdf)

        tiles_of(hidden, columns)

        @pl.when(c == 0)
        def _():
            weights_ready(1, down_s)

        def back(n):
            part[c, :, n] = dot_three(
                (act_hi[c], act_lo[c]), (down_s[0, n, :], down_s[1, n, :]), 1, 1
            )

        tiles_of(width, back)
        scatter0(1, c).start()
        trailing(c, functools.partial(finish0, 1), functools.partial(forward1, 0))

    def second_norm(c):
        trailing(c, None, functools.partial(finish0, 1))
        ffn = finish1(1, c) + full[0, c, own, :] + b_down[...]
        n_2, r_2 = normalized(ffn)
        out_own[c] = n_2 * gain_2[...] + shift_2[...]
        grad = cot[c]
        second = norm_back(grad, gain_2[...], n_2, r_2)
        full[1, c, own, :] = second
        gather1(1, c).start()
        vec[3:4, :] += jnp.sum(second, axis=0, keepdims=True)
        vec[4:5, :] += jnp.sum(grad * n_2, axis=0, keepdims=True)
        vec[5:6, :] += jnp.sum(grad, axis=0, keepdims=True)
        trailing(c, functools.partial(forward1, 1), None)

    def feed_back(c):
        gather0(1, c).wait()
        split_into(xs, full[1, c])

        def columns(n):
            grad = dot_three((xs[0], xs[1]), (down_s[0, :, n], down_s[1, :, n]), 1, 0)
            grad = grad * slope[c, :, n]
            slope[c, :, n] = grad
            ys[0, :, n], ys[1, :, n] = halves(grad)
            d_bup[:, n] += jnp.sum(grad, axis=0, keepdims=True)

        tiles_of(hidden, columns)

        def back(n):
            part[c, :, n] = dot_three((ys[0], ys[1]), (up_s[0, n, :], up_s[1, n, :]), 1, 1)

        tiles_of(width, back)
        scatter0(2, c).start()
        trailing(c, functools.partial(finish0, 2), functools.partial(forward1, 1))
        split_into(ts, full[1, c].T)

        def down_columns(n):
            d_down[:, n] += dot_three((ts[0], ts[1]), (act_hi[c, :, n], act_lo[c, :, n]), 1, 0)

        tiles_of(hidden, down_columns)

    def ring_step(slot):
        if blocked:
            for k in range(1, n_f + 1):

                @pl.when(slot == 2 * chunks * k // n_f - 1)
                def _(k=k):
                    ring.event(k)

    def middle_norm(c):
        trailing(c, None, functools.partial(finish0, 2))
        first = finish1(2, c) + full[1, c, own, :]
        n_1 = norm_1[c]
        mid = norm_back(first, gain_1[...], n_1, recip_1[c, :, :1])
        mid_own[c] = mid
        full[2, c, own, :] = mid
        gather1(2, c).start()
        vec[0:1, :] += jnp.sum(mid, axis=0, keepdims=True)
        vec[1:2, :] += jnp.sum(first * n_1, axis=0, keepdims=True)
        vec[2:3, :] += jnp.sum(first, axis=0, keepdims=True)
        trailing(c, functools.partial(forward1, 2), None)
        ring_step(c)

    def last(c):
        gather0(2, c).wait()
        mid = full[2, c]
        gatt[at_rows(c), :] = dot_three(halves(mid), (outw_s[0], outw_s[1]), 1, 0)
        trailing(c, None, functools.partial(forward1, 2))
        split_into(ts, mid.T)
        d_out[...] += dot_three((ts[0], ts[1]), halves(att_ref[at_rows(c), :]), 1, 0)
        split_into(ts, full[0, c].T)

        def columns(n):
            d_up[:, n] += dot_three((ts[0], ts[1]), halves(slope[c, :, n]), 1, 0)

        tiles_of(hidden, columns)
        ring_step(chunks + c)

    weights_ready(0, up_s)
    stage(feed_forward)
    stage(second_norm)
    stage(feed_back)
    if blocked:
        ring.begin()
    stage(middle_norm)
    stage(last)


def middle_whole(chunks, rows, n_c, att, up, down, *refs):
    middle_kernel(chunks, rows, n_c, att, (up, down), *refs)


def middle(attended, weights, wide_out_t, vectors, tokens, cot, hidden, n_c, chunks=4):
    blocked = not isinstance(weights, tuple)
    count, width = tokens.shape
    split_at = attended.shape[1]
    rows = count // chunks
    half, quarter = rows // 2, rows // 4
    vmem = pl.BlockSpec(memory_space=pltpu.VMEM)
    anywhere = pl.BlockSpec(memory_space=pl.ANY)
    f32, bf16 = jnp.float32, jnp.bfloat16
    sems = pltpu.SemaphoreType.DMA((2, 3, chunks))
    extra = [pltpu.VMEM((8, width), f32), pltpu.VMEM((1, hidden), f32)]
    if blocked:
        n_f, own = weights.shape[0], weights.shape[1]
        extra += [
            pltpu.VMEM((n_f, n_c, own, 2 * hidden), f32),
            pltpu.SemaphoreType.DMA((2, 2, n_f, n_c - 1)),
            pltpu.SemaphoreType.DMA((2, n_f)),
            pltpu.VMEM((width, hidden), f32),
            *ring_scratch(n_f, n_c, own, hidden),
        ]
    shape = jax.ShapeDtypeStruct
    return pl.pallas_call(
        functools.partial(middle_kernel if blocked else middle_whole, chunks, rows, n_c),
        in_specs=[vmem]
        + ([anywhere] if blocked else [vmem] * 2)
        + [vmem] * 8
        + [anywhere] * 2,
        out_specs=[vmem] * 8,
        out_shape=[
            shape((chunks, quarter, width), f32),
            shape((chunks, quarter, width), f32),
            shape((count, split_at), f32),
            shape((width, hidden), f32),
            shape((width, split_at), f32),
            shape((own if blocked else width, hidden), f32),
            shape((8, width), f32),
            shape((1, hidden), f32),
        ],
        scratch_shapes=[
            pltpu.VMEM((chunks, rows, width), f32),
            pltpu.VMEM((3, chunks, half, width), f32),
            pltpu.VMEM((3, chunks, quarter, width), f32),
            pltpu.VMEM((3, chunks, rows, width), f32),
            pltpu.VMEM((chunks, rows, hidden), bf16),
            pltpu.VMEM((chunks, rows, hidden), bf16),
            pltpu.VMEM((chunks, rows, hidden), f32),
            pltpu.VMEM((chunks, quarter, width), f32),
            pltpu.VMEM((chunks, quarter, width), f32),
            pltpu.VMEM((chunks, quarter, width), f32),
            pltpu.VMEM((chunks, quarter, 128), f32),
            pltpu.VMEM((2, width, hidden), bf16),
            pltpu.VMEM((2, width, hidden), bf16),
            pltpu.VMEM((2, width, split_at), bf16),
            pltpu.VMEM((2, rows, width), bf16),
            pltpu.VMEM((2, rows, hidden), bf16),
            pltpu.VMEM((2, width, rows), bf16),
            sems, sems, sems, sems,
            pltpu.SemaphoreType.DMA((2, chunks)),
            *extra,
        ],
        compiler_params=pltpu.CompilerParams(
            collective_id=1, has_side_effects=True, vmem_limit_bytes=62 << 20
        ),
        cost_estimate=pl.CostEstimate(
            flops=6 * count * width * (6 * hidden + 3 * split_at),
            bytes_accessed=4 * width * (5 * hidden + 3 * split_at),
            transcendentals=2 * count * hidden,
        ),
        name="middle",
    )(
        attended,
        *([weights] if blocked else weights),
        wide_out_t,
        *vectors,
        tokens,
        cot,
    )


def front_kernel(
    heads, n_c, n_f, tile, rows, meta_ref, tok, w_qkv, up, down_t, outw_t, b_q, b_v,
    att, lse, q_out, kv_out, kv_far, wide, up_down, out_all,
    shard, q_s, kv_s, kv_t, wv, w_s, ud_own, ow_own, kp, vt, bias, qd, acc, top_s, total_s,
    hop_sem, side_sem, ud_sem, ow_sem, ow_side_sem, kv_sem, local_sem,
):
    block, head, step = pl.program_id(0), pl.program_id(1), pl.program_id(2)
    n_q = pl.num_programs(2)
    span, hidden, split_at = tok.shape[0], up.shape[1], heads * HD
    own = shard.shape[0]
    f, c = lax.axis_index("fsdp"), lax.axis_index("ctx")

    def at_f(k):
        return (f + (n_f - k)) % n_f

    def at_c(m):
        return (c + (n_c - m)) % n_c

    def lanes(h):
        return pl.ds(pl.multiple_of(h * 2 * HD, 2 * HD), 2 * HD)

    columns = (pl.ds(0, 2 * split_at), pl.ds(2 * split_at, split_at))

    def hop(p, k):
        to = wv.at[at_f(k - 1), c, :, columns[p]]
        src = shard.at[:, columns[p]] if k == 1 else to
        return remote(
            src, to, hop_sem.at[0, p, k - 1], hop_sem.at[1, p, k - 1], fsdp=at_f(-1)
        )

    def side(p, k, m):
        to = wv.at[at_f(k), c, :, columns[p]]
        src = shard.at[:, columns[p]] if k == 0 else to
        return remote(
            src, to, side_sem.at[0, p, k, m - 1], side_sem.at[1, p, k, m - 1], ctx=at_c(-m)
        )

    def ud_hop(k):
        src = ud_own if k == 1 else up_down.at[at_f(k - 1)]
        return remote(
            src, up_down.at[at_f(k - 1)], ud_sem.at[0, k - 1], ud_sem.at[1, k - 1], fsdp=at_f(-1)
        )

    def ow_hop(k):
        src = ow_own if k == 1 else out_all.at[at_f(k - 1), c]
        return remote(
            src, out_all.at[at_f(k - 1), c], ow_sem.at[0, k - 1], ow_sem.at[1, k - 1], fsdp=at_f(-1)
        )

    def ow_side(k, m):
        src = ow_own if k == 0 else out_all.at[at_f(k), c]
        return remote(
            src,
            out_all.at[at_f(k), c],
            ow_side_sem.at[0, k, m - 1],
            ow_side_sem.at[1, k, m - 1],
            ctx=at_c(-m),
        )

    def kv_send(h, m):
        return remote(
            kv_s.at[:, lanes(h)],
            kv_far.at[m - 1, :, lanes(h)],
            kv_sem.at[0, h, m - 1],
            kv_sem.at[1, h, m - 1],
            ctx=at_c(-m),
        )

    def locals_of():
        return [
            pltpu.make_async_copy(a, b, local_sem.at[i])
            for i, (a, b) in enumerate(
                (
                    (ud_own, up_down.at[f]),
                    (ow_own, out_all.at[f, c]),
                    (wv, wide),
                    (q_s, q_out),
                    (kv_s, kv_out),
                )
            )
        ]

    def gathered(p):
        for k in range(n_f):
            for m in range(1, n_c):
                side(p, k, m).wait()

        def split(j, _):
            to = pl.ds(pl.multiple_of(j * own, own), own)
            w_s[0, to, columns[p]], w_s[1, to, columns[p]] = halves(
                wv[j // n_c, j % n_c, :, columns[p]]
            )
            return 0

        lax.fori_loop(0, n_f * n_c, split, 0)

    @pl.when((block == 0) & (head == 0) & (step == 0))
    def _():
        barrier = pltpu.get_barrier_semaphore()
        peers = [{"fsdp": at_f(-1)}] + ([{"fsdp": at_f(1)}] if n_f > 2 else [])
        peers += [{"ctx": at_c(m)} for m in range(1, n_c)]
        for peer in peers:
            pl.semaphore_signal(
                barrier, inc=1, device_id=peer, device_id_type=pl.DeviceIdType.MESH
            )
        for h in range(heads):
            at = 3 * HD * h
            shard[:, 2 * HD * h : 2 * HD * (h + 1)] = w_qkv[:, at + HD : at + 3 * HD]
            shard[:, 2 * split_at + HD * h : 2 * split_at + HD * (h + 1)] = w_qkv[:, at : at + HD]
        pl.semaphore_wait(barrier, len(peers))
        for p in range(2):
            hop(p, 1).start()
            for m in range(1, n_c):
                side(p, 0, m).start()
        wv[f, c] = shard[...]
        ud_own[:, :hidden] = up[...]
        ud_own[:, hidden:] = down_t[...]
        ow_own[...] = outw_t[...]
        for k in range(1, n_f):
            for p in range(2):
                hop(p, k).wait()
                if k < n_f - 1:
                    hop(p, k + 1).start()
                for m in range(1, n_c):
                    side(p, k, m).start()
        ud_hop(1).start()
        ow_hop(1).start()
        copies = locals_of()
        copies[0].start()
        copies[1].start()
        gathered(0)
        blank = jnp.zeros((1, HD), jnp.float32)
        v_row = row(b_v)
        b_kv = jnp.concatenate(
            sum(([blank, v_row[:, h * HD : (h + 1) * HD]] for h in range(heads)), []), axis=1
        )
        q_row = row(b_q)

        def keys(i, _):
            at = pl.ds(pl.multiple_of(i * rows, rows), rows)
            right = (w_s[0, :, : 2 * split_at], w_s[1, :, : 2 * split_at])
            kv_s[at, :] = dot_three(halves(tok[at, :]), right, 1, 0) + b_kv
            return 0

        lax.fori_loop(0, span // rows, keys, 0)
        for h in range(heads):
            for m in range(1, n_c):
                kv_send(h, m).start()

        gathered(1)
        copies[2].start()

        def asking(i, _):
            at = pl.ds(pl.multiple_of(i * rows, rows), rows)
            right = (w_s[0, :, 2 * split_at :], w_s[1, :, 2 * split_at :])
            q_s[at, :] = dot_three(halves(tok[at, :]), right, 1, 0) + q_row
            return 0

        lax.fori_loop(0, span // rows, asking, 0)
        copies[3].start()
        copies[4].start()
        for m in range(1, n_c):
            ow_side(0, m).start()

    @pl.when((block == 0) & (step == 0))
    def _():
        kv_t[...] = kv_s[:, lanes(head)]

    @pl.when((block > 0) & (step == 0))
    def _():
        kv_send(head, block).wait_recv()
        copy = pltpu.make_async_copy(
            kv_far.at[block - 1, :, lanes(head)], kv_t, local_sem.at[5]
        )
        copy.start()
        copy.wait()

    @pl.when(step == 0)
    def _():
        def prepare(j, _):
            at = pl.ds(pl.multiple_of(j * tile, tile), tile)
            pair = kv_t[at, :]
            kp[at, :] = packed(pair, True)
            vt[:, at] = stacked(pair.T[HD:, :])
            bias[at, :] = key_bias(meta_ref[0], at_c(block) * span + j * tile, tile, 128)
            return 0

        lax.fori_loop(0, span // tile, prepare, 0)

    here = pl.ds(pl.multiple_of(step * rows, rows), rows)

    @pl.when(block == 0)
    def _():
        acc[head, :, here] = jnp.zeros((2 * HD, rows), jnp.float32)
        top_s[head, :, here] = jnp.full((1, rows), MASKED, jnp.float32)
        total_s[head, :, here] = jnp.zeros((1, rows), jnp.float32)

    doubled(q_s, here, head, qd, heads)
    q_high, q_low = halves(qd[...] * (LOG2E * HD**-0.5))
    q_four = jnp.concatenate([q_high, q_low], axis=1)

    def key_tile(j, carry):
        top, total = carry
        at = pl.ds(pl.multiple_of(j * tile, tile), tile)
        k_two = kp[at, :]
        scores = dot(jnp.concatenate([k_two, k_two], axis=1), q_four, 1, 1)
        scores = scores + jnp.concatenate([bias[at, :]] * (rows // 128), axis=1)
        new_top = jnp.maximum(top, jnp.max(scores, axis=0, keepdims=True))
        fade = jnp.exp2(top - new_top)
        probs = jnp.exp2(scores - new_top)
        total = total * fade + jnp.sum(probs, axis=0, keepdims=True)
        high, low = halves(probs)
        v_two = vt[:, at]
        acc[head, :, here] = acc[head, :, here] * fade + (
            dot(v_two, high, 1, 0) + dot(v_two, low, 1, 0)
        )
        return new_top, total

    top, total = lax.fori_loop(
        0, span // tile, key_tile, (top_s[head, :, here], total_s[head, :, here])
    )
    top_s[head, :, here] = top
    total_s[head, :, here] = total

    @pl.when(block == n_c - 1)
    def _():
        result = ((acc[head, :HD, here] + acc[head, HD:, here]) / total).T
        for j in range(heads):

            @pl.when(head == j)
            def _(j=j):
                att[here, j * HD : (j + 1) * HD] = result
                lse[j : j + 1, here] = top + jnp.log2(total)

    def arrived(k):
        ud_hop(k).wait()
        ow_hop(k).wait()
        if k < n_f - 1:
            ud_hop(k + 1).start()
            ow_hop(k + 1).start()
        for m in range(1, n_c):
            ow_side(k, m).start()

    count = n_c * heads * STEPS_PER_HEAD
    now = (block * heads + head) * n_q + step
    for k in range(1, n_f):

        @pl.when(now == min(count - 1, k * count // (n_f - 1) - 1))
        def _(k=k):
            arrived(k)

    @pl.when(now == count - 1)
    def _():
        for k in range(n_f):
            for m in range(1, n_c):
                ow_side(k, m).wait()
        for h in range(heads):
            for m in range(1, n_c):
                kv_send(h, m).wait_send()
        for copy in locals_of():
            copy.wait()


def front(tokens, w_qkv, w_up, w_down_t, w_out_t, b_query, b_value, lengths, heads, n_f, n_c, tile=512):
    span, width = tokens.shape
    own, total = w_qkv.shape
    hidden, split_at = w_up.shape[1], heads * HD
    rows = span // STEPS_PER_HEAD
    shape, sem, f32, bf16 = jax.ShapeDtypeStruct, pltpu.SemaphoreType.DMA, jnp.float32, jnp.bfloat16
    anywhere = pl.BlockSpec(memory_space=pl.ANY)

    def held(dims):
        return pl.BlockSpec(dims, lambda b, h, i, m: (0,) * len(dims))

    operands = (tokens, w_qkv, w_up, w_down_t, w_out_t, b_query, b_value)
    return pl.pallas_call(
        functools.partial(front_kernel, heads, n_c, n_f, tile, rows),
        grid_spec=pltpu.PrefetchScalarGridSpec(
            num_scalar_prefetch=1,
            grid=(n_c, heads, STEPS_PER_HEAD),
            in_specs=[held(x.shape) for x in operands],
            out_specs=[held((span, split_at)), held((heads, span))] + [anywhere] * 6,
            scratch_shapes=[
                pltpu.VMEM((own, total), f32),
                pltpu.VMEM((span, split_at), f32),
                pltpu.VMEM((span, 2 * split_at), f32),
                pltpu.VMEM((span, 2 * HD), f32),
                pltpu.VMEM((n_f, n_c, own, total), f32),
                pltpu.VMEM((2, width, total), bf16),
                pltpu.VMEM((own, 2 * hidden), f32),
                pltpu.VMEM((own, split_at), f32),
                pltpu.VMEM((span, 2 * HD), bf16),
                pltpu.VMEM((2 * HD, span), bf16),
                pltpu.VMEM((span, 128), f32),
                pltpu.VMEM((rows, 2 * HD), f32),
                pltpu.VMEM((heads, 2 * HD, span), f32),
                pltpu.VMEM((heads, 1, span), f32),
                pltpu.VMEM((heads, 1, span), f32),
                sem((2, 2, n_f - 1)),
                sem((2, 2, n_f, n_c - 1)),
                sem((2, n_f - 1)),
                sem((2, n_f - 1)),
                sem((2, n_f, n_c - 1)),
                sem((2, heads, n_c - 1)),
                sem((6,)),
            ],
        ),
        out_shape=[
            shape((span, split_at), f32),
            shape((heads, span), f32),
            shape((span, split_at), f32),
            shape((span, 2 * split_at), f32),
            shape((n_c - 1, span, 2 * split_at), f32),
            shape((n_f, n_c, own, total), f32),
            shape((n_f, own, 2 * hidden), f32),
            shape((n_f, n_c, own, split_at), f32),
        ],
        compiler_params=pltpu.CompilerParams(
            dimension_semantics=("arbitrary",) * 3,
            collective_id=3,
            has_side_effects=True,
            vmem_limit_bytes=62 << 20,
        ),
        name="front",
    )(lengths, *operands)

def tail_kernel(
    chunks, rows, n_c, n_f, own,
    tok, grad_q, grad_kv, far, wide, mid, vec, d_bup, d_out,
    d_in, d_w, d_wout, d_bq, d_bv, d_bu, s_0, s_1, s_2, s_3, s_4, s_5,
    part, rx0, rx1, full, w_s, gs, ts, dw, side_rx, hop_rx, out_side, out_hop, small, small_rx,
    near_sem, far_sem, side_sem, hop_sem, out_side_sem, out_hop_sem, small_sem, local_sem,
):
    half, quarter = rows // 2, rows // 4
    me, f, c_at = lax.axis_index("tp"), lax.axis_index("fsdp"), lax.axis_index("ctx")
    bit0, bit1 = me % 2, me // 2 % 2
    peer0, peer1 = me + 1 - 2 * bit0, me + 2 - 4 * bit1
    home0 = pl.multiple_of(bit0 * half, half)
    away0 = pl.multiple_of((1 - bit0) * half, half)
    mine = pl.multiple_of(home0 + bit1 * quarter, quarter)
    away1 = pl.multiple_of(home0 + (1 - bit1) * quarter, quarter)
    keep = pl.ds(mine, quarter)
    width, kv_width, total = tok.shape[1], grad_kv.shape[1], wide.shape[1]

    def at_f(k):
        return (f + (n_f - k)) % n_f

    def at_c(m):
        return (c_at + (n_c - m)) % n_c

    def exchange(src, dst, sems, kind, c, peer):
        return remote(src, dst, sems.at[0, kind, c], sems.at[1, kind, c], tp=peer)

    def scatter0(c):
        return exchange(part.at[c, pl.ds(away0, half)], rx0.at[c], near_sem, 0, c, peer0)

    def scatter1(c):
        return exchange(part.at[c, pl.ds(away1, quarter)], rx1.at[c], far_sem, 0, c, peer1)

    def gather1(c):
        return exchange(full.at[c, keep], full.at[c, keep], far_sem, 1, c, peer1)

    def gather0(c):
        place = pl.ds(home0, half)
        return exchange(full.at[c, place], full.at[c, place], near_sem, 1, c, peer0)

    def powers(count):
        bits, bit = [], 1
        while bit < count:
            bits.append(bit)
            bit *= 2
        return bits

    def flipped(at, bit):
        return at + bit - 2 * bit * (at // bit % 2)

    rounds = [("tp", peer0), ("tp", peer1)]
    rounds += [("fsdp", flipped(f, bit)) for bit in powers(n_f)]
    rounds += [("ctx", flipped(c_at, bit)) for bit in powers(n_c)]

    def small_copy(r):
        axis, peer = rounds[r]
        return remote(
            small.at[r], small_rx.at[r], small_sem.at[0, r], small_sem.at[1, r], **{axis: peer}
        )

    def small_event(r):
        small_copy(r).wait()
        if rounds[r][0] == "tp":
            small[r + 1, :8, :] = small[r, :8, :] + small_rx[r, :8, :]
            small[r + 1, 8:, :] = small[r, 8:, :]
        else:
            small[r + 1] = small[r] + small_rx[r]
        if r + 1 < len(rounds):
            small_copy(r + 1).start()

    barrier = pltpu.get_barrier_semaphore()
    peers = [{"tp": peer0}, {"tp": peer1}]
    peers += [{"fsdp": at_f(k)} for k in range(1, n_f)]
    peers += [{"ctx": at_c(m)} for m in range(1, n_c)]
    for peer in peers:
        pl.semaphore_signal(barrier, inc=1, device_id=peer, device_id_type=pl.DeviceIdType.MESH)

    def split(i, _):
        at = pl.ds(pl.multiple_of(i * 128, 128), 128)
        w_s[0, at, :], w_s[1, at, :] = halves(wide[at, :])
        return 0

    lax.fori_loop(0, width // 128, split, 0)
    small[0, :8, :] = vec[...]
    small[0, 8:, :] = jnp.zeros_like(small[0, 8:, :])
    small[0, 8:9, :] = d_bup[...]
    dw[...] = jnp.zeros_like(dw)
    pl.semaphore_wait(barrier, len(peers))

    out_ring = Ring(
        n_f, n_c, row_block(d_out, own, n_f, n_c), out_side, out_hop, out_side_sem,
        out_hop_sem, keeper(d_wout),
    )
    out_ring.begin()

    def finish0(c):
        scatter0(c).wait()
        part[c, pl.ds(away1, quarter), :] += rx0[c, pl.ds(away1 - home0, quarter), :]
        scatter1(c).start()
        part[c, keep, :] += rx0[c, pl.ds(mine - home0, quarter), :]

    def partial(c, _):
        at = pl.ds(pl.multiple_of(c * rows, rows), rows)
        kv = grad_kv[at, :]
        for m in range(n_c - 1):
            kv = kv + far[m, at, :]
        grad = jnp.concatenate([kv, grad_q[at, :]], axis=1)
        gs[c, 0], gs[c, 1] = halves(grad)
        small[0, 9:10, :total] += jnp.sum(grad, axis=0, keepdims=True)

        def columns(n):
            part[c, :, n] = dot_three((gs[c, 0], gs[c, 1]), (w_s[0, n, :], w_s[1, n, :]), 1, 1)

        tiles_of(width, columns)
        scatter0(c).start()

        @pl.when(c > 0)
        def _():
            finish0(c - 1)

        return 0

    lax.fori_loop(0, chunks, partial, 0)
    finish0(chunks - 1)
    small_copy(0).start()

    def weights(c, _):
        at = pl.ds(pl.multiple_of(c * rows, rows), rows)
        ts[0], ts[1] = halves(tok[at, :].T)

        def lines(n):
            dw[n, :] += dot_three((ts[0, n, :], ts[1, n, :]), (gs[c, 0], gs[c, 1]), 1, 0)

        tiles_of(width, lines)
        return 0

    lax.fori_loop(0, chunks, weights, 0)
    qkv_ring = Ring(
        n_f, n_c, row_block(dw, own, n_f, n_c), side_rx, hop_rx, side_sem, hop_sem,
        lambda result: grouped(d_w, result),
    )
    qkv_ring.begin()
    heads = (total - kv_width) // HD

    def grouped(target, value):
        for h in range(heads):
            at = 3 * HD * h
            target[:, at : at + HD] = value[:, kv_width + HD * h : kv_width + HD * (h + 1)]
            target[:, at + HD : at + 3 * HD] = value[:, 2 * HD * h : 2 * HD * (h + 1)]

    def finish1(c):
        scatter1(c).wait()
        full[c, keep, :] = part[c, keep, :] + rx1[c] + mid[c]
        gather1(c).start()

    def forward1(c):
        gather1(c).wait()
        gather0(c).start()

    def leave(c):
        return pltpu.make_async_copy(full.at[c], d_in.at[c], local_sem.at[c])

    plan = [(18 + 4.4 * c, lambda c=c: finish1(c)) for c in range(chunks)]
    plan += [(30 + 6.5 * c, lambda c=c: forward1(c)) for c in range(chunks)]
    plan += [(5 + 10 * k / n_f, lambda k=k: out_ring.event(k)) for k in range(1, n_f + 1)]
    plan += [(17 + 24 * k / n_f, lambda k=k: qkv_ring.event(k)) for k in range(1, n_f + 1)]
    plan += [
        (15 + 30 * (r + 1) / len(rounds), lambda r=r: small_event(r)) for r in range(len(rounds))
    ]
    plan.sort(key=lambda item: item[0])
    for _, event in plan:
        event()
    last = len(rounds)
    for i, target in enumerate((s_0, s_1, s_2, s_3, s_4, s_5)):
        target[...] = small[last, i : i + 1, :].reshape(-1)
    d_bu[...] = small[last, 8:9, :].reshape(-1)
    d_bq[...] = small[last, 9:10, kv_width:total].reshape(-1)
    by_value = [
        small[last, 9:10, 2 * HD * h + HD : 2 * HD * (h + 1)] for h in range(heads)
    ]
    d_bv[...] = jnp.concatenate(by_value, axis=1).reshape(-1)
    for c in range(chunks):
        gather0(c).wait()
        leave(c).start()
    for c in range(chunks):
        leave(c).wait()


def tail(tokens, grad_q, grad_kv, far, wide, mid, vec, d_bup, d_out, n_f, n_c, own):
    count, width = tokens.shape
    total, chunks, quarter = wide.shape[1], mid.shape[0], mid.shape[1]
    rows = 4 * quarter
    vmem, anywhere = pl.BlockSpec(memory_space=pltpu.VMEM), pl.BlockSpec(memory_space=pl.ANY)
    shape, sem, f32, bf16 = jax.ShapeDtypeStruct, pltpu.SemaphoreType.DMA, jnp.float32, jnp.bfloat16
    rounds = 2 + (n_f - 1).bit_length() + (n_c - 1).bit_length()
    return pl.pallas_call(
        functools.partial(tail_kernel, chunks, rows, n_c, n_f, own),
        in_specs=[vmem] * 9,
        out_specs=[anywhere] + [vmem] * 11,
        out_shape=[
            shape((chunks, rows, width), f32),
            shape((own, total), f32),
            shape((own, d_out.shape[1]), f32),
            shape((total - grad_kv.shape[1],), f32),
            shape((total - grad_kv.shape[1],), f32),
        ]
        + [shape((width,), f32)] * 7,
        scratch_shapes=[
            pltpu.VMEM((chunks, rows, width), f32),
            pltpu.VMEM((chunks, rows // 2, width), f32),
            pltpu.VMEM((chunks, quarter, width), f32),
            pltpu.VMEM((chunks, rows, width), f32),
            pltpu.VMEM((2, width, total), bf16),
            pltpu.VMEM((chunks, 2, rows, total), bf16),
            pltpu.VMEM((2, width, rows), bf16),
            pltpu.VMEM((width, total), f32),
            pltpu.VMEM((n_f, n_c - 1, own, total), f32),
            pltpu.VMEM((n_f - 1, own, total), f32),
            pltpu.VMEM((n_f, n_c - 1, own, d_out.shape[1]), f32),
            pltpu.VMEM((n_f - 1, own, d_out.shape[1]), f32),
            pltpu.VMEM((rounds + 1, 16, width), f32),
            pltpu.VMEM((rounds, 16, width), f32),
            sem((2, 2, chunks)),
            sem((2, 2, chunks)),
            sem((2, n_f, n_c - 1)),
            sem((2, n_f - 1)),
            sem((2, n_f, n_c - 1)),
            sem((2, n_f - 1)),
            sem((2, rounds)),
            sem((chunks,)),
        ],
        compiler_params=pltpu.CompilerParams(
            collective_id=4, has_side_effects=True, vmem_limit_bytes=62 << 20
        ),
        name="tail",
    )(tokens, grad_q, grad_kv, far, wide, mid, vec, d_bup, d_out)

def finish_kernel(bigs, *refs):
    count = (len(refs) - bigs - 1) // 2
    given, results, stages, sem = refs[:count], refs[count : 2 * count], refs[2 * count : -1], refs[-1]
    pieces = [(i, c) for i in range(bigs) for c in range(given[i].shape[0])]

    def inward(i, c):
        return pltpu.make_async_copy(given[i].at[c], stages[i].at[c], sem.at[0, i, c])

    def outward(i, c):
        return pltpu.make_async_copy(stages[i].at[c], results[i].at[c], sem.at[1, i, c])

    for i, c in pieces:
        inward(i, c).start()
    for source, target in zip(given[bigs:], results[bigs:]):
        target[...] = source[...]
    for i, c in pieces:
        inward(i, c).wait()
        outward(i, c).start()
    for i, c in pieces:
        outward(i, c).wait()


def finish(large, small):
    anywhere, vmem = pl.BlockSpec(memory_space=pl.ANY), pl.BlockSpec(memory_space=pltpu.VMEM)
    specs = [anywhere] * len(large) + [vmem] * len(small)
    return pl.pallas_call(
        functools.partial(finish_kernel, len(large)),
        in_specs=specs,
        out_specs=specs,
        out_shape=[jax.ShapeDtypeStruct(x.shape, x.dtype) for x in (*large, *small)],
        scratch_shapes=[pltpu.VMEM(x.shape, x.dtype) for x in large]
        + [pltpu.SemaphoreType.DMA((2, len(large), max(x.shape[0] for x in large)))],
        name="finish",
    )(*large, *small)


def per_device(
    inputs,
    lengths,
    w_qkv,
    b_query,
    b_value,
    w_out,
    b_out,
    gain_attn,
    shift_attn,
    w_up,
    b_up,
    w_down,
    b_down,
    gain_ffn,
    shift_ffn,
    cotangent,
):
    width = inputs.shape[-1]
    block_len = inputs.shape[1]
    heads = b_query.shape[0] // HD
    split_at = heads * HD
    hidden = b_up.shape[0]
    tokens = inputs.reshape(block_len, width)
    cot = cotangent.reshape(block_len, width)
    length = lengths[0]
    n_c = lax.axis_size("ctx")
    at_c = lax.axis_index("ctx")

    def regroup(columns):
        parts = columns.reshape(columns.shape[:-1] + (heads, 3 * HD))
        lead = columns.shape[:-1]
        return jnp.concatenate(
            [
                parts[..., HD:].reshape(lead + (2 * split_at,)),
                parts[..., :HD].reshape(lead + (split_at,)),
            ],
            axis=-1,
        )

    bias_kv = jnp.stack(
        [jnp.zeros((heads, HD), jnp.float32), b_value.reshape(heads, HD)], axis=1
    ).reshape(-1)
    n_f, own = lax.axis_size("fsdp"), w_up.shape[0]
    fused = own % 16 == 0 and n_c > 1 and n_f > 1 and hidden == width
    if fused:
        attended, log_sums, queries, kv_own, kv_far, wide, weights, wide_out_t = front(
            tokens, w_qkv, w_up, w_down.T, w_out.T, b_query, b_value, lengths, heads, n_f, n_c,
        )
        wide = wide.reshape(width, 3 * split_at)
        wide_kv, wide_q = wide[:, : 2 * split_at], wide[:, 2 * split_at :]
        wide_out_t = wide_out_t.reshape(width, split_at)
        kv_blocks = [kv_own] + [kv_far[m] for m in range(n_c - 1)]
    else:
        wide_kv, wide_q = weight_gather(regroup(w_qkv), [2 * split_at, split_at])
        rest = jnp.concatenate([w_up, w_down.T, w_out.T], axis=1)
        wide_up, wide_down_t, wide_out_t = weight_gather(rest, [hidden, hidden, split_at])
        weights = (wide_up, wide_down_t)
        kv_blocks = [contract(tokens, wide_kv, 1, 0) + bias_kv]
        for m in range(1, n_c):
            kv_blocks.append(ringed(kv_blocks[-1], "ctx", 1))
        queries = contract(tokens, wide_q, 1, 0) + b_query
        meta = jnp.stack([length] + [(at_c - m) % n_c * block_len for m in range(n_c)])
        attended, log_sums = attention(queries, kv_blocks, meta, heads)

    vectors = (b_out, gain_attn, shift_attn, b_up, b_down, gain_ffn, shift_ffn)
    outs, grad_mid, grad_att, d_up, d_out, d_wdown_t, vec_rows, d_bup = middle(
        attended, weights, wide_out_t, vectors, tokens, cot, hidden, n_c
    )
    blocked = (lax.axis_size("fsdp"), n_c, w_up.shape[0])
    grad_q, grad_kv, d_wup, kv_back, outputs = attention_back(
        queries,
        grad_att,
        attended,
        log_sums,
        kv_blocks,
        lengths,
        heads,
        d_up.reshape(blocked + (hidden,)),
        outs,
    )
    if fused:
        d_inputs, *small = tail(
            tokens, grad_q, grad_kv, kv_back, wide, grad_mid, vec_rows, d_bup, d_out, n_f, n_c, own
        )
        outputs, d_inputs, d_wup, d_wdown_t, d_wqkv, d_wout_t, d_bquery, d_bvalue, d_bup, *sums = (
            finish([outputs.reshape(d_inputs.shape), d_inputs], [d_wup, d_wdown_t, *small])
        )
        d_inputs = d_inputs.reshape(block_len, width)
    else:
        for m in range(n_c - 1):
            grad_kv = grad_kv + kv_back[m]
        back = contract(grad_kv, wide_kv, 1, 1) + contract(grad_q, wide_q, 1, 1)
        tail_sums = small_sum(
            jnp.concatenate([jnp.sum(grad_kv, axis=0), jnp.sum(grad_q, axis=0), d_bup[0]]),
            ("fsdp", "ctx"),
        )
        d_wdown_t, d_wout_t = grad_scatter([d_wdown_t]), grad_scatter([d_out])
        proj_sums, d_bup = tail_sums[: 3 * split_at], tail_sums[3 * split_at :]
        sums = small_sum(vec_rows, ("tp", "fsdp", "ctx"))
        d_inputs = quarter_gather(grad_mid + quarter_scatter(back, grad_mid.shape[0]))
        own_dw = grad_scatter([contract(tokens, grad_kv, 0, 0), contract(tokens, grad_q, 0, 0)])
        d_wqkv = jnp.concatenate(
            [
                own_dw[:, 2 * split_at :].reshape(own, heads, HD),
                own_dw[:, : 2 * split_at].reshape(own, heads, 2 * HD),
            ],
            axis=2,
        ).reshape(own, 3 * split_at)
        d_bvalue = proj_sums[: 2 * split_at].reshape(heads, 2, HD)[:, 1].reshape(-1)
        d_bquery = proj_sums[2 * split_at : 3 * split_at]
    d_wdown, d_wout = d_wdown_t.T, d_wout_t.T
    return (
        outputs.reshape(1, block_len, width),
        d_inputs.reshape(1, block_len, width),
        d_wqkv,
        d_bquery,
        d_bvalue,
        d_wout,
        sums[0],
        sums[1],
        sums[2],
        d_wup,
        d_bup,
        d_wdown,
        sums[3],
        sums[4],
        sums[5],
    )


def solution(mesh):
    rows_of, cols_of = P(("fsdp", "ctx"), "tp"), P("tp", ("fsdp", "ctx"))
    seq, by_tp, same = P("fsdp", "ctx", None), P("tp"), P()
    in_specs = (
        seq, P("fsdp"), rows_of, by_tp, by_tp, cols_of, same, same, same,
        rows_of, by_tp, cols_of, same, same, same, seq,
    )
    out_specs = (
        seq, seq, rows_of, by_tp, by_tp, cols_of, same, same, same,
        rows_of, by_tp, cols_of, same, same, same,
    )
    return jax.shard_map(
        per_device, mesh=mesh, in_specs=in_specs, out_specs=out_specs, check_vma=False
    )
```

```python
import functools
import math

import jax
import jax.numpy as jnp
from jax import lax
from jax.experimental import pallas as pl
from jax.experimental.pallas import tpu as pltpu
from jax.sharding import PartitionSpec as P

HD = 64
LOG2E = math.log2(math.e)
NORM_EPS = 1e-12
MASKED = -1e30
THREE = lax.Precision.HIGH


def contract(left, right, left_dim, right_dim):
    return lax.dot_general(
        left,
        right,
        (((left_dim,), (right_dim,)), ((), ())),
        precision=THREE,
        preferred_element_type=jnp.float32,
    )


def ringed(block, axis, distance):
    count = lax.axis_size(axis)
    return lax.ppermute(block, axis, [(i, (i + distance) % count) for i in range(count)])


def swapped(block, axis, bit):
    return lax.ppermute(block, axis, [(i, i ^ bit) for i in range(lax.axis_size(axis))])


def bits_of(axis):
    bits, bit = [], 1
    while bit < lax.axis_size(axis):
        bits.append(bit)
        bit *= 2
    return bits


def half_scatter(part, chunks):
    upper = lax.axis_index("tp") % 2
    count, width = part.shape
    block = part.reshape(chunks, 2, count // (2 * chunks), width)
    leaving = lax.dynamic_index_in_dim(block, 1 - upper, 1, keepdims=False)
    staying = lax.dynamic_index_in_dim(block, upper, 1, keepdims=False)
    block = staying + swapped(leaving, "tp", 1)
    return block + swapped(block, "tp", 2)


def half_gather(block):
    other = swapped(block, "tp", 1)
    upper = lax.axis_index("tp") % 2 == 1
    block = jnp.where(upper, jnp.stack([other, block], axis=1), jnp.stack([block, other], axis=1))
    return block.reshape(-1, block.shape[-1])


def small_sum(vector, axes):
    for axis in axes:
        for bit in bits_of(axis):
            vector = vector + swapped(vector, axis, bit)
    return vector


def weight_gather(shard, widths):
    rows = shard.shape[0]
    n_f, n_c = lax.axis_size("fsdp"), lax.axis_size("ctx")
    at_f, at_c = lax.axis_index("fsdp"), lax.axis_index("ctx")
    wholes = [jnp.zeros((n_f * n_c * rows, width), jnp.float32) for width in widths]
    along_f = shard
    for k in range(n_f):
        if k:
            along_f = ringed(along_f, "fsdp", 1)
        along_c = along_f
        for m in range(n_c):
            if m:
                along_c = ringed(along_c, "ctx", 1)
            place = ((at_f - k) % n_f * n_c + (at_c - m) % n_c) * rows
            start = 0
            for i, width in enumerate(widths):
                wholes[i] = lax.dynamic_update_slice(
                    wholes[i], along_c[:, start : start + width], (place, 0)
                )
                start += width
    return wholes


def grad_scatter(pieces):
    n_f, n_c = lax.axis_size("fsdp"), lax.axis_size("ctx")
    at_f, at_c = lax.axis_index("fsdp"), lax.axis_index("ctx")
    rows = pieces[0].shape[0] // (n_f * n_c)

    def piece(f, c):
        start = (f % n_f * n_c + c % n_c) * rows
        cut = [lax.dynamic_slice_in_dim(p, start, rows, 0) for p in pieces]
        return cut[0] if len(cut) == 1 else jnp.concatenate(cut, axis=1)

    total = None
    for k in range(1, n_f + 1):
        over_c = piece(at_f - k, at_c - 1)
        for m in range(2, n_c + 1):
            over_c = ringed(over_c, "ctx", 1) + piece(at_f - k, at_c - m)
        total = over_c if total is None else ringed(total, "fsdp", 1) + over_c
    return total


def normalized(values):
    centred = values - jnp.mean(values, axis=-1, keepdims=True)
    spread = jnp.mean(centred * centred, axis=-1, keepdims=True)
    recip = lax.rsqrt(spread + NORM_EPS)
    return centred * recip, recip


def norm_back(grad, gain, normed, recip):
    scaled = grad * gain
    return recip * (
        scaled
        - jnp.mean(scaled, axis=-1, keepdims=True)
        - normed * jnp.mean(scaled * normed, axis=-1, keepdims=True)
    )


def halves(values):
    high = values.astype(jnp.bfloat16)
    return high, (values - high.astype(jnp.float32)).astype(jnp.bfloat16)


def low_half(shape):
    return lax.broadcasted_iota(jnp.int32, shape, 1) < HD


def dot(left, right, left_dim, right_dim):
    return lax.dot_general(
        left, right, (((left_dim,), (right_dim,)), ((), ())), preferred_element_type=jnp.float32
    )


def doubled(ref, rows, head, scratch, heads):
    for j in range(heads):

        @pl.when(head == j)
        def _():
            piece = ref[rows, j * HD : (j + 1) * HD]
            scratch[...] = jnp.concatenate([piece, piece], axis=1)


def packed(pair, first):
    low = low_half(pair.shape)
    turned = pltpu.roll(pair, HD, 1)
    twice = jnp.where(low, pair, turned) if first else jnp.where(low, turned, pair)
    high, rest = halves(twice)
    return jnp.where(low, high.astype(jnp.float32), rest.astype(jnp.float32)).astype(jnp.bfloat16)


def stacked(half):
    high, rest = halves(half)
    return jnp.concatenate([high, rest], axis=0)


def key_bias(limit, first, count, width):
    place = first + lax.broadcasted_iota(jnp.int32, (count, width), 0)
    return jnp.where(place < limit, 0.0, MASKED)


def row(ref):
    return ref[...].reshape(1, -1)


def forward_kernel(heads, blocks, tile, rows, meta_ref, q_ref, *refs):
    kv_refs, (out_ref, lse_ref, kp, vt, bias, qd, acc) = refs[:blocks], refs[blocks:]
    head, step = pl.program_id(0), pl.program_id(1)
    span = kv_refs[0].shape[0]
    per = span // tile

    @pl.when(step == 0)
    def _():
        for b in range(blocks):

            def prepare(j, _, b=b):
                at = pl.ds(pl.multiple_of(j * tile, tile), tile)
                to = pl.ds(pl.multiple_of(b * span + j * tile, tile), tile)
                pair = kv_refs[b][at, :]
                kp[to, :] = packed(pair, True)
                vt[:, to] = stacked(pair.T[HD:, :])
                bias[to, :] = key_bias(meta_ref[0], meta_ref[1 + b] + j * tile, tile, 128)
                return 0

            lax.fori_loop(0, per, prepare, 0)

    here = pl.ds(pl.multiple_of(step * rows, rows), rows)
    doubled(q_ref, here, head, qd, heads)
    q_high, q_low = halves(qd[...] * (LOG2E * HD**-0.5))
    q_four = jnp.concatenate([q_high, q_low], axis=1)
    acc[...] = jnp.zeros_like(acc)

    def key_tile(j, carry):
        top, total = carry
        at = pl.ds(pl.multiple_of(j * tile, tile), tile)
        k_two = kp[at, :]
        scores = dot(jnp.concatenate([k_two, k_two], axis=1), q_four, 1, 1)
        scores = scores + jnp.concatenate([bias[at, :]] * (rows // 128), axis=1)
        new_top = jnp.maximum(top, jnp.max(scores, axis=0, keepdims=True))
        fade = jnp.exp2(top - new_top)
        probs = jnp.exp2(scores - new_top)
        total = total * fade + jnp.sum(probs, axis=0, keepdims=True)
        high, low = halves(probs)
        v_two = vt[:, at]
        acc[...] = acc[...] * fade + (dot(v_two, high, 1, 0) + dot(v_two, low, 1, 0))
        return new_top, total

    top, total = lax.fori_loop(
        0,
        blocks * per,
        key_tile,
        (jnp.full((1, rows), MASKED, jnp.float32), jnp.zeros((1, rows), jnp.float32)),
    )
    result = acc[:HD, :] + acc[HD:, :]
    result = (result / total).T
    for j in range(heads):

        @pl.when(head == j)
        def _():
            out_ref[here, j * HD : (j + 1) * HD] = result
            lse_ref[j : j + 1, here] = top + jnp.log2(total)


def attention(queries, kv_blocks, meta, heads, rows=256, tile=512):
    count, span, blocks = queries.shape[0], kv_blocks[0].shape[0], len(kv_blocks)
    keys = span * blocks
    whole = lambda h, i, m: (0, 0)
    return pl.pallas_call(
        functools.partial(forward_kernel, heads, blocks, tile, rows),
        grid_spec=pltpu.PrefetchScalarGridSpec(
            num_scalar_prefetch=1,
            grid=(heads, count // rows),
            in_specs=[pl.BlockSpec((count, heads * HD), whole)]
            + [pl.BlockSpec((span, 2 * HD), lambda h, i, m: (0, h))] * blocks,
            out_specs=[
                pl.BlockSpec((count, heads * HD), whole),
                pl.BlockSpec((heads, count), whole),
            ],
            scratch_shapes=[
                pltpu.VMEM((keys, 2 * HD), jnp.bfloat16),
                pltpu.VMEM((2 * HD, keys), jnp.bfloat16),
                pltpu.VMEM((keys, 128), jnp.float32),
                pltpu.VMEM((rows, 2 * HD), jnp.float32),
                pltpu.VMEM((2 * HD, rows), jnp.float32),
            ],
        ),
        out_shape=[
            jax.ShapeDtypeStruct((count, heads * HD), jnp.float32),
            jax.ShapeDtypeStruct((heads, count), jnp.float32),
        ],
        compiler_params=pltpu.CompilerParams(dimension_semantics=("arbitrary", "arbitrary")),
        cost_estimate=pl.CostEstimate(
            flops=24 * heads * count * keys * HD,
            bytes_accessed=8 * keys * heads * HD + 8 * count * heads * HD,
            transcendentals=heads * count * keys,
        ),
        name="attention_forward",
    )(meta, queries, *kv_blocks)


def backward_kernel(
    heads, blocks, n_f, tile, rows, meta_ref, q_ref, do_ref, out_ref, lse_ref, up_g, outs,
    *refs,
):
    kv_refs = refs[:blocks]
    dq_ref, dkv_ref, up_out, kv_far, outs_all = refs[blocks : blocks + 5]
    (
        kp, vp, kt, bias, qd, dd, od, dk, dv, acc, stage, q_all, do_all, q_mix, do_mix, delta_all
    ) = refs[blocks + 5 : blocks + 21]
    transfers = Transfers(
        blocks, n_f, heads, up_g, outs, up_out, kv_far, outs_all, stage,
        *refs[blocks + 21 :],
    )
    head, order, step = pl.program_id(0), pl.program_id(1), pl.program_id(2)
    steps = pl.num_programs(2)
    now = (head * blocks + order) * steps + step
    transfers.run(now, before=True)
    span = kv_refs[0].shape[0]
    per = span // tile

    @pl.when(step == 0)
    def _():
        dk[...] = jnp.zeros_like(dk)
        dv[...] = jnp.zeros_like(dv)
        for b in range(blocks):

            @pl.when((order + 1) % blocks == b)
            def _(b=b):
                def prepare(j, _):
                    at = pl.ds(pl.multiple_of(j * tile, tile), tile)
                    pair = kv_refs[b][at, :]
                    kp[at, :] = packed(pair, True)
                    vp[at, :] = packed(pair, False)
                    kt[:, at] = stacked(pair.T[:HD, :])
                    bias[at, :] = key_bias(
                        meta_ref[0], transfers.at_c(b) * span + j * tile, tile, 128
                    )
                    return 0

                lax.fori_loop(0, per, prepare, 0)

    here = pl.ds(pl.multiple_of(step * rows, rows), rows)

    @pl.when(order == 0)
    def _():
        doubled(q_ref, here, head, qd, heads)
        doubled(do_ref, here, head, dd, heads)
        doubled(out_ref, here, head, od, heads)
        low = low_half((rows, 2 * HD))
        for value, four, mix in (
            (qd[...] * (LOG2E * HD**-0.5), q_all, q_mix),
            (dd[...], do_all, do_mix),
        ):
            high, rest = halves(value)
            four[here, : 2 * HD] = high
            four[here, 2 * HD :] = rest
            mixed = jnp.where(low, high.astype(jnp.float32), rest.astype(jnp.float32))
            mix[here, :] = mixed.astype(jnp.bfloat16)
        delta_all[:, here] = jnp.sum((dd[...] * od[...]).T[:HD, :], axis=0, keepdims=True)
        acc[:, here] = jnp.zeros((2 * HD, rows), jnp.float32)

    q_four, q_two, do_four, do_two = q_all[here, :], q_mix[here, :], do_all[here, :], do_mix[here, :]
    delta = delta_all[:, here]
    lse = lse_ref[0:1, here]
    for j in range(1, heads):
        lse = jnp.where(head == j, lse_ref[j : j + 1, here], lse)
    def key_tile(j, _):
        at = pl.ds(pl.multiple_of(j * tile, tile), tile)
        k_two, v_two = kp[at, :], vp[at, :]
        scores = dot(jnp.concatenate([k_two, k_two], axis=1), q_four, 1, 1)
        scores = scores + jnp.concatenate([bias[at, :]] * (rows // 128), axis=1)
        probs = jnp.exp2(scores - lse)
        high, rest = halves(probs)
        dv[at, :] += dot(high, do_two, 1, 0) + dot(rest, do_two, 1, 0)
        grad_p = dot(jnp.concatenate([v_two, v_two], axis=1), do_four, 1, 1)
        grad_s = probs * (grad_p - delta)
        high, rest = halves(grad_s)
        dk[at, :] += dot(high, q_two, 1, 0) + dot(rest, q_two, 1, 0)
        k_t = kt[:, at]
        acc[:, here] += dot(k_t, high, 1, 0) + dot(k_t, rest, 1, 0)
        return 0

    lax.fori_loop(0, per, key_tile, 0)

    @pl.when(order == blocks - 1)
    def _():
        result = ((acc[:HD, here] + acc[HD:, here]) * HD**-0.5).T
        for j in range(heads):

            @pl.when(head == j)
            def _(j=j):
                dq_ref[here, j * HD : (j + 1) * HD] = result

    def turned(at):
        grad_k, grad_v = dk[at, :], dv[at, :]
        grad_k = (grad_k + pltpu.roll(grad_k, HD, 1)) * (1.0 / LOG2E)
        grad_v = grad_v + pltpu.roll(grad_v, HD, 1)
        return jnp.where(low_half(grad_k.shape), grad_k, grad_v)

    for b in range(1, blocks):

        @pl.when((step == steps - 1) & (order == b - 1))
        def _(b=b):
            @pl.when(head >= 2)
            def _():
                transfers.kv_copy(head - 2, b).wait_send()

            def far(j, _):
                at = pl.ds(pl.multiple_of(j * tile, tile), tile)
                stage[head % 2, b - 1, at, :] = turned(at)
                return 0

            lax.fori_loop(0, per, far, 0)
            transfers.kv_copy(head, b).start()

    @pl.when((step == steps - 1) & (order == blocks - 1))
    def _():
        def keep(j, _):
            at = pl.ds(pl.multiple_of(j * tile, tile), tile)
            dkv_ref[at, :] = turned(at)
            return 0

        lax.fori_loop(0, per, keep, 0)

    transfers.run(now, before=False)


def remote(src, dst, send, recv, **peer):
    return pltpu.make_async_remote_copy(
        src_ref=src,
        dst_ref=dst,
        send_sem=send,
        recv_sem=recv,
        device_id=peer,
        device_id_type=pl.DeviceIdType.MESH,
    )


class Ring:
    def __init__(self, n_f, n_c, pick, side_rx, hop_rx, side_sem, hop_sem, emit):
        self.n_f, self.n_c, self.pick, self.emit = n_f, n_c, pick, emit
        self.side_rx, self.hop_rx, self.side_sem, self.hop_sem = side_rx, hop_rx, side_sem, hop_sem
        self.next_f = (lax.axis_index("fsdp") + 1) % n_f
        self.next_c = (lax.axis_index("ctx") + 1) % n_c

    def side(self, k, m):
        return remote(
            self.pick(k, 1) if m == 1 else self.side_rx.at[k - 1, m - 2],
            self.side_rx.at[k - 1, m - 1],
            self.side_sem.at[0, k - 1, m - 1],
            self.side_sem.at[1, k - 1, m - 1],
            ctx=self.next_c,
        )

    def hop(self, k):
        src = self.side_rx.at[0, self.n_c - 2] if k == 1 else self.hop_rx.at[k - 2]
        sem = self.hop_sem
        return remote(
            src, self.hop_rx.at[k - 1], sem.at[0, k - 1], sem.at[1, k - 1], fsdp=self.next_f
        )

    def begin(self):
        for k in range(1, self.n_f + 1):
            self.side(k, 1).start()

    def event(self, k):
        for m in range(2, self.n_c + 1):
            self.side(k, m - 1).wait()
            self.side_rx[k - 1, m - 2] += self.pick(k, m)[...]
            if m < self.n_c:
                self.side(k, m).start()
        if k > 1:
            self.hop(k - 1).wait()
            result = self.hop_rx[k - 2] + self.side_rx[k - 1, self.n_c - 2]
            if k < self.n_f:
                self.hop_rx[k - 2] = result
            else:
                self.emit(result)
        if k < self.n_f:
            self.hop(k).start()


def ring_scratch(n_f, n_c, own, wide):
    sem = pltpu.SemaphoreType.DMA
    return [
        pltpu.VMEM((n_f, n_c - 1, own, wide), jnp.float32),
        pltpu.VMEM((n_f - 1, own, wide), jnp.float32),
        sem((2, n_f, n_c - 1)),
        sem((2, n_f - 1)),
    ]


def row_block(ref, own, n_f, n_c):
    f, c = lax.axis_index("fsdp"), lax.axis_index("ctx")

    def pick(k, m):
        at = (f + (n_f - k)) % n_f * n_c + (c + (n_c - m)) % n_c
        return ref.at[pl.ds(pl.multiple_of(at * own, own), own)]

    return pick


def keeper(target):
    def emit(value):
        target[...] = value

    return emit


class Transfers:
    def __init__(
        self, n_c, n_f, heads, up_g, outs, up_out, kv_far, outs_all, stage,
        side_rx, hop_rx, side_sem, hop_sem, kv_sem, out_sem,
    ):
        self.n_c, self.n_f, self.heads = n_c, n_f, heads
        self.outs, self.kv_far, self.outs_all = outs, kv_far, outs_all
        self.stage = stage
        self.kv_sem = kv_sem
        self.out_sem = out_sem
        self.f, self.c, me = lax.axis_index("fsdp"), lax.axis_index("ctx"), lax.axis_index("tp")
        self.bit0 = me % 2
        self.peer0 = me + 1 - 2 * self.bit0
        self.ring = Ring(
            n_f, n_c, lambda k, m: up_g.at[self.at_f(k), self.at_c(m)],
            side_rx, hop_rx, side_sem, hop_sem, keeper(up_out),
        )

    def at_f(self, k):
        return (self.f + (self.n_f - k)) % self.n_f

    def at_c(self, m):
        return (self.c + (self.n_c - m)) % self.n_c

    def kv_copy(self, head, m):
        lanes = pl.ds(pl.multiple_of(head * 2 * HD, 2 * HD), 2 * HD)
        return remote(
            self.stage.at[head % 2, m - 1],
            self.kv_far.at[m - 1, :, lanes],
            self.kv_sem.at[0, head, m - 1],
            self.kv_sem.at[1, head, m - 1],
            ctx=self.at_c(m),
        )

    def out_local(self):
        return pltpu.make_async_copy(
            self.outs, self.outs_all.at[:, self.bit0], self.out_sem.at[0, 1]
        )

    def out_near(self):
        return remote(
            self.outs,
            self.outs_all.at[:, self.bit0],
            self.out_sem.at[0, 0],
            self.out_sem.at[1, 0],
            tp=self.peer0,
        )

    def begin(self):
        barrier = pltpu.get_barrier_semaphore()
        peers = [{"tp": self.peer0}, {"fsdp": self.at_f(-1)}]
        if self.n_f > 2:
            peers.append({"fsdp": self.at_f(1)})
        peers += [{"ctx": self.at_c(m)} for m in range(1, self.n_c)]
        for peer in peers:
            pl.semaphore_signal(
                barrier, inc=1, device_id=peer, device_id_type=pl.DeviceIdType.MESH
            )
        pl.semaphore_wait(barrier, len(peers))
        self.ring.begin()
        self.out_local().start()
        self.out_near().start()

    def end(self):
        self.out_local().wait()
        self.out_near().wait()
        for head in range(self.heads):
            for m in range(1, self.n_c):
                if head >= self.heads - 2:
                    self.kv_copy(head, m).wait_send()
                self.kv_copy(head, m).wait_recv()

    def run(self, now, before):
        count = self.heads * self.n_c * STEPS_PER_HEAD
        plan = []
        for k in range(1, self.n_f + 1):
            plan.append((0.85 * k / self.n_f, lambda k=k: self.ring.event(k)))
        plan.sort(key=lambda item: item[0])
        late = [self.end]
        if before:

            @pl.when(now == 0)
            def _():
                self.begin()

            return
        for at in range(count):
            todo = [f for p, f in plan if min(int(p * count), count - 1) == at]
            if at == count - 1:
                todo = todo + late
            if todo:

                @pl.when(now == at)
                def _(todo=todo):
                    for f in todo:
                        f()


STEPS_PER_HEAD = 4


def attention_back(
    queries, grads, result, lse, kv_blocks, meta, heads, up_g, outs, tile=512
):
    rows = queries.shape[0] // STEPS_PER_HEAD
    n_f, n_c, own, wide_up = up_g.shape
    count, span, blocks = queries.shape[0], kv_blocks[0].shape[0], len(kv_blocks)
    keys = span * blocks
    whole = lambda h, b, i, m: (0, 0)
    wide = pl.BlockSpec((count, heads * HD), whole)
    kv_spec = pl.BlockSpec((span, 2 * HD), lambda h, b, i, m: (0, h))
    anywhere = pl.BlockSpec(memory_space=pl.ANY)
    sem, shape = pltpu.SemaphoreType.DMA, jax.ShapeDtypeStruct

    def held(array):
        return pl.BlockSpec(array.shape, lambda h, b, i, m: (0,) * array.ndim)

    return pl.pallas_call(
        functools.partial(backward_kernel, heads, blocks, n_f, tile, rows),
        grid_spec=pltpu.PrefetchScalarGridSpec(
            num_scalar_prefetch=1,
            grid=(heads, blocks, count // rows),
            in_specs=[wide] * 3
            + [pl.BlockSpec((heads, count), whole)]
            + [held(up_g), held(outs)]
            + [kv_spec] * blocks,
            out_specs=[
                wide,
                kv_spec,
                pl.BlockSpec((own, wide_up), whole),
                anywhere,
                anywhere,
            ],
            scratch_shapes=[
                pltpu.VMEM((span, 2 * HD), jnp.bfloat16),
                pltpu.VMEM((span, 2 * HD), jnp.bfloat16),
                pltpu.VMEM((2 * HD, span), jnp.bfloat16),
                pltpu.VMEM((span, 128), jnp.float32),
                pltpu.VMEM((rows, 2 * HD), jnp.float32),
                pltpu.VMEM((rows, 2 * HD), jnp.float32),
                pltpu.VMEM((rows, 2 * HD), jnp.float32),
                pltpu.VMEM((span, 2 * HD), jnp.float32),
                pltpu.VMEM((span, 2 * HD), jnp.float32),
                pltpu.VMEM((2 * HD, count), jnp.float32),
                pltpu.VMEM((2, n_c - 1, span, 2 * HD), jnp.float32),
                pltpu.VMEM((count, 4 * HD), jnp.bfloat16),
                pltpu.VMEM((count, 4 * HD), jnp.bfloat16),
                pltpu.VMEM((count, 2 * HD), jnp.bfloat16),
                pltpu.VMEM((count, 2 * HD), jnp.bfloat16),
                pltpu.VMEM((1, count), jnp.float32),
                *ring_scratch(n_f, n_c, own, wide_up),
                sem((2, heads, n_c - 1)),
                sem((2, 2)),
            ],
        ),
        out_shape=[
            shape((count, heads * HD), jnp.float32),
            shape((span, 2 * heads * HD), jnp.float32),
            shape((own, wide_up), jnp.float32),
            shape((n_c - 1, span, 2 * heads * HD), jnp.float32),
            shape((outs.shape[0], 2) + outs.shape[1:], jnp.float32),
        ],
        compiler_params=pltpu.CompilerParams(
            dimension_semantics=("arbitrary",) * 3,
            collective_id=2,
            has_side_effects=True,
            vmem_limit_bytes=62 << 20,
        ),
        cost_estimate=pl.CostEstimate(
            flops=60 * heads * count * keys * HD,
            bytes_accessed=16 * keys * heads * HD + 16 * count * heads * HD,
            transcendentals=heads * count * keys,
        ),
        name="attention_backward",
    )(meta, queries, grads, result, lse, up_g, outs, *kv_blocks)


def dot_three(left, right, left_dim, right_dim):
    left_high, left_low = left
    right_high, right_low = right
    return dot(left_high, right_high, left_dim, right_dim) + (
        dot(left_high, right_low, left_dim, right_dim)
        + dot(left_low, right_high, left_dim, right_dim)
    )


def tiles_of(count, body):
    tile = 256 if count % 256 == 0 else count

    def step(n, _):
        body(pl.ds(pl.multiple_of(n * tile, tile), tile))
        return 0

    lax.fori_loop(0, count // tile, step, 0)


def middle_kernel(
    chunks, rows, n_c,
    att_ref, ups, downs, outw_ref,
    b_out_1, gain_1_1, shift_1_1, b_up_1, b_down_1, gain_2_1, shift_2_1, tok_hbm, cot_hbm,
    out_own, mid_own, gatt, d_up, d_out, d_down_out, vec, d_bup,
    part, rx0, rx1, full, act_hi, act_lo, slope, tok, cot, norm_1, recip_1,
    up_s, down_s, outw_s, xs, ys, ts, send0, recv0, send1, recv1, own_sem,
    lines, b_up, *blocked,
):
    half = rows // 2
    me = lax.axis_index("tp")
    bit0, bit1 = me % 2, me // 2 % 2
    peer0, peer1 = me + 1 - 2 * bit0, me + 2 - 4 * bit1
    home0 = pl.multiple_of(bit0 * half, half)
    away0 = pl.multiple_of((1 - bit0) * half, half)
    own = pl.ds(home0, half)

    def remote_tp(src, dst, send, recv, peer):
        return remote(src, dst, send, recv, tp=peer)

    width, hidden = up_s.shape[1], up_s.shape[2]
    d_down = d_down_out
    if blocked:
        whole, w_sem, wl_sem, d_down, *ring_refs = blocked
        n_f, own_w = ups.shape[0], ups.shape[1]
        at = lax.axis_index("ctx")
        ring = Ring(
            n_f, n_c, row_block(d_down, own_w, n_f, n_c), *ring_refs, keeper(d_down_out)
        )

        def columns_of(part_at):
            return pl.ds(part_at * hidden, hidden)

        def w_copies(part_at):
            cols = columns_of(part_at)
            for k in range(n_f):
                if part_at:
                    for m in range(n_c):
                        yield pltpu.make_async_copy(
                            downs.at[k, m], whole.at[k, m, :, cols], wl_sem.at[1, k, m]
                        )
                    continue
                yield pltpu.make_async_copy(
                    ups.at[k], whole.at[k, at, :, cols], wl_sem.at[0, k, 0]
                )
                for m in range(1, n_c):
                    yield remote(
                        ups.at[k],
                        whole.at[k, at, :, cols],
                        w_sem.at[0, k, m - 1],
                        w_sem.at[1, k, m - 1],
                        ctx=(at + m) % n_c,
                    )

    def scatter0(s, c):
        return remote_tp(
            part.at[c, pl.ds(away0, half)], rx0.at[c], send0.at[0, s, c], recv0.at[0, s, c], peer0
        )

    def swap1(s, c):
        return remote_tp(
            part.at[c, own], rx1.at[s % 2, c], send1.at[s, c], recv1.at[s, c], peer1
        )

    def gather0(s, c):
        return remote_tp(
            full.at[s, c, own], full.at[s, c, own], send0.at[1, s, c], recv0.at[1, s, c], peer0
        )

    def own_copies(c):
        where = pl.ds(pl.multiple_of(c * rows + home0, half), half)
        return (
            pltpu.make_async_copy(tok_hbm.at[where], tok.at[c], own_sem.at[0, c]),
            pltpu.make_async_copy(cot_hbm.at[where], cot.at[c], own_sem.at[1, c]),
        )

    for c in range(chunks):
        for copy in own_copies(c):
            copy.start()
    barrier = pltpu.get_barrier_semaphore()
    peers = [{"tp": peer0}, {"tp": peer1}]
    if blocked:
        peers += [{"ctx": (at + m) % n_c} for m in range(1, n_c)]
        at_f = lax.axis_index("fsdp")
        peers += [{"fsdp": (at_f + k) % n_f} for k in sorted({1, n_f - 1})]
    for peer in peers:
        pl.semaphore_signal(barrier, inc=1, device_id=peer, device_id_type=pl.DeviceIdType.MESH)

    firsts = (b_out_1, gain_1_1, shift_1_1, b_down_1, gain_2_1, shift_2_1)
    for i, vector in enumerate(firsts):
        lines[i : i + 1, :] = row(vector)
    b_up[...] = row(b_up_1)
    b_out, gain_1, shift_1, b_down, gain_2, shift_2 = (
        lines.at[i : i + 1] for i in range(len(firsts))
    )

    def split_rows(source, target):
        count = source.shape[0]
        step = 128

        def one(i, _):
            at = pl.ds(pl.multiple_of(i * step, step), step)
            target[0, at, :], target[1, at, :] = halves(source[at, :])
            return 0

        lax.fori_loop(0, count // step, one, 0)

    split_rows(outw_ref, outw_s)

    def weights_ready(part_at, target):
        if not blocked:
            split_rows((ups, downs)[part_at], target)
            return
        for copy in w_copies(part_at):
            copy.wait()

        def one(j, _):
            to = pl.ds(pl.multiple_of(j * own_w, own_w), own_w)
            piece = whole[j // n_c, j % n_c, :, columns_of(part_at)]
            target[0, to, :], target[1, to, :] = halves(piece)
            return 0

        lax.fori_loop(0, n_f * n_c, one, 0)

    d_bup[...] = jnp.zeros_like(d_bup)
    vec[...] = jnp.zeros_like(vec)
    d_up[...] = jnp.zeros_like(d_up)
    d_down[...] = jnp.zeros_like(d_down)
    d_out[...] = jnp.zeros_like(d_out)
    for c in range(chunks):
        for copy in own_copies(c):
            copy.wait()
    pl.semaphore_wait(barrier, len(peers))
    if blocked:
        for part_at in range(2):
            for copy in w_copies(part_at):
                copy.start()

    def split_into(target, value):
        target[0], target[1] = halves(value)

    def finish0(s, c):
        scatter0(s, c).wait()
        part[c, own, :] += rx0[c]
        swap1(s, c).start()

    def finish1(s, c):
        swap1(s, c).wait()
        return part[c, own, :] + rx1[s % 2, c]

    def pair(first, second, after):
        def one(t, _):
            @pl.when(t < chunks)
            def _():
                first(t)

            if after is not None:

                @pl.when(t >= 2)
                def _():
                    finish0(after, t - 2)

            @pl.when(t >= 1)
            def _():
                second(t - 1)

            if after is None:
                ring_step(t)
            return 0

        lax.fori_loop(0, chunks + 1, one, 0)
        if after is not None:
            finish0(after, chunks - 1)

    def at_rows(c):
        return pl.ds(pl.multiple_of(c * rows, rows), rows)

    def attention_out(c):
        left = halves(att_ref[at_rows(c), :])

        def columns(n):
            part[c, :, n] = dot_three(left, (outw_s[0, n, :], outw_s[1, n, :]), 1, 1)

        tiles_of(width, columns)
        scatter0(0, c).start()

    def nothing(c):
        del c

    pair(attention_out, nothing, 0)

    def first_norm(c):
        resid = finish1(0, c) + tok[c] + b_out[...]
        n_1, r_1 = normalized(resid)
        norm_1[c] = n_1
        recip_1[c] = jnp.broadcast_to(r_1, recip_1.shape[1:])
        full[0, c, own, :] = n_1 * gain_1[...] + shift_1[...]
        gather0(0, c).start()

    def feed_forward(c):
        @pl.when(c == 0)
        def _():
            weights_ready(0, up_s)

        gather0(0, c).wait()
        split_into(xs, full[0, c])

        def columns(n):
            pre = dot_three((xs[0], xs[1]), (up_s[0, :, n], up_s[1, :, n]), 1, 0) + b_up[:, n]
            cdf = 0.5 + 0.5 * lax.erf(pre * math.sqrt(0.5))
            slope[c, :, n] = cdf + pre * (
                jnp.exp(-0.5 * pre * pre) * (1.0 / math.sqrt(2.0 * math.pi))
            )
            act_hi[c, :, n], act_lo[c, :, n] = halves(pre * cdf)

        tiles_of(hidden, columns)

        @pl.when(c == 0)
        def _():
            weights_ready(1, down_s)

        def back(n):
            part[c, :, n] = dot_three(
                (act_hi[c], act_lo[c]), (down_s[0, n, :], down_s[1, n, :]), 1, 1
            )

        tiles_of(width, back)
        scatter0(1, c).start()

    def second_norm(c):
        ffn = finish1(1, c) + full[0, c, own, :] + b_down[...]
        n_2, r_2 = normalized(ffn)
        out_own[c] = n_2 * gain_2[...] + shift_2[...]
        grad = cot[c]
        second = norm_back(grad, gain_2[...], n_2, r_2)
        full[1, c, own, :] = second
        gather0(1, c).start()
        vec[3:4, :] += jnp.sum(second, axis=0, keepdims=True)
        vec[4:5, :] += jnp.sum(grad * n_2, axis=0, keepdims=True)
        vec[5:6, :] += jnp.sum(grad, axis=0, keepdims=True)

    def feed_back(c):
        gather0(1, c).wait()
        split_into(xs, full[1, c])

        def columns(n):
            grad = dot_three((xs[0], xs[1]), (down_s[0, :, n], down_s[1, :, n]), 1, 0)
            grad = grad * slope[c, :, n]
            slope[c, :, n] = grad
            ys[0, :, n], ys[1, :, n] = halves(grad)
            d_bup[:, n] += jnp.sum(grad, axis=0, keepdims=True)

        tiles_of(hidden, columns)

        def back(n):
            part[c, :, n] = dot_three((ys[0], ys[1]), (up_s[0, n, :], up_s[1, n, :]), 1, 1)

        tiles_of(width, back)
        scatter0(2, c).start()
        split_into(ts, full[1, c].T)

        def down_columns(n):
            d_down[:, n] += dot_three((ts[0], ts[1]), (act_hi[c, :, n], act_lo[c, :, n]), 1, 0)

        tiles_of(hidden, down_columns)

    def ring_step(slot):
        if blocked:
            for k in range(1, n_f + 1):

                @pl.when(slot == min(chunks, max(1, -(-k * chunks // n_f))))
                def _(k=k):
                    ring.event(k)

    def middle_norm(c):
        first = finish1(2, c) + full[1, c, own, :]
        n_1 = norm_1[c]
        mid = norm_back(first, gain_1[...], n_1, recip_1[c, :, :1])
        mid_own[c] = mid
        full[2, c, own, :] = mid
        gather0(2, c).start()
        vec[0:1, :] += jnp.sum(mid, axis=0, keepdims=True)
        vec[1:2, :] += jnp.sum(first * n_1, axis=0, keepdims=True)
        vec[2:3, :] += jnp.sum(first, axis=0, keepdims=True)

    def last(c):
        gather0(2, c).wait()
        mid = full[2, c]
        gatt[at_rows(c), :] = dot_three(halves(mid), (outw_s[0], outw_s[1]), 1, 0)
        split_into(ts, mid.T)
        d_out[...] += dot_three((ts[0], ts[1]), halves(att_ref[at_rows(c), :]), 1, 0)
        split_into(ts, full[0, c].T)

        def columns(n):
            d_up[:, n] += dot_three((ts[0], ts[1]), halves(slope[c, :, n]), 1, 0)

        tiles_of(hidden, columns)

    pair(first_norm, feed_forward, 1)
    pair(second_norm, feed_back, 2)
    if blocked:
        ring.begin()
    pair(middle_norm, last, None)


def middle(attended, weights, wide_out_t, vectors, tokens, cot, hidden, n_c, chunks=4):
    blocked = weights[0].ndim > 2
    count, width = tokens.shape
    split_at = attended.shape[1]
    rows = count // chunks
    half = rows // 2
    vmem = pl.BlockSpec(memory_space=pltpu.VMEM)
    anywhere = pl.BlockSpec(memory_space=pl.ANY)
    f32, bf16 = jnp.float32, jnp.bfloat16
    sems = pltpu.SemaphoreType.DMA((2, 3, chunks))
    swap_sems = pltpu.SemaphoreType.DMA((3, chunks))
    extra = [pltpu.VMEM((8, width), f32), pltpu.VMEM((1, hidden), f32)]
    if blocked:
        n_f, own = weights[0].shape[:2]
        extra += [
            pltpu.VMEM((n_f, n_c, own, 2 * hidden), f32),
            pltpu.SemaphoreType.DMA((2, n_f, n_c - 1)),
            pltpu.SemaphoreType.DMA((2, n_f, n_c)),
            pltpu.VMEM((width, hidden), f32),
            *ring_scratch(n_f, n_c, own, hidden),
        ]
    shape = jax.ShapeDtypeStruct
    return pl.pallas_call(
        functools.partial(middle_kernel, chunks, rows, n_c),
        in_specs=[vmem]
        + [anywhere if blocked else vmem] * 2
        + [vmem] * 8
        + [anywhere] * 2,
        out_specs=[vmem] * 8,
        out_shape=[
            shape((chunks, half, width), f32),
            shape((chunks, half, width), f32),
            shape((count, split_at), f32),
            shape((width, hidden), f32),
            shape((width, split_at), f32),
            shape((own if blocked else width, hidden), f32),
            shape((8, width), f32),
            shape((1, hidden), f32),
        ],
        scratch_shapes=[
            pltpu.VMEM((chunks, rows, width), f32),
            pltpu.VMEM((chunks, half, width), f32),
            pltpu.VMEM((2, chunks, half, width), f32),
            pltpu.VMEM((3, chunks, rows, width), f32),
            pltpu.VMEM((chunks, rows, hidden), bf16),
            pltpu.VMEM((chunks, rows, hidden), bf16),
            pltpu.VMEM((chunks, rows, hidden), f32),
            pltpu.VMEM((chunks, half, width), f32),
            pltpu.VMEM((chunks, half, width), f32),
            pltpu.VMEM((chunks, half, width), f32),
            pltpu.VMEM((chunks, half, 128), f32),
            pltpu.VMEM((2, width, hidden), bf16),
            pltpu.VMEM((2, width, hidden), bf16),
            pltpu.VMEM((2, width, split_at), bf16),
            pltpu.VMEM((2, rows, width), bf16),
            pltpu.VMEM((2, rows, hidden), bf16),
            pltpu.VMEM((2, width, rows), bf16),
            sems, sems, swap_sems, swap_sems,
            pltpu.SemaphoreType.DMA((2, chunks)),
            *extra,
        ],
        compiler_params=pltpu.CompilerParams(
            collective_id=1, has_side_effects=True, vmem_limit_bytes=62 << 20
        ),
        cost_estimate=pl.CostEstimate(
            flops=6 * count * width * (6 * hidden + 3 * split_at),
            bytes_accessed=4 * width * (5 * hidden + 3 * split_at),
            transcendentals=2 * count * hidden,
        ),
        name="middle",
    )(
        attended,
        *weights,
        wide_out_t,
        *vectors,
        tokens,
        cot,
    )


def front_kernel(
    heads, n_c, n_f, tile, rows, meta_ref, tok, w_qkv, up, down_t, outw_t, b_q, b_v,
    att, lse, q_out, kv_out, kv_far, wide, ups, downs, out_all,
    shard, q_s, kv_s, kv_t, wv, w_s, ow_own, kp, vt, bias, qd, acc, top_s, total_s,
    hop_sem, side_sem, up_sem, down_sem, down_side_sem, ow_sem, ow_side_sem, kv_sem, local_sem,
):
    block, head, step = pl.program_id(0), pl.program_id(1), pl.program_id(2)
    n_q = pl.num_programs(2)
    span, hidden, split_at = tok.shape[0], up.shape[1], heads * HD
    own = shard.shape[0]
    f, c = lax.axis_index("fsdp"), lax.axis_index("ctx")

    def at_f(k):
        return (f + (n_f - k)) % n_f

    def at_c(m):
        return (c + (n_c - m)) % n_c

    def lanes(h):
        return pl.ds(pl.multiple_of(h * 2 * HD, 2 * HD), 2 * HD)

    columns = (pl.ds(0, 2 * split_at), pl.ds(2 * split_at, split_at))

    def hop(p, k):
        to = wv.at[at_f(k - 1), c, :, columns[p]]
        src = shard.at[:, columns[p]] if k == 1 else to
        return remote(
            src, to, hop_sem.at[0, p, k - 1], hop_sem.at[1, p, k - 1], fsdp=at_f(-1)
        )

    def side(p, k, m):
        to = wv.at[at_f(k), c, :, columns[p]]
        src = shard.at[:, columns[p]] if k == 0 else to
        return remote(
            src, to, side_sem.at[0, p, k, m - 1], side_sem.at[1, p, k, m - 1], ctx=at_c(-m)
        )

    def up_hop(k):
        src = up if k == 1 else ups.at[at_f(k - 1)]
        return remote(
            src, ups.at[at_f(k - 1)], up_sem.at[0, k - 1], up_sem.at[1, k - 1], fsdp=at_f(-1)
        )

    def down_side(m):
        return remote(
            down_t,
            downs.at[f, c],
            down_side_sem.at[0, m - 1],
            down_side_sem.at[1, m - 1],
            ctx=at_c(-m),
        )

    def down_hop(k):
        pair = downs.at[at_f(k - 1)]
        return remote(
            pair, pair, down_sem.at[0, k - 1], down_sem.at[1, k - 1], fsdp=at_f(-1)
        )

    def ow_hop(k):
        src = ow_own if k == 1 else out_all.at[at_f(k - 1), c]
        return remote(
            src, out_all.at[at_f(k - 1), c], ow_sem.at[0, k - 1], ow_sem.at[1, k - 1], fsdp=at_f(-1)
        )

    def ow_side(k, m):
        src = ow_own if k == 0 else out_all.at[at_f(k), c]
        return remote(
            src,
            out_all.at[at_f(k), c],
            ow_side_sem.at[0, k, m - 1],
            ow_side_sem.at[1, k, m - 1],
            ctx=at_c(-m),
        )

    def kv_send(h, m):
        return remote(
            kv_s.at[:, lanes(h)],
            kv_far.at[m - 1, :, lanes(h)],
            kv_sem.at[0, h, m - 1],
            kv_sem.at[1, h, m - 1],
            ctx=at_c(-m),
        )

    def locals_of():
        return [
            pltpu.make_async_copy(a, b, local_sem.at[i])
            for i, (a, b) in enumerate(
                (
                    (up, ups.at[f]),
                    (ow_own, out_all.at[f, c]),
                    (wv, wide),
                    (q_s, q_out),
                    (kv_s, kv_out),
                    (down_t, downs.at[f, c]),
                )
            )
        ]

    def gathered(p):
        for k in range(n_f):
            for m in range(1, n_c):
                side(p, k, m).wait()

        def split(j, _):
            to = pl.ds(pl.multiple_of(j * own, own), own)
            w_s[0, to, columns[p]], w_s[1, to, columns[p]] = halves(
                wv[j // n_c, j % n_c, :, columns[p]]
            )
            return 0

        lax.fori_loop(0, n_f * n_c, split, 0)

    @pl.when((block == 0) & (head == 0) & (step == 0))
    def _():
        barrier = pltpu.get_barrier_semaphore()
        peers = [{"fsdp": at_f(-1)}] + ([{"fsdp": at_f(1)}] if n_f > 2 else [])
        peers += [{"ctx": at_c(m)} for m in range(1, n_c)]
        for peer in peers:
            pl.semaphore_signal(
                barrier, inc=1, device_id=peer, device_id_type=pl.DeviceIdType.MESH
            )
        for h in range(heads):
            at = 3 * HD * h
            shard[:, 2 * HD * h : 2 * HD * (h + 1)] = w_qkv[:, at + HD : at + 3 * HD]
            shard[:, 2 * split_at + HD * h : 2 * split_at + HD * (h + 1)] = w_qkv[:, at : at + HD]
        pl.semaphore_wait(barrier, len(peers))
        for p in range(2):
            hop(p, 1).start()
            for m in range(1, n_c):
                side(p, 0, m).start()
        wv[f, c] = shard[...]
        ow_own[...] = outw_t[...]
        for k in range(1, n_f):
            for p in range(2):
                hop(p, k).wait()
                if k < n_f - 1:
                    hop(p, k + 1).start()
                for m in range(1, n_c):
                    side(p, k, m).start()
        up_hop(1).start()
        ow_hop(1).start()
        for m in range(1, n_c):
            down_side(m).start()
        copies = locals_of()
        copies[0].start()
        copies[1].start()
        copies[5].start()
        gathered(0)
        blank = jnp.zeros((1, HD), jnp.float32)
        v_row = row(b_v)
        b_kv = jnp.concatenate(
            sum(([blank, v_row[:, h * HD : (h + 1) * HD]] for h in range(heads)), []), axis=1
        )
        q_row = row(b_q)

        def keys(i, _):
            at = pl.ds(pl.multiple_of(i * rows, rows), rows)
            right = (w_s[0, :, : 2 * split_at], w_s[1, :, : 2 * split_at])
            kv_s[at, :] = dot_three(halves(tok[at, :]), right, 1, 0) + b_kv
            return 0

        lax.fori_loop(0, span // rows, keys, 0)
        for h in range(heads):
            for m in range(1, n_c):
                kv_send(h, m).start()

        gathered(1)
        copies[2].start()

        def asking(i, _):
            at = pl.ds(pl.multiple_of(i * rows, rows), rows)
            right = (w_s[0, :, 2 * split_at :], w_s[1, :, 2 * split_at :])
            q_s[at, :] = dot_three(halves(tok[at, :]), right, 1, 0) + q_row
            return 0

        lax.fori_loop(0, span // rows, asking, 0)
        copies[3].start()
        copies[4].start()
        for m in range(1, n_c):
            ow_side(0, m).start()

    @pl.when((block == 0) & (step == 0))
    def _():
        kv_t[...] = kv_s[:, lanes(head)]

    @pl.when((block > 0) & (step == 0))
    def _():
        kv_send(head, block).wait_recv()
        copy = pltpu.make_async_copy(
            kv_far.at[block - 1, :, lanes(head)], kv_t, local_sem.at[6]
        )
        copy.start()
        copy.wait()

    @pl.when(step == 0)
    def _():
        def prepare(j, _):
            at = pl.ds(pl.multiple_of(j * tile, tile), tile)
            pair = kv_t[at, :]
            kp[at, :] = packed(pair, True)
            vt[:, at] = stacked(pair.T[HD:, :])
            bias[at, :] = key_bias(meta_ref[0], at_c(block) * span + j * tile, tile, 128)
            return 0

        lax.fori_loop(0, span // tile, prepare, 0)

    here = pl.ds(pl.multiple_of(step * rows, rows), rows)

    @pl.when(block == 0)
    def _():
        acc[head, :, here] = jnp.zeros((2 * HD, rows), jnp.float32)
        top_s[head, :, here] = jnp.full((1, rows), MASKED, jnp.float32)
        total_s[head, :, here] = jnp.zeros((1, rows), jnp.float32)

    doubled(q_s, here, head, qd, heads)
    q_high, q_low = halves(qd[...] * (LOG2E * HD**-0.5))
    q_four = jnp.concatenate([q_high, q_low], axis=1)

    def key_tile(j, carry):
        top, total = carry
        at = pl.ds(pl.multiple_of(j * tile, tile), tile)
        k_two = kp[at, :]
        scores = dot(jnp.concatenate([k_two, k_two], axis=1), q_four, 1, 1)
        scores = scores + jnp.concatenate([bias[at, :]] * (rows // 128), axis=1)
        new_top = jnp.maximum(top, jnp.max(scores, axis=0, keepdims=True))
        fade = jnp.exp2(top - new_top)
        probs = jnp.exp2(scores - new_top)
        total = total * fade + jnp.sum(probs, axis=0, keepdims=True)
        high, low = halves(probs)
        v_two = vt[:, at]
        acc[head, :, here] = acc[head, :, here] * fade + (
            dot(v_two, high, 1, 0) + dot(v_two, low, 1, 0)
        )
        return new_top, total

    top, total = lax.fori_loop(
        0, span // tile, key_tile, (top_s[head, :, here], total_s[head, :, here])
    )
    top_s[head, :, here] = top
    total_s[head, :, here] = total

    @pl.when(block == n_c - 1)
    def _():
        result = ((acc[head, :HD, here] + acc[head, HD:, here]) / total).T
        for j in range(heads):

            @pl.when(head == j)
            def _(j=j):
                att[here, j * HD : (j + 1) * HD] = result
                lse[j : j + 1, here] = top + jnp.log2(total)

    def arrived(k):
        up_hop(k).wait()
        ow_hop(k).wait()
        if k < n_f - 1:
            up_hop(k + 1).start()
            ow_hop(k + 1).start()
        for m in range(1, n_c):
            ow_side(k, m).start()

    def down_arrived(k):
        if k == 0:
            locals_of()[5].wait()
            for m in range(1, n_c):
                down_side(m).wait()
        else:
            down_hop(k).wait()
        if k < n_f - 1:
            down_hop(k + 1).start()

    count = n_c * heads * STEPS_PER_HEAD
    now = (block * heads + head) * n_q + step
    plan = [(0.03, lambda: down_arrived(0))]
    for k in range(1, n_f):
        plan.append((0.06 + 0.36 * k / (n_f - 1), lambda k=k: arrived(k)))
        plan.append((0.1 + 0.89 * k / (n_f - 1), lambda k=k: down_arrived(k)))
    plan.sort(key=lambda item: item[0])
    for share, event in plan:

        @pl.when(now == min(int(share * count), count - 1))
        def _(event=event):
            event()

    @pl.when(now == count - 1)
    def _():
        for k in range(n_f):
            for m in range(1, n_c):
                ow_side(k, m).wait()
        for h in range(heads):
            for m in range(1, n_c):
                kv_send(h, m).wait_send()
        for copy in locals_of()[:5]:
            copy.wait()


def front(tokens, w_qkv, w_up, w_down_t, w_out_t, b_query, b_value, lengths, heads, n_f, n_c, tile=512):
    span, width = tokens.shape
    own, total = w_qkv.shape
    hidden, split_at = w_up.shape[1], heads * HD
    rows = span // STEPS_PER_HEAD
    shape, sem, f32, bf16 = jax.ShapeDtypeStruct, pltpu.SemaphoreType.DMA, jnp.float32, jnp.bfloat16
    anywhere = pl.BlockSpec(memory_space=pl.ANY)

    def held(dims):
        return pl.BlockSpec(dims, lambda b, h, i, m: (0,) * len(dims))

    operands = (tokens, w_qkv, w_up, w_down_t, w_out_t, b_query, b_value)
    return pl.pallas_call(
        functools.partial(front_kernel, heads, n_c, n_f, tile, rows),
        grid_spec=pltpu.PrefetchScalarGridSpec(
            num_scalar_prefetch=1,
            grid=(n_c, heads, STEPS_PER_HEAD),
            in_specs=[held(x.shape) for x in operands],
            out_specs=[held((span, split_at)), held((heads, span))] + [anywhere] * 7,
            scratch_shapes=[
                pltpu.VMEM((own, total), f32),
                pltpu.VMEM((span, split_at), f32),
                pltpu.VMEM((span, 2 * split_at), f32),
                pltpu.VMEM((span, 2 * HD), f32),
                pltpu.VMEM((n_f, n_c, own, total), f32),
                pltpu.VMEM((2, width, total), bf16),
                pltpu.VMEM((own, split_at), f32),
                pltpu.VMEM((span, 2 * HD), bf16),
                pltpu.VMEM((2 * HD, span), bf16),
                pltpu.VMEM((span, 128), f32),
                pltpu.VMEM((rows, 2 * HD), f32),
                pltpu.VMEM((heads, 2 * HD, span), f32),
                pltpu.VMEM((heads, 1, span), f32),
                pltpu.VMEM((heads, 1, span), f32),
                sem((2, 2, n_f - 1)),
                sem((2, 2, n_f, n_c - 1)),
                sem((2, n_f - 1)),
                sem((2, n_f - 1)),
                sem((2, n_c - 1)),
                sem((2, n_f - 1)),
                sem((2, n_f, n_c - 1)),
                sem((2, heads, n_c - 1)),
                sem((7,)),
            ],
        ),
        out_shape=[
            shape((span, split_at), f32),
            shape((heads, span), f32),
            shape((span, split_at), f32),
            shape((span, 2 * split_at), f32),
            shape((n_c - 1, span, 2 * split_at), f32),
            shape((n_f, n_c, own, total), f32),
            shape((n_f, own, hidden), f32),
            shape((n_f, n_c, own, hidden), f32),
            shape((n_f, n_c, own, split_at), f32),
        ],
        compiler_params=pltpu.CompilerParams(
            dimension_semantics=("arbitrary",) * 3,
            collective_id=3,
            has_side_effects=True,
            vmem_limit_bytes=62 << 20,
        ),
        name="front",
    )(lengths, *operands)

def tail_kernel(
    chunks, rows, n_c, n_f, own,
    tok, grad_q, grad_kv, far, wide, mid, vec, d_bup, d_out,
    d_in, d_w, d_wout, d_bq, d_bv, d_bu, s_0, s_1, s_2, s_3, s_4, s_5,
    part, rx0, rx1, full, w_s, gs, ts, dw, side_rx, hop_rx, out_side, out_hop, small, small_rx,
    near_sem, far_sem, side_sem, hop_sem, out_side_sem, out_hop_sem, small_sem, local_sem,
):
    half = rows // 2
    me, f, c_at = lax.axis_index("tp"), lax.axis_index("fsdp"), lax.axis_index("ctx")
    bit0, bit1 = me % 2, me // 2 % 2
    peer0, peer1 = me + 1 - 2 * bit0, me + 2 - 4 * bit1
    home0 = pl.multiple_of(bit0 * half, half)
    away0 = pl.multiple_of((1 - bit0) * half, half)
    keep = pl.ds(home0, half)
    width, kv_width, total = tok.shape[1], grad_kv.shape[1], wide.shape[1]

    def at_f(k):
        return (f + (n_f - k)) % n_f

    def at_c(m):
        return (c_at + (n_c - m)) % n_c

    def exchange(src, dst, sems, kind, c, peer):
        return remote(src, dst, sems.at[0, kind, c], sems.at[1, kind, c], tp=peer)

    def scatter0(c):
        return exchange(part.at[c, pl.ds(away0, half)], rx0.at[c], near_sem, 0, c, peer0)

    def scatter1(c):
        return exchange(part.at[c, keep], rx1.at[c], far_sem, 0, c, peer1)

    def gather0(c):
        return exchange(full.at[c, keep], full.at[c, keep], near_sem, 1, c, peer0)

    def powers(count):
        bits, bit = [], 1
        while bit < count:
            bits.append(bit)
            bit *= 2
        return bits

    def flipped(at, bit):
        return at + bit - 2 * bit * (at // bit % 2)

    rounds = [("tp", peer0)]
    rounds += [("fsdp", flipped(f, bit)) for bit in powers(n_f)]
    rounds += [("ctx", flipped(c_at, bit)) for bit in powers(n_c)]

    def small_copy(r):
        axis, peer = rounds[r]
        return remote(
            small.at[r], small_rx.at[r], small_sem.at[0, r], small_sem.at[1, r], **{axis: peer}
        )

    def small_event(r):
        small_copy(r).wait()
        if rounds[r][0] == "tp":
            small[r + 1, :8, :] = small[r, :8, :] + small_rx[r, :8, :]
            small[r + 1, 8:, :] = small[r, 8:, :]
        else:
            small[r + 1] = small[r] + small_rx[r]
        if r + 1 < len(rounds):
            small_copy(r + 1).start()

    barrier = pltpu.get_barrier_semaphore()
    peers = [{"tp": peer0}, {"tp": peer1}]
    peers += [{"fsdp": at_f(k)} for k in range(1, n_f)]
    peers += [{"ctx": at_c(m)} for m in range(1, n_c)]
    for peer in peers:
        pl.semaphore_signal(barrier, inc=1, device_id=peer, device_id_type=pl.DeviceIdType.MESH)

    def split(i, _):
        at = pl.ds(pl.multiple_of(i * 128, 128), 128)
        w_s[0, at, :], w_s[1, at, :] = halves(wide[at, :])
        return 0

    lax.fori_loop(0, width // 128, split, 0)
    small[0, :8, :] = vec[...]
    small[0, 8:, :] = jnp.zeros_like(small[0, 8:, :])
    small[0, 8:9, :] = d_bup[...]
    dw[...] = jnp.zeros_like(dw)
    pl.semaphore_wait(barrier, len(peers))

    out_ring = Ring(
        n_f, n_c, row_block(d_out, own, n_f, n_c), out_side, out_hop, out_side_sem,
        out_hop_sem, keeper(d_wout),
    )
    out_ring.begin()

    def finish0(c):
        scatter0(c).wait()
        part[c, keep, :] += rx0[c]
        scatter1(c).start()

    def partial(c, _):
        at = pl.ds(pl.multiple_of(c * rows, rows), rows)
        kv = grad_kv[at, :]
        for m in range(n_c - 1):
            kv = kv + far[m, at, :]
        grad = jnp.concatenate([kv, grad_q[at, :]], axis=1)
        gs[c, 0], gs[c, 1] = halves(grad)
        small[0, 9:10, :total] += jnp.sum(grad, axis=0, keepdims=True)

        def columns(n):
            part[c, :, n] = dot_three((gs[c, 0], gs[c, 1]), (w_s[0, n, :], w_s[1, n, :]), 1, 1)

        tiles_of(width, columns)
        scatter0(c).start()

        @pl.when(c > 0)
        def _():
            finish0(c - 1)

        return 0

    lax.fori_loop(0, chunks, partial, 0)
    finish0(chunks - 1)
    small_copy(0).start()

    def weights(c, _):
        at = pl.ds(pl.multiple_of(c * rows, rows), rows)
        ts[0], ts[1] = halves(tok[at, :].T)

        def lines(n):
            dw[n, :] += dot_three((ts[0, n, :], ts[1, n, :]), (gs[c, 0], gs[c, 1]), 1, 0)

        tiles_of(width, lines)
        return 0

    lax.fori_loop(0, chunks, weights, 0)
    qkv_ring = Ring(
        n_f, n_c, row_block(dw, own, n_f, n_c), side_rx, hop_rx, side_sem, hop_sem,
        lambda result: grouped(d_w, result),
    )
    qkv_ring.begin()
    heads = (total - kv_width) // HD

    def grouped(target, value):
        for h in range(heads):
            at = 3 * HD * h
            target[:, at : at + HD] = value[:, kv_width + HD * h : kv_width + HD * (h + 1)]
            target[:, at + HD : at + 3 * HD] = value[:, 2 * HD * h : 2 * HD * (h + 1)]

    def finish1(c):
        scatter1(c).wait()
        full[c, keep, :] = part[c, keep, :] + rx1[c] + mid[c]
        gather0(c).start()

    def leave(c):
        return pltpu.make_async_copy(full.at[c], d_in.at[c], local_sem.at[c])

    plan = [(17 + 8.6 * c, lambda c=c: finish1(c)) for c in range(chunks)]
    plan += [(5 + 10 * k / n_f, lambda k=k: out_ring.event(k)) for k in range(1, n_f + 1)]
    plan += [(17 + 24 * k / n_f, lambda k=k: qkv_ring.event(k)) for k in range(1, n_f + 1)]
    plan += [
        (15 + 30 * (r + 1) / len(rounds), lambda r=r: small_event(r)) for r in range(len(rounds))
    ]
    plan.sort(key=lambda item: item[0])
    for _, event in plan:
        event()
    last = len(rounds)
    for i, target in enumerate((s_0, s_1, s_2, s_3, s_4, s_5)):
        target[...] = small[last, i : i + 1, :].reshape(-1)
    d_bu[...] = small[last, 8:9, :].reshape(-1)
    d_bq[...] = small[last, 9:10, kv_width:total].reshape(-1)
    by_value = [
        small[last, 9:10, 2 * HD * h + HD : 2 * HD * (h + 1)] for h in range(heads)
    ]
    d_bv[...] = jnp.concatenate(by_value, axis=1).reshape(-1)
    for c in range(chunks):
        gather0(c).wait()
        leave(c).start()
    for c in range(chunks):
        leave(c).wait()


def tail(tokens, grad_q, grad_kv, far, wide, mid, vec, d_bup, d_out, n_f, n_c, own):
    count, width = tokens.shape
    total, chunks, rows = wide.shape[1], mid.shape[0], 2 * mid.shape[1]
    vmem, anywhere = pl.BlockSpec(memory_space=pltpu.VMEM), pl.BlockSpec(memory_space=pl.ANY)
    shape, sem, f32, bf16 = jax.ShapeDtypeStruct, pltpu.SemaphoreType.DMA, jnp.float32, jnp.bfloat16
    rounds = 1 + (n_f - 1).bit_length() + (n_c - 1).bit_length()
    return pl.pallas_call(
        functools.partial(tail_kernel, chunks, rows, n_c, n_f, own),
        in_specs=[vmem] * 9,
        out_specs=[anywhere] + [vmem] * 11,
        out_shape=[
            shape((chunks, rows, width), f32),
            shape((own, total), f32),
            shape((own, d_out.shape[1]), f32),
            shape((total - grad_kv.shape[1],), f32),
            shape((total - grad_kv.shape[1],), f32),
        ]
        + [shape((width,), f32)] * 7,
        scratch_shapes=[
            pltpu.VMEM((chunks, rows, width), f32),
            pltpu.VMEM((chunks, rows // 2, width), f32),
            pltpu.VMEM((chunks, rows // 2, width), f32),
            pltpu.VMEM((chunks, rows, width), f32),
            pltpu.VMEM((2, width, total), bf16),
            pltpu.VMEM((chunks, 2, rows, total), bf16),
            pltpu.VMEM((2, width, rows), bf16),
            pltpu.VMEM((width, total), f32),
            pltpu.VMEM((n_f, n_c - 1, own, total), f32),
            pltpu.VMEM((n_f - 1, own, total), f32),
            pltpu.VMEM((n_f, n_c - 1, own, d_out.shape[1]), f32),
            pltpu.VMEM((n_f - 1, own, d_out.shape[1]), f32),
            pltpu.VMEM((rounds + 1, 16, width), f32),
            pltpu.VMEM((rounds, 16, width), f32),
            sem((2, 2, chunks)),
            sem((2, 2, chunks)),
            sem((2, n_f, n_c - 1)),
            sem((2, n_f - 1)),
            sem((2, n_f, n_c - 1)),
            sem((2, n_f - 1)),
            sem((2, rounds)),
            sem((chunks,)),
        ],
        compiler_params=pltpu.CompilerParams(
            collective_id=4, has_side_effects=True, vmem_limit_bytes=62 << 20
        ),
        name="tail",
    )(tokens, grad_q, grad_kv, far, wide, mid, vec, d_bup, d_out)

def finish_kernel(bigs, *refs):
    count = (len(refs) - bigs - 1) // 2
    given, results, stages, sem = refs[:count], refs[count : 2 * count], refs[2 * count : -1], refs[-1]
    pieces = [(i, c) for i in range(bigs) for c in range(given[i].shape[0])]

    def inward(i, c):
        return pltpu.make_async_copy(given[i].at[c], stages[i].at[c], sem.at[0, i, c])

    def outward(i, c):
        return pltpu.make_async_copy(stages[i].at[c], results[i].at[c], sem.at[1, i, c])

    for i, c in pieces:
        inward(i, c).start()
    for source, target in zip(given[bigs:], results[bigs:]):
        target[...] = source[...]
    for i, c in pieces:
        inward(i, c).wait()
        outward(i, c).start()
    for i, c in pieces:
        outward(i, c).wait()


def finish(large, small):
    anywhere, vmem = pl.BlockSpec(memory_space=pl.ANY), pl.BlockSpec(memory_space=pltpu.VMEM)
    specs = [anywhere] * len(large) + [vmem] * len(small)
    return pl.pallas_call(
        functools.partial(finish_kernel, len(large)),
        in_specs=specs,
        out_specs=specs,
        out_shape=[jax.ShapeDtypeStruct(x.shape, x.dtype) for x in (*large, *small)],
        scratch_shapes=[pltpu.VMEM(x.shape, x.dtype) for x in large]
        + [pltpu.SemaphoreType.DMA((2, len(large), max(x.shape[0] for x in large)))],
        name="finish",
    )(*large, *small)


def per_device(
    inputs,
    lengths,
    w_qkv,
    b_query,
    b_value,
    w_out,
    b_out,
    gain_attn,
    shift_attn,
    w_up,
    b_up,
    w_down,
    b_down,
    gain_ffn,
    shift_ffn,
    cotangent,
):
    width = inputs.shape[-1]
    block_len = inputs.shape[1]
    heads = b_query.shape[0] // HD
    split_at = heads * HD
    hidden = b_up.shape[0]
    tokens = inputs.reshape(block_len, width)
    cot = cotangent.reshape(block_len, width)
    length = lengths[0]
    n_c = lax.axis_size("ctx")
    at_c = lax.axis_index("ctx")

    def regroup(columns):
        parts = columns.reshape(columns.shape[:-1] + (heads, 3 * HD))
        lead = columns.shape[:-1]
        return jnp.concatenate(
            [
                parts[..., HD:].reshape(lead + (2 * split_at,)),
                parts[..., :HD].reshape(lead + (split_at,)),
            ],
            axis=-1,
        )

    bias_kv = jnp.stack(
        [jnp.zeros((heads, HD), jnp.float32), b_value.reshape(heads, HD)], axis=1
    ).reshape(-1)
    n_f, own = lax.axis_size("fsdp"), w_up.shape[0]
    fused = own % 16 == 0 and n_c > 1 and n_f > 1 and hidden == width
    if fused:
        attended, log_sums, queries, kv_own, kv_far, wide, *weights, wide_out_t = front(
            tokens, w_qkv, w_up, w_down.T, w_out.T, b_query, b_value, lengths, heads, n_f, n_c,
        )
        wide = wide.reshape(width, 3 * split_at)
        wide_kv, wide_q = wide[:, : 2 * split_at], wide[:, 2 * split_at :]
        wide_out_t = wide_out_t.reshape(width, split_at)
        kv_blocks = [kv_own] + [kv_far[m] for m in range(n_c - 1)]
    else:
        wide_kv, wide_q = weight_gather(regroup(w_qkv), [2 * split_at, split_at])
        rest = jnp.concatenate([w_up, w_down.T, w_out.T], axis=1)
        wide_up, wide_down_t, wide_out_t = weight_gather(rest, [hidden, hidden, split_at])
        weights = (wide_up, wide_down_t)
        kv_blocks = [contract(tokens, wide_kv, 1, 0) + bias_kv]
        for m in range(1, n_c):
            kv_blocks.append(ringed(kv_blocks[-1], "ctx", 1))
        queries = contract(tokens, wide_q, 1, 0) + b_query
        meta = jnp.stack([length] + [(at_c - m) % n_c * block_len for m in range(n_c)])
        attended, log_sums = attention(queries, kv_blocks, meta, heads)

    vectors = (b_out, gain_attn, shift_attn, b_up, b_down, gain_ffn, shift_ffn)
    outs, grad_mid, grad_att, d_up, d_out, d_wdown_t, vec_rows, d_bup = middle(
        attended, weights, wide_out_t, vectors, tokens, cot, hidden, n_c
    )
    blocked = (lax.axis_size("fsdp"), n_c, w_up.shape[0])
    grad_q, grad_kv, d_wup, kv_back, outputs = attention_back(
        queries,
        grad_att,
        attended,
        log_sums,
        kv_blocks,
        lengths,
        heads,
        d_up.reshape(blocked + (hidden,)),
        outs,
    )
    if fused:
        d_inputs, *small = tail(
            tokens, grad_q, grad_kv, kv_back, wide, grad_mid, vec_rows, d_bup, d_out, n_f, n_c, own
        )
        outputs, d_inputs, d_wup, d_wdown_t, d_wqkv, d_wout_t, d_bquery, d_bvalue, d_bup, *sums = (
            finish([outputs.reshape(d_inputs.shape), d_inputs], [d_wup, d_wdown_t, *small])
        )
        d_inputs = d_inputs.reshape(block_len, width)
    else:
        for m in range(n_c - 1):
            grad_kv = grad_kv + kv_back[m]
        back = contract(grad_kv, wide_kv, 1, 1) + contract(grad_q, wide_q, 1, 1)
        tail_sums = small_sum(
            jnp.concatenate([jnp.sum(grad_kv, axis=0), jnp.sum(grad_q, axis=0), d_bup[0]]),
            ("fsdp", "ctx"),
        )
        d_wdown_t, d_wout_t = grad_scatter([d_wdown_t]), grad_scatter([d_out])
        proj_sums, d_bup = tail_sums[: 3 * split_at], tail_sums[3 * split_at :]
        sums = small_sum(vec_rows + swapped(vec_rows, "tp", 1), ("fsdp", "ctx"))
        d_inputs = half_gather(grad_mid + half_scatter(back, grad_mid.shape[0]))
        own_dw = grad_scatter([contract(tokens, grad_kv, 0, 0), contract(tokens, grad_q, 0, 0)])
        d_wqkv = jnp.concatenate(
            [
                own_dw[:, 2 * split_at :].reshape(own, heads, HD),
                own_dw[:, : 2 * split_at].reshape(own, heads, 2 * HD),
            ],
            axis=2,
        ).reshape(own, 3 * split_at)
        d_bvalue = proj_sums[: 2 * split_at].reshape(heads, 2, HD)[:, 1].reshape(-1)
        d_bquery = proj_sums[2 * split_at : 3 * split_at]
    d_wdown, d_wout = d_wdown_t.T, d_wout_t.T
    return (
        outputs.reshape(1, block_len, width),
        d_inputs.reshape(1, block_len, width),
        d_wqkv,
        d_bquery,
        d_bvalue,
        d_wout,
        sums[0],
        sums[1],
        sums[2],
        d_wup,
        d_bup,
        d_wdown,
        sums[3],
        sums[4],
        sums[5],
    )


def solution(mesh):
    rows_of, cols_of = P(("fsdp", "ctx"), "tp"), P("tp", ("fsdp", "ctx"))
    seq, by_tp, same = P("fsdp", "ctx", None), P("tp"), P()
    in_specs = (
        seq, P("fsdp"), rows_of, by_tp, by_tp, cols_of, same, same, same,
        rows_of, by_tp, cols_of, same, same, same, seq,
    )
    out_specs = (
        seq, seq, rows_of, by_tp, by_tp, cols_of, same, same, same,
        rows_of, by_tp, cols_of, same, same, same,
    )
    return jax.shard_map(
        per_device, mesh=mesh, in_specs=in_specs, out_specs=out_specs, check_vma=False
    )
```

```python
import functools
import math

import jax
import jax.numpy as jnp
from jax import lax
from jax.experimental import pallas as pl
from jax.experimental.pallas import tpu as pltpu
from jax.sharding import PartitionSpec as P

HD = 64
LOG2E = math.log2(math.e)
NORM_EPS = 1e-12
MASKED = -1e30
THREE = lax.Precision.HIGH


def contract(left, right, left_dim, right_dim):
    return lax.dot_general(
        left,
        right,
        (((left_dim,), (right_dim,)), ((), ())),
        precision=THREE,
        preferred_element_type=jnp.float32,
    )


def ringed(block, axis, distance):
    count = lax.axis_size(axis)
    return lax.ppermute(block, axis, [(i, (i + distance) % count) for i in range(count)])


def swapped(block, axis, bit):
    return lax.ppermute(block, axis, [(i, i ^ bit) for i in range(lax.axis_size(axis))])


def bits_of(axis):
    bits, bit = [], 1
    while bit < lax.axis_size(axis):
        bits.append(bit)
        bit *= 2
    return bits


def half_scatter(part, chunks):
    upper = lax.axis_index("tp") % 2
    count, width = part.shape
    block = part.reshape(chunks, 2, count // (2 * chunks), width)
    leaving = lax.dynamic_index_in_dim(block, 1 - upper, 1, keepdims=False)
    staying = lax.dynamic_index_in_dim(block, upper, 1, keepdims=False)
    block = staying + swapped(leaving, "tp", 1)
    return block + swapped(block, "tp", 2)


def half_gather(block):
    other = swapped(block, "tp", 1)
    upper = lax.axis_index("tp") % 2 == 1
    block = jnp.where(upper, jnp.stack([other, block], axis=1), jnp.stack([block, other], axis=1))
    return block.reshape(-1, block.shape[-1])


def small_sum(vector, axes):
    for axis in axes:
        for bit in bits_of(axis):
            vector = vector + swapped(vector, axis, bit)
    return vector


def weight_gather(shard, widths):
    rows = shard.shape[0]
    n_f, n_c = lax.axis_size("fsdp"), lax.axis_size("ctx")
    at_f, at_c = lax.axis_index("fsdp"), lax.axis_index("ctx")
    wholes = [jnp.zeros((n_f * n_c * rows, width), jnp.float32) for width in widths]
    along_f = shard
    for k in range(n_f):
        if k:
            along_f = ringed(along_f, "fsdp", 1)
        along_c = along_f
        for m in range(n_c):
            if m:
                along_c = ringed(along_c, "ctx", 1)
            place = ((at_f - k) % n_f * n_c + (at_c - m) % n_c) * rows
            start = 0
            for i, width in enumerate(widths):
                wholes[i] = lax.dynamic_update_slice(
                    wholes[i], along_c[:, start : start + width], (place, 0)
                )
                start += width
    return wholes


def grad_scatter(pieces):
    n_f, n_c = lax.axis_size("fsdp"), lax.axis_size("ctx")
    at_f, at_c = lax.axis_index("fsdp"), lax.axis_index("ctx")
    rows = pieces[0].shape[0] // (n_f * n_c)

    def piece(f, c):
        start = (f % n_f * n_c + c % n_c) * rows
        cut = [lax.dynamic_slice_in_dim(p, start, rows, 0) for p in pieces]
        return cut[0] if len(cut) == 1 else jnp.concatenate(cut, axis=1)

    total = None
    for k in range(1, n_f + 1):
        over_c = piece(at_f - k, at_c - 1)
        for m in range(2, n_c + 1):
            over_c = ringed(over_c, "ctx", 1) + piece(at_f - k, at_c - m)
        total = over_c if total is None else ringed(total, "fsdp", 1) + over_c
    return total


def normalized(values):
    centred = values - jnp.mean(values, axis=-1, keepdims=True)
    spread = jnp.mean(centred * centred, axis=-1, keepdims=True)
    recip = lax.rsqrt(spread + NORM_EPS)
    return centred * recip, recip


def norm_back(grad, gain, normed, recip):
    scaled = grad * gain
    return recip * (
        scaled
        - jnp.mean(scaled, axis=-1, keepdims=True)
        - normed * jnp.mean(scaled * normed, axis=-1, keepdims=True)
    )


def halves(values):
    high = values.astype(jnp.bfloat16)
    return high, (values - high.astype(jnp.float32)).astype(jnp.bfloat16)


def low_half(shape):
    return lax.broadcasted_iota(jnp.int32, shape, 1) < HD


def dot(left, right, left_dim, right_dim):
    return lax.dot_general(
        left, right, (((left_dim,), (right_dim,)), ((), ())), preferred_element_type=jnp.float32
    )


def doubled(ref, rows, head, scratch, heads):
    for j in range(heads):

        @pl.when(head == j)
        def _():
            piece = ref[rows, j * HD : (j + 1) * HD]
            scratch[...] = jnp.concatenate([piece, piece], axis=1)


def packed(pair, first):
    low = low_half(pair.shape)
    turned = pltpu.roll(pair, HD, 1)
    twice = jnp.where(low, pair, turned) if first else jnp.where(low, turned, pair)
    high, rest = halves(twice)
    return jnp.where(low, high.astype(jnp.float32), rest.astype(jnp.float32)).astype(jnp.bfloat16)


def stacked(half):
    high, rest = halves(half)
    return jnp.concatenate([high, rest], axis=0)


def key_bias(limit, first, count, width):
    place = first + lax.broadcasted_iota(jnp.int32, (count, width), 0)
    return jnp.where(place < limit, 0.0, MASKED)


def row(ref):
    return ref[...].reshape(1, -1)


def forward_kernel(heads, blocks, tile, rows, meta_ref, q_ref, *refs):
    kv_refs, (out_ref, lse_ref, kp, vt, bias, qd, acc) = refs[:blocks], refs[blocks:]
    head, step = pl.program_id(0), pl.program_id(1)
    span = kv_refs[0].shape[0]
    per = span // tile

    @pl.when(step == 0)
    def _():
        for b in range(blocks):

            def prepare(j, _, b=b):
                at = pl.ds(pl.multiple_of(j * tile, tile), tile)
                to = pl.ds(pl.multiple_of(b * span + j * tile, tile), tile)
                pair = kv_refs[b][at, :]
                kp[to, :] = packed(pair, True)
                vt[:, to] = stacked(pair.T[HD:, :])
                bias[to, :] = key_bias(meta_ref[0], meta_ref[1 + b] + j * tile, tile, 128)
                return 0

            lax.fori_loop(0, per, prepare, 0)

    here = pl.ds(pl.multiple_of(step * rows, rows), rows)
    doubled(q_ref, here, head, qd, heads)
    q_high, q_low = halves(qd[...] * (LOG2E * HD**-0.5))
    q_four = jnp.concatenate([q_high, q_low], axis=1)
    acc[...] = jnp.zeros_like(acc)

    def key_tile(j, carry):
        top, total = carry
        at = pl.ds(pl.multiple_of(j * tile, tile), tile)
        k_two = kp[at, :]
        scores = dot(jnp.concatenate([k_two, k_two], axis=1), q_four, 1, 1)
        scores = scores + jnp.concatenate([bias[at, :]] * (rows // 128), axis=1)
        new_top = jnp.maximum(top, jnp.max(scores, axis=0, keepdims=True))
        fade = jnp.exp2(top - new_top)
        probs = jnp.exp2(scores - new_top)
        total = total * fade + jnp.sum(probs, axis=0, keepdims=True)
        high, low = halves(probs)
        v_two = vt[:, at]
        acc[...] = acc[...] * fade + (dot(v_two, high, 1, 0) + dot(v_two, low, 1, 0))
        return new_top, total

    top, total = lax.fori_loop(
        0,
        blocks * per,
        key_tile,
        (jnp.full((1, rows), MASKED, jnp.float32), jnp.zeros((1, rows), jnp.float32)),
    )
    result = acc[:HD, :] + acc[HD:, :]
    result = (result / total).T
    for j in range(heads):

        @pl.when(head == j)
        def _():
            out_ref[here, j * HD : (j + 1) * HD] = result
            lse_ref[j : j + 1, here] = top + jnp.log2(total)


def attention(queries, kv_blocks, meta, heads, rows=256, tile=512):
    count, span, blocks = queries.shape[0], kv_blocks[0].shape[0], len(kv_blocks)
    keys = span * blocks
    whole = lambda h, i, m: (0, 0)
    return pl.pallas_call(
        functools.partial(forward_kernel, heads, blocks, tile, rows),
        grid_spec=pltpu.PrefetchScalarGridSpec(
            num_scalar_prefetch=1,
            grid=(heads, count // rows),
            in_specs=[pl.BlockSpec((count, heads * HD), whole)]
            + [pl.BlockSpec((span, 2 * HD), lambda h, i, m: (0, h))] * blocks,
            out_specs=[
                pl.BlockSpec((count, heads * HD), whole),
                pl.BlockSpec((heads, count), whole),
            ],
            scratch_shapes=[
                pltpu.VMEM((keys, 2 * HD), jnp.bfloat16),
                pltpu.VMEM((2 * HD, keys), jnp.bfloat16),
                pltpu.VMEM((keys, 128), jnp.float32),
                pltpu.VMEM((rows, 2 * HD), jnp.float32),
                pltpu.VMEM((2 * HD, rows), jnp.float32),
            ],
        ),
        out_shape=[
            jax.ShapeDtypeStruct((count, heads * HD), jnp.float32),
            jax.ShapeDtypeStruct((heads, count), jnp.float32),
        ],
        compiler_params=pltpu.CompilerParams(dimension_semantics=("arbitrary", "arbitrary")),
        cost_estimate=pl.CostEstimate(
            flops=24 * heads * count * keys * HD,
            bytes_accessed=8 * keys * heads * HD + 8 * count * heads * HD,
            transcendentals=heads * count * keys,
        ),
        name="attention_forward",
    )(meta, queries, *kv_blocks)


def backward_kernel(
    heads, blocks, n_f, tile, rows, meta_ref, q_ref, do_ref, out_ref, lse_ref, up_g, outs,
    *refs,
):
    kv_refs = refs[:blocks]
    dq_ref, dkv_ref, up_out, kv_far, outs_all = refs[blocks : blocks + 5]
    (
        kp, vp, kt, bias, qd, dd, od, dk, dv, acc, stage, q_all, do_all, q_mix, do_mix, delta_all
    ) = refs[blocks + 5 : blocks + 21]
    transfers = Transfers(
        blocks, n_f, heads, up_g, outs, up_out, kv_far, outs_all, stage,
        *refs[blocks + 21 :],
    )
    head, order, step = pl.program_id(0), pl.program_id(1), pl.program_id(2)
    steps = pl.num_programs(2)
    now = (head * blocks + order) * steps + step
    transfers.run(now, before=True)
    span = kv_refs[0].shape[0]
    per = span // tile

    @pl.when(step == 0)
    def _():
        dk[...] = jnp.zeros_like(dk)
        dv[...] = jnp.zeros_like(dv)
        for b in range(blocks):

            @pl.when((order + 1) % blocks == b)
            def _(b=b):
                def prepare(j, _):
                    at = pl.ds(pl.multiple_of(j * tile, tile), tile)
                    pair = kv_refs[b][at, :]
                    kp[at, :] = packed(pair, True)
                    vp[at, :] = packed(pair, False)
                    kt[:, at] = stacked(pair.T[:HD, :])
                    bias[at, :] = key_bias(
                        meta_ref[0], transfers.at_c(b) * span + j * tile, tile, 128
                    )
                    return 0

                lax.fori_loop(0, per, prepare, 0)

    here = pl.ds(pl.multiple_of(step * rows, rows), rows)

    @pl.when(order == 0)
    def _():
        doubled(q_ref, here, head, qd, heads)
        doubled(do_ref, here, head, dd, heads)
        doubled(out_ref, here, head, od, heads)
        low = low_half((rows, 2 * HD))
        for value, four, mix in (
            (qd[...] * (LOG2E * HD**-0.5), q_all, q_mix),
            (dd[...], do_all, do_mix),
        ):
            high, rest = halves(value)
            four[here, : 2 * HD] = high
            four[here, 2 * HD :] = rest
            mixed = jnp.where(low, high.astype(jnp.float32), rest.astype(jnp.float32))
            mix[here, :] = mixed.astype(jnp.bfloat16)
        delta_all[:, here] = jnp.sum((dd[...] * od[...]).T[:HD, :], axis=0, keepdims=True)
        acc[:, here] = jnp.zeros((2 * HD, rows), jnp.float32)

    q_four, q_two, do_four, do_two = q_all[here, :], q_mix[here, :], do_all[here, :], do_mix[here, :]
    delta = delta_all[:, here]
    lse = lse_ref[0:1, here]
    for j in range(1, heads):
        lse = jnp.where(head == j, lse_ref[j : j + 1, here], lse)
    def key_tile(j, _):
        at = pl.ds(pl.multiple_of(j * tile, tile), tile)
        k_two, v_two = kp[at, :], vp[at, :]
        scores = dot(jnp.concatenate([k_two, k_two], axis=1), q_four, 1, 1)
        scores = scores + jnp.concatenate([bias[at, :]] * (rows // 128), axis=1)
        probs = jnp.exp2(scores - lse)
        high, rest = halves(probs)
        dv[at, :] += dot(high, do_two, 1, 0) + dot(rest, do_two, 1, 0)
        grad_p = dot(jnp.concatenate([v_two, v_two], axis=1), do_four, 1, 1)
        grad_s = probs * (grad_p - delta)
        high, rest = halves(grad_s)
        dk[at, :] += dot(high, q_two, 1, 0) + dot(rest, q_two, 1, 0)
        k_t = kt[:, at]
        acc[:, here] += dot(k_t, high, 1, 0) + dot(k_t, rest, 1, 0)
        return 0

    lax.fori_loop(0, per, key_tile, 0)

    @pl.when(order == blocks - 1)
    def _():
        result = ((acc[:HD, here] + acc[HD:, here]) * HD**-0.5).T
        for j in range(heads):

            @pl.when(head == j)
            def _(j=j):
                dq_ref[here, j * HD : (j + 1) * HD] = result

    def turned(at):
        grad_k, grad_v = dk[at, :], dv[at, :]
        grad_k = (grad_k + pltpu.roll(grad_k, HD, 1)) * (1.0 / LOG2E)
        grad_v = grad_v + pltpu.roll(grad_v, HD, 1)
        return jnp.where(low_half(grad_k.shape), grad_k, grad_v)

    for b in range(1, blocks):

        @pl.when((step == steps - 1) & (order == b - 1))
        def _(b=b):
            @pl.when(head >= 2)
            def _():
                transfers.kv_copy(head - 2, b).wait_send()

            def far(j, _):
                at = pl.ds(pl.multiple_of(j * tile, tile), tile)
                stage[head % 2, b - 1, at, :] = turned(at)
                return 0

            lax.fori_loop(0, per, far, 0)
            transfers.kv_copy(head, b).start()

    @pl.when((step == steps - 1) & (order == blocks - 1))
    def _():
        def keep(j, _):
            at = pl.ds(pl.multiple_of(j * tile, tile), tile)
            dkv_ref[at, :] = turned(at)
            return 0

        lax.fori_loop(0, per, keep, 0)

    transfers.run(now, before=False)


def remote(src, dst, send, recv, **peer):
    return pltpu.make_async_remote_copy(
        src_ref=src,
        dst_ref=dst,
        send_sem=send,
        recv_sem=recv,
        device_id=peer,
        device_id_type=pl.DeviceIdType.MESH,
    )


class Ring:
    def __init__(self, n_f, n_c, pick, side_rx, hop_rx, side_sem, hop_sem, emit):
        self.n_f, self.n_c, self.pick, self.emit = n_f, n_c, pick, emit
        self.side_rx, self.hop_rx, self.side_sem, self.hop_sem = side_rx, hop_rx, side_sem, hop_sem
        self.next_f = (lax.axis_index("fsdp") + 1) % n_f
        self.next_c = (lax.axis_index("ctx") + 1) % n_c

    def side(self, k, m):
        return remote(
            self.pick(k, 1) if m == 1 else self.side_rx.at[k - 1, m - 2],
            self.side_rx.at[k - 1, m - 1],
            self.side_sem.at[0, k - 1, m - 1],
            self.side_sem.at[1, k - 1, m - 1],
            ctx=self.next_c,
        )

    def hop(self, k):
        src = self.side_rx.at[0, self.n_c - 2] if k == 1 else self.hop_rx.at[k - 2]
        sem = self.hop_sem
        return remote(
            src, self.hop_rx.at[k - 1], sem.at[0, k - 1], sem.at[1, k - 1], fsdp=self.next_f
        )

    def begin(self):
        for k in range(1, self.n_f + 1):
            self.side(k, 1).start()

    def event(self, k):
        for m in range(2, self.n_c + 1):
            self.side(k, m - 1).wait()
            self.side_rx[k - 1, m - 2] += self.pick(k, m)[...]
            if m < self.n_c:
                self.side(k, m).start()
        if k > 1:
            self.hop(k - 1).wait()
            result = self.hop_rx[k - 2] + self.side_rx[k - 1, self.n_c - 2]
            if k < self.n_f:
                self.hop_rx[k - 2] = result
            else:
                self.emit(result)
        if k < self.n_f:
            self.hop(k).start()


def ring_scratch(n_f, n_c, own, wide):
    sem = pltpu.SemaphoreType.DMA
    return [
        pltpu.VMEM((n_f, n_c - 1, own, wide), jnp.float32),
        pltpu.VMEM((n_f - 1, own, wide), jnp.float32),
        sem((2, n_f, n_c - 1)),
        sem((2, n_f - 1)),
    ]


def row_block(ref, own, n_f, n_c):
    f, c = lax.axis_index("fsdp"), lax.axis_index("ctx")

    def pick(k, m):
        at = (f + (n_f - k)) % n_f * n_c + (c + (n_c - m)) % n_c
        return ref.at[pl.ds(pl.multiple_of(at * own, own), own)]

    return pick


def keeper(target):
    def emit(value):
        target[...] = value

    return emit


class Transfers:
    def __init__(
        self, n_c, n_f, heads, up_g, outs, up_out, kv_far, outs_all, stage,
        side_rx, hop_rx, side_sem, hop_sem, kv_sem, out_sem,
    ):
        self.n_c, self.n_f, self.heads = n_c, n_f, heads
        self.outs, self.kv_far, self.outs_all = outs, kv_far, outs_all
        self.stage = stage
        self.kv_sem = kv_sem
        self.out_sem = out_sem
        self.f, self.c, me = lax.axis_index("fsdp"), lax.axis_index("ctx"), lax.axis_index("tp")
        self.bit0 = me % 2
        self.peer0 = me + 1 - 2 * self.bit0
        self.ring = Ring(
            n_f, n_c, lambda k, m: up_g.at[self.at_f(k), self.at_c(m)],
            side_rx, hop_rx, side_sem, hop_sem, keeper(up_out),
        )

    def at_f(self, k):
        return (self.f + (self.n_f - k)) % self.n_f

    def at_c(self, m):
        return (self.c + (self.n_c - m)) % self.n_c

    def kv_copy(self, head, m):
        lanes = pl.ds(pl.multiple_of(head * 2 * HD, 2 * HD), 2 * HD)
        return remote(
            self.stage.at[head % 2, m - 1],
            self.kv_far.at[m - 1, :, lanes],
            self.kv_sem.at[0, head, m - 1],
            self.kv_sem.at[1, head, m - 1],
            ctx=self.at_c(m),
        )

    def out_local(self):
        return pltpu.make_async_copy(
            self.outs, self.outs_all.at[:, self.bit0], self.out_sem.at[0, 1]
        )

    def out_near(self):
        return remote(
            self.outs,
            self.outs_all.at[:, self.bit0],
            self.out_sem.at[0, 0],
            self.out_sem.at[1, 0],
            tp=self.peer0,
        )

    def begin(self):
        barrier = pltpu.get_barrier_semaphore()
        peers = [{"tp": self.peer0}, {"fsdp": self.at_f(-1)}]
        if self.n_f > 2:
            peers.append({"fsdp": self.at_f(1)})
        peers += [{"ctx": self.at_c(m)} for m in range(1, self.n_c)]
        for peer in peers:
            pl.semaphore_signal(
                barrier, inc=1, device_id=peer, device_id_type=pl.DeviceIdType.MESH
            )
        pl.semaphore_wait(barrier, len(peers))
        self.ring.begin()
        self.out_local().start()
        self.out_near().start()

    def end(self):
        self.out_local().wait()
        self.out_near().wait()
        for head in range(self.heads):
            for m in range(1, self.n_c):
                if head >= self.heads - 2:
                    self.kv_copy(head, m).wait_send()
                self.kv_copy(head, m).wait_recv()

    def run(self, now, before):
        count = self.heads * self.n_c * STEPS_PER_HEAD
        plan = []
        for k in range(1, self.n_f + 1):
            plan.append((0.85 * k / self.n_f, lambda k=k: self.ring.event(k)))
        plan.sort(key=lambda item: item[0])
        late = [self.end]
        if before:

            @pl.when(now == 0)
            def _():
                self.begin()

            return
        for at in range(count):
            todo = [f for p, f in plan if min(int(p * count), count - 1) == at]
            if at == count - 1:
                todo = todo + late
            if todo:

                @pl.when(now == at)
                def _(todo=todo):
                    for f in todo:
                        f()


STEPS_PER_HEAD = 4


def attention_back(
    queries, grads, result, lse, kv_blocks, meta, heads, up_g, outs, tile=512
):
    rows = queries.shape[0] // STEPS_PER_HEAD
    n_f, n_c, own, wide_up = up_g.shape
    count, span, blocks = queries.shape[0], kv_blocks[0].shape[0], len(kv_blocks)
    keys = span * blocks
    whole = lambda h, b, i, m: (0, 0)
    wide = pl.BlockSpec((count, heads * HD), whole)
    kv_spec = pl.BlockSpec((span, 2 * HD), lambda h, b, i, m: (0, h))
    anywhere = pl.BlockSpec(memory_space=pl.ANY)
    sem, shape = pltpu.SemaphoreType.DMA, jax.ShapeDtypeStruct

    def held(array):
        return pl.BlockSpec(array.shape, lambda h, b, i, m: (0,) * array.ndim)

    return pl.pallas_call(
        functools.partial(backward_kernel, heads, blocks, n_f, tile, rows),
        grid_spec=pltpu.PrefetchScalarGridSpec(
            num_scalar_prefetch=1,
            grid=(heads, blocks, count // rows),
            in_specs=[wide] * 3
            + [pl.BlockSpec((heads, count), whole)]
            + [held(up_g), held(outs)]
            + [kv_spec] * blocks,
            out_specs=[
                wide,
                kv_spec,
                pl.BlockSpec((own, wide_up), whole),
                anywhere,
                anywhere,
            ],
            scratch_shapes=[
                pltpu.VMEM((span, 2 * HD), jnp.bfloat16),
                pltpu.VMEM((span, 2 * HD), jnp.bfloat16),
                pltpu.VMEM((2 * HD, span), jnp.bfloat16),
                pltpu.VMEM((span, 128), jnp.float32),
                pltpu.VMEM((rows, 2 * HD), jnp.float32),
                pltpu.VMEM((rows, 2 * HD), jnp.float32),
                pltpu.VMEM((rows, 2 * HD), jnp.float32),
                pltpu.VMEM((span, 2 * HD), jnp.float32),
                pltpu.VMEM((span, 2 * HD), jnp.float32),
                pltpu.VMEM((2 * HD, count), jnp.float32),
                pltpu.VMEM((2, n_c - 1, span, 2 * HD), jnp.float32),
                pltpu.VMEM((count, 4 * HD), jnp.bfloat16),
                pltpu.VMEM((count, 4 * HD), jnp.bfloat16),
                pltpu.VMEM((count, 2 * HD), jnp.bfloat16),
                pltpu.VMEM((count, 2 * HD), jnp.bfloat16),
                pltpu.VMEM((1, count), jnp.float32),
                *ring_scratch(n_f, n_c, own, wide_up),
                sem((2, heads, n_c - 1)),
                sem((2, 2)),
            ],
        ),
        out_shape=[
            shape((count, heads * HD), jnp.float32),
            shape((span, 2 * heads * HD), jnp.float32),
            shape((own, wide_up), jnp.float32),
            shape((n_c - 1, span, 2 * heads * HD), jnp.float32),
            shape((outs.shape[0], 2) + outs.shape[1:], jnp.float32),
        ],
        compiler_params=pltpu.CompilerParams(
            dimension_semantics=("arbitrary",) * 3,
            collective_id=2,
            has_side_effects=True,
            vmem_limit_bytes=62 << 20,
        ),
        cost_estimate=pl.CostEstimate(
            flops=60 * heads * count * keys * HD,
            bytes_accessed=16 * keys * heads * HD + 16 * count * heads * HD,
            transcendentals=heads * count * keys,
        ),
        name="attention_backward",
    )(meta, queries, grads, result, lse, up_g, outs, *kv_blocks)


def dot_three(left, right, left_dim, right_dim):
    left_high, left_low = left
    right_high, right_low = right
    return dot(left_high, right_high, left_dim, right_dim) + (
        dot(left_high, right_low, left_dim, right_dim)
        + dot(left_low, right_high, left_dim, right_dim)
    )


def tiles_of(count, body):
    tile = 256 if count % 256 == 0 else count

    def step(n, _):
        body(pl.ds(pl.multiple_of(n * tile, tile), tile))
        return 0

    lax.fori_loop(0, count // tile, step, 0)


def middle_kernel(
    chunks, rows, n_c,
    att_ref, ups, downs, outw_ref,
    b_out_1, gain_1_1, shift_1_1, b_up_1, b_down_1, gain_2_1, shift_2_1, tok_hbm, cot_hbm,
    out_own, mid_own, gatt, d_up, d_out, d_down_out, vec, d_bup,
    part, rx0, rx1, full, act_hi, act_lo, slope, tok, cot, norm_1, recip_1,
    up_s, down_s, outw_s, xs, ys, ts, send0, recv0, send1, recv1, own_sem,
    lines, b_up, *blocked,
):
    half = rows // 2
    me = lax.axis_index("tp")
    bit0, bit1 = me % 2, me // 2 % 2
    peer0, peer1 = me + 1 - 2 * bit0, me + 2 - 4 * bit1
    home0 = pl.multiple_of(bit0 * half, half)
    away0 = pl.multiple_of((1 - bit0) * half, half)
    own = pl.ds(home0, half)

    def remote_tp(src, dst, send, recv, peer):
        return remote(src, dst, send, recv, tp=peer)

    width, hidden = up_s.shape[1], up_s.shape[2]
    d_down = d_down_out
    if blocked:
        whole, w_sem, wl_sem, last_sem, d_down, *ring_refs = blocked
        n_f, own_w = ups.shape[0], ups.shape[1]
        at, at_f = lax.axis_index("ctx"), lax.axis_index("fsdp")
        ring = Ring(
            n_f, n_c, row_block(d_down, own_w, n_f, n_c), *ring_refs, keeper(d_down_out)
        )

        def columns_of(part_at):
            return pl.ds(part_at * hidden, hidden)

        def up_copies():
            cols = columns_of(0)
            for k in range(n_f):
                yield pltpu.make_async_copy(
                    ups.at[k], whole.at[k, at, :, cols], wl_sem.at[0, k]
                )
                for m in range(1, n_c):
                    yield remote(
                        ups.at[k],
                        whole.at[k, at, :, cols],
                        w_sem.at[0, k, m - 1],
                        w_sem.at[1, k, m - 1],
                        ctx=(at + m) % n_c,
                    )

        def down_copies():
            cols = columns_of(1)
            for k in range(n_f - 1):
                slot = (at_f + (n_f - k)) % n_f
                yield pltpu.make_async_copy(
                    downs.at[slot], whole.at[slot, :, :, cols], wl_sem.at[1, k]
                )
            slot = (at_f + 2) % n_f
            yield remote(
                downs.at[slot],
                whole.at[slot, :, :, cols],
                last_sem.at[0],
                last_sem.at[1],
                fsdp=(at_f + 1) % n_f,
            )

        def w_copies(part_at):
            return down_copies() if part_at else up_copies()

    def scatter0(s, c):
        return remote_tp(
            part.at[c, pl.ds(away0, half)], rx0.at[c], send0.at[0, s, c], recv0.at[0, s, c], peer0
        )

    def swap1(s, c):
        return remote_tp(
            part.at[c, own], rx1.at[s % 2, c], send1.at[s, c], recv1.at[s, c], peer1
        )

    def gather0(s, c):
        return remote_tp(
            full.at[s, c, own], full.at[s, c, own], send0.at[1, s, c], recv0.at[1, s, c], peer0
        )

    def own_copies(c):
        where = pl.ds(pl.multiple_of(c * rows + home0, half), half)
        return (
            pltpu.make_async_copy(tok_hbm.at[where], tok.at[c], own_sem.at[0, c]),
            pltpu.make_async_copy(cot_hbm.at[where], cot.at[c], own_sem.at[1, c]),
        )

    for c in range(chunks):
        for copy in own_copies(c):
            copy.start()
    barrier = pltpu.get_barrier_semaphore()
    peers = [{"tp": peer0}, {"tp": peer1}]
    if blocked:
        peers += [{"ctx": (at + m) % n_c} for m in range(1, n_c)]
        peers += [{"fsdp": (at_f + k) % n_f} for k in sorted({1, n_f - 1})]
    for peer in peers:
        pl.semaphore_signal(barrier, inc=1, device_id=peer, device_id_type=pl.DeviceIdType.MESH)

    firsts = (b_out_1, gain_1_1, shift_1_1, b_down_1, gain_2_1, shift_2_1)
    for i, vector in enumerate(firsts):
        lines[i : i + 1, :] = row(vector)
    b_up[...] = row(b_up_1)
    b_out, gain_1, shift_1, b_down, gain_2, shift_2 = (
        lines.at[i : i + 1] for i in range(len(firsts))
    )

    def split_rows(source, target):
        count = source.shape[0]
        step = 128

        def one(i, _):
            at = pl.ds(pl.multiple_of(i * step, step), step)
            target[0, at, :], target[1, at, :] = halves(source[at, :])
            return 0

        lax.fori_loop(0, count // step, one, 0)

    split_rows(outw_ref, outw_s)

    def weights_ready(part_at, target):
        if not blocked:
            split_rows((ups, downs)[part_at], target)
            return
        for copy in w_copies(part_at):
            copy.wait()

        def one(j, _):
            to = pl.ds(pl.multiple_of(j * own_w, own_w), own_w)
            piece = whole[j // n_c, j % n_c, :, columns_of(part_at)]
            target[0, to, :], target[1, to, :] = halves(piece)
            return 0

        lax.fori_loop(0, n_f * n_c, one, 0)

    d_bup[...] = jnp.zeros_like(d_bup)
    vec[...] = jnp.zeros_like(vec)
    d_up[...] = jnp.zeros_like(d_up)
    d_down[...] = jnp.zeros_like(d_down)
    d_out[...] = jnp.zeros_like(d_out)
    for c in range(chunks):
        for copy in own_copies(c):
            copy.wait()
    pl.semaphore_wait(barrier, len(peers))
    if blocked:
        for part_at in range(2):
            for copy in w_copies(part_at):
                copy.start()

    def split_into(target, value):
        target[0], target[1] = halves(value)

    def finish0(s, c):
        scatter0(s, c).wait()
        part[c, own, :] += rx0[c]
        swap1(s, c).start()

    def finish1(s, c):
        swap1(s, c).wait()
        return part[c, own, :] + rx1[s % 2, c]

    def pair(first, second, after):
        def one(t, _):
            @pl.when(t < chunks)
            def _():
                first(t)

            if after is not None:

                @pl.when(t >= 2)
                def _():
                    finish0(after, t - 2)

            @pl.when(t >= 1)
            def _():
                second(t - 1)

            if after is None:
                ring_step(t)
            return 0

        lax.fori_loop(0, chunks + 1, one, 0)
        if after is not None:
            finish0(after, chunks - 1)

    def at_rows(c):
        return pl.ds(pl.multiple_of(c * rows, rows), rows)

    def attention_out(c):
        left = halves(att_ref[at_rows(c), :])

        def columns(n):
            part[c, :, n] = dot_three(left, (outw_s[0, n, :], outw_s[1, n, :]), 1, 1)

        tiles_of(width, columns)
        scatter0(0, c).start()

    def nothing(c):
        del c

    pair(attention_out, nothing, 0)

    def first_norm(c):
        resid = finish1(0, c) + tok[c] + b_out[...]
        n_1, r_1 = normalized(resid)
        norm_1[c] = n_1
        recip_1[c] = jnp.broadcast_to(r_1, recip_1.shape[1:])
        full[0, c, own, :] = n_1 * gain_1[...] + shift_1[...]
        gather0(0, c).start()

    def feed_forward(c):
        @pl.when(c == 0)
        def _():
            weights_ready(0, up_s)

        gather0(0, c).wait()
        split_into(xs, full[0, c])

        def columns(n):
            pre = dot_three((xs[0], xs[1]), (up_s[0, :, n], up_s[1, :, n]), 1, 0) + b_up[:, n]
            cdf = 0.5 + 0.5 * lax.erf(pre * math.sqrt(0.5))
            slope[c, :, n] = cdf + pre * (
                jnp.exp(-0.5 * pre * pre) * (1.0 / math.sqrt(2.0 * math.pi))
            )
            act_hi[c, :, n], act_lo[c, :, n] = halves(pre * cdf)

        tiles_of(hidden, columns)

        @pl.when(c == 0)
        def _():
            weights_ready(1, down_s)

        def back(n):
            part[c, :, n] = dot_three(
                (act_hi[c], act_lo[c]), (down_s[0, n, :], down_s[1, n, :]), 1, 1
            )

        tiles_of(width, back)
        scatter0(1, c).start()

    def second_norm(c):
        ffn = finish1(1, c) + full[0, c, own, :] + b_down[...]
        n_2, r_2 = normalized(ffn)
        out_own[c] = n_2 * gain_2[...] + shift_2[...]
        grad = cot[c]
        second = norm_back(grad, gain_2[...], n_2, r_2)
        full[1, c, own, :] = second
        gather0(1, c).start()
        vec[3:4, :] += jnp.sum(second, axis=0, keepdims=True)
        vec[4:5, :] += jnp.sum(grad * n_2, axis=0, keepdims=True)
        vec[5:6, :] += jnp.sum(grad, axis=0, keepdims=True)

    def feed_back(c):
        gather0(1, c).wait()
        split_into(xs, full[1, c])

        def columns(n):
            grad = dot_three((xs[0], xs[1]), (down_s[0, :, n], down_s[1, :, n]), 1, 0)
            grad = grad * slope[c, :, n]
            slope[c, :, n] = grad
            ys[0, :, n], ys[1, :, n] = halves(grad)
            d_bup[:, n] += jnp.sum(grad, axis=0, keepdims=True)

        tiles_of(hidden, columns)

        def back(n):
            part[c, :, n] = dot_three((ys[0], ys[1]), (up_s[0, n, :], up_s[1, n, :]), 1, 1)

        tiles_of(width, back)
        scatter0(2, c).start()
        split_into(ts, full[1, c].T)

        def down_columns(n):
            d_down[:, n] += dot_three((ts[0], ts[1]), (act_hi[c, :, n], act_lo[c, :, n]), 1, 0)

        tiles_of(hidden, down_columns)

    def ring_step(slot):
        if blocked:
            for k in range(1, n_f + 1):

                @pl.when(slot == min(chunks, max(1, -(-k * chunks // n_f))))
                def _(k=k):
                    ring.event(k)

    def middle_norm(c):
        first = finish1(2, c) + full[1, c, own, :]
        n_1 = norm_1[c]
        mid = norm_back(first, gain_1[...], n_1, recip_1[c, :, :1])
        mid_own[c] = mid
        full[2, c, own, :] = mid
        gather0(2, c).start()
        vec[0:1, :] += jnp.sum(mid, axis=0, keepdims=True)
        vec[1:2, :] += jnp.sum(first * n_1, axis=0, keepdims=True)
        vec[2:3, :] += jnp.sum(first, axis=0, keepdims=True)

    def last(c):
        gather0(2, c).wait()
        mid = full[2, c]
        gatt[at_rows(c), :] = dot_three(halves(mid), (outw_s[0], outw_s[1]), 1, 0)
        split_into(ts, mid.T)
        d_out[...] += dot_three((ts[0], ts[1]), halves(att_ref[at_rows(c), :]), 1, 0)
        split_into(ts, full[0, c].T)

        def columns(n):
            d_up[:, n] += dot_three((ts[0], ts[1]), halves(slope[c, :, n]), 1, 0)

        tiles_of(hidden, columns)

    pair(first_norm, feed_forward, 1)
    pair(second_norm, feed_back, 2)
    if blocked:
        ring.begin()
    pair(middle_norm, last, None)


def middle(attended, weights, wide_out_t, vectors, tokens, cot, hidden, n_c, chunks=4):
    blocked = weights[0].ndim > 2
    count, width = tokens.shape
    split_at = attended.shape[1]
    rows = count // chunks
    half = rows // 2
    vmem = pl.BlockSpec(memory_space=pltpu.VMEM)
    anywhere = pl.BlockSpec(memory_space=pl.ANY)
    f32, bf16 = jnp.float32, jnp.bfloat16
    sems = pltpu.SemaphoreType.DMA((2, 3, chunks))
    swap_sems = pltpu.SemaphoreType.DMA((3, chunks))
    extra = [pltpu.VMEM((8, width), f32), pltpu.VMEM((1, hidden), f32)]
    if blocked:
        n_f, own = weights[0].shape[:2]
        extra += [
            pltpu.VMEM((n_f, n_c, own, 2 * hidden), f32),
            pltpu.SemaphoreType.DMA((2, n_f, n_c - 1)),
            pltpu.SemaphoreType.DMA((2, n_f)),
            pltpu.SemaphoreType.DMA((2,)),
            pltpu.VMEM((width, hidden), f32),
            *ring_scratch(n_f, n_c, own, hidden),
        ]
    shape = jax.ShapeDtypeStruct
    return pl.pallas_call(
        functools.partial(middle_kernel, chunks, rows, n_c),
        in_specs=[vmem]
        + [anywhere if blocked else vmem] * 2
        + [vmem] * 8
        + [anywhere] * 2,
        out_specs=[vmem] * 8,
        out_shape=[
            shape((chunks, half, width), f32),
            shape((chunks, half, width), f32),
            shape((count, split_at), f32),
            shape((width, hidden), f32),
            shape((width, split_at), f32),
            shape((own if blocked else width, hidden), f32),
            shape((8, width), f32),
            shape((1, hidden), f32),
        ],
        scratch_shapes=[
            pltpu.VMEM((chunks, rows, width), f32),
            pltpu.VMEM((chunks, half, width), f32),
            pltpu.VMEM((2, chunks, half, width), f32),
            pltpu.VMEM((3, chunks, rows, width), f32),
            pltpu.VMEM((chunks, rows, hidden), bf16),
            pltpu.VMEM((chunks, rows, hidden), bf16),
            pltpu.VMEM((chunks, rows, hidden), f32),
            pltpu.VMEM((chunks, half, width), f32),
            pltpu.VMEM((chunks, half, width), f32),
            pltpu.VMEM((chunks, half, width), f32),
            pltpu.VMEM((chunks, half, 128), f32),
            pltpu.VMEM((2, width, hidden), bf16),
            pltpu.VMEM((2, width, hidden), bf16),
            pltpu.VMEM((2, width, split_at), bf16),
            pltpu.VMEM((2, rows, width), bf16),
            pltpu.VMEM((2, rows, hidden), bf16),
            pltpu.VMEM((2, width, rows), bf16),
            sems, sems, swap_sems, swap_sems,
            pltpu.SemaphoreType.DMA((2, chunks)),
            *extra,
        ],
        compiler_params=pltpu.CompilerParams(
            collective_id=1, has_side_effects=True, vmem_limit_bytes=62 << 20
        ),
        cost_estimate=pl.CostEstimate(
            flops=6 * count * width * (6 * hidden + 3 * split_at),
            bytes_accessed=4 * width * (5 * hidden + 3 * split_at),
            transcendentals=2 * count * hidden,
        ),
        name="middle",
    )(
        attended,
        *weights,
        wide_out_t,
        *vectors,
        tokens,
        cot,
    )


def front_kernel(
    heads, n_c, n_f, tile, rows, meta_ref, tok, w_qkv, up, down_t, outw, b_q, b_v,
    att, lse, q_out, kv_out, kv_far, wide, ups, downs, out_all,
    shard, q_s, kv_s, kv_t, wv, w_s, ow_own, kp, vt, bias, qd, acc, top_s, total_s,
    hop_sem, side_sem, up_sem, down_sem, down_side_sem, ow_sem, ow_side_sem, kv_sem, local_sem,
):
    block, head, step = pl.program_id(0), pl.program_id(1), pl.program_id(2)
    n_q = pl.num_programs(2)
    span, hidden, split_at = tok.shape[0], up.shape[1], heads * HD
    own = shard.shape[0]
    f, c = lax.axis_index("fsdp"), lax.axis_index("ctx")

    def at_f(k):
        return (f + (n_f - k)) % n_f

    def at_c(m):
        return (c + (n_c - m)) % n_c

    def lanes(h):
        return pl.ds(pl.multiple_of(h * 2 * HD, 2 * HD), 2 * HD)

    columns = (pl.ds(0, 2 * split_at), pl.ds(2 * split_at, split_at))

    def hop(p, k):
        to = wv.at[at_f(k - 1), c, :, columns[p]]
        src = shard.at[:, columns[p]] if k == 1 else to
        return remote(
            src, to, hop_sem.at[0, p, k - 1], hop_sem.at[1, p, k - 1], fsdp=at_f(-1)
        )

    def side(p, k, m):
        to = wv.at[at_f(k), c, :, columns[p]]
        src = shard.at[:, columns[p]] if k == 0 else to
        return remote(
            src, to, side_sem.at[0, p, k, m - 1], side_sem.at[1, p, k, m - 1], ctx=at_c(-m)
        )

    def up_hop(k):
        src = up if k == 1 else ups.at[at_f(k - 1)]
        return remote(
            src, ups.at[at_f(k - 1)], up_sem.at[0, k - 1], up_sem.at[1, k - 1], fsdp=at_f(-1)
        )

    def down_side(m):
        return remote(
            down_t,
            downs.at[f, c],
            down_side_sem.at[0, m - 1],
            down_side_sem.at[1, m - 1],
            ctx=at_c(-m),
        )

    def down_hop(k):
        pair = downs.at[at_f(k - 1)]
        return remote(
            pair, pair, down_sem.at[0, k - 1], down_sem.at[1, k - 1], fsdp=at_f(-1)
        )

    def ow_hop(k):
        src = ow_own if k == 1 else out_all.at[at_f(k - 1), c]
        return remote(
            src, out_all.at[at_f(k - 1), c], ow_sem.at[0, k - 1], ow_sem.at[1, k - 1], fsdp=at_f(-1)
        )

    def ow_side(k, m):
        src = ow_own if k == 0 else out_all.at[at_f(k), c]
        return remote(
            src,
            out_all.at[at_f(k), c],
            ow_side_sem.at[0, k, m - 1],
            ow_side_sem.at[1, k, m - 1],
            ctx=at_c(-m),
        )

    def kv_send(h, m):
        return remote(
            kv_s.at[:, lanes(h)],
            kv_far.at[m - 1, :, lanes(h)],
            kv_sem.at[0, h, m - 1],
            kv_sem.at[1, h, m - 1],
            ctx=at_c(-m),
        )

    def locals_of():
        return [
            pltpu.make_async_copy(a, b, local_sem.at[i])
            for i, (a, b) in enumerate(
                (
                    (up, ups.at[f]),
                    (ow_own, out_all.at[f, c]),
                    (wv, wide),
                    (q_s, q_out),
                    (kv_s, kv_out),
                    (down_t, downs.at[f, c]),
                )
            )
        ]

    def gathered(p):
        for k in range(n_f):
            for m in range(1, n_c):
                side(p, k, m).wait()

        def split(j, _):
            to = pl.ds(pl.multiple_of(j * own, own), own)
            w_s[0, to, columns[p]], w_s[1, to, columns[p]] = halves(
                wv[j // n_c, j % n_c, :, columns[p]]
            )
            return 0

        lax.fori_loop(0, n_f * n_c, split, 0)

    @pl.when((block == 0) & (head == 0) & (step == 0))
    def _():
        barrier = pltpu.get_barrier_semaphore()
        peers = [{"fsdp": at_f(-1)}] + ([{"fsdp": at_f(1)}] if n_f > 2 else [])
        peers += [{"ctx": at_c(m)} for m in range(1, n_c)]
        for peer in peers:
            pl.semaphore_signal(
                barrier, inc=1, device_id=peer, device_id_type=pl.DeviceIdType.MESH
            )
        for h in range(heads):
            at = 3 * HD * h
            shard[:, 2 * HD * h : 2 * HD * (h + 1)] = w_qkv[:, at + HD : at + 3 * HD]
            shard[:, 2 * split_at + HD * h : 2 * split_at + HD * (h + 1)] = w_qkv[:, at : at + HD]
        pl.semaphore_wait(barrier, len(peers))
        for p in range(2):
            hop(p, 1).start()
            for m in range(1, n_c):
                side(p, 0, m).start()
        wv[f, c] = shard[...]
        ow_own[...] = outw[...].T
        for k in range(1, n_f):
            for p in range(2):
                hop(p, k).wait()
                if k < n_f - 1:
                    hop(p, k + 1).start()
                for m in range(1, n_c):
                    side(p, k, m).start()
        up_hop(1).start()
        ow_hop(1).start()
        for m in range(1, n_c):
            down_side(m).start()
        copies = locals_of()
        copies[0].start()
        copies[1].start()
        copies[5].start()
        gathered(0)
        blank = jnp.zeros((1, HD), jnp.float32)
        v_row = row(b_v)
        b_kv = jnp.concatenate(
            sum(([blank, v_row[:, h * HD : (h + 1) * HD]] for h in range(heads)), []), axis=1
        )
        q_row = row(b_q)

        def keys(i, _):
            at = pl.ds(pl.multiple_of(i * rows, rows), rows)
            right = (w_s[0, :, : 2 * split_at], w_s[1, :, : 2 * split_at])
            kv_s[at, :] = dot_three(halves(tok[at, :]), right, 1, 0) + b_kv
            return 0

        lax.fori_loop(0, span // rows, keys, 0)
        for h in range(heads):
            for m in range(1, n_c):
                kv_send(h, m).start()

        gathered(1)
        copies[2].start()

        def asking(i, _):
            at = pl.ds(pl.multiple_of(i * rows, rows), rows)
            right = (w_s[0, :, 2 * split_at :], w_s[1, :, 2 * split_at :])
            q_s[at, :] = dot_three(halves(tok[at, :]), right, 1, 0) + q_row
            return 0

        lax.fori_loop(0, span // rows, asking, 0)
        copies[3].start()
        copies[4].start()
        for m in range(1, n_c):
            ow_side(0, m).start()

    @pl.when((block == 0) & (step == 0))
    def _():
        kv_t[...] = kv_s[:, lanes(head)]

    @pl.when((block > 0) & (step == 0))
    def _():
        kv_send(head, block).wait_recv()
        copy = pltpu.make_async_copy(
            kv_far.at[block - 1, :, lanes(head)], kv_t, local_sem.at[6]
        )
        copy.start()
        copy.wait()

    @pl.when(step == 0)
    def _():
        def prepare(j, _):
            at = pl.ds(pl.multiple_of(j * tile, tile), tile)
            pair = kv_t[at, :]
            kp[at, :] = packed(pair, True)
            vt[:, at] = stacked(pair.T[HD:, :])
            bias[at, :] = key_bias(meta_ref[0], at_c(block) * span + j * tile, tile, 128)
            return 0

        lax.fori_loop(0, span // tile, prepare, 0)

    here = pl.ds(pl.multiple_of(step * rows, rows), rows)

    @pl.when(block == 0)
    def _():
        acc[head, :, here] = jnp.zeros((2 * HD, rows), jnp.float32)
        top_s[head, :, here] = jnp.full((1, rows), MASKED, jnp.float32)
        total_s[head, :, here] = jnp.zeros((1, rows), jnp.float32)

    doubled(q_s, here, head, qd, heads)
    q_high, q_low = halves(qd[...] * (LOG2E * HD**-0.5))
    q_four = jnp.concatenate([q_high, q_low], axis=1)

    def key_tile(j, carry):
        top, total = carry
        at = pl.ds(pl.multiple_of(j * tile, tile), tile)
        k_two = kp[at, :]
        scores = dot(jnp.concatenate([k_two, k_two], axis=1), q_four, 1, 1)
        scores = scores + jnp.concatenate([bias[at, :]] * (rows // 128), axis=1)
        new_top = jnp.maximum(top, jnp.max(scores, axis=0, keepdims=True))
        fade = jnp.exp2(top - new_top)
        probs = jnp.exp2(scores - new_top)
        total = total * fade + jnp.sum(probs, axis=0, keepdims=True)
        high, low = halves(probs)
        v_two = vt[:, at]
        acc[head, :, here] = acc[head, :, here] * fade + (
            dot(v_two, high, 1, 0) + dot(v_two, low, 1, 0)
        )
        return new_top, total

    top, total = lax.fori_loop(
        0, span // tile, key_tile, (top_s[head, :, here], total_s[head, :, here])
    )
    top_s[head, :, here] = top
    total_s[head, :, here] = total

    @pl.when(block == n_c - 1)
    def _():
        result = ((acc[head, :HD, here] + acc[head, HD:, here]) / total).T
        for j in range(heads):

            @pl.when(head == j)
            def _(j=j):
                att[here, j * HD : (j + 1) * HD] = result
                lse[j : j + 1, here] = top + jnp.log2(total)

    def arrived(k):
        up_hop(k).wait()
        ow_hop(k).wait()
        if k < n_f - 1:
            up_hop(k + 1).start()
            ow_hop(k + 1).start()
        for m in range(1, n_c):
            ow_side(k, m).start()

    def down_arrived(k):
        if k == 0:
            locals_of()[5].wait()
            for m in range(1, n_c):
                down_side(m).wait()
        else:
            down_hop(k).wait()
        if k < n_f - 2:
            down_hop(k + 1).start()

    count = n_c * heads * STEPS_PER_HEAD
    now = (block * heads + head) * n_q + step
    plan = [(0.425, lambda: down_arrived(0))]
    for k in range(1, n_f):
        plan.append((0.05 + 0.37 * (k - 1) / max(1, n_f - 2), lambda k=k: arrived(k)))
    for k in range(1, n_f - 1):
        plan.append((0.425 + 0.575 * k / (n_f - 2), lambda k=k: down_arrived(k)))
    plan.sort(key=lambda item: item[0])
    for share, event in plan:

        @pl.when(now == min(int(share * count), count - 1))
        def _(event=event):
            event()

    @pl.when(now == count - 1)
    def _():
        for k in range(n_f):
            for m in range(1, n_c):
                ow_side(k, m).wait()
        for h in range(heads):
            for m in range(1, n_c):
                kv_send(h, m).wait_send()
        for copy in locals_of()[:5]:
            copy.wait()


def front(tokens, w_qkv, w_up, w_down_t, w_out, b_query, b_value, lengths, heads, n_f, n_c, tile=512):
    span, width = tokens.shape
    own, total = w_qkv.shape
    hidden, split_at = w_up.shape[1], heads * HD
    rows = span // STEPS_PER_HEAD
    shape, sem, f32, bf16 = jax.ShapeDtypeStruct, pltpu.SemaphoreType.DMA, jnp.float32, jnp.bfloat16
    anywhere = pl.BlockSpec(memory_space=pl.ANY)

    def held(dims):
        return pl.BlockSpec(dims, lambda b, h, i, m: (0,) * len(dims))

    operands = (tokens, w_qkv, w_up, w_down_t, w_out, b_query, b_value)
    return pl.pallas_call(
        functools.partial(front_kernel, heads, n_c, n_f, tile, rows),
        grid_spec=pltpu.PrefetchScalarGridSpec(
            num_scalar_prefetch=1,
            grid=(n_c, heads, STEPS_PER_HEAD),
            in_specs=[held(x.shape) for x in operands],
            out_specs=[held((span, split_at)), held((heads, span))] + [anywhere] * 7,
            scratch_shapes=[
                pltpu.VMEM((own, total), f32),
                pltpu.VMEM((span, split_at), f32),
                pltpu.VMEM((span, 2 * split_at), f32),
                pltpu.VMEM((span, 2 * HD), f32),
                pltpu.VMEM((n_f, n_c, own, total), f32),
                pltpu.VMEM((2, width, total), bf16),
                pltpu.VMEM((own, split_at), f32),
                pltpu.VMEM((span, 2 * HD), bf16),
                pltpu.VMEM((2 * HD, span), bf16),
                pltpu.VMEM((span, 128), f32),
                pltpu.VMEM((rows, 2 * HD), f32),
                pltpu.VMEM((heads, 2 * HD, span), f32),
                pltpu.VMEM((heads, 1, span), f32),
                pltpu.VMEM((heads, 1, span), f32),
                sem((2, 2, n_f - 1)),
                sem((2, 2, n_f, n_c - 1)),
                sem((2, n_f - 1)),
                sem((2, n_f - 1)),
                sem((2, n_c - 1)),
                sem((2, n_f - 1)),
                sem((2, n_f, n_c - 1)),
                sem((2, heads, n_c - 1)),
                sem((7,)),
            ],
        ),
        out_shape=[
            shape((span, split_at), f32),
            shape((heads, span), f32),
            shape((span, split_at), f32),
            shape((span, 2 * split_at), f32),
            shape((n_c - 1, span, 2 * split_at), f32),
            shape((n_f, n_c, own, total), f32),
            shape((n_f, own, hidden), f32),
            shape((n_f, n_c, own, hidden), f32),
            shape((n_f, n_c, own, split_at), f32),
        ],
        compiler_params=pltpu.CompilerParams(
            dimension_semantics=("arbitrary",) * 3,
            collective_id=3,
            has_side_effects=True,
            vmem_limit_bytes=62 << 20,
        ),
        name="front",
    )(lengths, *operands)

def tail_kernel(
    chunks, rows, n_c, n_f, own,
    tok, grad_q, grad_kv, far, wide, mid, vec, d_bup, d_out,
    d_in, d_w, d_wout, d_bq, d_bv, d_bu, s_0, s_1, s_2, s_3, s_4, s_5,
    part, rx0, rx1, full, w_s, gs, ts, dw, side_rx, hop_rx, out_side, out_hop, small, small_rx,
    near_sem, far_sem, side_sem, hop_sem, out_side_sem, out_hop_sem, small_sem, local_sem,
):
    half = rows // 2
    me, f, c_at = lax.axis_index("tp"), lax.axis_index("fsdp"), lax.axis_index("ctx")
    bit0, bit1 = me % 2, me // 2 % 2
    peer0, peer1 = me + 1 - 2 * bit0, me + 2 - 4 * bit1
    home0 = pl.multiple_of(bit0 * half, half)
    away0 = pl.multiple_of((1 - bit0) * half, half)
    keep = pl.ds(home0, half)
    width, kv_width, total = tok.shape[1], grad_kv.shape[1], wide.shape[1]

    def at_f(k):
        return (f + (n_f - k)) % n_f

    def at_c(m):
        return (c_at + (n_c - m)) % n_c

    def exchange(src, dst, sems, kind, c, peer):
        return remote(src, dst, sems.at[0, kind, c], sems.at[1, kind, c], tp=peer)

    def scatter0(c):
        return exchange(part.at[c, pl.ds(away0, half)], rx0.at[c], near_sem, 0, c, peer0)

    def scatter1(c):
        return exchange(part.at[c, keep], rx1.at[c], far_sem, 0, c, peer1)

    def gather0(c):
        return exchange(full.at[c, keep], full.at[c, keep], near_sem, 1, c, peer0)

    def powers(count):
        bits, bit = [], 1
        while bit < count:
            bits.append(bit)
            bit *= 2
        return bits

    def flipped(at, bit):
        return at + bit - 2 * bit * (at // bit % 2)

    rounds = [("tp", peer0)]
    rounds += [("fsdp", flipped(f, bit)) for bit in powers(n_f)]
    rounds += [("ctx", flipped(c_at, bit)) for bit in powers(n_c)]

    def small_copy(r):
        axis, peer = rounds[r]
        return remote(
            small.at[r], small_rx.at[r], small_sem.at[0, r], small_sem.at[1, r], **{axis: peer}
        )

    def small_event(r):
        small_copy(r).wait()
        if rounds[r][0] == "tp":
            small[r + 1, :8, :] = small[r, :8, :] + small_rx[r, :8, :]
            small[r + 1, 8:, :] = small[r, 8:, :]
        else:
            small[r + 1] = small[r] + small_rx[r]
        if r + 1 < len(rounds):
            small_copy(r + 1).start()

    barrier = pltpu.get_barrier_semaphore()
    peers = [{"tp": peer0}, {"tp": peer1}]
    peers += [{"fsdp": at_f(k)} for k in range(1, n_f)]
    peers += [{"ctx": at_c(m)} for m in range(1, n_c)]
    for peer in peers:
        pl.semaphore_signal(barrier, inc=1, device_id=peer, device_id_type=pl.DeviceIdType.MESH)

    def split(i, _):
        at = pl.ds(pl.multiple_of(i * 128, 128), 128)
        w_s[0, at, :], w_s[1, at, :] = halves(wide[at, :])
        return 0

    lax.fori_loop(0, width // 128, split, 0)
    small[0, :8, :] = vec[...]
    small[0, 8:, :] = jnp.zeros_like(small[0, 8:, :])
    small[0, 8:9, :] = d_bup[...]
    dw[...] = jnp.zeros_like(dw)
    pl.semaphore_wait(barrier, len(peers))

    out_ring = Ring(
        n_f, n_c, row_block(d_out, own, n_f, n_c), out_side, out_hop, out_side_sem,
        out_hop_sem, keeper(d_wout),
    )
    out_ring.begin()

    def finish0(c):
        scatter0(c).wait()
        part[c, keep, :] += rx0[c]
        scatter1(c).start()

    def partial(c, _):
        at = pl.ds(pl.multiple_of(c * rows, rows), rows)
        kv = grad_kv[at, :]
        for m in range(n_c - 1):
            kv = kv + far[m, at, :]
        grad = jnp.concatenate([kv, grad_q[at, :]], axis=1)
        gs[c, 0], gs[c, 1] = halves(grad)
        small[0, 9:10, :total] += jnp.sum(grad, axis=0, keepdims=True)

        def columns(n):
            part[c, :, n] = dot_three((gs[c, 0], gs[c, 1]), (w_s[0, n, :], w_s[1, n, :]), 1, 1)

        tiles_of(width, columns)
        scatter0(c).start()

        @pl.when(c > 0)
        def _():
            finish0(c - 1)

        return 0

    lax.fori_loop(0, chunks, partial, 0)
    finish0(chunks - 1)
    small_copy(0).start()

    def weights(c, _):
        at = pl.ds(pl.multiple_of(c * rows, rows), rows)
        ts[0], ts[1] = halves(tok[at, :].T)

        def lines(n):
            dw[n, :] += dot_three((ts[0, n, :], ts[1, n, :]), (gs[c, 0], gs[c, 1]), 1, 0)

        tiles_of(width, lines)
        return 0

    lax.fori_loop(0, chunks, weights, 0)
    qkv_ring = Ring(
        n_f, n_c, row_block(dw, own, n_f, n_c), side_rx, hop_rx, side_sem, hop_sem,
        lambda result: grouped(d_w, result),
    )
    qkv_ring.begin()
    heads = (total - kv_width) // HD

    def grouped(target, value):
        for h in range(heads):
            at = 3 * HD * h
            target[:, at : at + HD] = value[:, kv_width + HD * h : kv_width + HD * (h + 1)]
            target[:, at + HD : at + 3 * HD] = value[:, 2 * HD * h : 2 * HD * (h + 1)]

    def finish1(c):
        scatter1(c).wait()
        full[c, keep, :] = part[c, keep, :] + rx1[c] + mid[c]
        gather0(c).start()

    def leave(c):
        return pltpu.make_async_copy(full.at[c], d_in.at[c], local_sem.at[c])

    plan = [(17 + 8.6 * c, lambda c=c: finish1(c)) for c in range(chunks)]
    plan += [(5 + 10 * k / n_f, lambda k=k: out_ring.event(k)) for k in range(1, n_f + 1)]
    plan += [(17 + 24 * k / n_f, lambda k=k: qkv_ring.event(k)) for k in range(1, n_f + 1)]
    plan += [
        (15 + 30 * (r + 1) / len(rounds), lambda r=r: small_event(r)) for r in range(len(rounds))
    ]
    plan.sort(key=lambda item: item[0])
    for _, event in plan:
        event()
    last = len(rounds)
    for i, target in enumerate((s_0, s_1, s_2, s_3, s_4, s_5)):
        target[...] = small[last, i : i + 1, :].reshape(-1)
    d_bu[...] = small[last, 8:9, :].reshape(-1)
    d_bq[...] = small[last, 9:10, kv_width:total].reshape(-1)
    by_value = [
        small[last, 9:10, 2 * HD * h + HD : 2 * HD * (h + 1)] for h in range(heads)
    ]
    d_bv[...] = jnp.concatenate(by_value, axis=1).reshape(-1)
    for c in range(chunks):
        gather0(c).wait()
        leave(c).start()
    for c in range(chunks):
        leave(c).wait()


def tail(tokens, grad_q, grad_kv, far, wide, mid, vec, d_bup, d_out, n_f, n_c, own):
    count, width = tokens.shape
    total, chunks, rows = wide.shape[1], mid.shape[0], 2 * mid.shape[1]
    vmem, anywhere = pl.BlockSpec(memory_space=pltpu.VMEM), pl.BlockSpec(memory_space=pl.ANY)
    shape, sem, f32, bf16 = jax.ShapeDtypeStruct, pltpu.SemaphoreType.DMA, jnp.float32, jnp.bfloat16
    rounds = 1 + (n_f - 1).bit_length() + (n_c - 1).bit_length()
    return pl.pallas_call(
        functools.partial(tail_kernel, chunks, rows, n_c, n_f, own),
        in_specs=[vmem] * 9,
        out_specs=[anywhere] + [vmem] * 11,
        out_shape=[
            shape((chunks, rows, width), f32),
            shape((own, total), f32),
            shape((own, d_out.shape[1]), f32),
            shape((total - grad_kv.shape[1],), f32),
            shape((total - grad_kv.shape[1],), f32),
        ]
        + [shape((width,), f32)] * 7,
        scratch_shapes=[
            pltpu.VMEM((chunks, rows, width), f32),
            pltpu.VMEM((chunks, rows // 2, width), f32),
            pltpu.VMEM((chunks, rows // 2, width), f32),
            pltpu.VMEM((chunks, rows, width), f32),
            pltpu.VMEM((2, width, total), bf16),
            pltpu.VMEM((chunks, 2, rows, total), bf16),
            pltpu.VMEM((2, width, rows), bf16),
            pltpu.VMEM((width, total), f32),
            pltpu.VMEM((n_f, n_c - 1, own, total), f32),
            pltpu.VMEM((n_f - 1, own, total), f32),
            pltpu.VMEM((n_f, n_c - 1, own, d_out.shape[1]), f32),
            pltpu.VMEM((n_f - 1, own, d_out.shape[1]), f32),
            pltpu.VMEM((rounds + 1, 16, width), f32),
            pltpu.VMEM((rounds, 16, width), f32),
            sem((2, 2, chunks)),
            sem((2, 2, chunks)),
            sem((2, n_f, n_c - 1)),
            sem((2, n_f - 1)),
            sem((2, n_f, n_c - 1)),
            sem((2, n_f - 1)),
            sem((2, rounds)),
            sem((chunks,)),
        ],
        compiler_params=pltpu.CompilerParams(
            collective_id=4, has_side_effects=True, vmem_limit_bytes=62 << 20
        ),
        name="tail",
    )(tokens, grad_q, grad_kv, far, wide, mid, vec, d_bup, d_out)

def finish_kernel(bigs, *refs):
    count = (len(refs) - bigs - 1) // 2
    given, results, stages, sem = refs[:count], refs[count : 2 * count], refs[2 * count : -1], refs[-1]
    pieces = [(i, c) for i in range(bigs) for c in range(given[i].shape[0])]

    def inward(i, c):
        return pltpu.make_async_copy(given[i].at[c], stages[i].at[c], sem.at[0, i, c])

    def outward(i, c):
        return pltpu.make_async_copy(stages[i].at[c], results[i].at[c], sem.at[1, i, c])

    for i, c in pieces:
        inward(i, c).start()
    for source, target in zip(given[bigs:], results[bigs:]):
        target[...] = source[...] if source.shape == target.shape else source[...].T
    for i, c in pieces:
        inward(i, c).wait()
        outward(i, c).start()
    for i, c in pieces:
        outward(i, c).wait()


def finish(large, small, turned):
    anywhere, vmem = pl.BlockSpec(memory_space=pl.ANY), pl.BlockSpec(memory_space=pltpu.VMEM)
    specs = [anywhere] * len(large) + [vmem] * len(small)
    shapes = [x.shape for x in (*large, *small)]
    shapes[turned] = shapes[turned][::-1]
    return pl.pallas_call(
        functools.partial(finish_kernel, len(large)),
        in_specs=specs,
        out_specs=specs,
        out_shape=[jax.ShapeDtypeStruct(dims, jnp.float32) for dims in shapes],
        scratch_shapes=[pltpu.VMEM(x.shape, x.dtype) for x in large]
        + [pltpu.SemaphoreType.DMA((2, len(large), max(x.shape[0] for x in large)))],
        name="finish",
    )(*large, *small)


def per_device(
    inputs,
    lengths,
    w_qkv,
    b_query,
    b_value,
    w_out,
    b_out,
    gain_attn,
    shift_attn,
    w_up,
    b_up,
    w_down,
    b_down,
    gain_ffn,
    shift_ffn,
    cotangent,
):
    width = inputs.shape[-1]
    block_len = inputs.shape[1]
    heads = b_query.shape[0] // HD
    split_at = heads * HD
    hidden = b_up.shape[0]
    tokens = inputs.reshape(block_len, width)
    cot = cotangent.reshape(block_len, width)
    length = lengths[0]
    n_c = lax.axis_size("ctx")
    at_c = lax.axis_index("ctx")

    def regroup(columns):
        parts = columns.reshape(columns.shape[:-1] + (heads, 3 * HD))
        lead = columns.shape[:-1]
        return jnp.concatenate(
            [
                parts[..., HD:].reshape(lead + (2 * split_at,)),
                parts[..., :HD].reshape(lead + (split_at,)),
            ],
            axis=-1,
        )

    bias_kv = jnp.stack(
        [jnp.zeros((heads, HD), jnp.float32), b_value.reshape(heads, HD)], axis=1
    ).reshape(-1)
    n_f, own = lax.axis_size("fsdp"), w_up.shape[0]
    fused = own % 16 == 0 and n_c > 1 and n_f > 1 and hidden == width
    if fused:
        attended, log_sums, queries, kv_own, kv_far, wide, *weights, wide_out_t = front(
            tokens, w_qkv, w_up, w_down.T, w_out, b_query, b_value, lengths, heads, n_f, n_c,
        )
        wide = wide.reshape(width, 3 * split_at)
        wide_kv, wide_q = wide[:, : 2 * split_at], wide[:, 2 * split_at :]
        wide_out_t = wide_out_t.reshape(width, split_at)
        kv_blocks = [kv_own] + [kv_far[m] for m in range(n_c - 1)]
    else:
        wide_kv, wide_q = weight_gather(regroup(w_qkv), [2 * split_at, split_at])
        rest = jnp.concatenate([w_up, w_down.T, w_out.T], axis=1)
        wide_up, wide_down_t, wide_out_t = weight_gather(rest, [hidden, hidden, split_at])
        weights = (wide_up, wide_down_t)
        kv_blocks = [contract(tokens, wide_kv, 1, 0) + bias_kv]
        for m in range(1, n_c):
            kv_blocks.append(ringed(kv_blocks[-1], "ctx", 1))
        queries = contract(tokens, wide_q, 1, 0) + b_query
        meta = jnp.stack([length] + [(at_c - m) % n_c * block_len for m in range(n_c)])
        attended, log_sums = attention(queries, kv_blocks, meta, heads)

    vectors = (b_out, gain_attn, shift_attn, b_up, b_down, gain_ffn, shift_ffn)
    outs, grad_mid, grad_att, d_up, d_out, d_wdown_t, vec_rows, d_bup = middle(
        attended, weights, wide_out_t, vectors, tokens, cot, hidden, n_c
    )
    blocked = (lax.axis_size("fsdp"), n_c, w_up.shape[0])
    grad_q, grad_kv, d_wup, kv_back, outputs = attention_back(
        queries,
        grad_att,
        attended,
        log_sums,
        kv_blocks,
        lengths,
        heads,
        d_up.reshape(blocked + (hidden,)),
        outs,
    )
    if fused:
        d_inputs, *small = tail(
            tokens, grad_q, grad_kv, kv_back, wide, grad_mid, vec_rows, d_bup, d_out, n_f, n_c, own
        )
        outputs, d_inputs, d_wup, d_wdown_t, d_wqkv, d_wout, d_bquery, d_bvalue, d_bup, *sums = (
            finish([outputs.reshape(d_inputs.shape), d_inputs], [d_wup, d_wdown_t, *small], 5)
        )
        d_inputs = d_inputs.reshape(block_len, width)
    else:
        for m in range(n_c - 1):
            grad_kv = grad_kv + kv_back[m]
        back = contract(grad_kv, wide_kv, 1, 1) + contract(grad_q, wide_q, 1, 1)
        tail_sums = small_sum(
            jnp.concatenate([jnp.sum(grad_kv, axis=0), jnp.sum(grad_q, axis=0), d_bup[0]]),
            ("fsdp", "ctx"),
        )
        d_wdown_t, d_wout = grad_scatter([d_wdown_t]), grad_scatter([d_out]).T
        proj_sums, d_bup = tail_sums[: 3 * split_at], tail_sums[3 * split_at :]
        sums = small_sum(vec_rows + swapped(vec_rows, "tp", 1), ("fsdp", "ctx"))
        d_inputs = half_gather(grad_mid + half_scatter(back, grad_mid.shape[0]))
        own_dw = grad_scatter([contract(tokens, grad_kv, 0, 0), contract(tokens, grad_q, 0, 0)])
        d_wqkv = jnp.concatenate(
            [
                own_dw[:, 2 * split_at :].reshape(own, heads, HD),
                own_dw[:, : 2 * split_at].reshape(own, heads, 2 * HD),
            ],
            axis=2,
        ).reshape(own, 3 * split_at)
        d_bvalue = proj_sums[: 2 * split_at].reshape(heads, 2, HD)[:, 1].reshape(-1)
        d_bquery = proj_sums[2 * split_at : 3 * split_at]
    d_wdown = d_wdown_t.T
    return (
        outputs.reshape(1, block_len, width),
        d_inputs.reshape(1, block_len, width),
        d_wqkv,
        d_bquery,
        d_bvalue,
        d_wout,
        sums[0],
        sums[1],
        sums[2],
        d_wup,
        d_bup,
        d_wdown,
        sums[3],
        sums[4],
        sums[5],
    )


def solution(mesh):
    rows_of, cols_of = P(("fsdp", "ctx"), "tp"), P("tp", ("fsdp", "ctx"))
    seq, by_tp, same = P("fsdp", "ctx", None), P("tp"), P()
    in_specs = (
        seq, P("fsdp"), rows_of, by_tp, by_tp, cols_of, same, same, same,
        rows_of, by_tp, cols_of, same, same, same, seq,
    )
    out_specs = (
        seq, seq, rows_of, by_tp, by_tp, cols_of, same, same, same,
        rows_of, by_tp, cols_of, same, same, same,
    )
    return jax.shard_map(
        per_device, mesh=mesh, in_specs=in_specs, out_specs=out_specs, check_vma=False
    )
```

```python
import functools
import math

import jax
import jax.numpy as jnp
from jax import lax
from jax.experimental import pallas as pl
from jax.experimental.pallas import tpu as pltpu
from jax.sharding import PartitionSpec as P

HD = 64
LOG2E = math.log2(math.e)
NORM_EPS = 1e-12
MASKED = -1e30
THREE = lax.Precision.HIGH


def contract(left, right, left_dim, right_dim):
    return lax.dot_general(
        left,
        right,
        (((left_dim,), (right_dim,)), ((), ())),
        precision=THREE,
        preferred_element_type=jnp.float32,
    )


def ringed(block, axis, distance):
    count = lax.axis_size(axis)
    return lax.ppermute(block, axis, [(i, (i + distance) % count) for i in range(count)])


def swapped(block, axis, bit):
    return lax.ppermute(block, axis, [(i, i ^ bit) for i in range(lax.axis_size(axis))])


def bits_of(axis):
    bits, bit = [], 1
    while bit < lax.axis_size(axis):
        bits.append(bit)
        bit *= 2
    return bits


def half_scatter(part, chunks):
    upper = lax.axis_index("tp") % 2
    count, width = part.shape
    block = part.reshape(chunks, 2, count // (2 * chunks), width)
    leaving = lax.dynamic_index_in_dim(block, 1 - upper, 1, keepdims=False)
    staying = lax.dynamic_index_in_dim(block, upper, 1, keepdims=False)
    block = staying + swapped(leaving, "tp", 1)
    return block + swapped(block, "tp", 2)


def half_gather(block):
    other = swapped(block, "tp", 1)
    upper = lax.axis_index("tp") % 2 == 1
    block = jnp.where(upper, jnp.stack([other, block], axis=1), jnp.stack([block, other], axis=1))
    return block.reshape(-1, block.shape[-1])


def small_sum(vector, axes):
    for axis in axes:
        for bit in bits_of(axis):
            vector = vector + swapped(vector, axis, bit)
    return vector


def weight_gather(shard, widths):
    rows = shard.shape[0]
    n_f, n_c = lax.axis_size("fsdp"), lax.axis_size("ctx")
    at_f, at_c = lax.axis_index("fsdp"), lax.axis_index("ctx")
    wholes = [jnp.zeros((n_f * n_c * rows, width), jnp.float32) for width in widths]
    along_f = shard
    for k in range(n_f):
        if k:
            along_f = ringed(along_f, "fsdp", 1)
        along_c = along_f
        for m in range(n_c):
            if m:
                along_c = ringed(along_c, "ctx", 1)
            place = ((at_f - k) % n_f * n_c + (at_c - m) % n_c) * rows
            start = 0
            for i, width in enumerate(widths):
                wholes[i] = lax.dynamic_update_slice(
                    wholes[i], along_c[:, start : start + width], (place, 0)
                )
                start += width
    return wholes


def grad_scatter(pieces):
    n_f, n_c = lax.axis_size("fsdp"), lax.axis_size("ctx")
    at_f, at_c = lax.axis_index("fsdp"), lax.axis_index("ctx")
    rows = pieces[0].shape[0] // (n_f * n_c)

    def piece(f, c):
        start = (f % n_f * n_c + c % n_c) * rows
        cut = [lax.dynamic_slice_in_dim(p, start, rows, 0) for p in pieces]
        return cut[0] if len(cut) == 1 else jnp.concatenate(cut, axis=1)

    total = None
    for k in range(1, n_f + 1):
        over_c = piece(at_f - k, at_c - 1)
        for m in range(2, n_c + 1):
            over_c = ringed(over_c, "ctx", 1) + piece(at_f - k, at_c - m)
        total = over_c if total is None else ringed(total, "fsdp", 1) + over_c
    return total


def normalized(values):
    centred = values - jnp.mean(values, axis=-1, keepdims=True)
    spread = jnp.mean(centred * centred, axis=-1, keepdims=True)
    recip = lax.rsqrt(spread + NORM_EPS)
    return centred * recip, recip


def norm_back(grad, gain, normed, recip):
    scaled = grad * gain
    return recip * (
        scaled
        - jnp.mean(scaled, axis=-1, keepdims=True)
        - normed * jnp.mean(scaled * normed, axis=-1, keepdims=True)
    )


def halves(values):
    high = values.astype(jnp.bfloat16)
    return high, (values - high.astype(jnp.float32)).astype(jnp.bfloat16)


def low_half(shape):
    return lax.broadcasted_iota(jnp.int32, shape, 1) < HD


def dot(left, right, left_dim, right_dim):
    return lax.dot_general(
        left, right, (((left_dim,), (right_dim,)), ((), ())), preferred_element_type=jnp.float32
    )


def doubled(ref, rows, head, scratch, heads):
    for j in range(heads):

        @pl.when(head == j)
        def _():
            piece = ref[rows, j * HD : (j + 1) * HD]
            scratch[...] = jnp.concatenate([piece, piece], axis=1)


def packed(pair, first):
    low = low_half(pair.shape)
    turned = pltpu.roll(pair, HD, 1)
    twice = jnp.where(low, pair, turned) if first else jnp.where(low, turned, pair)
    high, rest = halves(twice)
    return jnp.where(low, high.astype(jnp.float32), rest.astype(jnp.float32)).astype(jnp.bfloat16)


def stacked(half):
    high, rest = halves(half)
    return jnp.concatenate([high, rest], axis=0)


def key_bias(limit, first, count, width):
    place = first + lax.broadcasted_iota(jnp.int32, (count, width), 0)
    return jnp.where(place < limit, 0.0, MASKED)


def row(ref):
    return ref[...].reshape(1, -1)


def forward_kernel(heads, blocks, tile, rows, meta_ref, q_ref, *refs):
    kv_refs, (out_ref, lse_ref, kp, vt, bias, qd, acc) = refs[:blocks], refs[blocks:]
    head, step = pl.program_id(0), pl.program_id(1)
    span = kv_refs[0].shape[0]
    per = span // tile

    @pl.when(step == 0)
    def _():
        for b in range(blocks):

            def prepare(j, _, b=b):
                at = pl.ds(pl.multiple_of(j * tile, tile), tile)
                to = pl.ds(pl.multiple_of(b * span + j * tile, tile), tile)
                pair = kv_refs[b][at, :]
                kp[to, :] = packed(pair, True)
                vt[:, to] = stacked(pair.T[HD:, :])
                bias[to, :] = key_bias(meta_ref[0], meta_ref[1 + b] + j * tile, tile, 128)
                return 0

            lax.fori_loop(0, per, prepare, 0)

    here = pl.ds(pl.multiple_of(step * rows, rows), rows)
    doubled(q_ref, here, head, qd, heads)
    q_high, q_low = halves(qd[...] * (LOG2E * HD**-0.5))
    q_four = jnp.concatenate([q_high, q_low], axis=1)
    acc[...] = jnp.zeros_like(acc)

    def key_tile(j, carry):
        top, total = carry
        at = pl.ds(pl.multiple_of(j * tile, tile), tile)
        k_two = kp[at, :]
        scores = dot(jnp.concatenate([k_two, k_two], axis=1), q_four, 1, 1)
        scores = scores + jnp.concatenate([bias[at, :]] * (rows // 128), axis=1)
        new_top = jnp.maximum(top, jnp.max(scores, axis=0, keepdims=True))
        fade = jnp.exp2(top - new_top)
        probs = jnp.exp2(scores - new_top)
        total = total * fade + jnp.sum(probs, axis=0, keepdims=True)
        high, low = halves(probs)
        v_two = vt[:, at]
        acc[...] = acc[...] * fade + (dot(v_two, high, 1, 0) + dot(v_two, low, 1, 0))
        return new_top, total

    top, total = lax.fori_loop(
        0,
        blocks * per,
        key_tile,
        (jnp.full((1, rows), MASKED, jnp.float32), jnp.zeros((1, rows), jnp.float32)),
    )
    result = acc[:HD, :] + acc[HD:, :]
    result = (result / total).T
    for j in range(heads):

        @pl.when(head == j)
        def _():
            out_ref[here, j * HD : (j + 1) * HD] = result
            lse_ref[j : j + 1, here] = top + jnp.log2(total)


def attention(queries, kv_blocks, meta, heads, rows=256, tile=512):
    count, span, blocks = queries.shape[0], kv_blocks[0].shape[0], len(kv_blocks)
    keys = span * blocks
    whole = lambda h, i, m: (0, 0)
    return pl.pallas_call(
        functools.partial(forward_kernel, heads, blocks, tile, rows),
        grid_spec=pltpu.PrefetchScalarGridSpec(
            num_scalar_prefetch=1,
            grid=(heads, count // rows),
            in_specs=[pl.BlockSpec((count, heads * HD), whole)]
            + [pl.BlockSpec((span, 2 * HD), lambda h, i, m: (0, h))] * blocks,
            out_specs=[
                pl.BlockSpec((count, heads * HD), whole),
                pl.BlockSpec((heads, count), whole),
            ],
            scratch_shapes=[
                pltpu.VMEM((keys, 2 * HD), jnp.bfloat16),
                pltpu.VMEM((2 * HD, keys), jnp.bfloat16),
                pltpu.VMEM((keys, 128), jnp.float32),
                pltpu.VMEM((rows, 2 * HD), jnp.float32),
                pltpu.VMEM((2 * HD, rows), jnp.float32),
            ],
        ),
        out_shape=[
            jax.ShapeDtypeStruct((count, heads * HD), jnp.float32),
            jax.ShapeDtypeStruct((heads, count), jnp.float32),
        ],
        compiler_params=pltpu.CompilerParams(dimension_semantics=("arbitrary", "arbitrary")),
        cost_estimate=pl.CostEstimate(
            flops=24 * heads * count * keys * HD,
            bytes_accessed=8 * keys * heads * HD + 8 * count * heads * HD,
            transcendentals=heads * count * keys,
        ),
        name="attention_forward",
    )(meta, queries, *kv_blocks)


def backward_kernel(
    heads, blocks, n_f, tile, rows, meta_ref, q_ref, do_ref, out_ref, lse_ref, up_g, outs,
    *refs,
):
    kv_refs = refs[:blocks]
    dq_ref, dkv_ref, up_out, kv_far, outs_all = refs[blocks : blocks + 5]
    (
        kp, vp, kt, bias, qd, dd, od, dk, dv, acc, stage, q_all, do_all, q_mix, do_mix, delta_all
    ) = refs[blocks + 5 : blocks + 21]
    transfers = Transfers(
        blocks, n_f, heads, up_g, outs, up_out, kv_far, outs_all, stage,
        *refs[blocks + 21 :],
    )
    head, order, step = pl.program_id(0), pl.program_id(1), pl.program_id(2)
    steps = pl.num_programs(2)
    now = (head * blocks + order) * steps + step
    transfers.run(now, before=True)
    span = kv_refs[0].shape[0]
    per = span // tile

    @pl.when(step == 0)
    def _():
        dk[...] = jnp.zeros_like(dk)
        dv[...] = jnp.zeros_like(dv)
        for b in range(blocks):

            @pl.when((order + 1) % blocks == b)
            def _(b=b):
                def prepare(j, _):
                    at = pl.ds(pl.multiple_of(j * tile, tile), tile)
                    pair = kv_refs[b][at, :]
                    kp[at, :] = packed(pair, True)
                    vp[at, :] = packed(pair, False)
                    kt[:, at] = stacked(pair.T[:HD, :])
                    bias[at, :] = key_bias(
                        meta_ref[0], transfers.at_c(b) * span + j * tile, tile, 128
                    )
                    return 0

                lax.fori_loop(0, per, prepare, 0)

    here = pl.ds(pl.multiple_of(step * rows, rows), rows)

    @pl.when(order == 0)
    def _():
        doubled(q_ref, here, head, qd, heads)
        doubled(do_ref, here, head, dd, heads)
        doubled(out_ref, here, head, od, heads)
        low = low_half((rows, 2 * HD))
        for value, four, mix in (
            (qd[...] * (LOG2E * HD**-0.5), q_all, q_mix),
            (dd[...], do_all, do_mix),
        ):
            high, rest = halves(value)
            four[here, : 2 * HD] = high
            four[here, 2 * HD :] = rest
            mixed = jnp.where(low, high.astype(jnp.float32), rest.astype(jnp.float32))
            mix[here, :] = mixed.astype(jnp.bfloat16)
        delta_all[:, here] = jnp.sum((dd[...] * od[...]).T[:HD, :], axis=0, keepdims=True)
        acc[:, here] = jnp.zeros((2 * HD, rows), jnp.float32)

    q_four, q_two, do_four, do_two = q_all[here, :], q_mix[here, :], do_all[here, :], do_mix[here, :]
    delta = delta_all[:, here]
    lse = lse_ref[0:1, here]
    for j in range(1, heads):
        lse = jnp.where(head == j, lse_ref[j : j + 1, here], lse)
    def key_tile(j, _):
        at = pl.ds(pl.multiple_of(j * tile, tile), tile)
        k_two, v_two = kp[at, :], vp[at, :]
        scores = dot(jnp.concatenate([k_two, k_two], axis=1), q_four, 1, 1)
        scores = scores + jnp.concatenate([bias[at, :]] * (rows // 128), axis=1)
        probs = jnp.exp2(scores - lse)
        high, rest = halves(probs)
        dv[at, :] += dot(high, do_two, 1, 0) + dot(rest, do_two, 1, 0)
        grad_p = dot(jnp.concatenate([v_two, v_two], axis=1), do_four, 1, 1)
        grad_s = probs * (grad_p - delta)
        high, rest = halves(grad_s)
        dk[at, :] += dot(high, q_two, 1, 0) + dot(rest, q_two, 1, 0)
        k_t = kt[:, at]
        acc[:, here] += dot(k_t, high, 1, 0) + dot(k_t, rest, 1, 0)
        return 0

    lax.fori_loop(0, per, key_tile, 0)

    @pl.when(order == blocks - 1)
    def _():
        result = ((acc[:HD, here] + acc[HD:, here]) * HD**-0.5).T
        for j in range(heads):

            @pl.when(head == j)
            def _(j=j):
                dq_ref[here, j * HD : (j + 1) * HD] = result

    def turned(at):
        grad_k, grad_v = dk[at, :], dv[at, :]
        grad_k = (grad_k + pltpu.roll(grad_k, HD, 1)) * (1.0 / LOG2E)
        grad_v = grad_v + pltpu.roll(grad_v, HD, 1)
        return jnp.where(low_half(grad_k.shape), grad_k, grad_v)

    for b in range(1, blocks):

        @pl.when((step == steps - 1) & (order == b - 1))
        def _(b=b):
            @pl.when(head >= 2)
            def _():
                transfers.kv_copy(head - 2, b).wait_send()

            def far(j, _):
                at = pl.ds(pl.multiple_of(j * tile, tile), tile)
                stage[head % 2, b - 1, at, :] = turned(at)
                return 0

            lax.fori_loop(0, per, far, 0)
            transfers.kv_copy(head, b).start()

    @pl.when((step == steps - 1) & (order == blocks - 1))
    def _():
        def keep(j, _):
            at = pl.ds(pl.multiple_of(j * tile, tile), tile)
            dkv_ref[at, :] = turned(at)
            return 0

        lax.fori_loop(0, per, keep, 0)

    transfers.run(now, before=False)


def remote(src, dst, send, recv, **peer):
    return pltpu.make_async_remote_copy(
        src_ref=src,
        dst_ref=dst,
        send_sem=send,
        recv_sem=recv,
        device_id=peer,
        device_id_type=pl.DeviceIdType.MESH,
    )


class Ring:
    def __init__(self, n_f, n_c, pick, side_rx, hop_rx, side_sem, hop_sem, emit):
        self.n_f, self.n_c, self.pick, self.emit = n_f, n_c, pick, emit
        self.side_rx, self.hop_rx, self.side_sem, self.hop_sem = side_rx, hop_rx, side_sem, hop_sem
        self.next_f = (lax.axis_index("fsdp") + 1) % n_f
        self.next_c = (lax.axis_index("ctx") + 1) % n_c

    def side(self, k, m):
        return remote(
            self.pick(k, 1) if m == 1 else self.side_rx.at[k - 1, m - 2],
            self.side_rx.at[k - 1, m - 1],
            self.side_sem.at[0, k - 1, m - 1],
            self.side_sem.at[1, k - 1, m - 1],
            ctx=self.next_c,
        )

    def hop(self, k):
        src = self.side_rx.at[0, self.n_c - 2] if k == 1 else self.hop_rx.at[k - 2]
        sem = self.hop_sem
        return remote(
            src, self.hop_rx.at[k - 1], sem.at[0, k - 1], sem.at[1, k - 1], fsdp=self.next_f
        )

    def begin(self):
        for k in range(1, self.n_f + 1):
            self.side(k, 1).start()

    def event(self, k):
        for m in range(2, self.n_c + 1):
            self.side(k, m - 1).wait()
            self.side_rx[k - 1, m - 2] += self.pick(k, m)[...]
            if m < self.n_c:
                self.side(k, m).start()
        if k > 1:
            self.hop(k - 1).wait()
            result = self.hop_rx[k - 2] + self.side_rx[k - 1, self.n_c - 2]
            if k < self.n_f:
                self.hop_rx[k - 2] = result
            else:
                self.emit(result)
        if k < self.n_f:
            self.hop(k).start()


def ring_scratch(n_f, n_c, own, wide):
    sem = pltpu.SemaphoreType.DMA
    return [
        pltpu.VMEM((n_f, n_c - 1, own, wide), jnp.float32),
        pltpu.VMEM((n_f - 1, own, wide), jnp.float32),
        sem((2, n_f, n_c - 1)),
        sem((2, n_f - 1)),
    ]


def row_block(ref, own, n_f, n_c):
    f, c = lax.axis_index("fsdp"), lax.axis_index("ctx")

    def pick(k, m):
        at = (f + (n_f - k)) % n_f * n_c + (c + (n_c - m)) % n_c
        return ref.at[pl.ds(pl.multiple_of(at * own, own), own)]

    return pick


def keeper(target):
    def emit(value):
        target[...] = value

    return emit


class Transfers:
    def __init__(
        self, n_c, n_f, heads, up_g, outs, up_out, kv_far, outs_all, stage,
        side_rx, hop_rx, side_sem, hop_sem, kv_sem, out_sem,
    ):
        self.n_c, self.n_f, self.heads = n_c, n_f, heads
        self.outs, self.kv_far, self.outs_all = outs, kv_far, outs_all
        self.stage = stage
        self.kv_sem = kv_sem
        self.out_sem = out_sem
        self.f, self.c, me = lax.axis_index("fsdp"), lax.axis_index("ctx"), lax.axis_index("tp")
        self.bit0 = me % 2
        self.peer0 = me + 1 - 2 * self.bit0
        self.ring = Ring(
            n_f, n_c, lambda k, m: up_g.at[self.at_f(k), self.at_c(m)],
            side_rx, hop_rx, side_sem, hop_sem, keeper(up_out),
        )

    def at_f(self, k):
        return (self.f + (self.n_f - k)) % self.n_f

    def at_c(self, m):
        return (self.c + (self.n_c - m)) % self.n_c

    def kv_copy(self, head, m):
        lanes = pl.ds(pl.multiple_of(head * 2 * HD, 2 * HD), 2 * HD)
        return remote(
            self.stage.at[head % 2, m - 1],
            self.kv_far.at[m - 1, :, lanes],
            self.kv_sem.at[0, head, m - 1],
            self.kv_sem.at[1, head, m - 1],
            ctx=self.at_c(m),
        )

    def out_local(self):
        return pltpu.make_async_copy(
            self.outs, self.outs_all.at[:, self.bit0], self.out_sem.at[0, 1]
        )

    def out_near(self):
        return remote(
            self.outs,
            self.outs_all.at[:, self.bit0],
            self.out_sem.at[0, 0],
            self.out_sem.at[1, 0],
            tp=self.peer0,
        )

    def begin(self):
        barrier = pltpu.get_barrier_semaphore()
        peers = [{"tp": self.peer0}, {"fsdp": self.at_f(-1)}]
        if self.n_f > 2:
            peers.append({"fsdp": self.at_f(1)})
        peers += [{"ctx": self.at_c(m)} for m in range(1, self.n_c)]
        for peer in peers:
            pl.semaphore_signal(
                barrier, inc=1, device_id=peer, device_id_type=pl.DeviceIdType.MESH
            )
        pl.semaphore_wait(barrier, len(peers))
        self.ring.begin()
        self.out_local().start()
        self.out_near().start()

    def end(self):
        self.out_local().wait()
        self.out_near().wait()
        for head in range(self.heads):
            for m in range(1, self.n_c):
                if head >= self.heads - 2:
                    self.kv_copy(head, m).wait_send()
                self.kv_copy(head, m).wait_recv()

    def run(self, now, before):
        count = self.heads * self.n_c * STEPS_PER_HEAD
        plan = []
        for k in range(1, self.n_f + 1):
            plan.append((0.85 * k / self.n_f, lambda k=k: self.ring.event(k)))
        plan.sort(key=lambda item: item[0])
        late = [self.end]
        if before:

            @pl.when(now == 0)
            def _():
                self.begin()

            return
        for at in range(count):
            todo = [f for p, f in plan if min(int(p * count), count - 1) == at]
            if at == count - 1:
                todo = todo + late
            if todo:

                @pl.when(now == at)
                def _(todo=todo):
                    for f in todo:
                        f()


STEPS_PER_HEAD = 4


def attention_back(
    queries, grads, result, lse, kv_blocks, meta, heads, up_g, outs, tile=512
):
    rows = queries.shape[0] // STEPS_PER_HEAD
    n_f, n_c, own, wide_up = up_g.shape
    count, span, blocks = queries.shape[0], kv_blocks[0].shape[0], len(kv_blocks)
    keys = span * blocks
    whole = lambda h, b, i, m: (0, 0)
    wide = pl.BlockSpec((count, heads * HD), whole)
    kv_spec = pl.BlockSpec((span, 2 * HD), lambda h, b, i, m: (0, h))
    anywhere = pl.BlockSpec(memory_space=pl.ANY)
    sem, shape = pltpu.SemaphoreType.DMA, jax.ShapeDtypeStruct

    def held(array):
        return pl.BlockSpec(array.shape, lambda h, b, i, m: (0,) * array.ndim)

    return pl.pallas_call(
        functools.partial(backward_kernel, heads, blocks, n_f, tile, rows),
        grid_spec=pltpu.PrefetchScalarGridSpec(
            num_scalar_prefetch=1,
            grid=(heads, blocks, count // rows),
            in_specs=[wide] * 3
            + [pl.BlockSpec((heads, count), whole)]
            + [held(up_g), held(outs)]
            + [kv_spec] * blocks,
            out_specs=[
                wide,
                kv_spec,
                pl.BlockSpec((own, wide_up), whole),
                anywhere,
                anywhere,
            ],
            scratch_shapes=[
                pltpu.VMEM((span, 2 * HD), jnp.bfloat16),
                pltpu.VMEM((span, 2 * HD), jnp.bfloat16),
                pltpu.VMEM((2 * HD, span), jnp.bfloat16),
                pltpu.VMEM((span, 128), jnp.float32),
                pltpu.VMEM((rows, 2 * HD), jnp.float32),
                pltpu.VMEM((rows, 2 * HD), jnp.float32),
                pltpu.VMEM((rows, 2 * HD), jnp.float32),
                pltpu.VMEM((span, 2 * HD), jnp.float32),
                pltpu.VMEM((span, 2 * HD), jnp.float32),
                pltpu.VMEM((2 * HD, count), jnp.float32),
                pltpu.VMEM((2, n_c - 1, span, 2 * HD), jnp.float32),
                pltpu.VMEM((count, 4 * HD), jnp.bfloat16),
                pltpu.VMEM((count, 4 * HD), jnp.bfloat16),
                pltpu.VMEM((count, 2 * HD), jnp.bfloat16),
                pltpu.VMEM((count, 2 * HD), jnp.bfloat16),
                pltpu.VMEM((1, count), jnp.float32),
                *ring_scratch(n_f, n_c, own, wide_up),
                sem((2, heads, n_c - 1)),
                sem((2, 2)),
            ],
        ),
        out_shape=[
            shape((count, heads * HD), jnp.float32),
            shape((span, 2 * heads * HD), jnp.float32),
            shape((own, wide_up), jnp.float32),
            shape((n_c - 1, span, 2 * heads * HD), jnp.float32),
            shape((outs.shape[0], 2) + outs.shape[1:], jnp.float32),
        ],
        compiler_params=pltpu.CompilerParams(
            dimension_semantics=("arbitrary",) * 3,
            collective_id=2,
            has_side_effects=True,
            vmem_limit_bytes=62 << 20,
        ),
        cost_estimate=pl.CostEstimate(
            flops=60 * heads * count * keys * HD,
            bytes_accessed=16 * keys * heads * HD + 16 * count * heads * HD,
            transcendentals=heads * count * keys,
        ),
        name="attention_backward",
    )(meta, queries, grads, result, lse, up_g, outs, *kv_blocks)


def dot_three(left, right, left_dim, right_dim):
    left_high, left_low = left
    right_high, right_low = right
    return dot(left_high, right_high, left_dim, right_dim) + (
        dot(left_high, right_low, left_dim, right_dim)
        + dot(left_low, right_high, left_dim, right_dim)
    )


def tiles_of(count, body):
    tile = 256 if count % 256 == 0 else count

    def step(n, _):
        body(pl.ds(pl.multiple_of(n * tile, tile), tile))
        return 0

    lax.fori_loop(0, count // tile, step, 0)


def middle_kernel(
    chunks, rows, n_c,
    att_ref, ups, downs, outw_ref,
    b_out_1, gain_1_1, shift_1_1, b_up_1, b_down_1, gain_2_1, shift_2_1, tok_hbm, cot_hbm,
    out_own, mid_own, gatt, d_up, d_out, d_down_out, vec, d_bup,
    part, rx0, rx1, full, act_hi, act_lo, slope, tok, cot, norm_1, recip_1,
    up_s, down_s, outw_s, xs, ys, ts, send0, recv0, send1, recv1, own_sem,
    lines, b_up, *blocked,
):
    half = rows // 2
    me = lax.axis_index("tp")
    bit0, bit1 = me % 2, me // 2 % 2
    peer0, peer1 = me + 1 - 2 * bit0, me + 2 - 4 * bit1
    home0 = pl.multiple_of(bit0 * half, half)
    away0 = pl.multiple_of((1 - bit0) * half, half)
    own = pl.ds(home0, half)

    def remote_tp(src, dst, send, recv, peer):
        return remote(src, dst, send, recv, tp=peer)

    width, hidden = up_s.shape[1], up_s.shape[2]
    d_down = d_down_out
    if blocked:
        whole, w_sem, wl_sem, last_sem, d_down, *ring_refs = blocked
        n_f, own_w = ups.shape[0], ups.shape[1]
        at, at_f = lax.axis_index("ctx"), lax.axis_index("fsdp")
        ring = Ring(
            n_f, n_c, row_block(d_down, own_w, n_f, n_c), *ring_refs, keeper(d_down_out)
        )

        def columns_of(part_at):
            return pl.ds(part_at * hidden, hidden)

        def up_copies():
            cols = columns_of(0)
            for k in range(n_f):
                yield pltpu.make_async_copy(
                    ups.at[k], whole.at[k, at, :, cols], wl_sem.at[0, k]
                )
                for m in range(1, n_c):
                    yield remote(
                        ups.at[k],
                        whole.at[k, at, :, cols],
                        w_sem.at[0, k, m - 1],
                        w_sem.at[1, k, m - 1],
                        ctx=(at + m) % n_c,
                    )

        def down_copies():
            cols = columns_of(1)
            for k in range(n_f - 1):
                slot = (at_f + (n_f - k)) % n_f
                yield pltpu.make_async_copy(
                    downs.at[slot], whole.at[slot, :, :, cols], wl_sem.at[1, k]
                )
            slot = (at_f + 2) % n_f
            yield remote(
                downs.at[slot],
                whole.at[slot, :, :, cols],
                last_sem.at[0],
                last_sem.at[1],
                fsdp=(at_f + 1) % n_f,
            )

        def w_copies(part_at):
            return down_copies() if part_at else up_copies()

    def scatter0(s, c):
        return remote_tp(
            part.at[c, pl.ds(away0, half)], rx0.at[c], send0.at[0, s, c], recv0.at[0, s, c], peer0
        )

    def swap1(s, c):
        return remote_tp(
            part.at[c, own], rx1.at[s % 2, c], send1.at[s, c], recv1.at[s, c], peer1
        )

    def gather0(s, c):
        return remote_tp(
            full.at[s, c, own], full.at[s, c, own], send0.at[1, s, c], recv0.at[1, s, c], peer0
        )

    def own_copies(c):
        where = pl.ds(pl.multiple_of(c * rows + home0, half), half)
        return (
            pltpu.make_async_copy(tok_hbm.at[where], tok.at[c], own_sem.at[0, c]),
            pltpu.make_async_copy(cot_hbm.at[where], cot.at[c], own_sem.at[1, c]),
        )

    for c in range(chunks):
        for copy in own_copies(c):
            copy.start()
    barrier = pltpu.get_barrier_semaphore()
    peers = [{"tp": peer0}, {"tp": peer1}]
    if blocked:
        peers += [{"ctx": (at + m) % n_c} for m in range(1, n_c)]
        peers += [{"fsdp": (at_f + k) % n_f} for k in sorted({1, n_f - 1})]
    for peer in peers:
        pl.semaphore_signal(barrier, inc=1, device_id=peer, device_id_type=pl.DeviceIdType.MESH)

    firsts = (b_out_1, gain_1_1, shift_1_1, b_down_1, gain_2_1, shift_2_1)
    for i, vector in enumerate(firsts):
        lines[i : i + 1, :] = row(vector)
    b_up[...] = row(b_up_1)
    b_out, gain_1, shift_1, b_down, gain_2, shift_2 = (
        lines.at[i : i + 1] for i in range(len(firsts))
    )

    def split_rows(source, target):
        count = source.shape[0]
        step = 128

        def one(i, _):
            at = pl.ds(pl.multiple_of(i * step, step), step)
            target[0, at, :], target[1, at, :] = halves(source[at, :])
            return 0

        lax.fori_loop(0, count // step, one, 0)

    split_rows(outw_ref, outw_s)

    def weights_ready(part_at, target):
        if not blocked:
            split_rows((ups, downs)[part_at], target)
            return
        for copy in w_copies(part_at):
            copy.wait()

        def one(j, _):
            to = pl.ds(pl.multiple_of(j * own_w, own_w), own_w)
            piece = whole[j // n_c, j % n_c, :, columns_of(part_at)]
            target[0, to, :], target[1, to, :] = halves(piece)
            return 0

        lax.fori_loop(0, n_f * n_c, one, 0)

    d_bup[...] = jnp.zeros_like(d_bup)
    vec[...] = jnp.zeros_like(vec)
    d_up[...] = jnp.zeros_like(d_up)
    d_down[...] = jnp.zeros_like(d_down)
    d_out[...] = jnp.zeros_like(d_out)
    for c in range(chunks):
        for copy in own_copies(c):
            copy.wait()
    pl.semaphore_wait(barrier, len(peers))
    if blocked:
        for part_at in range(2):
            for copy in w_copies(part_at):
                copy.start()

    def split_into(target, value):
        target[0], target[1] = halves(value)

    def finish0(s, c):
        scatter0(s, c).wait()
        part[c, own, :] += rx0[c]
        swap1(s, c).start()

    def finish1(s, c):
        swap1(s, c).wait()
        return part[c, own, :] + rx1[s % 2, c]

    def pair(first, second, after):
        def one(t, _):
            @pl.when(t < chunks)
            def _():
                first(t)

            if after is not None:

                @pl.when(t >= 2)
                def _():
                    finish0(after, t - 2)

            @pl.when(t >= 1)
            def _():
                second(t - 1)

            if after is None:
                ring_step(t)
            return 0

        lax.fori_loop(0, chunks + 1, one, 0)
        if after is not None:
            finish0(after, chunks - 1)

    def at_rows(c):
        return pl.ds(pl.multiple_of(c * rows, rows), rows)

    def attention_out(c):
        left = halves(att_ref[at_rows(c), :])

        def columns(n):
            part[c, :, n] = dot_three(left, (outw_s[0, n, :], outw_s[1, n, :]), 1, 1)

        tiles_of(width, columns)
        scatter0(0, c).start()

    def nothing(c):
        del c

    pair(attention_out, nothing, 0)

    def first_norm(c):
        resid = finish1(0, c) + tok[c] + b_out[...]
        n_1, r_1 = normalized(resid)
        norm_1[c] = n_1
        recip_1[c] = jnp.broadcast_to(r_1, recip_1.shape[1:])
        full[0, c, own, :] = n_1 * gain_1[...] + shift_1[...]
        gather0(0, c).start()

    def feed_forward(c):
        @pl.when(c == 0)
        def _():
            weights_ready(0, up_s)

        gather0(0, c).wait()
        split_into(xs, full[0, c])

        def columns(n):
            pre = dot_three((xs[0], xs[1]), (up_s[0, :, n], up_s[1, :, n]), 1, 0) + b_up[:, n]
            cdf = 0.5 + 0.5 * lax.erf(pre * math.sqrt(0.5))
            slope[c, :, n] = cdf + pre * (
                jnp.exp(-0.5 * pre * pre) * (1.0 / math.sqrt(2.0 * math.pi))
            )
            act_hi[c, :, n], act_lo[c, :, n] = halves(pre * cdf)

        tiles_of(hidden, columns)

        @pl.when(c == 0)
        def _():
            weights_ready(1, down_s)

        def back(n):
            part[c, :, n] = dot_three(
                (act_hi[c], act_lo[c]), (down_s[0, n, :], down_s[1, n, :]), 1, 1
            )

        tiles_of(width, back)
        scatter0(1, c).start()

    def second_norm(c):
        ffn = finish1(1, c) + full[0, c, own, :] + b_down[...]
        n_2, r_2 = normalized(ffn)
        out_own[c] = n_2 * gain_2[...] + shift_2[...]
        grad = cot[c]
        second = norm_back(grad, gain_2[...], n_2, r_2)
        full[1, c, own, :] = second
        gather0(1, c).start()
        vec[3:4, :] += jnp.sum(second, axis=0, keepdims=True)
        vec[4:5, :] += jnp.sum(grad * n_2, axis=0, keepdims=True)
        vec[5:6, :] += jnp.sum(grad, axis=0, keepdims=True)

    def feed_back(c):
        gather0(1, c).wait()
        split_into(xs, full[1, c])

        def columns(n):
            grad = dot_three((xs[0], xs[1]), (down_s[0, :, n], down_s[1, :, n]), 1, 0)
            grad = grad * slope[c, :, n]
            slope[c, :, n] = grad
            ys[0, :, n], ys[1, :, n] = halves(grad)
            d_bup[:, n] += jnp.sum(grad, axis=0, keepdims=True)

        tiles_of(hidden, columns)

        def back(n):
            part[c, :, n] = dot_three((ys[0], ys[1]), (up_s[0, n, :], up_s[1, n, :]), 1, 1)

        tiles_of(width, back)
        scatter0(2, c).start()
        split_into(ts, full[1, c].T)

        def down_columns(n):
            d_down[:, n] += dot_three((ts[0], ts[1]), (act_hi[c, :, n], act_lo[c, :, n]), 1, 0)

        tiles_of(hidden, down_columns)

    def ring_step(slot):
        if blocked:
            for k in range(1, n_f + 1):

                @pl.when(slot == min(chunks, max(1, -(-k * chunks // n_f))))
                def _(k=k):
                    ring.event(k)

    def middle_norm(c):
        first = finish1(2, c) + full[1, c, own, :]
        n_1 = norm_1[c]
        mid = norm_back(first, gain_1[...], n_1, recip_1[c, :, :1])
        mid_own[c] = mid
        full[2, c, own, :] = mid
        gather0(2, c).start()
        vec[0:1, :] += jnp.sum(mid, axis=0, keepdims=True)
        vec[1:2, :] += jnp.sum(first * n_1, axis=0, keepdims=True)
        vec[2:3, :] += jnp.sum(first, axis=0, keepdims=True)

    def last(c):
        gather0(2, c).wait()
        mid = full[2, c]
        gatt[at_rows(c), :] = dot_three(halves(mid), (outw_s[0], outw_s[1]), 1, 0)
        split_into(ts, mid.T)
        d_out[...] += dot_three((ts[0], ts[1]), halves(att_ref[at_rows(c), :]), 1, 0)
        split_into(ts, full[0, c].T)

        def columns(n):
            d_up[:, n] += dot_three((ts[0], ts[1]), halves(slope[c, :, n]), 1, 0)

        tiles_of(hidden, columns)

    pair(first_norm, feed_forward, 1)
    pair(second_norm, feed_back, 2)
    if blocked:
        ring.begin()
    pair(middle_norm, last, None)


def middle(attended, weights, wide_out_t, vectors, tokens, cot, hidden, n_c, chunks=4):
    blocked = weights[0].ndim > 2
    count, width = tokens.shape
    split_at = attended.shape[1]
    rows = count // chunks
    half = rows // 2
    vmem = pl.BlockSpec(memory_space=pltpu.VMEM)
    anywhere = pl.BlockSpec(memory_space=pl.ANY)
    f32, bf16 = jnp.float32, jnp.bfloat16
    sems = pltpu.SemaphoreType.DMA((2, 3, chunks))
    swap_sems = pltpu.SemaphoreType.DMA((3, chunks))
    extra = [pltpu.VMEM((8, width), f32), pltpu.VMEM((1, hidden), f32)]
    if blocked:
        n_f, own = weights[0].shape[:2]
        extra += [
            pltpu.VMEM((n_f, n_c, own, 2 * hidden), f32),
            pltpu.SemaphoreType.DMA((2, n_f, n_c - 1)),
            pltpu.SemaphoreType.DMA((2, n_f)),
            pltpu.SemaphoreType.DMA((2,)),
            pltpu.VMEM((width, hidden), f32),
            *ring_scratch(n_f, n_c, own, hidden),
        ]
    shape = jax.ShapeDtypeStruct
    return pl.pallas_call(
        functools.partial(middle_kernel, chunks, rows, n_c),
        in_specs=[vmem]
        + [anywhere if blocked else vmem] * 2
        + [vmem] * 8
        + [anywhere] * 2,
        out_specs=[vmem] * 8,
        out_shape=[
            shape((chunks, half, width), f32),
            shape((chunks, half, width), f32),
            shape((count, split_at), f32),
            shape((width, hidden), f32),
            shape((width, split_at), f32),
            shape((own if blocked else width, hidden), f32),
            shape((8, width), f32),
            shape((1, hidden), f32),
        ],
        scratch_shapes=[
            pltpu.VMEM((chunks, rows, width), f32),
            pltpu.VMEM((chunks, half, width), f32),
            pltpu.VMEM((2, chunks, half, width), f32),
            pltpu.VMEM((3, chunks, rows, width), f32),
            pltpu.VMEM((chunks, rows, hidden), bf16),
            pltpu.VMEM((chunks, rows, hidden), bf16),
            pltpu.VMEM((chunks, rows, hidden), f32),
            pltpu.VMEM((chunks, half, width), f32),
            pltpu.VMEM((chunks, half, width), f32),
            pltpu.VMEM((chunks, half, width), f32),
            pltpu.VMEM((chunks, half, 128), f32),
            pltpu.VMEM((2, width, hidden), bf16),
            pltpu.VMEM((2, width, hidden), bf16),
            pltpu.VMEM((2, width, split_at), bf16),
            pltpu.VMEM((2, rows, width), bf16),
            pltpu.VMEM((2, rows, hidden), bf16),
            pltpu.VMEM((2, width, rows), bf16),
            sems, sems, swap_sems, swap_sems,
            pltpu.SemaphoreType.DMA((2, chunks)),
            *extra,
        ],
        compiler_params=pltpu.CompilerParams(
            collective_id=1, has_side_effects=True, vmem_limit_bytes=62 << 20
        ),
        cost_estimate=pl.CostEstimate(
            flops=6 * count * width * (6 * hidden + 3 * split_at),
            bytes_accessed=4 * width * (5 * hidden + 3 * split_at),
            transcendentals=2 * count * hidden,
        ),
        name="middle",
    )(
        attended,
        *weights,
        wide_out_t,
        *vectors,
        tokens,
        cot,
    )


def front_kernel(
    heads, n_c, n_f, tile, rows, meta_ref, tok, w_qkv, up, down_t, outw, b_q, b_v,
    att, lse, q_out, kv_out, kv_far, wide, ups, downs, out_all,
    shard, q_s, kv_s, kv_t, wv, w_s, ow_own, kp, vt, bias, qd, acc, top_s, total_s,
    hop_sem, side_sem, up_sem, down_sem, down_side_sem, ow_sem, ow_side_sem, kv_sem, local_sem,
):
    block, head, step = pl.program_id(0), pl.program_id(1), pl.program_id(2)
    n_q = pl.num_programs(2)
    span, hidden, split_at = tok.shape[0], up.shape[1], heads * HD
    own = shard.shape[0]
    f, c = lax.axis_index("fsdp"), lax.axis_index("ctx")

    def at_f(k):
        return (f + (n_f - k)) % n_f

    def at_c(m):
        return (c + (n_c - m)) % n_c

    def lanes(h):
        return pl.ds(pl.multiple_of(h * 2 * HD, 2 * HD), 2 * HD)

    columns = (pl.ds(0, 2 * split_at), pl.ds(2 * split_at, split_at))

    def hop(p, k):
        to = wv.at[at_f(k - 1), c, :, columns[p]]
        src = shard.at[:, columns[p]] if k == 1 else to
        return remote(
            src, to, hop_sem.at[0, p, k - 1], hop_sem.at[1, p, k - 1], fsdp=at_f(-1)
        )

    def side(p, k, m):
        to = wv.at[at_f(k), c, :, columns[p]]
        src = shard.at[:, columns[p]] if k == 0 else to
        return remote(
            src, to, side_sem.at[0, p, k, m - 1], side_sem.at[1, p, k, m - 1], ctx=at_c(-m)
        )

    def up_hop(k):
        src = up if k == 1 else ups.at[at_f(k - 1)]
        return remote(
            src, ups.at[at_f(k - 1)], up_sem.at[0, k - 1], up_sem.at[1, k - 1], fsdp=at_f(-1)
        )

    def down_side(m):
        return remote(
            down_t,
            downs.at[f, c],
            down_side_sem.at[0, m - 1],
            down_side_sem.at[1, m - 1],
            ctx=at_c(-m),
        )

    def down_hop(k):
        pair = downs.at[at_f(k - 1)]
        return remote(
            pair, pair, down_sem.at[0, k - 1], down_sem.at[1, k - 1], fsdp=at_f(-1)
        )

    def ow_hop(k):
        src = ow_own if k == 1 else out_all.at[at_f(k - 1), c]
        return remote(
            src, out_all.at[at_f(k - 1), c], ow_sem.at[0, k - 1], ow_sem.at[1, k - 1], fsdp=at_f(-1)
        )

    def ow_side(k, m):
        src = ow_own if k == 0 else out_all.at[at_f(k), c]
        return remote(
            src,
            out_all.at[at_f(k), c],
            ow_side_sem.at[0, k, m - 1],
            ow_side_sem.at[1, k, m - 1],
            ctx=at_c(-m),
        )

    def kv_send(h, m):
        return remote(
            kv_s.at[:, lanes(h)],
            kv_far.at[m - 1, :, lanes(h)],
            kv_sem.at[0, h, m - 1],
            kv_sem.at[1, h, m - 1],
            ctx=at_c(-m),
        )

    def locals_of():
        return [
            pltpu.make_async_copy(a, b, local_sem.at[i])
            for i, (a, b) in enumerate(
                (
                    (up, ups.at[f]),
                    (ow_own, out_all.at[f, c]),
                    (wv, wide),
                    (q_s, q_out),
                    (kv_s, kv_out),
                    (down_t, downs.at[f, c]),
                )
            )
        ]

    def gathered(p):
        for k in range(n_f):
            for m in range(1, n_c):
                side(p, k, m).wait()

        def split(j, _):
            to = pl.ds(pl.multiple_of(j * own, own), own)
            w_s[0, to, columns[p]], w_s[1, to, columns[p]] = halves(
                wv[j // n_c, j % n_c, :, columns[p]]
            )
            return 0

        lax.fori_loop(0, n_f * n_c, split, 0)

    @pl.when((block == 0) & (head == 0) & (step == 0))
    def _():
        barrier = pltpu.get_barrier_semaphore()
        peers = [{"fsdp": at_f(-1)}] + ([{"fsdp": at_f(1)}] if n_f > 2 else [])
        peers += [{"ctx": at_c(m)} for m in range(1, n_c)]
        for peer in peers:
            pl.semaphore_signal(
                barrier, inc=1, device_id=peer, device_id_type=pl.DeviceIdType.MESH
            )
        for h in range(heads):
            at = 3 * HD * h
            shard[:, 2 * HD * h : 2 * HD * (h + 1)] = w_qkv[:, at + HD : at + 3 * HD]
            shard[:, 2 * split_at + HD * h : 2 * split_at + HD * (h + 1)] = w_qkv[:, at : at + HD]
        pl.semaphore_wait(barrier, len(peers))
        for p in range(2):
            hop(p, 1).start()
            for m in range(1, n_c):
                side(p, 0, m).start()
        wv[f, c] = shard[...]
        ow_own[...] = outw[...].T
        for k in range(1, n_f):
            for p in range(2):
                hop(p, k).wait()
                if k < n_f - 1:
                    hop(p, k + 1).start()
                for m in range(1, n_c):
                    side(p, k, m).start()
        up_hop(1).start()
        ow_hop(1).start()
        for m in range(1, n_c):
            down_side(m).start()
        copies = locals_of()
        copies[0].start()
        copies[1].start()
        copies[5].start()
        gathered(0)
        blank = jnp.zeros((1, HD), jnp.float32)
        v_row = row(b_v)
        b_kv = jnp.concatenate(
            sum(([blank, v_row[:, h * HD : (h + 1) * HD]] for h in range(heads)), []), axis=1
        )
        q_row = row(b_q)

        def keys(i, _):
            at = pl.ds(pl.multiple_of(i * rows, rows), rows)
            right = (w_s[0, :, : 2 * split_at], w_s[1, :, : 2 * split_at])
            kv_s[at, :] = dot_three(halves(tok[at, :]), right, 1, 0) + b_kv
            return 0

        lax.fori_loop(0, span // rows, keys, 0)
        for h in range(heads):
            for m in range(1, n_c):
                kv_send(h, m).start()

        gathered(1)
        copies[2].start()

        def asking(i, _):
            at = pl.ds(pl.multiple_of(i * rows, rows), rows)
            right = (w_s[0, :, 2 * split_at :], w_s[1, :, 2 * split_at :])
            q_s[at, :] = dot_three(halves(tok[at, :]), right, 1, 0) + q_row
            return 0

        lax.fori_loop(0, span // rows, asking, 0)
        copies[3].start()
        copies[4].start()
        for m in range(1, n_c):
            ow_side(0, m).start()

    @pl.when((block == 0) & (step == 0))
    def _():
        kv_t[...] = kv_s[:, lanes(head)]

    @pl.when((block > 0) & (step == 0))
    def _():
        kv_send(head, block).wait_recv()
        copy = pltpu.make_async_copy(
            kv_far.at[block - 1, :, lanes(head)], kv_t, local_sem.at[6]
        )
        copy.start()
        copy.wait()

    @pl.when(step == 0)
    def _():
        def prepare(j, _):
            at = pl.ds(pl.multiple_of(j * tile, tile), tile)
            pair = kv_t[at, :]
            kp[at, :] = packed(pair, True)
            vt[:, at] = stacked(pair.T[HD:, :])
            bias[at, :] = key_bias(meta_ref[0], at_c(block) * span + j * tile, tile, 128)
            return 0

        lax.fori_loop(0, span // tile, prepare, 0)

    here = pl.ds(pl.multiple_of(step * rows, rows), rows)

    @pl.when(block == 0)
    def _():
        acc[head, :, here] = jnp.zeros((2 * HD, rows), jnp.float32)
        top_s[head, :, here] = jnp.full((1, rows), MASKED, jnp.float32)
        total_s[head, :, here] = jnp.zeros((1, rows), jnp.float32)

    doubled(q_s, here, head, qd, heads)
    q_high, q_low = halves(qd[...] * (LOG2E * HD**-0.5))
    q_four = jnp.concatenate([q_high, q_low], axis=1)

    def key_tile(j, carry):
        top, total = carry
        at = pl.ds(pl.multiple_of(j * tile, tile), tile)
        k_two = kp[at, :]
        scores = dot(jnp.concatenate([k_two, k_two], axis=1), q_four, 1, 1)
        scores = scores + jnp.concatenate([bias[at, :]] * (rows // 128), axis=1)
        new_top = jnp.maximum(top, jnp.max(scores, axis=0, keepdims=True))
        fade = jnp.exp2(top - new_top)
        probs = jnp.exp2(scores - new_top)
        total = total * fade + jnp.sum(probs, axis=0, keepdims=True)
        high, low = halves(probs)
        v_two = vt[:, at]
        acc[head, :, here] = acc[head, :, here] * fade + (
            dot(v_two, high, 1, 0) + dot(v_two, low, 1, 0)
        )
        return new_top, total

    top, total = lax.fori_loop(
        0, span // tile, key_tile, (top_s[head, :, here], total_s[head, :, here])
    )
    top_s[head, :, here] = top
    total_s[head, :, here] = total

    @pl.when(block == n_c - 1)
    def _():
        result = ((acc[head, :HD, here] + acc[head, HD:, here]) / total).T
        for j in range(heads):

            @pl.when(head == j)
            def _(j=j):
                att[here, j * HD : (j + 1) * HD] = result
                lse[j : j + 1, here] = top + jnp.log2(total)

    def arrived(k):
        up_hop(k).wait()
        ow_hop(k).wait()
        if k < n_f - 1:
            up_hop(k + 1).start()
            ow_hop(k + 1).start()
        for m in range(1, n_c):
            ow_side(k, m).start()

    def down_arrived(k):
        if k == 0:
            locals_of()[5].wait()
            for m in range(1, n_c):
                down_side(m).wait()
        else:
            down_hop(k).wait()
        if k < n_f - 2:
            down_hop(k + 1).start()

    count = n_c * heads * STEPS_PER_HEAD
    now = (block * heads + head) * n_q + step
    plan = [(0.425, lambda: down_arrived(0))]
    for k in range(1, n_f):
        plan.append((0.05 + 0.37 * (k - 1) / max(1, n_f - 2), lambda k=k: arrived(k)))
    for k in range(1, n_f - 1):
        plan.append((0.425 + 0.575 * k / (n_f - 2), lambda k=k: down_arrived(k)))
    plan.sort(key=lambda item: item[0])
    for share, event in plan:

        @pl.when(now == min(int(share * count), count - 1))
        def _(event=event):
            event()

    @pl.when(now == count - 1)
    def _():
        for k in range(n_f):
            for m in range(1, n_c):
                ow_side(k, m).wait()
        for h in range(heads):
            for m in range(1, n_c):
                kv_send(h, m).wait_send()
        for copy in locals_of()[:5]:
            copy.wait()


def front(tokens, w_qkv, w_up, w_down_t, w_out, b_query, b_value, lengths, heads, n_f, n_c, tile=1024):
    span, width = tokens.shape
    tile = min(tile, span)
    own, total = w_qkv.shape
    hidden, split_at = w_up.shape[1], heads * HD
    rows = span // STEPS_PER_HEAD
    shape, sem, f32, bf16 = jax.ShapeDtypeStruct, pltpu.SemaphoreType.DMA, jnp.float32, jnp.bfloat16
    anywhere = pl.BlockSpec(memory_space=pl.ANY)

    def held(dims):
        return pl.BlockSpec(dims, lambda b, h, i, m: (0,) * len(dims))

    operands = (tokens, w_qkv, w_up, w_down_t, w_out, b_query, b_value)
    return pl.pallas_call(
        functools.partial(front_kernel, heads, n_c, n_f, tile, rows),
        grid_spec=pltpu.PrefetchScalarGridSpec(
            num_scalar_prefetch=1,
            grid=(n_c, heads, STEPS_PER_HEAD),
            in_specs=[held(x.shape) for x in operands],
            out_specs=[held((span, split_at)), held((heads, span))] + [anywhere] * 7,
            scratch_shapes=[
                pltpu.VMEM((own, total), f32),
                pltpu.VMEM((span, split_at), f32),
                pltpu.VMEM((span, 2 * split_at), f32),
                pltpu.VMEM((span, 2 * HD), f32),
                pltpu.VMEM((n_f, n_c, own, total), f32),
                pltpu.VMEM((2, width, total), bf16),
                pltpu.VMEM((own, split_at), f32),
                pltpu.VMEM((span, 2 * HD), bf16),
                pltpu.VMEM((2 * HD, span), bf16),
                pltpu.VMEM((span, 128), f32),
                pltpu.VMEM((rows, 2 * HD), f32),
                pltpu.VMEM((heads, 2 * HD, span), f32),
                pltpu.VMEM((heads, 1, span), f32),
                pltpu.VMEM((heads, 1, span), f32),
                sem((2, 2, n_f - 1)),
                sem((2, 2, n_f, n_c - 1)),
                sem((2, n_f - 1)),
                sem((2, n_f - 1)),
                sem((2, n_c - 1)),
                sem((2, n_f - 1)),
                sem((2, n_f, n_c - 1)),
                sem((2, heads, n_c - 1)),
                sem((7,)),
            ],
        ),
        out_shape=[
            shape((span, split_at), f32),
            shape((heads, span), f32),
            shape((span, split_at), f32),
            shape((span, 2 * split_at), f32),
            shape((n_c - 1, span, 2 * split_at), f32),
            shape((n_f, n_c, own, total), f32),
            shape((n_f, own, hidden), f32),
            shape((n_f, n_c, own, hidden), f32),
            shape((n_f, n_c, own, split_at), f32),
        ],
        compiler_params=pltpu.CompilerParams(
            dimension_semantics=("arbitrary",) * 3,
            collective_id=3,
            has_side_effects=True,
            vmem_limit_bytes=62 << 20,
        ),
        name="front",
    )(lengths, *operands)

def tail_kernel(
    chunks, rows, n_c, n_f, own,
    tok, grad_q, grad_kv, far, wide, mid, vec, d_bup, d_out,
    d_in, d_w, d_wout, d_bq, d_bv, d_bu, s_0, s_1, s_2, s_3, s_4, s_5,
    part, rx0, rx1, full, w_s, gs, ts, dw, side_rx, hop_rx, out_side, out_hop, small, small_rx,
    near_sem, far_sem, side_sem, hop_sem, out_side_sem, out_hop_sem, small_sem, local_sem,
):
    half = rows // 2
    me, f, c_at = lax.axis_index("tp"), lax.axis_index("fsdp"), lax.axis_index("ctx")
    bit0, bit1 = me % 2, me // 2 % 2
    peer0, peer1 = me + 1 - 2 * bit0, me + 2 - 4 * bit1
    home0 = pl.multiple_of(bit0 * half, half)
    away0 = pl.multiple_of((1 - bit0) * half, half)
    keep = pl.ds(home0, half)
    width, kv_width, total = tok.shape[1], grad_kv.shape[1], wide.shape[1]

    def at_f(k):
        return (f + (n_f - k)) % n_f

    def at_c(m):
        return (c_at + (n_c - m)) % n_c

    def exchange(src, dst, sems, kind, c, peer):
        return remote(src, dst, sems.at[0, kind, c], sems.at[1, kind, c], tp=peer)

    def scatter0(c):
        return exchange(part.at[c, pl.ds(away0, half)], rx0.at[c], near_sem, 0, c, peer0)

    def scatter1(c):
        return exchange(part.at[c, keep], rx1.at[c], far_sem, 0, c, peer1)

    def gather0(c):
        return exchange(full.at[c, keep], full.at[c, keep], near_sem, 1, c, peer0)

    def powers(count):
        bits, bit = [], 1
        while bit < count:
            bits.append(bit)
            bit *= 2
        return bits

    def flipped(at, bit):
        return at + bit - 2 * bit * (at // bit % 2)

    rounds = [("tp", peer0)]
    rounds += [("fsdp", flipped(f, bit)) for bit in powers(n_f)]
    rounds += [("ctx", flipped(c_at, bit)) for bit in powers(n_c)]

    def small_copy(r):
        axis, peer = rounds[r]
        return remote(
            small.at[r], small_rx.at[r], small_sem.at[0, r], small_sem.at[1, r], **{axis: peer}
        )

    def small_event(r):
        small_copy(r).wait()
        if rounds[r][0] == "tp":
            small[r + 1, :8, :] = small[r, :8, :] + small_rx[r, :8, :]
            small[r + 1, 8:, :] = small[r, 8:, :]
        else:
            small[r + 1] = small[r] + small_rx[r]
        if r + 1 < len(rounds):
            small_copy(r + 1).start()

    barrier = pltpu.get_barrier_semaphore()
    peers = [{"tp": peer0}, {"tp": peer1}]
    peers += [{"fsdp": at_f(k)} for k in range(1, n_f)]
    peers += [{"ctx": at_c(m)} for m in range(1, n_c)]
    for peer in peers:
        pl.semaphore_signal(barrier, inc=1, device_id=peer, device_id_type=pl.DeviceIdType.MESH)

    def split(i, _):
        at = pl.ds(pl.multiple_of(i * 128, 128), 128)
        w_s[0, at, :], w_s[1, at, :] = halves(wide[at, :])
        return 0

    lax.fori_loop(0, width // 128, split, 0)
    small[0, :8, :] = vec[...]
    small[0, 8:, :] = jnp.zeros_like(small[0, 8:, :])
    small[0, 8:9, :] = d_bup[...]
    dw[...] = jnp.zeros_like(dw)
    pl.semaphore_wait(barrier, len(peers))

    out_ring = Ring(
        n_f, n_c, row_block(d_out, own, n_f, n_c), out_side, out_hop, out_side_sem,
        out_hop_sem, keeper(d_wout),
    )
    out_ring.begin()

    def finish0(c):
        scatter0(c).wait()
        part[c, keep, :] += rx0[c]
        scatter1(c).start()

    def partial(c, _):
        at = pl.ds(pl.multiple_of(c * rows, rows), rows)
        kv = grad_kv[at, :]
        for m in range(n_c - 1):
            kv = kv + far[m, at, :]
        grad = jnp.concatenate([kv, grad_q[at, :]], axis=1)
        gs[c, 0], gs[c, 1] = halves(grad)
        small[0, 9:10, :total] += jnp.sum(grad, axis=0, keepdims=True)

        def columns(n):
            part[c, :, n] = dot_three((gs[c, 0], gs[c, 1]), (w_s[0, n, :], w_s[1, n, :]), 1, 1)

        tiles_of(width, columns)
        scatter0(c).start()

        @pl.when(c > 0)
        def _():
            finish0(c - 1)

        return 0

    lax.fori_loop(0, chunks, partial, 0)
    finish0(chunks - 1)
    small_copy(0).start()

    def weights(c, _):
        at = pl.ds(pl.multiple_of(c * rows, rows), rows)
        ts[0], ts[1] = halves(tok[at, :].T)

        def lines(n):
            dw[n, :] += dot_three((ts[0, n, :], ts[1, n, :]), (gs[c, 0], gs[c, 1]), 1, 0)

        tiles_of(width, lines)
        return 0

    lax.fori_loop(0, chunks, weights, 0)
    qkv_ring = Ring(
        n_f, n_c, row_block(dw, own, n_f, n_c), side_rx, hop_rx, side_sem, hop_sem,
        lambda result: grouped(d_w, result),
    )
    qkv_ring.begin()
    heads = (total - kv_width) // HD

    def grouped(target, value):
        for h in range(heads):
            at = 3 * HD * h
            target[:, at : at + HD] = value[:, kv_width + HD * h : kv_width + HD * (h + 1)]
            target[:, at + HD : at + 3 * HD] = value[:, 2 * HD * h : 2 * HD * (h + 1)]

    def finish1(c):
        scatter1(c).wait()
        full[c, keep, :] = part[c, keep, :] + rx1[c] + mid[c]
        gather0(c).start()

    def leave(c):
        return pltpu.make_async_copy(full.at[c], d_in.at[c], local_sem.at[c])

    plan = [(17 + 8.6 * c, lambda c=c: finish1(c)) for c in range(chunks)]
    plan += [(5 + 10 * k / n_f, lambda k=k: out_ring.event(k)) for k in range(1, n_f + 1)]
    plan += [(17 + 24 * k / n_f, lambda k=k: qkv_ring.event(k)) for k in range(1, n_f + 1)]
    plan += [
        (15 + 30 * (r + 1) / len(rounds), lambda r=r: small_event(r)) for r in range(len(rounds))
    ]
    plan.sort(key=lambda item: item[0])
    for _, event in plan:
        event()
    last = len(rounds)
    for i, target in enumerate((s_0, s_1, s_2, s_3, s_4, s_5)):
        target[...] = small[last, i : i + 1, :].reshape(-1)
    d_bu[...] = small[last, 8:9, :].reshape(-1)
    d_bq[...] = small[last, 9:10, kv_width:total].reshape(-1)
    by_value = [
        small[last, 9:10, 2 * HD * h + HD : 2 * HD * (h + 1)] for h in range(heads)
    ]
    d_bv[...] = jnp.concatenate(by_value, axis=1).reshape(-1)
    for c in range(chunks):
        gather0(c).wait()
        leave(c).start()
    for c in range(chunks):
        leave(c).wait()


def tail(tokens, grad_q, grad_kv, far, wide, mid, vec, d_bup, d_out, n_f, n_c, own):
    count, width = tokens.shape
    total, chunks, rows = wide.shape[1], mid.shape[0], 2 * mid.shape[1]
    vmem, anywhere = pl.BlockSpec(memory_space=pltpu.VMEM), pl.BlockSpec(memory_space=pl.ANY)
    shape, sem, f32, bf16 = jax.ShapeDtypeStruct, pltpu.SemaphoreType.DMA, jnp.float32, jnp.bfloat16
    rounds = 1 + (n_f - 1).bit_length() + (n_c - 1).bit_length()
    return pl.pallas_call(
        functools.partial(tail_kernel, chunks, rows, n_c, n_f, own),
        in_specs=[vmem] * 9,
        out_specs=[anywhere] + [vmem] * 11,
        out_shape=[
            shape((chunks, rows, width), f32),
            shape((own, total), f32),
            shape((own, d_out.shape[1]), f32),
            shape((total - grad_kv.shape[1],), f32),
            shape((total - grad_kv.shape[1],), f32),
        ]
        + [shape((width,), f32)] * 7,
        scratch_shapes=[
            pltpu.VMEM((chunks, rows, width), f32),
            pltpu.VMEM((chunks, rows // 2, width), f32),
            pltpu.VMEM((chunks, rows // 2, width), f32),
            pltpu.VMEM((chunks, rows, width), f32),
            pltpu.VMEM((2, width, total), bf16),
            pltpu.VMEM((chunks, 2, rows, total), bf16),
            pltpu.VMEM((2, width, rows), bf16),
            pltpu.VMEM((width, total), f32),
            pltpu.VMEM((n_f, n_c - 1, own, total), f32),
            pltpu.VMEM((n_f - 1, own, total), f32),
            pltpu.VMEM((n_f, n_c - 1, own, d_out.shape[1]), f32),
            pltpu.VMEM((n_f - 1, own, d_out.shape[1]), f32),
            pltpu.VMEM((rounds + 1, 16, width), f32),
            pltpu.VMEM((rounds, 16, width), f32),
            sem((2, 2, chunks)),
            sem((2, 2, chunks)),
            sem((2, n_f, n_c - 1)),
            sem((2, n_f - 1)),
            sem((2, n_f, n_c - 1)),
            sem((2, n_f - 1)),
            sem((2, rounds)),
            sem((chunks,)),
        ],
        compiler_params=pltpu.CompilerParams(
            collective_id=4, has_side_effects=True, vmem_limit_bytes=62 << 20
        ),
        name="tail",
    )(tokens, grad_q, grad_kv, far, wide, mid, vec, d_bup, d_out)

def finish_kernel(bigs, *refs):
    count = (len(refs) - bigs - 1) // 2
    given, results, stages, sem = refs[:count], refs[count : 2 * count], refs[2 * count : -1], refs[-1]
    pieces = [(i, c) for i in range(bigs) for c in range(given[i].shape[0])]

    def inward(i, c):
        return pltpu.make_async_copy(given[i].at[c], stages[i].at[c], sem.at[0, i, c])

    def outward(i, c):
        return pltpu.make_async_copy(stages[i].at[c], results[i].at[c], sem.at[1, i, c])

    for i, c in pieces:
        inward(i, c).start()
    for source, target in zip(given[bigs:], results[bigs:]):
        target[...] = source[...] if source.shape == target.shape else source[...].T
    for i, c in pieces:
        inward(i, c).wait()
        outward(i, c).start()
    for i, c in pieces:
        outward(i, c).wait()


def finish(large, small, turned):
    anywhere, vmem = pl.BlockSpec(memory_space=pl.ANY), pl.BlockSpec(memory_space=pltpu.VMEM)
    specs = [anywhere] * len(large) + [vmem] * len(small)
    shapes = [x.shape for x in (*large, *small)]
    shapes[turned] = shapes[turned][::-1]
    return pl.pallas_call(
        functools.partial(finish_kernel, len(large)),
        in_specs=specs,
        out_specs=specs,
        out_shape=[jax.ShapeDtypeStruct(dims, jnp.float32) for dims in shapes],
        scratch_shapes=[pltpu.VMEM(x.shape, x.dtype) for x in large]
        + [pltpu.SemaphoreType.DMA((2, len(large), max(x.shape[0] for x in large)))],
        name="finish",
    )(*large, *small)


def per_device(
    inputs,
    lengths,
    w_qkv,
    b_query,
    b_value,
    w_out,
    b_out,
    gain_attn,
    shift_attn,
    w_up,
    b_up,
    w_down,
    b_down,
    gain_ffn,
    shift_ffn,
    cotangent,
):
    width = inputs.shape[-1]
    block_len = inputs.shape[1]
    heads = b_query.shape[0] // HD
    split_at = heads * HD
    hidden = b_up.shape[0]
    tokens = inputs.reshape(block_len, width)
    cot = cotangent.reshape(block_len, width)
    length = lengths[0]
    n_c = lax.axis_size("ctx")
    at_c = lax.axis_index("ctx")

    def regroup(columns):
        parts = columns.reshape(columns.shape[:-1] + (heads, 3 * HD))
        lead = columns.shape[:-1]
        return jnp.concatenate(
            [
                parts[..., HD:].reshape(lead + (2 * split_at,)),
                parts[..., :HD].reshape(lead + (split_at,)),
            ],
            axis=-1,
        )

    bias_kv = jnp.stack(
        [jnp.zeros((heads, HD), jnp.float32), b_value.reshape(heads, HD)], axis=1
    ).reshape(-1)
    n_f, own = lax.axis_size("fsdp"), w_up.shape[0]
    fused = own % 16 == 0 and n_c > 1 and n_f > 1 and hidden == width
    if fused:
        attended, log_sums, queries, kv_own, kv_far, wide, *weights, wide_out_t = front(
            tokens, w_qkv, w_up, w_down.T, w_out, b_query, b_value, lengths, heads, n_f, n_c,
        )
        wide = wide.reshape(width, 3 * split_at)
        wide_kv, wide_q = wide[:, : 2 * split_at], wide[:, 2 * split_at :]
        wide_out_t = wide_out_t.reshape(width, split_at)
        kv_blocks = [kv_own] + [kv_far[m] for m in range(n_c - 1)]
    else:
        wide_kv, wide_q = weight_gather(regroup(w_qkv), [2 * split_at, split_at])
        rest = jnp.concatenate([w_up, w_down.T, w_out.T], axis=1)
        wide_up, wide_down_t, wide_out_t = weight_gather(rest, [hidden, hidden, split_at])
        weights = (wide_up, wide_down_t)
        kv_blocks = [contract(tokens, wide_kv, 1, 0) + bias_kv]
        for m in range(1, n_c):
            kv_blocks.append(ringed(kv_blocks[-1], "ctx", 1))
        queries = contract(tokens, wide_q, 1, 0) + b_query
        meta = jnp.stack([length] + [(at_c - m) % n_c * block_len for m in range(n_c)])
        attended, log_sums = attention(queries, kv_blocks, meta, heads)

    vectors = (b_out, gain_attn, shift_attn, b_up, b_down, gain_ffn, shift_ffn)
    outs, grad_mid, grad_att, d_up, d_out, d_wdown_t, vec_rows, d_bup = middle(
        attended, weights, wide_out_t, vectors, tokens, cot, hidden, n_c
    )
    blocked = (lax.axis_size("fsdp"), n_c, w_up.shape[0])
    grad_q, grad_kv, d_wup, kv_back, outputs = attention_back(
        queries,
        grad_att,
        attended,
        log_sums,
        kv_blocks,
        lengths,
        heads,
        d_up.reshape(blocked + (hidden,)),
        outs,
    )
    if fused:
        d_inputs, *small = tail(
            tokens, grad_q, grad_kv, kv_back, wide, grad_mid, vec_rows, d_bup, d_out, n_f, n_c, own
        )
        outputs, d_inputs, d_wup, d_wdown_t, d_wqkv, d_wout, d_bquery, d_bvalue, d_bup, *sums = (
            finish([outputs.reshape(d_inputs.shape), d_inputs], [d_wup, d_wdown_t, *small], 5)
        )
        d_inputs = d_inputs.reshape(block_len, width)
    else:
        for m in range(n_c - 1):
            grad_kv = grad_kv + kv_back[m]
        back = contract(grad_kv, wide_kv, 1, 1) + contract(grad_q, wide_q, 1, 1)
        tail_sums = small_sum(
            jnp.concatenate([jnp.sum(grad_kv, axis=0), jnp.sum(grad_q, axis=0), d_bup[0]]),
            ("fsdp", "ctx"),
        )
        d_wdown_t, d_wout = grad_scatter([d_wdown_t]), grad_scatter([d_out]).T
        proj_sums, d_bup = tail_sums[: 3 * split_at], tail_sums[3 * split_at :]
        sums = small_sum(vec_rows + swapped(vec_rows, "tp", 1), ("fsdp", "ctx"))
        d_inputs = half_gather(grad_mid + half_scatter(back, grad_mid.shape[0]))
        own_dw = grad_scatter([contract(tokens, grad_kv, 0, 0), contract(tokens, grad_q, 0, 0)])
        d_wqkv = jnp.concatenate(
            [
                own_dw[:, 2 * split_at :].reshape(own, heads, HD),
                own_dw[:, : 2 * split_at].reshape(own, heads, 2 * HD),
            ],
            axis=2,
        ).reshape(own, 3 * split_at)
        d_bvalue = proj_sums[: 2 * split_at].reshape(heads, 2, HD)[:, 1].reshape(-1)
        d_bquery = proj_sums[2 * split_at : 3 * split_at]
    d_wdown = d_wdown_t.T
    return (
        outputs.reshape(1, block_len, width),
        d_inputs.reshape(1, block_len, width),
        d_wqkv,
        d_bquery,
        d_bvalue,
        d_wout,
        sums[0],
        sums[1],
        sums[2],
        d_wup,
        d_bup,
        d_wdown,
        sums[3],
        sums[4],
        sums[5],
    )


def solution(mesh):
    rows_of, cols_of = P(("fsdp", "ctx"), "tp"), P("tp", ("fsdp", "ctx"))
    seq, by_tp, same = P("fsdp", "ctx", None), P("tp"), P()
    in_specs = (
        seq, P("fsdp"), rows_of, by_tp, by_tp, cols_of, same, same, same,
        rows_of, by_tp, cols_of, same, same, same, seq,
    )
    out_specs = (
        seq, seq, rows_of, by_tp, by_tp, cols_of, same, same, same,
        rows_of, by_tp, cols_of, same, same, same,
    )
    return jax.shard_map(
        per_device, mesh=mesh, in_specs=in_specs, out_specs=out_specs, check_vma=False
    )
```
